32 devices in a mesh: ctx: 4 (over y, x), fsdp: 8 (over z, core).
Axes of the slice: x: 2, y: 2, z: 4, core: 2. Of those that a mesh axis runs over, the one named last changes fastest.
Arguments:
- layer_input: bfloat16 [1280, 4, 1536], P(('ctx', 'fsdp')), may hold values from -6 to 6
- block_order: int32 [2, 8], replicated, may hold values from 0 to 7, each once within a row
- first_gain: bfloat16 [1536], P('fsdp'), may hold values from 0.25 to 1.75
- w_qkv: bfloat16 [1536, 2048], P('fsdp'), may hold values from -0.15625 to 0.15625
- b_qkv: bfloat16 [2048], P('fsdp'), may hold values from -1.5 to 1.5
- w_o: bfloat16 [1536, 1536], P('fsdp'), may hold values from -1.25 to 1.25
- second_gain: bfloat16 [1536], P('fsdp'), may hold values from 0.25 to 1.75
- w_gate: bfloat16 [1536, 8960], P('fsdp'), may hold values from -0.15625 to 0.15625
- w_up: bfloat16 [1536, 8960], P('fsdp'), may hold values from -0.15625 to 0.15625
- w_down: bfloat16 [8960, 1536], P('fsdp'), may hold values from -0.0625 to 0.0625
- cotangent: bfloat16 [1280, 4, 1536], P(('ctx', 'fsdp')), may hold values from -6 to 6
Outputs:
- mixed: bfloat16 [1280, 4, 1536], P(('ctx', 'fsdp'))
- input_grad: float32 [1280, 4, 1536], P(('ctx', 'fsdp'))
- first_gain_grad: float32 [1536], P('fsdp')
- w_qkv_grad: float32 [1536, 2048], P('fsdp')
- b_qkv_grad: float32 [1792], P('fsdp')
- value_bias_grad: float32 [256], P('fsdp')
- w_o_grad: float32 [1536, 1536], P('fsdp')
- second_gain_grad: float32 [1536], P('fsdp')
- w_gate_grad: float32 [1536, 8960], P('fsdp')
- w_up_grad: float32 [1536, 8960], P('fsdp')
- w_down_grad: float32 [8960, 1536], P('fsdp')
The draws below stay inside these ranges and needn't reach their ends.
Inputs may be any that keep to these rules, and one draw needn't show every extreme that they name: `block_order`: each row is a permutation.
All inputs are finite; a program needn't handle non-finite values.
Results may differ from the reference program's by a relative error of at most 0.02.
Values may be sent and summed in bfloat16 or wider, within the bound.
A program may use at most 576 MiB of HBM per device.

```python
import math
import jax
import jax.numpy as jnp
from jax import lax

D = 1536
H = 12
KVH = 2
HD = 128
FF = 8960
SEQS = 2
QKV = 2048
QK = 1792
SPAN = 1280
LEN = 2560
N_CTX = 4


def block_levels(rng, extent, cuts, least, top_value):
    level, own = 1.0, jax.random.fold_in(rng, 6)
    for dim, parts in cuts:
        steps = jnp.exp(jax.random.uniform(jax.random.fold_in(own, dim), (parts,), jnp.float32, least / len(cuts), top_value / len(cuts)))
        level = level * jnp.repeat(steps, extent[dim] // parts).reshape([-1 if axis == dim else 1 for axis in range(len(extent))])
    return level


def bell_draw(own_key, extent, spread, bound, pieces=(), kind=jnp.bfloat16):
    loudness = block_levels(own_key, extent, pieces, -0.22, 0.18) if pieces else 1.0
    array = jax.random.normal(own_key, extent, jnp.float32) * spread * loudness
    return jnp.minimum(jnp.maximum(array, -bound), bound).astype(kind)


def setup_inputs(seed: int = 0) -> dict:
    key_of = jax.random.split(jax.random.key(seed), 12)
    layer_input = bell_draw(key_of[0], (SPAN, 2 * SEQS, D), 1.0, 6.0, ((0, 32),))
    block_order = jax.vmap(lambda own: jax.random.permutation(own, 2 * N_CTX))(jax.random.split(key_of[1], SEQS)).reshape((SEQS, 2 * N_CTX)).astype(jnp.int32)
    first_gain = jnp.clip(1.0 + 0.15 * jax.random.normal(key_of[2], (D,), jnp.float32), 0.25, 1.75).astype(jnp.bfloat16)
    w_qkv = bell_draw(key_of[3], (D, QKV), D ** -0.5, 0.15625, ((0, 8),))
    b_qkv = bell_draw(key_of[4], (QKV,), 0.5, 1.5, ((0, 8),))
    w_o = bell_draw(key_of[5], (D, D), (max(1, 32 * D // LEN)) ** -0.5, 1.25, ((0, 8),))
    second_gain = jnp.clip(1.0 + 0.15 * jax.random.normal(key_of[6], (D,), jnp.float32), 0.25, 1.75).astype(jnp.bfloat16)
    w_gate = bell_draw(key_of[7], (D, FF), D ** -0.5, 0.15625, ((0, 8),))
    w_up = bell_draw(key_of[8], (D, FF), D ** -0.5, 0.15625, ((0, 8),))
    w_down = bell_draw(key_of[9], (FF, D), FF ** -0.5, 0.0625, ((0, 8),))
    cotangent = bell_draw(key_of[10], (SPAN, 2 * SEQS, D), 1.0, 6.0, ((0, 32),))
    return dict(layer_input=layer_input, block_order=block_order, first_gain=first_gain, w_qkv=w_qkv, b_qkv=b_qkv, w_o=w_o, second_gain=second_gain, w_gate=w_gate, w_up=w_up, w_down=w_down, cotangent=cotangent)


EPS = 1e-06
THETA = 1000000.0
HIGH = lax.Precision.HIGHEST

@jax.custom_vjp
def low(v):
    return lax.optimization_barrier(v.astype(jnp.bfloat16)).astype(jnp.float32)

@jax.custom_vjp
def low_back(v):
    return v

def low_keep(v):
    return (low(v), None)

def low_pass(kept, grad):
    return (grad,)

def back_keep(v):
    return (v, None)

def back_low(kept, grad):
    return (low(grad),)
low.defvjp(low_keep, low_pass)
low_back.defvjp(back_keep, back_low)

def token_positions(block_order):
    block_rows = SPAN // N_CTX
    row_index = jnp.arange(SPAN, dtype=jnp.int32)
    slot_index = jnp.arange(2 * SEQS, dtype=jnp.int32)
    entries = (slot_index // SEQS)[None, :] * N_CTX + (row_index // block_rows)[:, None]
    picked = block_order[(slot_index % SEQS)[None, :], entries]
    return (picked * block_rows + (row_index % block_rows)[:, None]).astype(jnp.int32)

def rope_tables(positions):
    half_width = HD // 2
    frequency = THETA ** (-jnp.arange(half_width, dtype=jnp.float32) * 2.0 / HD)
    angles = positions.astype(jnp.float32)[:, None] * frequency[None, :]
    cosine_table = jnp.concatenate([jnp.cos(angles), jnp.cos(angles)], -1)[:, None, :]
    sine_table = jnp.concatenate([jnp.sin(angles), jnp.sin(angles)], -1)[:, None, :]
    return (cosine_table, sine_table)

def rotate(head_values, cosine_table, sine_table):
    half_width = HD // 2
    turned = jnp.concatenate([-head_values[..., half_width:], head_values[..., :half_width]], -1)
    return head_values * cosine_table + turned * sine_table

def by_sequence(tokens):
    shaped = tokens.reshape((SPAN, 2, SEQS) + tokens.shape[1:])
    return jnp.moveaxis(shaped, 2, 0).reshape((SEQS, LEN) + tokens.shape[1:])

def from_sequences(per_sequence):
    shaped = per_sequence.reshape((SEQS, SPAN, 2) + per_sequence.shape[2:])
    return jnp.moveaxis(shaped, 0, 2).reshape((SPAN * 2 * SEQS,) + per_sequence.shape[2:])

def attend_sequence(query_heads, key_heads, value_heads, positions):
    group_size = H // KVH
    query_block = math.gcd(LEN, 512)
    block_count = LEN // query_block
    query_blocks = query_heads.reshape(block_count, query_block, KVH, group_size, HD)
    pos_blocks = positions.reshape(block_count, query_block)

    def one_block(pair):
        query_part, query_pos = pair
        scores = jnp.einsum('qngd,knd->ngqk', query_part, key_heads, precision=HIGH)
        scores = low_back(scores)
        visible = (query_pos[:, None] >= positions[None, :])[None, None]
        scores = jnp.where(visible, scores, -1e+30)
        largest = lax.optimization_barrier(jnp.max(scores, -1, keepdims=True))
        weights = jnp.where(visible, jnp.exp(scores - largest), 0.0)
        totals = lax.optimization_barrier(jnp.sum(weights, -1, keepdims=True))
        mixed_part = jnp.einsum('ngqk,knd->qngd', low(weights), value_heads, precision=HIGH)
        return mixed_part / jnp.transpose(totals, (2, 0, 1, 3))
    outputs = lax.map(jax.checkpoint(one_block), (query_blocks, pos_blocks))
    return outputs.reshape(LEN, H * HD)

def rms_scale(values):
    return lax.rsqrt(lax.optimization_barrier(jnp.mean(values * values, -1, keepdims=True)) + EPS)

def layer(inputs, gain_one, w_qkv, b_qkv, w_o, gain_two, w_gate, w_up, w_down, positions):
    token_rows = inputs.reshape(-1, D)
    normed_one = low(token_rows * rms_scale(token_rows) * gain_one)
    projected = low_back(jnp.dot(normed_one, w_qkv, precision=HIGH) + b_qkv)
    flat_pos = positions.reshape(-1)
    cosine_table, sine_table = rope_tables(flat_pos)
    query_heads = rotate(projected[:, :H * HD].reshape(-1, H, HD), cosine_table, sine_table)
    key_heads = rotate(projected[:, H * HD:(H + KVH) * HD].reshape(-1, KVH, HD), cosine_table, sine_table)
    value_heads = projected[:, (H + KVH) * HD:].reshape(-1, KVH, HD)
    query_heads = low_back(low(query_heads * HD ** (-0.5)))
    key_heads = low_back(low(key_heads))
    value_heads = low_back(low(value_heads))
    seq_queries = by_sequence(query_heads)
    seq_keys = by_sequence(key_heads)
    seq_values = by_sequence(value_heads)
    seq_pos = by_sequence(flat_pos)
    outputs = jnp.stack([attend_sequence(seq_queries[seq_index], seq_keys[seq_index], seq_values[seq_index], seq_pos[seq_index]) for seq_index in range(SEQS)])
    attended = low(low_back(from_sequences(outputs)))
    middle = token_rows + low_back(jnp.dot(attended, w_o, precision=HIGH))
    normed_two = low(middle * rms_scale(middle) * gain_two)
    gate_part = low_back(jnp.dot(normed_two, w_gate, precision=HIGH))
    up_part = low_back(jnp.dot(normed_two, w_up, precision=HIGH))
    hidden = low(jax.nn.silu(gate_part) * up_part)
    mixed_out = middle + low_back(jnp.dot(hidden, w_down, precision=HIGH))
    return mixed_out.reshape(SPAN, 2 * SEQS, D)

def reference(layer_input, block_order, first_gain, w_qkv, b_qkv, w_o, second_gain, w_gate, w_up, w_down, cotangent):
    positions = token_positions(block_order)
    params = tuple((item.astype(jnp.float32) for item in (layer_input, first_gain, w_qkv, b_qkv, w_o, second_gain, w_gate, w_up, w_down)))

    def forward(inputs, gain_one, w_one, bias_one, w_two, gain_two, w_three, w_four, w_five):
        return layer(inputs, gain_one, w_one, bias_one, w_two, gain_two, w_three, w_four, w_five, positions)
    mixed_out, pull_back = jax.vjp(forward, *params)
    grads = pull_back(cotangent.astype(jnp.float32))
    return (mixed_out.astype(jnp.bfloat16), grads[0], grads[1], grads[2], grads[3][:QK], grads[3][QK:], grads[4], grads[5], grads[6], grads[7], grads[8])
```

```python
import functools

import jax
import jax.numpy as jnp
from jax import lax
from jax.experimental import pallas as pl
from jax.experimental.pallas import tpu as pltpu
from jax.sharding import PartitionSpec as P

D = 1536
H = 12
KVH = 2
HD = 128
FF = 8960
SEQS = 2
QKV = 2048
QK = 1792


EPS = 1e-06
THETA = 1000000.0
NEG_FILL = -1e30
CONTRACT_LAST = (((1,), (1,)), ((), ()))
CONTRACT_FIRST = (((0,), (0,)), ((), ()))


def narrowed(values):
    return lax.optimization_barrier(values.astype(jnp.bfloat16)).astype(jnp.float32)


def block_positions(block_order, first_row, row_count, block_rows, ctx_size):
    row_index = first_row + jnp.arange(row_count, dtype=jnp.int32)
    slot_index = jnp.arange(2 * SEQS, dtype=jnp.int32)
    entries = (slot_index // SEQS)[None, :] * ctx_size + (row_index // block_rows)[:, None]
    tiled = jnp.tile(block_order, (2, 1))
    entry_ids = jnp.arange(2 * ctx_size, dtype=jnp.int32)
    picked = jnp.sum(
        jnp.where(entries[:, :, None] == entry_ids[None, None, :], tiled[None, :, :], 0), -1
    )
    return picked * block_rows + (row_index % block_rows)[:, None]


def to_groups(tokens, row_count):
    shaped = tokens.reshape(row_count, 2, SEQS, KVH, H // KVH, HD)
    return shaped.transpose(2, 1, 3, 4, 0, 5).reshape(SEQS, 2, KVH, H // KVH * row_count, HD)


def from_groups(grouped, row_count):
    shaped = grouped.reshape(SEQS, 2, KVH, H // KVH, row_count, HD).transpose(4, 1, 0, 2, 3, 5)
    return shaped.reshape(row_count * 2 * SEQS, H * HD)


def rope_tables(positions):
    half_width = HD // 2
    frequency = THETA ** (-jnp.arange(half_width, dtype=jnp.float32) * 2.0 / HD)
    angles = positions.astype(jnp.float32)[:, None] * frequency[None, :]
    cosine_table = jnp.concatenate([jnp.cos(angles), jnp.cos(angles)], -1)[:, None, :]
    sine_table = jnp.concatenate([jnp.sin(angles), jnp.sin(angles)], -1)[:, None, :]
    return (cosine_table, sine_table)


def rotate(head_values, cosine_table, sine_table):
    half_width = HD // 2
    turned = jnp.concatenate([-head_values[..., half_width:], head_values[..., :half_width]], -1)
    return head_values * cosine_table + turned * sine_table


def rotate_back(grad_values, cosine_table, sine_table):
    half_width = HD // 2
    moved = grad_values * sine_table
    return grad_values * cosine_table + jnp.concatenate(
        [moved[..., half_width:], -moved[..., :half_width]], -1
    )


def normalize(values, gain):
    scale = lax.rsqrt(jnp.mean(values * values, -1, keepdims=True) + EPS)
    unit = values * scale
    return (unit, scale, unit * gain)


def norm_back(grad_out, unit, scale, gain):
    grad_unit = grad_out * gain
    inner = jnp.mean(grad_unit * unit, -1, keepdims=True)
    return (scale * (grad_unit - unit * inner), jnp.sum(grad_out * unit, 0))


def attend_forward_kernel(ctx_size, block_rows, rows_here, scalars, q_ref, kv_ref, out_ref, stat_ref, best_ref, total_ref, accum_ref):
    seq = pl.program_id(0)
    blocks = 2 * ctx_size
    own_ctx = scalars[SEQS * blocks]
    own_shard = scalars[SEQS * blocks + 1]
    lanes = q_ref.shape[3]
    best_ref[...] = jnp.full(best_ref.shape, NEG_FILL, jnp.float32)
    total_ref[...] = jnp.zeros(total_ref.shape, jnp.float32)
    accum_ref[...] = jnp.zeros(accum_ref.shape, jnp.float32)

    def step(key_ctx, half_key, half):
        order_key = scalars[seq * blocks + half_key * ctx_size + key_ctx]
        order_query = scalars[seq * blocks + half * ctx_size + own_ctx]

        def work(masked):
            rows = pl.ds(pl.multiple_of(key_ctx * block_rows, block_rows), block_rows)
            keys = kv_ref[rows, half_key * 2 * HD : half_key * 2 * HD + HD]
            values = kv_ref[rows, half_key * 2 * HD + HD : half_key * 2 * HD + 2 * HD]
            scores = lax.dot_general(
                keys, q_ref[0, half, 0], CONTRACT_LAST, preferred_element_type=jnp.float32
            )
            if masked:
                row = lax.broadcasted_iota(jnp.int32, (block_rows, lanes), 0)
                lane = lax.broadcasted_iota(jnp.int32, (block_rows, lanes), 1)
                scores = jnp.where(
                    row <= own_shard * rows_here + lax.rem(lane, rows_here), scores, NEG_FILL
                )
            best = best_ref[half]
            fresh = jnp.maximum(best, jnp.max(scores, 0, keepdims=True))
            decay = jnp.exp(best - fresh)
            weights = jnp.exp(scores - fresh)
            total_ref[half] = total_ref[half] * decay + jnp.sum(weights, 0, keepdims=True)
            accum_ref[half] = accum_ref[half] * decay + lax.dot_general(
                values,
                weights.astype(jnp.bfloat16),
                CONTRACT_FIRST,
                preferred_element_type=jnp.float32,
            )
            best_ref[half] = fresh

        @pl.when(order_key < order_query)
        def full():
            work(False)

        @pl.when(order_key == order_query)
        def diagonal():
            work(True)

    @pl.loop(0, ctx_size)
    def sweep(key_ctx):
        for half_key in range(2):
            for half in range(2):
                step(key_ctx, half_key, half)

    for half in range(2):
        totals = total_ref[half]
        out_ref[0, half, 0] = (accum_ref[half] / totals).T
        stat_ref[0, half, 0] = best_ref[half] + jnp.log(totals)


def attend_forward(scalars, queries, all_kv, ctx_size, block_rows, rows_here):
    lanes = queries.shape[3]
    kernel = functools.partial(attend_forward_kernel, ctx_size, block_rows, rows_here)
    group = pl.BlockSpec((1, 2, 1, lanes, HD), lambda s, n, _: (s, 0, n, 0, 0))
    stat = pl.BlockSpec((1, 2, 1, 1, lanes), lambda s, n, _: (s, 0, n, 0, 0))
    return pl.pallas_call(
        kernel,
        grid_spec=pltpu.PrefetchScalarGridSpec(
            num_scalar_prefetch=1,
            grid=(SEQS, KVH),
            in_specs=[
                group,
                pl.BlockSpec((all_kv.shape[0], 4 * HD), lambda s, n, _: (0, s * KVH + n)),
            ],
            out_specs=[group, stat],
            scratch_shapes=[
                pltpu.VMEM((2, 1, lanes), jnp.float32),
                pltpu.VMEM((2, 1, lanes), jnp.float32),
                pltpu.VMEM((2, HD, lanes), jnp.float32),
            ],
        ),
        out_shape=(
            jax.ShapeDtypeStruct(queries.shape, jnp.float32),
            jax.ShapeDtypeStruct((SEQS, 2, KVH, 1, lanes), jnp.float32),
        ),
        compiler_params=pltpu.CompilerParams(vmem_limit_bytes=56 * 2**20),
        name="attend_forward",
    )(scalars, queries, all_kv)


def attend_backward_kernel(ctx_size, block_rows, rows_here, scalars, q_ref, go_ref, att_ref, stat_ref, kv_ref, gq_ref, gkv_ref, delta_ref, gq_acc, gk_acc, gv_acc):
    seq = pl.program_id(0)
    blocks = 2 * ctx_size
    own_ctx = scalars[SEQS * blocks]
    own_shard = scalars[SEQS * blocks + 1]
    lanes = q_ref.shape[3]
    gq_acc[...] = jnp.zeros(gq_acc.shape, jnp.float32)
    for half in range(2):
        product = go_ref[0, half, 0].astype(jnp.float32) * att_ref[0, half, 0]
        delta_ref[half] = jnp.sum(product.T, 0, keepdims=True)

    def step(key_ctx, half_key, half):
        order_key = scalars[seq * blocks + half_key * ctx_size + key_ctx]
        order_query = scalars[seq * blocks + half * ctx_size + own_ctx]

        def work(masked):
            rows = pl.ds(pl.multiple_of(key_ctx * block_rows, block_rows), block_rows)
            keys = kv_ref[rows, half_key * 2 * HD : half_key * 2 * HD + HD]
            values = kv_ref[rows, half_key * 2 * HD + HD : half_key * 2 * HD + 2 * HD]
            queries = q_ref[0, half, 0]
            grad_out = go_ref[0, half, 0]
            scores = lax.dot_general(
                keys, queries, CONTRACT_LAST, preferred_element_type=jnp.float32
            )
            probs = jnp.exp(scores - stat_ref[0, half, 0])
            if masked:
                row = lax.broadcasted_iota(jnp.int32, (block_rows, lanes), 0)
                lane = lax.broadcasted_iota(jnp.int32, (block_rows, lanes), 1)
                probs = jnp.where(
                    row <= own_shard * rows_here + lax.rem(lane, rows_here), probs, 0.0
                )
            grad_probs = lax.dot_general(
                values, grad_out, CONTRACT_LAST, preferred_element_type=jnp.float32
            )
            grad_scores = (probs * (grad_probs - delta_ref[half])).astype(jnp.bfloat16)
            gv_acc[...] += jnp.dot(
                probs.astype(jnp.bfloat16), grad_out, preferred_element_type=jnp.float32
            )
            gk_acc[...] += jnp.dot(grad_scores, queries, preferred_element_type=jnp.float32)
            gq_acc[half] += lax.dot_general(
                keys, grad_scores, CONTRACT_FIRST, preferred_element_type=jnp.float32
            )

        @pl.when(order_key < order_query)
        def full():
            work(False)

        @pl.when(order_key == order_query)
        def diagonal():
            work(True)

    @pl.loop(0, ctx_size)
    def sweep(key_ctx):
        rows = pl.ds(pl.multiple_of(key_ctx * block_rows, block_rows), block_rows)
        for half_key in range(2):
            gk_acc[...] = jnp.zeros(gk_acc.shape, jnp.float32)
            gv_acc[...] = jnp.zeros(gv_acc.shape, jnp.float32)
            for half in range(2):
                step(key_ctx, half_key, half)
            at = half_key * 2 * HD
            gkv_ref[rows, at : at + HD] = gk_acc[...].astype(jnp.bfloat16)
            gkv_ref[rows, at + HD : at + 2 * HD] = gv_acc[...].astype(jnp.bfloat16)

    for half in range(2):
        gq_ref[0, half, 0] = gq_acc[half].T


def attend_backward(scalars, queries, grad_out, attended, stats, all_kv, ctx_size, block_rows, rows_here):
    lanes = queries.shape[3]
    kernel = functools.partial(attend_backward_kernel, ctx_size, block_rows, rows_here)
    group = pl.BlockSpec((1, 2, 1, lanes, HD), lambda s, n, _: (s, 0, n, 0, 0))
    stat = pl.BlockSpec((1, 2, 1, 1, lanes), lambda s, n, _: (s, 0, n, 0, 0))
    full = pl.BlockSpec((all_kv.shape[0], 4 * HD), lambda s, n, _: (0, s * KVH + n))
    return pl.pallas_call(
        kernel,
        grid_spec=pltpu.PrefetchScalarGridSpec(
            num_scalar_prefetch=1,
            grid=(SEQS, KVH),
            in_specs=[group, group, group, stat, full],
            out_specs=[group, full],
            scratch_shapes=[
                pltpu.VMEM((2, 1, lanes), jnp.float32),
                pltpu.VMEM((2, HD, lanes), jnp.float32),
                pltpu.VMEM((block_rows, HD), jnp.float32),
                pltpu.VMEM((block_rows, HD), jnp.float32),
            ],
        ),
        out_shape=(
            jax.ShapeDtypeStruct(queries.shape, jnp.float32),
            jax.ShapeDtypeStruct(all_kv.shape, jnp.bfloat16),
        ),
        compiler_params=pltpu.CompilerParams(vmem_limit_bytes=56 * 2**20),
        name="attend_backward",
    )(scalars, queries, grad_out, attended, stats, all_kv)


def column_terms_to_rows(terms):
    ctx_size = lax.axis_size("ctx")
    shard_count = lax.axis_size("fsdp")
    cut = D // (ctx_size * shard_count)
    columns = terms.shape[1]
    stacked = terms.reshape(shard_count, ctx_size, cut, columns).transpose(1, 0, 2, 3)
    summed = lax.psum_scatter(stacked, "ctx", scatter_dimension=0, tiled=True)
    summed = summed.reshape(shard_count * cut, columns)
    rows = lax.all_to_all(summed, "fsdp", 0, 1, tiled=True)
    return lax.all_gather(rows, "ctx", axis=0, tiled=True).astype(jnp.float32)


def shards(
    layer_input,
    block_order,
    first_gain,
    w_qkv,
    b_qkv,
    w_o,
    second_gain,
    w_gate,
    w_up,
    w_down,
    cotangent,
):
    ctx_size = lax.axis_size("ctx")
    shard_count = lax.axis_size("fsdp")
    rows_here = layer_input.shape[0]
    slots = layer_input.shape[1]
    block_rows = rows_here * shard_count
    kv_width = KVH * HD
    first_row = (lax.axis_index("ctx") * shard_count + lax.axis_index("fsdp")) * rows_here
    own_pos = block_positions(block_order, first_row, rows_here, block_rows, ctx_size)
    cosine_table, sine_table = rope_tables(own_pos.reshape(-1))
    query_scale = HD ** (-0.5)
    w_qkv_all, w_o_all, bias_all, gain_one, gain_two = (
        lax.all_gather(w_qkv, "fsdp", axis=0, tiled=True),
        lax.all_gather(w_o, "fsdp", axis=0, tiled=True),
        lax.all_gather(b_qkv, "fsdp", axis=0, tiled=True),
        lax.all_gather(first_gain, "fsdp", axis=0, tiled=True),
        lax.all_gather(second_gain, "fsdp", axis=0, tiled=True),
    )
    gate_cols = lax.all_to_all(w_gate, "fsdp", 1, 0, tiled=True)
    up_cols = lax.all_to_all(w_up, "fsdp", 1, 0, tiled=True)
    cotangent_all = lax.all_gather(cotangent.reshape(-1, D), "fsdp", axis=0, tiled=True)
    gain_one = gain_one.astype(jnp.float32)
    gain_two = gain_two.astype(jnp.float32)
    inputs = layer_input.reshape(-1, D).astype(jnp.float32)
    unit_one, scale_one, normed = normalize(inputs, gain_one)
    normed_one = normed.astype(jnp.bfloat16)
    projected = jnp.dot(
        normed_one, w_qkv_all, preferred_element_type=jnp.float32
    ) + bias_all.astype(jnp.float32)
    query_raw = projected[:, : H * HD].reshape(-1, H, HD)
    key_raw = projected[:, H * HD : H * HD + kv_width].reshape(-1, KVH, HD)
    value_raw = projected[:, H * HD + kv_width :]
    query_tokens = (
        (rotate(query_raw, cosine_table, sine_table) * query_scale)
        .astype(jnp.bfloat16)
        .reshape(-1, H * HD)
    )
    key_tokens = (
        rotate(key_raw, cosine_table, sine_table).astype(jnp.bfloat16).reshape(-1, kv_width)
    )
    own_kv = jnp.stack([key_tokens, value_raw.astype(jnp.bfloat16)], 1)
    own_kv = own_kv.reshape(rows_here, 2, SEQS, 2, KVH, HD).transpose(0, 2, 4, 1, 3, 5)
    own_kv = own_kv.reshape(rows_here, SEQS * KVH * 4 * HD)
    all_kv = lax.all_gather(own_kv, ("ctx", "fsdp"), axis=0, tiled=True)
    queries = to_groups(query_tokens, rows_here)
    scalars = jnp.concatenate(
        [
            block_order.reshape(-1),
            jnp.stack([lax.axis_index("ctx"), lax.axis_index("fsdp")]).astype(jnp.int32),
        ]
    )
    attended_grouped, stats = attend_forward(
        scalars, queries, all_kv, ctx_size, block_rows, rows_here
    )
    attended_low = from_groups(attended_grouped, rows_here).astype(jnp.bfloat16)
    middle = inputs + jnp.dot(attended_low, w_o_all, preferred_element_type=jnp.float32)
    unit_two, scale_two, normed = normalize(middle, gain_two)
    normed_two = normed.astype(jnp.bfloat16)
    tokens_all = lax.all_gather(normed_two, "fsdp", axis=0, tiled=True)
    gate_part = jnp.dot(tokens_all, gate_cols, preferred_element_type=jnp.float32)
    up_part = jnp.dot(tokens_all, up_cols, preferred_element_type=jnp.float32)
    sigmoid_gate = jax.nn.sigmoid(gate_part)
    activated = gate_part * sigmoid_gate
    hidden = (activated * up_part).astype(jnp.bfloat16)
    grad_hidden = lax.dot_general(
        cotangent_all, w_down, CONTRACT_LAST, preferred_element_type=jnp.float32
    )
    grad_gate = (
        grad_hidden * up_part * sigmoid_gate * (1.0 + gate_part * (1.0 - sigmoid_gate))
    ).astype(jnp.bfloat16)
    grad_up = (grad_hidden * activated).astype(jnp.bfloat16)
    grad_tokens = lax.dot_general(
        grad_gate, gate_cols, CONTRACT_LAST, preferred_element_type=jnp.float32
    ) + lax.dot_general(grad_up, up_cols, CONTRACT_LAST, preferred_element_type=jnp.float32)
    grad_normed_two = lax.psum_scatter(
        grad_tokens.astype(jnp.bfloat16), "fsdp", scatter_dimension=0, tiled=True
    ).astype(jnp.float32)
    mixed_terms = jnp.dot(hidden, w_down, preferred_element_type=jnp.float32)
    mixed_out = middle + lax.psum_scatter(
        mixed_terms.astype(jnp.bfloat16), "fsdp", scatter_dimension=0, tiled=True
    ).astype(jnp.float32)
    output = mixed_out.astype(jnp.bfloat16).reshape(rows_here, slots, D)
    down_terms = lax.dot_general(
        hidden, cotangent_all, CONTRACT_FIRST, preferred_element_type=jnp.float32
    ).astype(jnp.bfloat16)
    gate_terms = lax.dot_general(
        tokens_all, grad_gate, CONTRACT_FIRST, preferred_element_type=jnp.float32
    ).astype(jnp.bfloat16)
    up_terms = lax.dot_general(
        tokens_all, grad_up, CONTRACT_FIRST, preferred_element_type=jnp.float32
    ).astype(jnp.bfloat16)
    down_rows = lax.psum(down_terms, "ctx").astype(jnp.float32)
    gate_rows = column_terms_to_rows(gate_terms)
    up_rows = column_terms_to_rows(up_terms)
    grad_middle_norm, grad_gain_two = norm_back(grad_normed_two, unit_two, scale_two, gain_two)
    grad_middle = cotangent.reshape(-1, D).astype(jnp.float32) + grad_middle_norm
    grad_branch_one = grad_middle.astype(jnp.bfloat16)
    grad_attended = lax.dot_general(
        grad_branch_one, w_o_all, CONTRACT_LAST, preferred_element_type=jnp.float32
    ).astype(jnp.bfloat16)
    grad_queries, grad_kv_full = attend_backward(
        scalars,
        queries,
        to_groups(grad_attended, rows_here),
        attended_grouped,
        stats,
        all_kv,
        ctx_size,
        block_rows,
        rows_here,
    )
    grad_kv = lax.psum_scatter(
        grad_kv_full, ("ctx", "fsdp"), scatter_dimension=0, tiled=True
    ).astype(jnp.float32)
    grad_kv_low = narrowed(grad_kv).reshape(rows_here, SEQS, KVH, 2, 2, HD)
    grad_kv_low = grad_kv_low.transpose(0, 3, 1, 4, 2, 5).reshape(-1, 2 * kv_width)
    grad_query_tokens = from_groups(narrowed(grad_queries), rows_here) * query_scale
    grad_query_raw = rotate_back(
        grad_query_tokens.reshape(-1, H, HD), cosine_table, sine_table
    ).reshape(-1, H * HD)
    grad_key_raw = rotate_back(
        grad_kv_low[:, :kv_width].reshape(-1, KVH, HD), cosine_table, sine_table
    ).reshape(-1, kv_width)
    grad_projected = jnp.concatenate(
        [grad_query_raw, grad_key_raw, grad_kv_low[:, kv_width:]], -1
    ).astype(jnp.bfloat16)
    grad_bias = jnp.sum(grad_projected, 0, dtype=jnp.float32)
    grad_bias_qk = grad_bias[:QK]
    grad_bias_value = grad_bias[QK:]
    grad_normed_one = lax.dot_general(
        grad_projected, w_qkv_all, CONTRACT_LAST, preferred_element_type=jnp.float32
    )
    grad_input_norm, grad_gain_one = norm_back(grad_normed_one, unit_one, scale_one, gain_one)
    grad_input = (grad_middle + grad_input_norm).reshape(rows_here, slots, D)
    qkv_rows = lax.psum_scatter(
        lax.dot_general(
            normed_one, grad_projected, CONTRACT_FIRST, preferred_element_type=jnp.float32
        ).astype(jnp.bfloat16),
        "fsdp",
        scatter_dimension=0,
        tiled=True,
    )
    o_rows = lax.psum_scatter(
        lax.dot_general(
            attended_low, grad_branch_one, CONTRACT_FIRST, preferred_element_type=jnp.float32
        ).astype(jnp.bfloat16),
        "fsdp",
        scatter_dimension=0,
        tiled=True,
    )
    qkv_rows = lax.psum(qkv_rows, "ctx").astype(jnp.float32)
    o_rows = lax.psum(o_rows, "ctx").astype(jnp.float32)
    gain_one_rows, gain_two_rows, bias_rows, value_bias_rows = (
        lax.psum_scatter(grad_gain_one, "fsdp", scatter_dimension=0, tiled=True),
        lax.psum_scatter(grad_gain_two, "fsdp", scatter_dimension=0, tiled=True),
        lax.psum_scatter(grad_bias_qk, "fsdp", scatter_dimension=0, tiled=True),
        lax.psum_scatter(grad_bias_value, "fsdp", scatter_dimension=0, tiled=True),
    )
    gain_one_rows, gain_two_rows, bias_rows, value_bias_rows = (
        lax.psum(gain_one_rows, "ctx"),
        lax.psum(gain_two_rows, "ctx"),
        lax.psum(bias_rows, "ctx"),
        lax.psum(value_bias_rows, "ctx"),
    )
    return (
        output,
        grad_input,
        gain_one_rows,
        qkv_rows,
        bias_rows,
        value_bias_rows,
        o_rows,
        gain_two_rows,
        gate_rows,
        up_rows,
        down_rows,
    )


def solution(mesh):
    in_specs = (
        P(("ctx", "fsdp"), None, None),
        P(),
        P("fsdp"),
        P("fsdp", None),
        P("fsdp"),
        P("fsdp", None),
        P("fsdp"),
        P("fsdp", None),
        P("fsdp", None),
        P("fsdp", None),
        P(("ctx", "fsdp"), None, None),
    )
    out_specs = (
        P(("ctx", "fsdp"), None, None),
        P(("ctx", "fsdp"), None, None),
        P("fsdp"),
        P("fsdp", None),
        P("fsdp"),
        P("fsdp"),
        P("fsdp", None),
        P("fsdp"),
        P("fsdp", None),
        P("fsdp", None),
        P("fsdp", None),
    )
    return jax.shard_map(shards, mesh=mesh, in_specs=in_specs, out_specs=out_specs, check_vma=False)
```

```python
import functools

import jax
import jax.numpy as jnp
from jax import lax
from jax.experimental import pallas as pl
from jax.experimental.pallas import tpu as pltpu
from jax.sharding import PartitionSpec as P

D = 1536
H = 12
KVH = 2
HD = 128
FF = 8960
SEQS = 2
QKV = 2048
QK = 1792


EPS = 1e-06
THETA = 1000000.0
NEG_FILL = -1e30
MESH_ID = pl.DeviceIdType.MESH
CONTRACT_LAST = (((1,), (1,)), ((), ()))
CONTRACT_FIRST = (((0,), (0,)), ((), ()))


def narrowed(values):
    return lax.optimization_barrier(values.astype(jnp.bfloat16)).astype(jnp.float32)


def block_positions(block_order, first_row, row_count, block_rows, ctx_size):
    row_index = first_row + jnp.arange(row_count, dtype=jnp.int32)
    slot_index = jnp.arange(2 * SEQS, dtype=jnp.int32)
    entries = (slot_index // SEQS)[None, :] * ctx_size + (row_index // block_rows)[:, None]
    tiled = jnp.tile(block_order, (2, 1))
    entry_ids = jnp.arange(2 * ctx_size, dtype=jnp.int32)
    picked = jnp.sum(
        jnp.where(entries[:, :, None] == entry_ids[None, None, :], tiled[None, :, :], 0), -1
    )
    return picked * block_rows + (row_index % block_rows)[:, None]


def to_groups(tokens, row_count):
    shaped = tokens.reshape(row_count, 2, SEQS, KVH, H // KVH, HD)
    return shaped.transpose(2, 1, 3, 4, 0, 5).reshape(SEQS, 2, KVH, H // KVH * row_count, HD)


def from_groups(grouped, row_count):
    shaped = grouped.reshape(SEQS, 2, KVH, H // KVH, row_count, HD).transpose(4, 1, 0, 2, 3, 5)
    return shaped.reshape(row_count * 2 * SEQS, H * HD)


def rope_tables(positions):
    half_width = HD // 2
    frequency = THETA ** (-jnp.arange(half_width, dtype=jnp.float32) * 2.0 / HD)
    angles = positions.astype(jnp.float32)[:, None] * frequency[None, :]
    cosine_table = jnp.concatenate([jnp.cos(angles), jnp.cos(angles)], -1)[:, None, :]
    sine_table = jnp.concatenate([jnp.sin(angles), jnp.sin(angles)], -1)[:, None, :]
    return (cosine_table, sine_table)


def rotate(head_values, cosine_table, sine_table):
    half_width = HD // 2
    turned = jnp.concatenate([-head_values[..., half_width:], head_values[..., :half_width]], -1)
    return head_values * cosine_table + turned * sine_table


def rotate_back(grad_values, cosine_table, sine_table):
    half_width = HD // 2
    moved = grad_values * sine_table
    return grad_values * cosine_table + jnp.concatenate(
        [moved[..., half_width:], -moved[..., :half_width]], -1
    )


def normalize(values, gain):
    scale = lax.rsqrt(jnp.mean(values * values, -1, keepdims=True) + EPS)
    unit = values * scale
    return (unit, scale, unit * gain)


def norm_back(grad_out, unit, scale, gain):
    grad_unit = grad_out * gain
    inner = jnp.mean(grad_unit * unit, -1, keepdims=True)
    return (scale * (grad_unit - unit * inner), jnp.sum(grad_out * unit, 0))


def attend_forward_kernel(ctx_size, block_rows, rows_here, scalars, q_ref, kv_ref, out_ref, stat_ref, best_ref, total_ref, accum_ref):
    seq = pl.program_id(0)
    blocks = 2 * ctx_size
    own_ctx = scalars[SEQS * blocks]
    own_shard = scalars[SEQS * blocks + 1]
    lanes = q_ref.shape[3]
    best_ref[...] = jnp.full(best_ref.shape, NEG_FILL, jnp.float32)
    total_ref[...] = jnp.zeros(total_ref.shape, jnp.float32)
    accum_ref[...] = jnp.zeros(accum_ref.shape, jnp.float32)

    def step(key_ctx, half_key, half):
        order_key = scalars[seq * blocks + half_key * ctx_size + key_ctx]
        order_query = scalars[seq * blocks + half * ctx_size + own_ctx]

        def work(masked):
            rows = pl.ds(pl.multiple_of(key_ctx * block_rows, block_rows), block_rows)
            keys = kv_ref[rows, half_key * 2 * HD : half_key * 2 * HD + HD]
            values = kv_ref[rows, half_key * 2 * HD + HD : half_key * 2 * HD + 2 * HD]
            scores = lax.dot_general(
                keys, q_ref[0, half, 0], CONTRACT_LAST, preferred_element_type=jnp.float32
            )
            if masked:
                row = lax.broadcasted_iota(jnp.int32, (block_rows, lanes), 0)
                lane = lax.broadcasted_iota(jnp.int32, (block_rows, lanes), 1)
                scores = jnp.where(
                    row <= own_shard * rows_here + lax.rem(lane, rows_here), scores, NEG_FILL
                )
            best = best_ref[half]
            fresh = jnp.maximum(best, jnp.max(scores, 0, keepdims=True))
            decay = jnp.exp(best - fresh)
            weights = jnp.exp(scores - fresh)
            total_ref[half] = total_ref[half] * decay + jnp.sum(weights, 0, keepdims=True)
            accum_ref[half] = accum_ref[half] * decay + lax.dot_general(
                values,
                weights.astype(jnp.bfloat16),
                CONTRACT_FIRST,
                preferred_element_type=jnp.float32,
            )
            best_ref[half] = fresh

        @pl.when(order_key < order_query)
        def full():
            work(False)

        @pl.when(order_key == order_query)
        def diagonal():
            work(True)

    @pl.loop(0, ctx_size)
    def sweep(key_ctx):
        for half_key in range(2):
            for half in range(2):
                step(key_ctx, half_key, half)

    for half in range(2):
        totals = total_ref[half]
        out_ref[0, half, 0] = (accum_ref[half] / totals).T
        stat_ref[0, half, 0] = best_ref[half] + jnp.log(totals)


def attend_forward(scalars, queries, all_kv, ctx_size, block_rows, rows_here):
    lanes = queries.shape[3]
    kernel = functools.partial(attend_forward_kernel, ctx_size, block_rows, rows_here)
    group = pl.BlockSpec((1, 2, 1, lanes, HD), lambda s, n, _: (s, 0, n, 0, 0))
    stat = pl.BlockSpec((1, 2, 1, 1, lanes), lambda s, n, _: (s, 0, n, 0, 0))
    return pl.pallas_call(
        kernel,
        grid_spec=pltpu.PrefetchScalarGridSpec(
            num_scalar_prefetch=1,
            grid=(SEQS, KVH),
            in_specs=[
                group,
                pl.BlockSpec((all_kv.shape[0], 4 * HD), lambda s, n, _: (0, s * KVH + n)),
            ],
            out_specs=[group, stat],
            scratch_shapes=[
                pltpu.VMEM((2, 1, lanes), jnp.float32),
                pltpu.VMEM((2, 1, lanes), jnp.float32),
                pltpu.VMEM((2, HD, lanes), jnp.float32),
            ],
        ),
        out_shape=(
            jax.ShapeDtypeStruct(queries.shape, jnp.float32),
            jax.ShapeDtypeStruct((SEQS, 2, KVH, 1, lanes), jnp.float32),
        ),
        compiler_params=pltpu.CompilerParams(vmem_limit_bytes=56 * 2**20),
        name="attend_forward",
    )(scalars, queries, all_kv)


def attend_backward_kernel(ctx_size, block_rows, rows_here, scalars, q_ref, go_ref, att_ref, stat_ref, kv_ref, gq_ref, gkv_ref, delta_ref, gq_acc, gk_acc, gv_acc):
    seq = pl.program_id(0)
    blocks = 2 * ctx_size
    own_ctx = scalars[SEQS * blocks]
    own_shard = scalars[SEQS * blocks + 1]
    lanes = q_ref.shape[3]
    gq_acc[...] = jnp.zeros(gq_acc.shape, jnp.float32)
    for half in range(2):
        product = go_ref[0, half, 0].astype(jnp.float32) * att_ref[0, half, 0]
        delta_ref[half] = jnp.sum(product.T, 0, keepdims=True)

    def step(key_ctx, half_key, half):
        order_key = scalars[seq * blocks + half_key * ctx_size + key_ctx]
        order_query = scalars[seq * blocks + half * ctx_size + own_ctx]

        def work(masked):
            rows = pl.ds(pl.multiple_of(key_ctx * block_rows, block_rows), block_rows)
            keys = kv_ref[rows, half_key * 2 * HD : half_key * 2 * HD + HD]
            values = kv_ref[rows, half_key * 2 * HD + HD : half_key * 2 * HD + 2 * HD]
            queries = q_ref[0, half, 0]
            grad_out = go_ref[0, half, 0]
            scores = lax.dot_general(
                keys, queries, CONTRACT_LAST, preferred_element_type=jnp.float32
            )
            probs = jnp.exp(scores - stat_ref[0, half, 0])
            if masked:
                row = lax.broadcasted_iota(jnp.int32, (block_rows, lanes), 0)
                lane = lax.broadcasted_iota(jnp.int32, (block_rows, lanes), 1)
                probs = jnp.where(
                    row <= own_shard * rows_here + lax.rem(lane, rows_here), probs, 0.0
                )
            grad_probs = lax.dot_general(
                values, grad_out, CONTRACT_LAST, preferred_element_type=jnp.float32
            )
            grad_scores = (probs * (grad_probs - delta_ref[half])).astype(jnp.bfloat16)
            gv_acc[...] += jnp.dot(
                probs.astype(jnp.bfloat16), grad_out, preferred_element_type=jnp.float32
            )
            gk_acc[...] += jnp.dot(grad_scores, queries, preferred_element_type=jnp.float32)
            gq_acc[half] += lax.dot_general(
                keys, grad_scores, CONTRACT_FIRST, preferred_element_type=jnp.float32
            )

        @pl.when(order_key < order_query)
        def full():
            work(False)

        @pl.when(order_key == order_query)
        def diagonal():
            work(True)

    @pl.loop(0, ctx_size)
    def sweep(key_ctx):
        rows = pl.ds(pl.multiple_of(key_ctx * block_rows, block_rows), block_rows)
        for half_key in range(2):
            gk_acc[...] = jnp.zeros(gk_acc.shape, jnp.float32)
            gv_acc[...] = jnp.zeros(gv_acc.shape, jnp.float32)
            for half in range(2):
                step(key_ctx, half_key, half)
            at = half_key * 2 * HD
            gkv_ref[rows, at : at + HD] = gk_acc[...].astype(jnp.bfloat16)
            gkv_ref[rows, at + HD : at + 2 * HD] = gv_acc[...].astype(jnp.bfloat16)

    for half in range(2):
        gq_ref[0, half, 0] = gq_acc[half].T


def attend_backward(scalars, queries, grad_out, attended, stats, all_kv, ctx_size, block_rows, rows_here):
    lanes = queries.shape[3]
    kernel = functools.partial(attend_backward_kernel, ctx_size, block_rows, rows_here)
    group = pl.BlockSpec((1, 2, 1, lanes, HD), lambda s, n, _: (s, 0, n, 0, 0))
    stat = pl.BlockSpec((1, 2, 1, 1, lanes), lambda s, n, _: (s, 0, n, 0, 0))
    full = pl.BlockSpec((all_kv.shape[0], 4 * HD), lambda s, n, _: (0, s * KVH + n))
    return pl.pallas_call(
        kernel,
        grid_spec=pltpu.PrefetchScalarGridSpec(
            num_scalar_prefetch=1,
            grid=(SEQS, KVH),
            in_specs=[group, group, group, stat, full],
            out_specs=[group, full],
            scratch_shapes=[
                pltpu.VMEM((2, 1, lanes), jnp.float32),
                pltpu.VMEM((2, HD, lanes), jnp.float32),
                pltpu.VMEM((block_rows, HD), jnp.float32),
                pltpu.VMEM((block_rows, HD), jnp.float32),
            ],
        ),
        out_shape=(
            jax.ShapeDtypeStruct(queries.shape, jnp.float32),
            jax.ShapeDtypeStruct(all_kv.shape, jnp.bfloat16),
        ),
        compiler_params=pltpu.CompilerParams(vmem_limit_bytes=56 * 2**20),
        name="attend_backward",
    )(scalars, queries, grad_out, attended, stats, all_kv)


def peers_of(ctx_size):
    return ctx_size == 4, range(1, ctx_size)


def ctx_target(position, way, square, ctx_size):
    return position ^ way if square else lax.rem(position + way, ctx_size)


def ctx_source(position, way, square, ctx_size):
    return position ^ way if square else lax.rem(position + ctx_size - way, ctx_size)


def greet(ctx_size, pair_count, with_ctx):
    ctx = lax.axis_index("ctx")
    shard = lax.axis_index("fsdp")
    pair, core = shard // 2, shard % 2
    barrier = pltpu.get_barrier_semaphore()
    count = 0
    for step in range(1, pair_count):
        there = lax.rem(pair + step, pair_count) * 2 + core
        pl.semaphore_signal(barrier, inc=1, device_id=(ctx, there), device_id_type=MESH_ID)
        count += 1
    if with_ctx:
        for way in range(1, ctx_size):
            there = lax.rem(ctx + way, ctx_size)
            pl.semaphore_signal(barrier, inc=1, device_id=(there, shard), device_id_type=MESH_ID)
            count += 1
    pl.semaphore_signal(barrier, inc=1, device_id=(ctx, pair * 2 + 1 - core), device_id_type=MESH_ID)
    pl.semaphore_wait(barrier, count + 1)
    return ctx, pair, core


def gather_kernel(arity, ctx_size, pair_count, slot, *refs):
    sources, outs = refs[:arity], refs[arity : 2 * arity]
    pair_send, pair_recv, ctx_send, ctx_recv, core_send, core_recv, local_sem = refs[2 * arity :]
    square, ways = peers_of(ctx_size)
    ctx, pair, core = greet(ctx_size, pair_count, True)
    started = []

    def send(item, source, place, target, sems, at):
        copy = pltpu.make_async_remote_copy(
            src_ref=source,
            dst_ref=outs[item].at[place],
            send_sem=sems[0].at[at],
            recv_sem=sems[1].at[at],
            device_id=target,
            device_id_type=MESH_ID,
        )
        copy.start()
        started.append(copy)

    def arrive(item, place, sems, at):
        pltpu.make_async_remote_copy(
            src_ref=outs[item].at[place],
            dst_ref=outs[item].at[place],
            send_sem=sems[0].at[at],
            recv_sem=sems[1].at[at],
            device_id=(ctx, pair * 2 + core),
            device_id_type=MESH_ID,
        ).wait_recv()

    pair_sems, ctx_sems, core_sems = (pair_send, pair_recv), (ctx_send, ctx_recv), (core_send, core_recv)
    home = slot(ctx, pair * 2 + core)
    locals_ = []
    for item in range(arity):
        copy = pltpu.make_async_copy(sources[item], outs[item].at[home], local_sem.at[item])
        copy.start()
        locals_.append(copy)

    def origin(step):
        return lax.rem(pair + pair_count - step, pair_count)

    def to_core(item, source, from_ctx, way, step):
        send(
            item,
            source,
            slot(from_ctx, origin(step) * 2 + core),
            (ctx, pair * 2 + 1 - core),
            core_sems,
            (way, step, item),
        )

    def spread(step):
        for item in range(arity):
            place = slot(ctx, origin(step) * 2 + core)
            if step == 0:
                source = sources[item]
            else:
                arrive(item, place, pair_sems, (step - 1, item))
                source = outs[item].at[place]
            for way in ways:
                if square and way == 3:
                    continue
                there = ctx_target(ctx, way, square, ctx_size)
                send(item, source, place, (there, pair * 2 + core), ctx_sems, (way - 1, step, item))
            to_core(item, source, ctx, 0, step)

    def collect(step):
        for way in ways:
            if square and way == 3:
                continue
            for item in range(arity):
                come = ctx_source(ctx, way, square, ctx_size)
                place = slot(come, origin(step) * 2 + core)
                arrive(item, place, ctx_sems, (way - 1, step, item))
                source = outs[item].at[place]
                if square and (step % 2 == 0) == (way == 1):
                    send(
                        item,
                        source,
                        place,
                        (ctx ^ (3 - way), pair * 2 + core),
                        ctx_sems,
                        (2, step, item),
                    )
                to_core(item, source, come, way, step)

    def collect_far(step):
        for item in range(arity):
            place = slot(ctx ^ 3, origin(step) * 2 + core)
            arrive(item, place, ctx_sems, (2, step, item))
            to_core(item, outs[item].at[place], ctx ^ 3, 3, step)

    for item in range(arity):
        for step in range(1, pair_count):
            there = lax.rem(pair + step, pair_count) * 2 + core
            send(item, sources[item], home, (ctx, there), pair_sems, (step - 1, item))
    for step in range(pair_count + 2):
        if step < pair_count:
            spread(step)
        if 1 <= step <= pair_count:
            collect(step - 1)
        if square and step >= 2:
            collect_far(step - 2)
    for step in range(pair_count):
        for way in range(ctx_size):
            come = ctx_source(ctx, way, square, ctx_size) if way else ctx
            for item in range(arity):
                arrive(item, slot(come, origin(step) * 2 + 1 - core), core_sems, (way, step, item))
    for copy in locals_:
        copy.wait()
    for copy in started:
        copy.wait_send()


def gather(pieces, slot, collective_id, name):
    ctx_size, shard_count = lax.axis_size("ctx"), lax.axis_size("fsdp")
    pair_count = shard_count // 2
    arity = len(pieces)
    dma = pltpu.SemaphoreType.DMA
    moved = sum(piece.size for piece in pieces) * 2
    return pl.pallas_call(
        functools.partial(gather_kernel, arity, ctx_size, pair_count, slot),
        in_specs=[pl.BlockSpec(memory_space=pltpu.VMEM)] * arity,
        out_specs=[pl.BlockSpec(memory_space=pl.ANY)] * arity,
        out_shape=[
            jax.ShapeDtypeStruct((ctx_size * shard_count,) + piece.shape, piece.dtype) for piece in pieces
        ],
        scratch_shapes=[dma((pair_count - 1, arity))] * 2
        + [dma((ctx_size - 1, pair_count, arity))] * 2
        + [dma((ctx_size, pair_count, arity))] * 2
        + [dma((arity,))],
        compiler_params=pltpu.CompilerParams(collective_id=collective_id, has_side_effects=True),
        cost_estimate=pl.CostEstimate(
            flops=0, bytes_accessed=moved * ctx_size * shard_count * 4, transcendentals=0
        ),
        name=name,
    )(*pieces)


def scatter_kernel(arity, ctx_size, pair_count, slot, spread_ctx, *refs):
    sources, outs, refs = refs[:arity], refs[arity : 2 * arity], refs[2 * arity :]
    halves, relays, asides, ends, finals = (refs[i * arity : (i + 1) * arity] for i in range(5))
    sems = refs[5 * arity :]
    core_sems, relay_sems, ctx_sems, pair_sems, last_sems = (sems[2 * i : 2 * i + 2] for i in range(5))
    square, ways = peers_of(ctx_size)
    ctx, pair, core = greet(ctx_size, pair_count, True)
    order = list(range(1, pair_count)) + [0]
    started = []

    def send(source, target, device, pair_of_sems, at):
        copy = pltpu.make_async_remote_copy(
            src_ref=source,
            dst_ref=target,
            send_sem=pair_of_sems[0].at[at],
            recv_sem=pair_of_sems[1].at[at],
            device_id=device,
            device_id_type=MESH_ID,
        )
        copy.start()
        started.append(copy)

    def arrive(target, pair_of_sems, at):
        pltpu.make_async_remote_copy(
            src_ref=target,
            dst_ref=target,
            send_sem=pair_of_sems[0].at[at],
            recv_sem=pair_of_sems[1].at[at],
            device_id=(ctx, pair * 2 + core),
            device_id_type=MESH_ID,
        ).wait_recv()

    def toward(step):
        return lax.rem(pair + step, pair_count)

    def target_ctx(way):
        return ctx_target(ctx, way, square, ctx_size) if way else ctx

    def f32(value):
        return value.astype(jnp.float32)

    far_first = [3, 1, 2, 0] if square else list(ways) + [0]
    for step in order:
        for way in far_first:
            for item in range(arity):
                send(
                    sources[item].at[slot(target_ctx(way), toward(step) * 2 + 1 - core)],
                    halves[item].at[way, step],
                    (ctx, pair * 2 + 1 - core),
                    core_sems,
                    (way, step, item),
                )

    def fold_core(step):
        for way in far_first:
            for item in range(arity):
                half = halves[item].at[way, step]
                arrive(half, core_sems, (way, step, item))
                mine = sources[item][slot(target_ctx(way), toward(step) * 2 + core)]
                half[...] = (f32(mine) + f32(half[...])).astype(half.dtype)
                if square and way == 3:
                    there = ctx ^ (1 if step % 2 == 0 else 2)
                    send(
                        half,
                        relays[item].at[step],
                        (there, pair * 2 + core),
                        relay_sems,
                        (step, item),
                    )

    def fold_relay(step):
        for item in range(arity):
            if square:
                relay = relays[item].at[step]
                arrive(relay, relay_sems, (step, item))
                half = halves[item].at[2 if step % 2 == 0 else 1, step]
                half[...] = (f32(half[...]) + f32(relay[...])).astype(half.dtype)
            for way in ways:
                if square and way == 3:
                    continue
                send(
                    halves[item].at[way, step],
                    asides[item].at[way - 1, step],
                    (target_ctx(way), pair * 2 + core),
                    ctx_sems,
                    (way - 1, step, item),
                )

    def fold_ctx(step):
        for item in range(arity):
            half = halves[item].at[0, step]
            total = f32(half[...])
            for way in ways:
                if square and way == 3:
                    continue
                aside = asides[item].at[way - 1, step]
                arrive(aside, ctx_sems, (way - 1, step, item))
                total = total + f32(aside[...])
            if step:
                half[...] = total.astype(half.dtype)
                send(
                    half,
                    ends[item].at[step - 1],
                    (ctx, toward(step) * 2 + core),
                    pair_sems,
                    (step - 1, item),
                )
            else:
                for other in range(1, pair_count):
                    end = ends[item].at[other - 1]
                    arrive(end, pair_sems, (other - 1, item))
                    total = total + f32(end[...])
                if spread_ctx:
                    finals[item][...] = total.astype(finals[item].dtype)
                else:
                    outs[item][...] = total.astype(outs[item].dtype)

    for turn in range(pair_count + 2):
        if turn < pair_count:
            fold_core(order[turn])
        if 1 <= turn <= pair_count:
            fold_relay(order[turn - 1])
        if turn >= 2:
            fold_ctx(order[turn - 2])
    if spread_ctx:
        for item in range(arity):
            for way in ways:
                send(
                    finals[item],
                    outs[item].at[ctx],
                    (target_ctx(way), pair * 2 + core),
                    last_sems,
                    (way - 1, item),
                )
            outs[item][ctx] = finals[item][...]
        for item in range(arity):
            for way in ways:
                arrive(outs[item].at[ctx_source(ctx, way, square, ctx_size)], last_sems, (way - 1, item))
    for copy in started:
        copy.wait_send()


def scatter(terms, slot, collective_id, name, spread_ctx=False, out_dtype=None):
    ctx_size, shard_count = lax.axis_size("ctx"), lax.axis_size("fsdp")
    pair_count = shard_count // 2
    arity = len(terms)
    dma = pltpu.SemaphoreType.DMA
    lead = (ctx_size,) if spread_ctx else ()
    asides = 2 if ctx_size == 4 else ctx_size - 1

    def room(*extent):
        return [pltpu.VMEM(extent + term.shape[1:], term.dtype) for term in terms]

    moved = sum(term.size * term.dtype.itemsize for term in terms)
    return pl.pallas_call(
        functools.partial(scatter_kernel, arity, ctx_size, pair_count, slot, spread_ctx),
        in_specs=[pl.BlockSpec(memory_space=pltpu.VMEM)] * arity,
        out_specs=[pl.BlockSpec(memory_space=pltpu.VMEM)] * arity,
        out_shape=[
            jax.ShapeDtypeStruct(lead + term.shape[1:], out_dtype or term.dtype) for term in terms
        ],
        scratch_shapes=room(ctx_size, pair_count)
        + room(pair_count)
        + room(asides, pair_count)
        + room(pair_count - 1)
        + room()
        + [dma((ctx_size, pair_count, arity))] * 2
        + [dma((pair_count, arity))] * 2
        + [dma((ctx_size - 1, pair_count, arity))] * 2
        + [dma((pair_count - 1, arity))] * 2
        + [dma((ctx_size - 1, arity))] * 2,
        compiler_params=pltpu.CompilerParams(
            collective_id=collective_id, has_side_effects=True, vmem_limit_bytes=60 * 2**20
        ),
        cost_estimate=pl.CostEstimate(flops=0, bytes_accessed=moved * 16, transcendentals=0),
        name=name,
    )(*terms)

def shards(
    layer_input,
    block_order,
    first_gain,
    w_qkv,
    b_qkv,
    w_o,
    second_gain,
    w_gate,
    w_up,
    w_down,
    cotangent,
):
    ctx_size = lax.axis_size("ctx")
    shard_count = lax.axis_size("fsdp")
    own_ctx = lax.axis_index("ctx")
    own_shard = lax.axis_index("fsdp")
    rows_here = layer_input.shape[0]
    slots = layer_input.shape[1]
    block_rows = rows_here * shard_count
    kv_width = KVH * HD
    cut = D // (ctx_size * shard_count)
    columns = FF // shard_count
    first_row = (own_ctx * shard_count + own_shard) * rows_here
    own_pos = block_positions(block_order, first_row, rows_here, block_rows, ctx_size)
    cosine_table, sine_table = rope_tables(own_pos.reshape(-1))
    query_scale = HD ** (-0.5)

    def by_rows(ctx, shard):
        return shard * ctx_size + ctx

    def by_tokens(ctx, shard):
        return ctx * shard_count + shard

    def own_cut(weight):
        return lax.dynamic_slice_in_dim(weight, own_ctx * cut, cut, 0)

    def mix_features(values):
        shaped = values.reshape(-1, shard_count, ctx_size, cut)
        return shaped.transpose(0, 2, 1, 3).reshape(-1, D)

    def unmix_features(values):
        shaped = values.reshape(-1, ctx_size, shard_count, cut)
        return shaped.transpose(0, 2, 1, 3).reshape(-1, D)

    small = jnp.concatenate([b_qkv, first_gain, second_gain]).reshape(ctx_size, -1)
    small_width = small.shape[1]
    small = lax.dynamic_slice_in_dim(small, own_ctx, 1, 0)
    small = jnp.pad(small, ((0, 0), (0, 16 * HD - small_width))).reshape(16, HD)
    w_qkv_all, w_o_all, small_all = gather(
        [own_cut(w_qkv), own_cut(w_o), small], by_rows, 1, "gather_weights"
    )
    w_qkv_all = w_qkv_all.reshape(D, QKV)
    w_o_all = w_o_all.reshape(D, D)
    small_all = small_all.reshape(shard_count, ctx_size, -1)[:, :, :small_width]
    small_all = small_all.reshape(shard_count, -1).astype(jnp.float32)
    bias_width = QKV // shard_count
    gain_width = D // shard_count
    bias_all = small_all[:, :bias_width].reshape(-1)
    gain_one = small_all[:, bias_width : bias_width + gain_width].reshape(-1)
    gain_two = small_all[:, bias_width + gain_width :].reshape(-1)

    gate_up_cut = jnp.concatenate(
        [
            own_cut(w_gate).reshape(cut, shard_count, columns),
            own_cut(w_up).reshape(cut, shard_count, columns),
        ],
        2,
    ).transpose(1, 0, 2)
    gate_up_cut = lax.all_to_all(gate_up_cut, "fsdp", 0, 0, tiled=True)
    gate_up_cols = lax.all_gather(
        gate_up_cut.reshape(shard_count * cut, 2 * columns), "ctx", axis=0, tiled=True
    )
    cotangent_all = lax.all_gather(cotangent.reshape(-1, D), "fsdp", axis=0, tiled=True)

    inputs = layer_input.reshape(-1, D).astype(jnp.float32)
    unit_one, scale_one, normed = normalize(inputs, gain_one)
    normed_one = normed.astype(jnp.bfloat16)
    projected = jnp.dot(normed_one, w_qkv_all, preferred_element_type=jnp.float32) + bias_all
    query_raw = projected[:, : H * HD].reshape(-1, H, HD)
    key_raw = projected[:, H * HD : H * HD + kv_width].reshape(-1, KVH, HD)
    value_raw = projected[:, H * HD + kv_width :]
    query_tokens = (
        (rotate(query_raw, cosine_table, sine_table) * query_scale)
        .astype(jnp.bfloat16)
        .reshape(-1, H * HD)
    )
    key_tokens = (
        rotate(key_raw, cosine_table, sine_table).astype(jnp.bfloat16).reshape(-1, kv_width)
    )
    own_kv = jnp.stack([key_tokens, value_raw.astype(jnp.bfloat16)], 1)
    own_kv = own_kv.reshape(rows_here, 2, SEQS, 2, KVH, HD).transpose(0, 2, 4, 1, 3, 5)
    own_kv = own_kv.reshape(rows_here, SEQS * KVH * 4 * HD)
    (all_kv,) = gather([own_kv], by_tokens, 2, "gather_keys")
    all_kv = all_kv.reshape(-1, SEQS * KVH * 4 * HD)
    queries = to_groups(query_tokens, rows_here)
    scalars = jnp.concatenate(
        [block_order.reshape(-1), jnp.stack([own_ctx, own_shard]).astype(jnp.int32)]
    )
    attended_grouped, stats = attend_forward(
        scalars, queries, all_kv, ctx_size, block_rows, rows_here
    )
    attended_low = from_groups(attended_grouped, rows_here).astype(jnp.bfloat16)
    middle = inputs + jnp.dot(attended_low, w_o_all, preferred_element_type=jnp.float32)
    unit_two, scale_two, normed = normalize(middle, gain_two)
    normed_two = mix_features(normed.astype(jnp.bfloat16))

    tokens_all = lax.all_gather(normed_two, "fsdp", axis=0, tiled=True)
    gate_up_part = jnp.dot(tokens_all, gate_up_cols, preferred_element_type=jnp.float32)
    gate_part, up_part = gate_up_part[:, :columns], gate_up_part[:, columns:]
    sigmoid_gate = jax.nn.sigmoid(gate_part)
    activated = gate_part * sigmoid_gate
    hidden = (activated * up_part).astype(jnp.bfloat16)
    grad_hidden = lax.dot_general(
        cotangent_all, w_down, CONTRACT_LAST, preferred_element_type=jnp.float32
    )
    grad_gate = grad_hidden * up_part * sigmoid_gate * (1.0 + gate_part * (1.0 - sigmoid_gate))
    grad_gate_up = jnp.concatenate([grad_gate, grad_hidden * activated], -1).astype(jnp.bfloat16)
    grad_tokens = lax.dot_general(
        grad_gate_up, gate_up_cols, CONTRACT_LAST, preferred_element_type=jnp.float32
    )
    grad_normed_two = lax.psum_scatter(
        grad_tokens.astype(jnp.bfloat16), "fsdp", scatter_dimension=0, tiled=True
    )
    down_terms = lax.dot_general(
        hidden, cotangent_all, CONTRACT_FIRST, preferred_element_type=jnp.float32
    ).astype(jnp.bfloat16)
    gate_up_terms = lax.dot_general(
        tokens_all, grad_gate_up, CONTRACT_FIRST, preferred_element_type=jnp.float32
    ).astype(jnp.bfloat16)
    mixed_terms = jnp.dot(hidden, w_down, preferred_element_type=jnp.float32).astype(jnp.bfloat16)
    down_rows = lax.psum(down_terms, "ctx")
    gate_up_rows = lax.psum_scatter(gate_up_terms, "ctx", scatter_dimension=0, tiled=True)
    gate_up_rows = lax.all_to_all(
        gate_up_rows.reshape(shard_count, cut, 2 * columns), "fsdp", 0, 0, tiled=True
    )
    gate_up_rows = lax.all_gather(gate_up_rows, "ctx", axis=0, tiled=False)
    mixed_out = middle + lax.psum_scatter(
        mixed_terms, "fsdp", scatter_dimension=0, tiled=True
    ).astype(jnp.float32)
    output = mixed_out.astype(jnp.bfloat16).reshape(rows_here, slots, D)

    grad_normed_two, down_terms, gate_up_terms, mixed_terms = lax.optimization_barrier(
        (grad_normed_two, down_terms, gate_up_terms, mixed_terms)
    )
    grad_normed_two = unmix_features(grad_normed_two.astype(jnp.float32))
    grad_middle_norm, grad_gain_two = norm_back(grad_normed_two, unit_two, scale_two, gain_two)
    grad_middle = cotangent.reshape(-1, D).astype(jnp.float32) + grad_middle_norm
    grad_branch_one = grad_middle.astype(jnp.bfloat16)
    grad_attended = lax.dot_general(
        grad_branch_one, w_o_all, CONTRACT_LAST, preferred_element_type=jnp.float32
    ).astype(jnp.bfloat16)
    o_terms = lax.dot_general(
        attended_low, grad_branch_one, CONTRACT_FIRST, preferred_element_type=jnp.float32
    ).astype(jnp.bfloat16)
    grad_queries, grad_kv_full = attend_backward(
        scalars,
        queries,
        to_groups(grad_attended, rows_here),
        attended_grouped,
        stats,
        all_kv,
        ctx_size,
        block_rows,
        rows_here,
    )
    (grad_kv,) = scatter(
        [grad_kv_full.reshape(-1, rows_here, SEQS * KVH * 4 * HD)],
        by_tokens,
        3,
        "scatter_keys",
        out_dtype=jnp.float32,
    )
    grad_kv_low = narrowed(grad_kv).reshape(rows_here, SEQS, KVH, 2, 2, HD)
    grad_kv_low = grad_kv_low.transpose(0, 3, 1, 4, 2, 5).reshape(-1, 2 * kv_width)
    grad_query_tokens = from_groups(narrowed(grad_queries), rows_here) * query_scale
    grad_query_raw = rotate_back(
        grad_query_tokens.reshape(-1, H, HD), cosine_table, sine_table
    ).reshape(-1, H * HD)
    grad_key_raw = rotate_back(
        grad_kv_low[:, :kv_width].reshape(-1, KVH, HD), cosine_table, sine_table
    ).reshape(-1, kv_width)
    grad_projected = jnp.concatenate(
        [grad_query_raw, grad_key_raw, grad_kv_low[:, kv_width:]], -1
    ).astype(jnp.bfloat16)
    grad_bias = jnp.sum(grad_projected, 0, dtype=jnp.float32)
    grad_normed_one = lax.dot_general(
        grad_projected, w_qkv_all, CONTRACT_LAST, preferred_element_type=jnp.float32
    )
    grad_input_norm, grad_gain_one = norm_back(grad_normed_one, unit_one, scale_one, gain_one)
    grad_input = (grad_middle + grad_input_norm).reshape(rows_here, slots, D)
    qkv_terms = lax.dot_general(
        normed_one, grad_projected, CONTRACT_FIRST, preferred_element_type=jnp.float32
    ).astype(jnp.bfloat16)
    small_terms = jnp.concatenate(
        [
            part.reshape(shard_count, -1)
            for part in (grad_gain_one, grad_gain_two, grad_bias[:QK], grad_bias[QK:])
        ],
        1,
    )
    small_terms = small_terms.reshape(ctx_size * shard_count, small_width)
    small_terms = jnp.pad(small_terms, ((0, 0), (0, 8 * HD - small_width)))
    qkv_rows, o_rows, small_rows = scatter(
        [
            qkv_terms.reshape(-1, cut, QKV),
            o_terms.reshape(-1, cut, D),
            small_terms.reshape(-1, 8, HD),
        ],
        by_rows,
        4,
        "scatter_weights",
        spread_ctx=True,
    )
    small_rows = small_rows.reshape(ctx_size, -1)[:, :small_width].reshape(-1)
    bias_start = 2 * gain_width
    value_start = bias_start + QK // shard_count

    def own_rows(part):
        shaped = part.transpose(0, 2, 1, 3)
        return shaped.reshape(ctx_size * cut, FF).astype(jnp.float32)

    return (
        output,
        grad_input,
        small_rows[:gain_width],
        qkv_rows.reshape(-1, QKV).astype(jnp.float32),
        small_rows[bias_start:value_start],
        small_rows[value_start:],
        o_rows.reshape(-1, D).astype(jnp.float32),
        small_rows[gain_width:bias_start],
        own_rows(gate_up_rows[:, :, :, :columns]),
        own_rows(gate_up_rows[:, :, :, columns:]),
        down_rows.astype(jnp.float32),
    )


def solution(mesh):
    in_specs = (
        P(("ctx", "fsdp"), None, None),
        P(),
        P("fsdp"),
        P("fsdp", None),
        P("fsdp"),
        P("fsdp", None),
        P("fsdp"),
        P("fsdp", None),
        P("fsdp", None),
        P("fsdp", None),
        P(("ctx", "fsdp"), None, None),
    )
    out_specs = (
        P(("ctx", "fsdp"), None, None),
        P(("ctx", "fsdp"), None, None),
        P("fsdp"),
        P("fsdp", None),
        P("fsdp"),
        P("fsdp"),
        P("fsdp", None),
        P("fsdp"),
        P("fsdp", None),
        P("fsdp", None),
        P("fsdp", None),
    )
    return jax.shard_map(shards, mesh=mesh, in_specs=in_specs, out_specs=out_specs, check_vma=False)
```

```python
import functools

import jax
import jax.numpy as jnp
from jax import lax
from jax.experimental import pallas as pl
from jax.experimental.pallas import tpu as pltpu
from jax.sharding import PartitionSpec as P

D = 1536
H = 12
KVH = 2
HD = 128
FF = 8960
SEQS = 2
QKV = 2048
QK = 1792


EPS = 1e-06
THETA = 1000000.0
NEG_FILL = -1e30
MESH_ID = pl.DeviceIdType.MESH
CONTRACT_LAST = (((1,), (1,)), ((), ()))
CONTRACT_FIRST = (((0,), (0,)), ((), ()))


def narrowed(values):
    return lax.optimization_barrier(values.astype(jnp.bfloat16)).astype(jnp.float32)


def block_positions(block_order, first_row, row_count, block_rows, ctx_size):
    row_index = first_row + jnp.arange(row_count, dtype=jnp.int32)
    slot_index = jnp.arange(2 * SEQS, dtype=jnp.int32)
    entries = (slot_index // SEQS)[None, :] * ctx_size + (row_index // block_rows)[:, None]
    tiled = jnp.tile(block_order, (2, 1))
    entry_ids = jnp.arange(2 * ctx_size, dtype=jnp.int32)
    picked = jnp.sum(
        jnp.where(entries[:, :, None] == entry_ids[None, None, :], tiled[None, :, :], 0), -1
    )
    return picked * block_rows + (row_index % block_rows)[:, None]


def to_groups(tokens, row_count):
    shaped = tokens.reshape(row_count, 2, SEQS, KVH, H // KVH, HD)
    return shaped.transpose(2, 1, 3, 4, 0, 5).reshape(SEQS, 2, KVH, H // KVH * row_count, HD)


def from_groups(grouped, row_count):
    shaped = grouped.reshape(SEQS, 2, KVH, H // KVH, row_count, HD).transpose(4, 1, 0, 2, 3, 5)
    return shaped.reshape(row_count * 2 * SEQS, H * HD)


def rope_tables(positions):
    half_width = HD // 2
    frequency = THETA ** (-jnp.arange(half_width, dtype=jnp.float32) * 2.0 / HD)
    angles = positions.astype(jnp.float32)[:, None] * frequency[None, :]
    cosine_table = jnp.concatenate([jnp.cos(angles), jnp.cos(angles)], -1)[:, None, :]
    sine_table = jnp.concatenate([jnp.sin(angles), jnp.sin(angles)], -1)[:, None, :]
    return (cosine_table, sine_table)


def rotate(head_values, cosine_table, sine_table):
    half_width = HD // 2
    turned = jnp.concatenate([-head_values[..., half_width:], head_values[..., :half_width]], -1)
    return head_values * cosine_table + turned * sine_table


def rotate_back(grad_values, cosine_table, sine_table):
    half_width = HD // 2
    moved = grad_values * sine_table
    return grad_values * cosine_table + jnp.concatenate(
        [moved[..., half_width:], -moved[..., :half_width]], -1
    )


def normalize(values, gain):
    scale = lax.rsqrt(jnp.mean(values * values, -1, keepdims=True) + EPS)
    unit = values * scale
    return (unit, scale, unit * gain)


def norm_back(grad_out, unit, scale, gain):
    grad_unit = grad_out * gain
    inner = jnp.mean(grad_unit * unit, -1, keepdims=True)
    return (scale * (grad_unit - unit * inner), jnp.sum(grad_out * unit, 0))


def attend_forward_kernel(ctx_size, block_rows, rows_here, scalars, q_ref, kv_ref, out_ref, stat_ref, best_ref, total_ref, accum_ref):
    seq = pl.program_id(0)
    blocks = 2 * ctx_size
    own_ctx = scalars[SEQS * blocks]
    own_shard = scalars[SEQS * blocks + 1]
    lanes = q_ref.shape[3]
    best_ref[...] = jnp.full(best_ref.shape, NEG_FILL, jnp.float32)
    total_ref[...] = jnp.zeros(total_ref.shape, jnp.float32)
    accum_ref[...] = jnp.zeros(accum_ref.shape, jnp.float32)

    def step(key_ctx, half_key, half):
        order_key = scalars[seq * blocks + half_key * ctx_size + key_ctx]
        order_query = scalars[seq * blocks + half * ctx_size + own_ctx]

        def work(masked):
            rows = pl.ds(pl.multiple_of(key_ctx * block_rows, block_rows), block_rows)
            keys = kv_ref[rows, half_key * 2 * HD : half_key * 2 * HD + HD]
            values = kv_ref[rows, half_key * 2 * HD + HD : half_key * 2 * HD + 2 * HD]
            scores = lax.dot_general(
                keys, q_ref[0, half, 0], CONTRACT_LAST, preferred_element_type=jnp.float32
            )
            if masked:
                row = lax.broadcasted_iota(jnp.int32, (block_rows, lanes), 0)
                lane = lax.broadcasted_iota(jnp.int32, (block_rows, lanes), 1)
                scores = jnp.where(
                    row <= own_shard * rows_here + lax.rem(lane, rows_here), scores, NEG_FILL
                )
            best = best_ref[half]
            fresh = jnp.maximum(best, jnp.max(scores, 0, keepdims=True))
            decay = jnp.exp(best - fresh)
            weights = jnp.exp(scores - fresh)
            total_ref[half] = total_ref[half] * decay + jnp.sum(weights, 0, keepdims=True)
            accum_ref[half] = accum_ref[half] * decay + lax.dot_general(
                values,
                weights.astype(jnp.bfloat16),
                CONTRACT_FIRST,
                preferred_element_type=jnp.float32,
            )
            best_ref[half] = fresh

        @pl.when(order_key < order_query)
        def full():
            work(False)

        @pl.when(order_key == order_query)
        def diagonal():
            work(True)

    @pl.loop(0, ctx_size)
    def sweep(key_ctx):
        for half_key in range(2):
            for half in range(2):
                step(key_ctx, half_key, half)

    for half in range(2):
        totals = total_ref[half]
        out_ref[0, half, 0] = (accum_ref[half] / totals).T
        stat_ref[0, half, 0] = best_ref[half] + jnp.log(totals)


def attend_forward(scalars, queries, all_kv, ctx_size, block_rows, rows_here):
    lanes = queries.shape[3]
    kernel = functools.partial(attend_forward_kernel, ctx_size, block_rows, rows_here)
    group = pl.BlockSpec((1, 2, 1, lanes, HD), lambda s, n, _: (s, 0, n, 0, 0))
    stat = pl.BlockSpec((1, 2, 1, 1, lanes), lambda s, n, _: (s, 0, n, 0, 0))
    return pl.pallas_call(
        kernel,
        grid_spec=pltpu.PrefetchScalarGridSpec(
            num_scalar_prefetch=1,
            grid=(SEQS, KVH),
            in_specs=[
                group,
                pl.BlockSpec((all_kv.shape[0], 4 * HD), lambda s, n, _: (0, s * KVH + n)),
            ],
            out_specs=[group, stat],
            scratch_shapes=[
                pltpu.VMEM((2, 1, lanes), jnp.float32),
                pltpu.VMEM((2, 1, lanes), jnp.float32),
                pltpu.VMEM((2, HD, lanes), jnp.float32),
            ],
        ),
        out_shape=(
            jax.ShapeDtypeStruct(queries.shape, jnp.float32),
            jax.ShapeDtypeStruct((SEQS, 2, KVH, 1, lanes), jnp.float32),
        ),
        compiler_params=pltpu.CompilerParams(vmem_limit_bytes=56 * 2**20),
        name="attend_forward",
    )(scalars, queries, all_kv)


def attend_backward_kernel(ctx_size, block_rows, rows_here, scalars, q_ref, go_ref, att_ref, stat_ref, kv_ref, gq_ref, gkv_ref, delta_ref, gq_acc, gk_acc, gv_acc):
    seq = pl.program_id(0)
    blocks = 2 * ctx_size
    own_ctx = scalars[SEQS * blocks]
    own_shard = scalars[SEQS * blocks + 1]
    lanes = q_ref.shape[3]
    gq_acc[...] = jnp.zeros(gq_acc.shape, jnp.float32)
    for half in range(2):
        product = go_ref[0, half, 0].astype(jnp.float32) * att_ref[0, half, 0]
        delta_ref[half] = jnp.sum(product.T, 0, keepdims=True)

    def step(key_ctx, half_key, half):
        order_key = scalars[seq * blocks + half_key * ctx_size + key_ctx]
        order_query = scalars[seq * blocks + half * ctx_size + own_ctx]

        def work(masked):
            rows = pl.ds(pl.multiple_of(key_ctx * block_rows, block_rows), block_rows)
            keys = kv_ref[rows, half_key * 2 * HD : half_key * 2 * HD + HD]
            values = kv_ref[rows, half_key * 2 * HD + HD : half_key * 2 * HD + 2 * HD]
            queries = q_ref[0, half, 0]
            grad_out = go_ref[0, half, 0]
            scores = lax.dot_general(
                keys, queries, CONTRACT_LAST, preferred_element_type=jnp.float32
            )
            probs = jnp.exp(scores - stat_ref[0, half, 0])
            if masked:
                row = lax.broadcasted_iota(jnp.int32, (block_rows, lanes), 0)
                lane = lax.broadcasted_iota(jnp.int32, (block_rows, lanes), 1)
                probs = jnp.where(
                    row <= own_shard * rows_here + lax.rem(lane, rows_here), probs, 0.0
                )
            grad_probs = lax.dot_general(
                values, grad_out, CONTRACT_LAST, preferred_element_type=jnp.float32
            )
            grad_scores = (probs * (grad_probs - delta_ref[half])).astype(jnp.bfloat16)
            gv_acc[...] += jnp.dot(
                probs.astype(jnp.bfloat16), grad_out, preferred_element_type=jnp.float32
            )
            gk_acc[...] += jnp.dot(grad_scores, queries, preferred_element_type=jnp.float32)
            gq_acc[half] += lax.dot_general(
                keys, grad_scores, CONTRACT_FIRST, preferred_element_type=jnp.float32
            )

        @pl.when(order_key < order_query)
        def full():
            work(False)

        @pl.when(order_key == order_query)
        def diagonal():
            work(True)

    @pl.loop(0, ctx_size)
    def sweep(key_ctx):
        rows = pl.ds(pl.multiple_of(key_ctx * block_rows, block_rows), block_rows)
        for half_key in range(2):
            gk_acc[...] = jnp.zeros(gk_acc.shape, jnp.float32)
            gv_acc[...] = jnp.zeros(gv_acc.shape, jnp.float32)
            for half in range(2):
                step(key_ctx, half_key, half)
            at = half_key * 2 * HD
            gkv_ref[rows, at : at + HD] = gk_acc[...].astype(jnp.bfloat16)
            gkv_ref[rows, at + HD : at + 2 * HD] = gv_acc[...].astype(jnp.bfloat16)

    for half in range(2):
        gq_ref[0, half, 0] = gq_acc[half].T


def attend_backward(scalars, queries, grad_out, attended, stats, all_kv, ctx_size, block_rows, rows_here):
    lanes = queries.shape[3]
    kernel = functools.partial(attend_backward_kernel, ctx_size, block_rows, rows_here)
    group = pl.BlockSpec((1, 2, 1, lanes, HD), lambda s, n, _: (s, 0, n, 0, 0))
    stat = pl.BlockSpec((1, 2, 1, 1, lanes), lambda s, n, _: (s, 0, n, 0, 0))
    full = pl.BlockSpec((all_kv.shape[0], 4 * HD), lambda s, n, _: (0, s * KVH + n))
    return pl.pallas_call(
        kernel,
        grid_spec=pltpu.PrefetchScalarGridSpec(
            num_scalar_prefetch=1,
            grid=(SEQS, KVH),
            in_specs=[group, group, group, stat, full],
            out_specs=[group, full],
            scratch_shapes=[
                pltpu.VMEM((2, 1, lanes), jnp.float32),
                pltpu.VMEM((2, HD, lanes), jnp.float32),
                pltpu.VMEM((block_rows, HD), jnp.float32),
                pltpu.VMEM((block_rows, HD), jnp.float32),
            ],
        ),
        out_shape=(
            jax.ShapeDtypeStruct(queries.shape, jnp.float32),
            jax.ShapeDtypeStruct(all_kv.shape, jnp.bfloat16),
        ),
        compiler_params=pltpu.CompilerParams(vmem_limit_bytes=56 * 2**20),
        name="attend_backward",
    )(scalars, queries, grad_out, attended, stats, all_kv)


def peers_of(ctx_size):
    return ctx_size == 4, range(1, ctx_size)


def ctx_target(position, way, square, ctx_size):
    return position ^ way if square else lax.rem(position + way, ctx_size)


def ctx_source(position, way, square, ctx_size):
    return position ^ way if square else lax.rem(position + ctx_size - way, ctx_size)


def greet(ctx_size, pair_count, with_ctx, all_shards):
    ctx = lax.axis_index("ctx")
    shard = lax.axis_index("fsdp")
    pair, core = shard // 2, shard % 2
    barrier = pltpu.get_barrier_semaphore()
    shard_count = 2 * pair_count
    partners = [(ctx, pair * 2 + 1 - core)]
    for step in range(1, pair_count):
        there = lax.rem(pair + step, pair_count) * 2
        partners.append((ctx, there + core))
        if all_shards:
            partners.append((ctx, there + 1 - core))
    if with_ctx:
        for way in range(1, ctx_size):
            partners.append((lax.rem(ctx + way, ctx_size), shard))
    for partner in partners:
        pl.semaphore_signal(barrier, inc=1, device_id=partner, device_id_type=MESH_ID)
    pl.semaphore_wait(barrier, len(partners))
    return ctx, pair, core


class Exchange:
    def __init__(self, source, out, sems, own_sem, pair_count):
        self.source, self.out, self.sems, self.own_sem = source, out, sems, own_sem
        self.shard_count = 2 * pair_count

    def start(self):
        ctx, shard = lax.axis_index("ctx"), lax.axis_index("fsdp")
        self.own = pltpu.make_async_copy(self.source.at[shard], self.out.at[shard], self.own_sem)
        self.own.start()
        self.copies = []
        for step in range(1, self.shard_count):
            there = lax.rem(shard + step, self.shard_count)
            copy = pltpu.make_async_remote_copy(
                src_ref=self.source.at[there],
                dst_ref=self.out.at[shard],
                send_sem=self.sems[0].at[step - 1],
                recv_sem=self.sems[1].at[step - 1],
                device_id=(ctx, there),
                device_id_type=MESH_ID,
            )
            copy.start()
            self.copies.append(copy)

    def finish(self):
        ctx, shard = lax.axis_index("ctx"), lax.axis_index("fsdp")
        for step in range(1, self.shard_count):
            come = lax.rem(shard + self.shard_count - step, self.shard_count)
            pltpu.make_async_remote_copy(
                src_ref=self.out.at[come],
                dst_ref=self.out.at[come],
                send_sem=self.sems[0].at[step - 1],
                recv_sem=self.sems[1].at[step - 1],
                device_id=(ctx, shard),
                device_id_type=MESH_ID,
            ).wait_recv()
        self.own.wait()
        for copy in self.copies:
            copy.wait_send()


def exchange_kernel(pair_count, source, out, send_sem, recv_sem, own_sem):
    greet(1, pair_count, False, True)
    flow = Exchange(source, out, (send_sem, recv_sem), own_sem, pair_count)
    flow.start()
    flow.finish()


def exchange(pieces, collective_id, name):
    shard_count = lax.axis_size("fsdp")
    dma = pltpu.SemaphoreType.DMA
    return pl.pallas_call(
        functools.partial(exchange_kernel, shard_count // 2),
        in_specs=[pl.BlockSpec(memory_space=pltpu.VMEM)],
        out_specs=pl.BlockSpec(memory_space=pl.ANY),
        out_shape=jax.ShapeDtypeStruct(pieces.shape, pieces.dtype),
        scratch_shapes=[dma((shard_count - 1,))] * 2 + [dma],
        compiler_params=pltpu.CompilerParams(collective_id=collective_id, has_side_effects=True),
        cost_estimate=pl.CostEstimate(
            flops=0, bytes_accessed=pieces.size * 64, transcendentals=0
        ),
        name=name,
    )(pieces)


def gather_kernel(arity, ctx_size, pair_count, slots, swaps, *refs):
    sources, refs = refs[:arity], refs[arity:]
    swap_sources, refs = refs[:swaps], refs[swaps:]
    outs, refs = refs[:arity], refs[arity:]
    swap_outs, refs = refs[:swaps], refs[swaps:]
    pair_sems, ctx_sems, core_sems = refs[0:2], refs[2:4], refs[4:6]
    local_sem = refs[6]
    square, ways = peers_of(ctx_size)
    near = [way for way in ways if not (square and way == 3)]
    ctx, pair, core = greet(ctx_size, pair_count, True, swaps > 0)
    homes = [place(ctx, pair * 2 + core) for place in slots]
    started = []
    steps = [(0, 1)] + [(far, way) for far in range(1, pair_count) for way in (1, -1)]

    def present(step):
        far, way = steps[step]
        if far == 0:
            return None
        return pair >= far if way == 1 else pair + far < pair_count

    def origin(step):
        far, way = steps[step]
        return pair - far * way

    def when(condition, work):
        if condition is None:
            work()
        else:
            pl.when(condition)(work)

    def send(item, source, place, target, sems, at, condition):
        copy = pltpu.make_async_remote_copy(
            src_ref=source,
            dst_ref=outs[item].at[place],
            send_sem=sems[0].at[at],
            recv_sem=sems[1].at[at],
            device_id=target,
            device_id_type=MESH_ID,
        )
        copy.start()
        started.append((condition, item, sems, at))

    def sent(item, sems, at):
        pltpu.make_async_remote_copy(
            src_ref=outs[item].at[0],
            dst_ref=outs[item].at[0],
            send_sem=sems[0].at[at],
            recv_sem=sems[1].at[at],
            device_id=(ctx, pair * 2 + core),
            device_id_type=MESH_ID,
        ).wait_send()

    def arrive(item, place, sems, at):
        pltpu.make_async_remote_copy(
            src_ref=outs[item].at[place],
            dst_ref=outs[item].at[place],
            send_sem=sems[0].at[at],
            recv_sem=sems[1].at[at],
            device_id=(ctx, pair * 2 + core),
            device_id_type=MESH_ID,
        ).wait_recv()

    def pass_on(step, item, source, place):
        far, way = steps[step]
        for side in (1, -1) if far == 0 else (way,):

            def further(side=side):
                return pair + 1 < pair_count if side == 1 else pair >= 1

            def both(further=further):
                return further() if far == 0 else jnp.logical_and(further(), present(step))

            def work(side=side, both=both):
                send(
                    item,
                    source,
                    place,
                    (ctx, (pair + side) * 2 + core),
                    pair_sems,
                    ((side + 1) // 2, far, item),
                    both,
                )

            if far + 1 < pair_count:
                pl.when(further())(work)

    def to_core(item, source, from_ctx, way, step):
        send(
            item,
            source,
            slots[item](from_ctx, origin(step) * 2 + core),
            (ctx, pair * 2 + 1 - core),
            core_sems,
            (way, step, item),
            functools.partial(present, step),
        )

    def spread(step):
        for item in range(arity):
            place = slots[item](ctx, origin(step) * 2 + core)
            source = sources[item]
            if step:
                far, way = steps[step]
                arrive(item, place, pair_sems, ((way + 1) // 2, far - 1, item))
                source = outs[item].at[place]
            pass_on(step, item, source, place)
            for way in near:
                there = ctx_target(ctx, way, square, ctx_size)
                send(
                    item,
                    source,
                    place,
                    (there, pair * 2 + core),
                    ctx_sems,
                    (way - 1, step, item),
                    functools.partial(present, step),
                )
            to_core(item, source, ctx, 0, step)

    def collect(step):
        for way in near:
            for item in range(arity):
                come = ctx_source(ctx, way, square, ctx_size)
                place = slots[item](come, origin(step) * 2 + core)
                arrive(item, place, ctx_sems, (way - 1, step, item))
                source = outs[item].at[place]
                if square and (steps[step][0] % 2 == 0) == (way == 1):
                    send(
                        item,
                        source,
                        place,
                        (ctx ^ (3 - way), pair * 2 + core),
                        ctx_sems,
                        (2, step, item),
                        functools.partial(present, step),
                    )
                to_core(item, source, come, way, step)

    def collect_far(step):
        for item in range(arity):
            place = slots[item](ctx ^ 3, origin(step) * 2 + core)
            arrive(item, place, ctx_sems, (2, step, item))
            to_core(item, outs[item].at[place], ctx ^ 3, 3, step)

    locals_ = []
    for item in range(arity):
        copy = pltpu.make_async_copy(sources[item], outs[item].at[homes[item]], local_sem.at[item])
        copy.start()
        locals_.append(copy)
    when(None, lambda: spread(0))
    flows = []
    count = len(steps)
    for turn in range(1, count + 4):
        if turn < count:
            when(present(turn), functools.partial(spread, turn))
        if turn == count:
            for item in range(swaps):
                flow = Exchange(
                    swap_sources[item],
                    swap_outs[item],
                    refs[7 + 3 * item : 9 + 3 * item],
                    refs[9 + 3 * item],
                    pair_count,
                )
                flow.start()
                flows.append(flow)
        if 0 <= turn - 2 < count:
            when(present(turn - 2), functools.partial(collect, turn - 2))
        if square and 0 <= turn - 4 < count:
            when(present(turn - 4), functools.partial(collect_far, turn - 4))

    def from_core(step):
        for way in range(ctx_size):
            come = ctx_source(ctx, way, square, ctx_size) if way else ctx
            for item in range(arity):
                arrive(item, slots[item](come, origin(step) * 2 + 1 - core), core_sems, (way, step, item))

    for step in range(count):
        when(present(step), functools.partial(from_core, step))
    for flow in flows:
        flow.finish()
    for copy in locals_:
        copy.wait()
    for condition, *which in started:
        when(condition(), functools.partial(sent, *which))


def gather(pieces, slots, collective_id, name, swaps=()):
    ctx_size, shard_count = lax.axis_size("ctx"), lax.axis_size("fsdp")
    pair_count = shard_count // 2
    arity = len(pieces)
    dma = pltpu.SemaphoreType.DMA
    moved = sum(piece.size for piece in pieces) * 2
    steps = 2 * pair_count - 1
    return pl.pallas_call(
        functools.partial(gather_kernel, arity, ctx_size, pair_count, slots, len(swaps)),
        in_specs=[pl.BlockSpec(memory_space=pltpu.VMEM)] * (arity + len(swaps)),
        out_specs=[pl.BlockSpec(memory_space=pl.ANY)] * (arity + len(swaps)),
        out_shape=[
            jax.ShapeDtypeStruct((ctx_size * shard_count,) + piece.shape, piece.dtype) for piece in pieces
        ]
        + [jax.ShapeDtypeStruct(swap.shape, swap.dtype) for swap in swaps],
        scratch_shapes=[dma((2, pair_count - 1, arity))] * 2
        + [dma((ctx_size - 1, steps, arity))] * 2
        + [dma((ctx_size, steps, arity))] * 2
        + [dma((arity,))]
        + [dma((shard_count - 1,)), dma((shard_count - 1,)), dma] * len(swaps),
        compiler_params=pltpu.CompilerParams(collective_id=collective_id, has_side_effects=True),
        cost_estimate=pl.CostEstimate(
            flops=0, bytes_accessed=moved * ctx_size * shard_count * 4, transcendentals=0
        ),
        name=name,
    )(*pieces, *swaps)


def scatter_kernel(arity, ctx_size, pair_count, slot, spread_ctx, *refs):
    sources, outs, refs = refs[:arity], refs[arity : 2 * arity], refs[2 * arity :]
    halves, relays, asides, ends, finals = (refs[i * arity : (i + 1) * arity] for i in range(5))
    sems = refs[5 * arity :]
    core_sems, relay_sems, ctx_sems, pair_sems, last_sems = (sems[2 * i : 2 * i + 2] for i in range(5))
    square, ways = peers_of(ctx_size)
    ctx, pair, core = greet(ctx_size, pair_count, True, False)
    order = list(range(1, pair_count)) + [0]
    started = []

    def send(source, target, device, pair_of_sems, at):
        copy = pltpu.make_async_remote_copy(
            src_ref=source,
            dst_ref=target,
            send_sem=pair_of_sems[0].at[at],
            recv_sem=pair_of_sems[1].at[at],
            device_id=device,
            device_id_type=MESH_ID,
        )
        copy.start()
        started.append(copy)

    def arrive(target, pair_of_sems, at):
        pltpu.make_async_remote_copy(
            src_ref=target,
            dst_ref=target,
            send_sem=pair_of_sems[0].at[at],
            recv_sem=pair_of_sems[1].at[at],
            device_id=(ctx, pair * 2 + core),
            device_id_type=MESH_ID,
        ).wait_recv()

    def toward(step):
        return lax.rem(pair + step, pair_count)

    def target_ctx(way):
        return ctx_target(ctx, way, square, ctx_size) if way else ctx

    def f32(value):
        return value.astype(jnp.float32)

    far_first = [3, 1, 2, 0] if square else list(ways) + [0]
    for step in order:
        for way in far_first:
            for item in range(arity):
                send(
                    sources[item].at[slot(target_ctx(way), toward(step) * 2 + 1 - core)],
                    halves[item].at[way, step],
                    (ctx, pair * 2 + 1 - core),
                    core_sems,
                    (way, step, item),
                )

    def fold_core(step):
        for way in far_first:
            for item in range(arity):
                half = halves[item].at[way, step]
                arrive(half, core_sems, (way, step, item))
                mine = sources[item][slot(target_ctx(way), toward(step) * 2 + core)]
                half[...] = (f32(mine) + f32(half[...])).astype(half.dtype)
                if square and way == 3:
                    there = ctx ^ (1 if step % 2 == 0 else 2)
                    send(
                        half,
                        relays[item].at[step],
                        (there, pair * 2 + core),
                        relay_sems,
                        (step, item),
                    )

    def fold_relay(step):
        for item in range(arity):
            if square:
                relay = relays[item].at[step]
                arrive(relay, relay_sems, (step, item))
                half = halves[item].at[2 if step % 2 == 0 else 1, step]
                half[...] = (f32(half[...]) + f32(relay[...])).astype(half.dtype)
            for way in ways:
                if square and way == 3:
                    continue
                send(
                    halves[item].at[way, step],
                    asides[item].at[way - 1, step],
                    (target_ctx(way), pair * 2 + core),
                    ctx_sems,
                    (way - 1, step, item),
                )

    def fold_ctx(step):
        for item in range(arity):
            half = halves[item].at[0, step]
            total = f32(half[...])
            for way in ways:
                if square and way == 3:
                    continue
                aside = asides[item].at[way - 1, step]
                arrive(aside, ctx_sems, (way - 1, step, item))
                total = total + f32(aside[...])
            if step:
                half[...] = total.astype(half.dtype)
                send(
                    half,
                    ends[item].at[step - 1],
                    (ctx, toward(step) * 2 + core),
                    pair_sems,
                    (step - 1, item),
                )
            else:
                for other in range(1, pair_count):
                    end = ends[item].at[other - 1]
                    arrive(end, pair_sems, (other - 1, item))
                    total = total + f32(end[...])
                if spread_ctx:
                    finals[item][...] = total.astype(finals[item].dtype)
                else:
                    outs[item][...] = total.astype(outs[item].dtype)

    for turn in range(pair_count + 2):
        if turn < pair_count:
            fold_core(order[turn])
        if 1 <= turn <= pair_count:
            fold_relay(order[turn - 1])
        if turn >= 2:
            fold_ctx(order[turn - 2])
    if spread_ctx:
        for item in range(arity):
            for way in ways:
                send(
                    finals[item],
                    outs[item].at[ctx],
                    (target_ctx(way), pair * 2 + core),
                    last_sems,
                    (way - 1, item),
                )
            outs[item][ctx] = finals[item][...]
        for item in range(arity):
            for way in ways:
                arrive(outs[item].at[ctx_source(ctx, way, square, ctx_size)], last_sems, (way - 1, item))
    for copy in started:
        copy.wait_send()


def scatter(terms, slot, collective_id, name, spread_ctx=False, out_dtype=None):
    ctx_size, shard_count = lax.axis_size("ctx"), lax.axis_size("fsdp")
    pair_count = shard_count // 2
    arity = len(terms)
    dma = pltpu.SemaphoreType.DMA
    lead = (ctx_size,) if spread_ctx else ()
    asides = 2 if ctx_size == 4 else ctx_size - 1

    def room(*extent):
        return [pltpu.VMEM(extent + term.shape[1:], term.dtype) for term in terms]

    moved = sum(term.size * term.dtype.itemsize for term in terms)
    return pl.pallas_call(
        functools.partial(scatter_kernel, arity, ctx_size, pair_count, slot, spread_ctx),
        in_specs=[pl.BlockSpec(memory_space=pltpu.VMEM)] * arity,
        out_specs=[pl.BlockSpec(memory_space=pltpu.VMEM)] * arity,
        out_shape=[
            jax.ShapeDtypeStruct(lead + term.shape[1:], out_dtype or term.dtype) for term in terms
        ],
        scratch_shapes=room(ctx_size, pair_count)
        + room(pair_count)
        + room(asides, pair_count)
        + room(pair_count - 1)
        + room()
        + [dma((ctx_size, pair_count, arity))] * 2
        + [dma((pair_count, arity))] * 2
        + [dma((ctx_size - 1, pair_count, arity))] * 2
        + [dma((pair_count - 1, arity))] * 2
        + [dma((ctx_size - 1, arity))] * 2,
        compiler_params=pltpu.CompilerParams(
            collective_id=collective_id, has_side_effects=True, vmem_limit_bytes=60 * 2**20
        ),
        cost_estimate=pl.CostEstimate(flops=0, bytes_accessed=moved * 16, transcendentals=0),
        name=name,
    )(*terms)

def pack_kernel(columns, gate_ref, up_ref, out_ref):
    width = out_ref.shape[2] // 2
    cut = out_ref.shape[1]
    for there in range(out_ref.shape[0]):
        for side, ref in enumerate((gate_ref, up_ref)):
            at = side * width
            out_ref[there, :, at + width - HD : at + width] = jnp.zeros((cut, HD), out_ref.dtype)
            out_ref[there, :, at : at + columns] = ref[:, there * columns : (there + 1) * columns]


def pack(gate, up, shard_count, columns, width):
    return pl.pallas_call(
        functools.partial(pack_kernel, columns),
        in_specs=[pl.BlockSpec(memory_space=pltpu.VMEM)] * 2,
        out_specs=pl.BlockSpec(memory_space=pltpu.VMEM),
        out_shape=jax.ShapeDtypeStruct((shard_count, gate.shape[0], 2 * width), gate.dtype),
        name="pack",
    )(gate, up)


def unpack_kernel(columns, in_ref, gate_ref, up_ref):
    width = in_ref.shape[3] // 2
    for there in range(in_ref.shape[1]):
        for side, ref in enumerate((gate_ref, up_ref)):
            part = in_ref[0, there, :, side * width : side * width + columns]
            ref[0, :, there * columns : (there + 1) * columns] = part.astype(jnp.float32)


def unpack(rows, columns):
    ctx_size, shard_count, cut, _ = rows.shape
    out = jax.ShapeDtypeStruct((ctx_size, cut, shard_count * columns), jnp.float32)
    return pl.pallas_call(
        functools.partial(unpack_kernel, columns),
        grid=(ctx_size,),
        in_specs=[pl.BlockSpec((1,) + rows.shape[1:], lambda c: (c, 0, 0, 0))],
        out_specs=[pl.BlockSpec((1, cut, shard_count * columns), lambda c: (c, 0, 0))] * 2,
        out_shape=[out, out],
        name="unpack",
    )(rows)


def shards(
    layer_input,
    block_order,
    first_gain,
    w_qkv,
    b_qkv,
    w_o,
    second_gain,
    w_gate,
    w_up,
    w_down,
    cotangent,
):
    ctx_size = lax.axis_size("ctx")
    shard_count = lax.axis_size("fsdp")
    own_ctx = lax.axis_index("ctx")
    own_shard = lax.axis_index("fsdp")
    rows_here = layer_input.shape[0]
    slots = layer_input.shape[1]
    block_rows = rows_here * shard_count
    kv_width = KVH * HD
    cut = D // (ctx_size * shard_count)
    columns = FF // shard_count
    first_row = (own_ctx * shard_count + own_shard) * rows_here
    own_pos = block_positions(block_order, first_row, rows_here, block_rows, ctx_size)
    cosine_table, sine_table = rope_tables(own_pos.reshape(-1))
    query_scale = HD ** (-0.5)

    def by_rows(ctx, shard):
        return shard * ctx_size + ctx

    def by_tokens(ctx, shard):
        return ctx * shard_count + shard

    def own_cut(weight):
        return lax.dynamic_slice_in_dim(weight, own_ctx * cut, cut, 0)

    def mix_features(values):
        shaped = values.reshape(-1, shard_count, ctx_size, cut)
        return shaped.transpose(0, 2, 1, 3).reshape(-1, D)

    def unmix_features(values):
        shaped = values.reshape(-1, ctx_size, shard_count, cut)
        return shaped.transpose(0, 2, 1, 3).reshape(-1, D)

    small = jnp.concatenate([b_qkv, first_gain, second_gain]).reshape(ctx_size, -1)
    small_width = small.shape[1]
    small = lax.dynamic_slice_in_dim(small, own_ctx, 1, 0)
    small = jnp.pad(small, ((0, 0), (0, 16 * HD - small_width))).reshape(16, HD)
    width = -(-columns // HD) * HD
    w_qkv_all, small_all, gate_up_cut = gather(
        [own_cut(w_qkv), small],
        [by_rows, by_rows],
        1,
        "gather_weights",
        swaps=[pack(own_cut(w_gate), own_cut(w_up), shard_count, columns, width)],
    )
    w_qkv_all = w_qkv_all.reshape(D, QKV)
    small_all = small_all.reshape(shard_count, ctx_size, -1)[:, :, :small_width]
    small_all = small_all.reshape(shard_count, -1).astype(jnp.float32)
    bias_width = QKV // shard_count
    gain_width = D // shard_count
    bias_all = small_all[:, :bias_width].reshape(-1)
    gain_one = small_all[:, bias_width : bias_width + gain_width].reshape(-1)
    gain_two = small_all[:, bias_width + gain_width :].reshape(-1)

    gate_up_cols = lax.all_gather(
        gate_up_cut.reshape(shard_count * cut, 2 * width), "ctx", axis=0, tiled=True
    )
    down_padded = jnp.pad(w_down, ((0, width - columns), (0, 0)))
    cotangent_all = lax.all_gather(cotangent.reshape(-1, D), "fsdp", axis=0, tiled=True)

    inputs = layer_input.reshape(-1, D).astype(jnp.float32)
    unit_one, scale_one, normed = normalize(inputs, gain_one)
    normed_one = normed.astype(jnp.bfloat16)
    projected = jnp.dot(normed_one, w_qkv_all, preferred_element_type=jnp.float32) + bias_all
    query_raw = projected[:, : H * HD].reshape(-1, H, HD)
    key_raw = projected[:, H * HD : H * HD + kv_width].reshape(-1, KVH, HD)
    value_raw = projected[:, H * HD + kv_width :]
    query_tokens = (
        (rotate(query_raw, cosine_table, sine_table) * query_scale)
        .astype(jnp.bfloat16)
        .reshape(-1, H * HD)
    )
    key_tokens = (
        rotate(key_raw, cosine_table, sine_table).astype(jnp.bfloat16).reshape(-1, kv_width)
    )
    own_kv = jnp.stack([key_tokens, value_raw.astype(jnp.bfloat16)], 1)
    own_kv = own_kv.reshape(rows_here, 2, SEQS, 2, KVH, HD).transpose(0, 2, 4, 1, 3, 5)
    own_kv = own_kv.reshape(rows_here, SEQS * KVH * 4 * HD)
    all_kv, w_o_all = gather([own_kv, own_cut(w_o)], [by_tokens, by_rows], 2, "gather_keys")
    w_o_all = w_o_all.reshape(D, D)
    all_kv = all_kv.reshape(-1, SEQS * KVH * 4 * HD)
    queries = to_groups(query_tokens, rows_here)
    scalars = jnp.concatenate(
        [block_order.reshape(-1), jnp.stack([own_ctx, own_shard]).astype(jnp.int32)]
    )
    attended_grouped, stats = attend_forward(
        scalars, queries, all_kv, ctx_size, block_rows, rows_here
    )
    attended_low = from_groups(attended_grouped, rows_here).astype(jnp.bfloat16)
    middle = inputs + jnp.dot(attended_low, w_o_all, preferred_element_type=jnp.float32)
    unit_two, scale_two, normed = normalize(middle, gain_two)
    normed_two = mix_features(normed.astype(jnp.bfloat16))

    tokens_all = lax.all_gather(normed_two, "fsdp", axis=0, tiled=True)
    gate_up_part = jnp.dot(tokens_all, gate_up_cols, preferred_element_type=jnp.float32)
    gate_part, up_part = gate_up_part[:, :width], gate_up_part[:, width:]
    sigmoid_gate = jax.nn.sigmoid(gate_part)
    activated = gate_part * sigmoid_gate
    hidden = (activated * up_part).astype(jnp.bfloat16)
    grad_hidden = lax.dot_general(
        cotangent_all, down_padded, CONTRACT_LAST, preferred_element_type=jnp.float32
    )
    grad_gate = grad_hidden * up_part * sigmoid_gate * (1.0 + gate_part * (1.0 - sigmoid_gate))
    grad_gate_up = jnp.concatenate([grad_gate, grad_hidden * activated], -1).astype(jnp.bfloat16)
    grad_tokens = lax.dot_general(
        grad_gate_up, gate_up_cols, CONTRACT_LAST, preferred_element_type=jnp.float32
    )
    grad_normed_two = lax.psum_scatter(
        grad_tokens.astype(jnp.bfloat16), "fsdp", scatter_dimension=0, tiled=True
    )
    down_terms = lax.dot_general(
        hidden, cotangent_all, CONTRACT_FIRST, preferred_element_type=jnp.float32
    ).astype(jnp.bfloat16)
    gate_up_terms = lax.dot_general(
        tokens_all, grad_gate_up, CONTRACT_FIRST, preferred_element_type=jnp.float32
    ).astype(jnp.bfloat16)
    mixed_terms = jnp.dot(hidden, down_padded, preferred_element_type=jnp.float32).astype(jnp.bfloat16)
    down_rows = lax.psum(down_terms, "ctx")
    gate_up_rows = lax.psum_scatter(gate_up_terms, "ctx", scatter_dimension=0, tiled=True)
    gate_up_rows = exchange(
        gate_up_rows.reshape(shard_count, cut, 2 * width), 5, "exchange_rows"
    )
    gate_up_rows, down_rows = lax.optimization_barrier((gate_up_rows, down_rows))
    gate_up_rows = lax.all_gather(gate_up_rows, "ctx", axis=0, tiled=False)

    grad_normed_two, down_terms, gate_up_terms, mixed_terms = lax.optimization_barrier(
        (grad_normed_two, down_terms, gate_up_terms, mixed_terms)
    )
    grad_normed_two = unmix_features(grad_normed_two.astype(jnp.float32))
    grad_middle_norm, grad_gain_two = norm_back(grad_normed_two, unit_two, scale_two, gain_two)
    grad_middle = cotangent.reshape(-1, D).astype(jnp.float32) + grad_middle_norm
    grad_branch_one = grad_middle.astype(jnp.bfloat16)
    grad_attended = lax.dot_general(
        grad_branch_one, w_o_all, CONTRACT_LAST, preferred_element_type=jnp.float32
    ).astype(jnp.bfloat16)
    o_terms = lax.dot_general(
        attended_low, grad_branch_one, CONTRACT_FIRST, preferred_element_type=jnp.float32
    ).astype(jnp.bfloat16)
    grad_queries, grad_kv_full = attend_backward(
        scalars,
        queries,
        to_groups(grad_attended, rows_here),
        attended_grouped,
        stats,
        all_kv,
        ctx_size,
        block_rows,
        rows_here,
    )
    (grad_kv,) = scatter(
        [grad_kv_full.reshape(-1, rows_here, SEQS * KVH * 4 * HD)],
        by_tokens,
        3,
        "scatter_keys",
        out_dtype=jnp.float32,
    )
    grad_kv, mixed_terms = lax.optimization_barrier((grad_kv, mixed_terms))
    mixed_out = middle + lax.psum_scatter(
        mixed_terms, "fsdp", scatter_dimension=0, tiled=True
    ).astype(jnp.float32)
    output = mixed_out.astype(jnp.bfloat16).reshape(rows_here, slots, D)
    grad_kv_low = narrowed(grad_kv).reshape(rows_here, SEQS, KVH, 2, 2, HD)
    grad_kv_low = grad_kv_low.transpose(0, 3, 1, 4, 2, 5).reshape(-1, 2 * kv_width)
    grad_query_tokens = from_groups(narrowed(grad_queries), rows_here) * query_scale
    grad_query_raw = rotate_back(
        grad_query_tokens.reshape(-1, H, HD), cosine_table, sine_table
    ).reshape(-1, H * HD)
    grad_key_raw = rotate_back(
        grad_kv_low[:, :kv_width].reshape(-1, KVH, HD), cosine_table, sine_table
    ).reshape(-1, kv_width)
    grad_projected = jnp.concatenate(
        [grad_query_raw, grad_key_raw, grad_kv_low[:, kv_width:]], -1
    ).astype(jnp.bfloat16)
    grad_bias = jnp.sum(grad_projected, 0, dtype=jnp.float32)
    grad_normed_one = lax.dot_general(
        grad_projected, w_qkv_all, CONTRACT_LAST, preferred_element_type=jnp.float32
    )
    grad_input_norm, grad_gain_one = norm_back(grad_normed_one, unit_one, scale_one, gain_one)
    grad_input = (grad_middle + grad_input_norm).reshape(rows_here, slots, D)
    qkv_terms = lax.dot_general(
        normed_one, grad_projected, CONTRACT_FIRST, preferred_element_type=jnp.float32
    ).astype(jnp.bfloat16)
    small_terms = jnp.concatenate(
        [
            part.reshape(shard_count, -1)
            for part in (grad_gain_one, grad_gain_two, grad_bias[:QK], grad_bias[QK:])
        ],
        1,
    )
    small_terms = small_terms.reshape(ctx_size * shard_count, small_width)
    small_terms = jnp.pad(small_terms, ((0, 0), (0, 8 * HD - small_width)))
    qkv_rows, o_rows, small_rows = scatter(
        [
            qkv_terms.reshape(-1, cut, QKV),
            o_terms.reshape(-1, cut, D),
            small_terms.reshape(-1, 8, HD),
        ],
        by_rows,
        4,
        "scatter_weights",
        spread_ctx=True,
    )
    small_rows = small_rows.reshape(ctx_size, -1)[:, :small_width].reshape(-1)
    bias_start = 2 * gain_width
    value_start = bias_start + QK // shard_count

    gate_rows, up_rows = unpack(gate_up_rows, columns)
    return (
        output,
        grad_input,
        small_rows[:gain_width],
        qkv_rows.reshape(-1, QKV).astype(jnp.float32),
        small_rows[bias_start:value_start],
        small_rows[value_start:],
        o_rows.reshape(-1, D).astype(jnp.float32),
        small_rows[gain_width:bias_start],
        gate_rows.reshape(-1, FF),
        up_rows.reshape(-1, FF),
        down_rows[:columns].astype(jnp.float32),
    )


def solution(mesh):
    in_specs = (
        P(("ctx", "fsdp"), None, None),
        P(),
        P("fsdp"),
        P("fsdp", None),
        P("fsdp"),
        P("fsdp", None),
        P("fsdp"),
        P("fsdp", None),
        P("fsdp", None),
        P("fsdp", None),
        P(("ctx", "fsdp"), None, None),
    )
    out_specs = (
        P(("ctx", "fsdp"), None, None),
        P(("ctx", "fsdp"), None, None),
        P("fsdp"),
        P("fsdp", None),
        P("fsdp"),
        P("fsdp"),
        P("fsdp", None),
        P("fsdp"),
        P("fsdp", None),
        P("fsdp", None),
        P("fsdp", None),
    )
    return jax.shard_map(shards, mesh=mesh, in_specs=in_specs, out_specs=out_specs, check_vma=False)
```

```python
import functools

import jax
import jax.numpy as jnp
from jax import lax
from jax.experimental import pallas as pl
from jax.experimental.pallas import tpu as pltpu
from jax.sharding import PartitionSpec as P

D = 1536
H = 12
KVH = 2
HD = 128
FF = 8960
SEQS = 2
QKV = 2048
QK = 1792


EPS = 1e-06
THETA = 1000000.0
NEG_FILL = -1e30
MESH_ID = pl.DeviceIdType.MESH
CONTRACT_LAST = (((1,), (1,)), ((), ()))
CONTRACT_FIRST = (((0,), (0,)), ((), ()))


def narrowed(values):
    return lax.optimization_barrier(values.astype(jnp.bfloat16)).astype(jnp.float32)


def block_positions(block_order, first_row, row_count, block_rows, ctx_size):
    row_index = first_row + jnp.arange(row_count, dtype=jnp.int32)
    slot_index = jnp.arange(2 * SEQS, dtype=jnp.int32)
    entries = (slot_index // SEQS)[None, :] * ctx_size + (row_index // block_rows)[:, None]
    tiled = jnp.tile(block_order, (2, 1))
    entry_ids = jnp.arange(2 * ctx_size, dtype=jnp.int32)
    picked = jnp.sum(
        jnp.where(entries[:, :, None] == entry_ids[None, None, :], tiled[None, :, :], 0), -1
    )
    return picked * block_rows + (row_index % block_rows)[:, None]


def to_groups(tokens, row_count):
    shaped = tokens.reshape(row_count, 2, SEQS, KVH, H // KVH, HD)
    return shaped.transpose(2, 1, 3, 4, 0, 5).reshape(SEQS, 2, KVH, H // KVH * row_count, HD)


def from_groups(grouped, row_count):
    shaped = grouped.reshape(SEQS, 2, KVH, H // KVH, row_count, HD).transpose(4, 1, 0, 2, 3, 5)
    return shaped.reshape(row_count * 2 * SEQS, H * HD)


def rope_tables(positions):
    half_width = HD // 2
    frequency = THETA ** (-jnp.arange(half_width, dtype=jnp.float32) * 2.0 / HD)
    angles = positions.astype(jnp.float32)[:, None] * frequency[None, :]
    cosine_table = jnp.concatenate([jnp.cos(angles), jnp.cos(angles)], -1)[:, None, :]
    sine_table = jnp.concatenate([jnp.sin(angles), jnp.sin(angles)], -1)[:, None, :]
    return (cosine_table, sine_table)


def rotate(head_values, cosine_table, sine_table):
    half_width = HD // 2
    turned = jnp.concatenate([-head_values[..., half_width:], head_values[..., :half_width]], -1)
    return head_values * cosine_table + turned * sine_table


def rotate_back(grad_values, cosine_table, sine_table):
    half_width = HD // 2
    moved = grad_values * sine_table
    return grad_values * cosine_table + jnp.concatenate(
        [moved[..., half_width:], -moved[..., :half_width]], -1
    )


def normalize(values, gain):
    scale = lax.rsqrt(jnp.mean(values * values, -1, keepdims=True) + EPS)
    unit = values * scale
    return (unit, scale, unit * gain)


def norm_back(grad_out, unit, scale, gain):
    grad_unit = grad_out * gain
    inner = jnp.mean(grad_unit * unit, -1, keepdims=True)
    return (scale * (grad_unit - unit * inner), jnp.sum(grad_out * unit, 0))


def attend_forward_kernel(ctx_size, block_rows, rows_here, scalars, q_ref, kv_ref, out_ref, stat_ref, best_ref, total_ref, accum_ref):
    seq = pl.program_id(0)
    blocks = 2 * ctx_size
    own_ctx = scalars[SEQS * blocks]
    own_shard = scalars[SEQS * blocks + 1]
    lanes = q_ref.shape[3]
    best_ref[...] = jnp.full(best_ref.shape, NEG_FILL, jnp.float32)
    total_ref[...] = jnp.zeros(total_ref.shape, jnp.float32)
    accum_ref[...] = jnp.zeros(accum_ref.shape, jnp.float32)

    def step(key_ctx, half_key, half):
        order_key = scalars[seq * blocks + half_key * ctx_size + key_ctx]
        order_query = scalars[seq * blocks + half * ctx_size + own_ctx]

        def work(masked):
            rows = pl.ds(pl.multiple_of(key_ctx * block_rows, block_rows), block_rows)
            keys = kv_ref[rows, half_key * 2 * HD : half_key * 2 * HD + HD]
            values = kv_ref[rows, half_key * 2 * HD + HD : half_key * 2 * HD + 2 * HD]
            scores = lax.dot_general(
                keys, q_ref[0, half, 0], CONTRACT_LAST, preferred_element_type=jnp.float32
            )
            if masked:
                row = lax.broadcasted_iota(jnp.int32, (block_rows, lanes), 0)
                lane = lax.broadcasted_iota(jnp.int32, (block_rows, lanes), 1)
                scores = jnp.where(
                    row <= own_shard * rows_here + lax.rem(lane, rows_here), scores, NEG_FILL
                )
            best = best_ref[half]
            fresh = jnp.maximum(best, jnp.max(scores, 0, keepdims=True))
            decay = jnp.exp(best - fresh)
            weights = jnp.exp(scores - fresh)
            total_ref[half] = total_ref[half] * decay + jnp.sum(weights, 0, keepdims=True)
            accum_ref[half] = accum_ref[half] * decay + lax.dot_general(
                values,
                weights.astype(jnp.bfloat16),
                CONTRACT_FIRST,
                preferred_element_type=jnp.float32,
            )
            best_ref[half] = fresh

        @pl.when(order_key < order_query)
        def full():
            work(False)

        @pl.when(order_key == order_query)
        def diagonal():
            work(True)

    @pl.loop(0, ctx_size)
    def sweep(key_ctx):
        for half_key in range(2):
            for half in range(2):
                step(key_ctx, half_key, half)

    for half in range(2):
        totals = total_ref[half]
        out_ref[0, half, 0] = (accum_ref[half] / totals).T
        stat_ref[0, half, 0] = best_ref[half] + jnp.log(totals)


def attend_forward(scalars, queries, all_kv, ctx_size, block_rows, rows_here):
    lanes = queries.shape[3]
    kernel = functools.partial(attend_forward_kernel, ctx_size, block_rows, rows_here)
    group = pl.BlockSpec((1, 2, 1, lanes, HD), lambda s, n, _: (s, 0, n, 0, 0))
    stat = pl.BlockSpec((1, 2, 1, 1, lanes), lambda s, n, _: (s, 0, n, 0, 0))
    return pl.pallas_call(
        kernel,
        grid_spec=pltpu.PrefetchScalarGridSpec(
            num_scalar_prefetch=1,
            grid=(SEQS, KVH),
            in_specs=[
                group,
                pl.BlockSpec((all_kv.shape[0], 4 * HD), lambda s, n, _: (0, s * KVH + n)),
            ],
            out_specs=[group, stat],
            scratch_shapes=[
                pltpu.VMEM((2, 1, lanes), jnp.float32),
                pltpu.VMEM((2, 1, lanes), jnp.float32),
                pltpu.VMEM((2, HD, lanes), jnp.float32),
            ],
        ),
        out_shape=(
            jax.ShapeDtypeStruct(queries.shape, jnp.float32),
            jax.ShapeDtypeStruct((SEQS, 2, KVH, 1, lanes), jnp.float32),
        ),
        compiler_params=pltpu.CompilerParams(vmem_limit_bytes=56 * 2**20),
        name="attend_forward",
    )(scalars, queries, all_kv)


def attend_backward_kernel(ctx_size, block_rows, rows_here, scalars, q_ref, go_ref, att_ref, stat_ref, kv_ref, gq_ref, gkv_ref, delta_ref, gq_acc, gk_acc, gv_acc):
    seq = pl.program_id(0)
    blocks = 2 * ctx_size
    own_ctx = scalars[SEQS * blocks]
    own_shard = scalars[SEQS * blocks + 1]
    lanes = q_ref.shape[3]
    gq_acc[...] = jnp.zeros(gq_acc.shape, jnp.float32)
    for half in range(2):
        product = go_ref[0, half, 0].astype(jnp.float32) * att_ref[0, half, 0]
        delta_ref[half] = jnp.sum(product.T, 0, keepdims=True)

    def step(key_ctx, half_key, half):
        order_key = scalars[seq * blocks + half_key * ctx_size + key_ctx]
        order_query = scalars[seq * blocks + half * ctx_size + own_ctx]

        def work(masked):
            rows = pl.ds(pl.multiple_of(key_ctx * block_rows, block_rows), block_rows)
            keys = kv_ref[rows, half_key * 2 * HD : half_key * 2 * HD + HD]
            values = kv_ref[rows, half_key * 2 * HD + HD : half_key * 2 * HD + 2 * HD]
            queries = q_ref[0, half, 0]
            grad_out = go_ref[0, half, 0]
            scores = lax.dot_general(
                keys, queries, CONTRACT_LAST, preferred_element_type=jnp.float32
            )
            probs = jnp.exp(scores - stat_ref[0, half, 0])
            if masked:
                row = lax.broadcasted_iota(jnp.int32, (block_rows, lanes), 0)
                lane = lax.broadcasted_iota(jnp.int32, (block_rows, lanes), 1)
                probs = jnp.where(
                    row <= own_shard * rows_here + lax.rem(lane, rows_here), probs, 0.0
                )
            grad_probs = lax.dot_general(
                values, grad_out, CONTRACT_LAST, preferred_element_type=jnp.float32
            )
            grad_scores = (probs * (grad_probs - delta_ref[half])).astype(jnp.bfloat16)
            gv_acc[...] += jnp.dot(
                probs.astype(jnp.bfloat16), grad_out, preferred_element_type=jnp.float32
            )
            gk_acc[...] += jnp.dot(grad_scores, queries, preferred_element_type=jnp.float32)
            gq_acc[half] += lax.dot_general(
                keys, grad_scores, CONTRACT_FIRST, preferred_element_type=jnp.float32
            )

        @pl.when(order_key < order_query)
        def full():
            work(False)

        @pl.when(order_key == order_query)
        def diagonal():
            work(True)

    @pl.loop(0, ctx_size)
    def sweep(key_ctx):
        rows = pl.ds(pl.multiple_of(key_ctx * block_rows, block_rows), block_rows)
        for half_key in range(2):
            gk_acc[...] = jnp.zeros(gk_acc.shape, jnp.float32)
            gv_acc[...] = jnp.zeros(gv_acc.shape, jnp.float32)
            for half in range(2):
                step(key_ctx, half_key, half)
            at = half_key * 2 * HD
            gkv_ref[rows, at : at + HD] = gk_acc[...].astype(jnp.bfloat16)
            gkv_ref[rows, at + HD : at + 2 * HD] = gv_acc[...].astype(jnp.bfloat16)

    for half in range(2):
        gq_ref[0, half, 0] = gq_acc[half].T


def attend_backward(scalars, queries, grad_out, attended, stats, all_kv, ctx_size, block_rows, rows_here):
    lanes = queries.shape[3]
    kernel = functools.partial(attend_backward_kernel, ctx_size, block_rows, rows_here)
    group = pl.BlockSpec((1, 2, 1, lanes, HD), lambda s, n, _: (s, 0, n, 0, 0))
    stat = pl.BlockSpec((1, 2, 1, 1, lanes), lambda s, n, _: (s, 0, n, 0, 0))
    full = pl.BlockSpec((all_kv.shape[0], 4 * HD), lambda s, n, _: (0, s * KVH + n))
    return pl.pallas_call(
        kernel,
        grid_spec=pltpu.PrefetchScalarGridSpec(
            num_scalar_prefetch=1,
            grid=(SEQS, KVH),
            in_specs=[group, group, group, stat, full],
            out_specs=[group, full],
            scratch_shapes=[
                pltpu.VMEM((2, 1, lanes), jnp.float32),
                pltpu.VMEM((2, HD, lanes), jnp.float32),
                pltpu.VMEM((block_rows, HD), jnp.float32),
                pltpu.VMEM((block_rows, HD), jnp.float32),
            ],
        ),
        out_shape=(
            jax.ShapeDtypeStruct(queries.shape, jnp.float32),
            jax.ShapeDtypeStruct(all_kv.shape, jnp.bfloat16),
        ),
        compiler_params=pltpu.CompilerParams(vmem_limit_bytes=56 * 2**20),
        name="attend_backward",
    )(scalars, queries, grad_out, attended, stats, all_kv)


def peers_of(ctx_size):
    return ctx_size == 4, range(1, ctx_size)


def ctx_target(position, way, square, ctx_size):
    return position ^ way if square else lax.rem(position + way, ctx_size)


def ctx_source(position, way, square, ctx_size):
    return position ^ way if square else lax.rem(position + ctx_size - way, ctx_size)


def greet(ctx_size, pair_count, with_ctx, all_shards):
    ctx = lax.axis_index("ctx")
    shard = lax.axis_index("fsdp")
    pair, core = shard // 2, shard % 2
    barrier = pltpu.get_barrier_semaphore()
    shard_count = 2 * pair_count
    partners = [(ctx, pair * 2 + 1 - core)]
    for step in range(1, pair_count):
        there = lax.rem(pair + step, pair_count) * 2
        partners.append((ctx, there + core))
        if all_shards:
            partners.append((ctx, there + 1 - core))
    if with_ctx:
        for way in range(1, ctx_size):
            partners.append((lax.rem(ctx + way, ctx_size), shard))
    for partner in partners:
        pl.semaphore_signal(barrier, inc=1, device_id=partner, device_id_type=MESH_ID)
    pl.semaphore_wait(barrier, len(partners))
    return ctx, pair, core


class Exchange:
    def __init__(self, source, out, sems, own_sem, pair_count):
        self.source, self.out, self.sems, self.own_sem = source, out, sems, own_sem
        self.shard_count = 2 * pair_count

    def start(self):
        ctx, shard = lax.axis_index("ctx"), lax.axis_index("fsdp")
        self.own = pltpu.make_async_copy(self.source.at[shard], self.out.at[shard], self.own_sem)
        self.own.start()
        self.copies = []
        for step in range(1, self.shard_count):
            there = lax.rem(shard + step, self.shard_count)
            copy = pltpu.make_async_remote_copy(
                src_ref=self.source.at[there],
                dst_ref=self.out.at[shard],
                send_sem=self.sems[0].at[step - 1],
                recv_sem=self.sems[1].at[step - 1],
                device_id=(ctx, there),
                device_id_type=MESH_ID,
            )
            copy.start()
            self.copies.append(copy)

    def finish(self):
        ctx, shard = lax.axis_index("ctx"), lax.axis_index("fsdp")
        for step in range(1, self.shard_count):
            come = lax.rem(shard + self.shard_count - step, self.shard_count)
            pltpu.make_async_remote_copy(
                src_ref=self.out.at[come],
                dst_ref=self.out.at[come],
                send_sem=self.sems[0].at[step - 1],
                recv_sem=self.sems[1].at[step - 1],
                device_id=(ctx, shard),
                device_id_type=MESH_ID,
            ).wait_recv()
        self.own.wait()
        for copy in self.copies:
            copy.wait_send()


def exchange_kernel(pair_count, source, out, send_sem, recv_sem, own_sem):
    greet(1, pair_count, False, True)
    flow = Exchange(source, out, (send_sem, recv_sem), own_sem, pair_count)
    flow.start()
    flow.finish()


def exchange(pieces, collective_id, name):
    shard_count = lax.axis_size("fsdp")
    dma = pltpu.SemaphoreType.DMA
    return pl.pallas_call(
        functools.partial(exchange_kernel, shard_count // 2),
        in_specs=[pl.BlockSpec(memory_space=pltpu.VMEM)],
        out_specs=pl.BlockSpec(memory_space=pl.ANY),
        out_shape=jax.ShapeDtypeStruct(pieces.shape, pieces.dtype),
        scratch_shapes=[dma((shard_count - 1,))] * 2 + [dma],
        compiler_params=pltpu.CompilerParams(collective_id=collective_id, has_side_effects=True),
        cost_estimate=pl.CostEstimate(
            flops=0, bytes_accessed=pieces.size * 64, transcendentals=0
        ),
        name=name,
    )(pieces)


def gather_kernel(arity, ctx_size, pair_count, slots, swaps, with_ctx, *refs):
    sources, refs = refs[:arity], refs[arity:]
    swap_sources, refs = refs[:swaps], refs[swaps:]
    outs, refs = refs[:arity], refs[arity:]
    swap_outs, refs = refs[:swaps], refs[swaps:]
    pair_sems, ctx_sems, core_sems = refs[0:2], refs[2:4], refs[4:6]
    local_sem = refs[6]
    square, ways = peers_of(ctx_size) if with_ctx else (False, ())
    near = [way for way in ways if not (square and way == 3)]
    ctx, pair, core = greet(ctx_size, pair_count, with_ctx, swaps > 0)
    homes = [place(ctx, pair * 2 + core) for place in slots]
    started = []
    steps = [(0, 1)] + [(far, way) for far in range(1, pair_count) for way in (1, -1)]

    def present(step):
        far, way = steps[step]
        if far == 0:
            return None
        return pair >= far if way == 1 else pair + far < pair_count

    def origin(step):
        far, way = steps[step]
        return pair - far * way

    def when(condition, work):
        if condition is None:
            work()
        else:
            pl.when(condition)(work)

    def send(item, source, place, target, sems, at, condition):
        copy = pltpu.make_async_remote_copy(
            src_ref=source,
            dst_ref=outs[item].at[place],
            send_sem=sems[0].at[at],
            recv_sem=sems[1].at[at],
            device_id=target,
            device_id_type=MESH_ID,
        )
        copy.start()
        started.append((condition, item, sems, at))

    def sent(item, sems, at):
        pltpu.make_async_remote_copy(
            src_ref=outs[item].at[0],
            dst_ref=outs[item].at[0],
            send_sem=sems[0].at[at],
            recv_sem=sems[1].at[at],
            device_id=(ctx, pair * 2 + core),
            device_id_type=MESH_ID,
        ).wait_send()

    def arrive(item, place, sems, at):
        pltpu.make_async_remote_copy(
            src_ref=outs[item].at[place],
            dst_ref=outs[item].at[place],
            send_sem=sems[0].at[at],
            recv_sem=sems[1].at[at],
            device_id=(ctx, pair * 2 + core),
            device_id_type=MESH_ID,
        ).wait_recv()

    def pass_on(step, item, source, place):
        far, way = steps[step]
        for side in (1, -1) if far == 0 else (way,):

            def further(side=side):
                return pair + 1 < pair_count if side == 1 else pair >= 1

            def both(further=further):
                return further() if far == 0 else jnp.logical_and(further(), present(step))

            def work(side=side, both=both):
                send(
                    item,
                    source,
                    place,
                    (ctx, (pair + side) * 2 + core),
                    pair_sems,
                    ((side + 1) // 2, far, item),
                    both,
                )

            if far + 1 < pair_count:
                pl.when(further())(work)

    def to_core(item, source, from_ctx, way, step):
        send(
            item,
            source,
            slots[item](from_ctx, origin(step) * 2 + core),
            (ctx, pair * 2 + 1 - core),
            core_sems,
            (way, step, item),
            functools.partial(present, step),
        )

    def spread(step):
        for item in range(arity):
            place = slots[item](ctx, origin(step) * 2 + core)
            source = sources[item]
            if step:
                far, way = steps[step]
                arrive(item, place, pair_sems, ((way + 1) // 2, far - 1, item))
                source = outs[item].at[place]
            pass_on(step, item, source, place)
            for way in near:
                there = ctx_target(ctx, way, square, ctx_size)
                send(
                    item,
                    source,
                    place,
                    (there, pair * 2 + core),
                    ctx_sems,
                    (way - 1, step, item),
                    functools.partial(present, step),
                )
            to_core(item, source, ctx, 0, step)

    def collect(step):
        for way in near:
            for item in range(arity):
                come = ctx_source(ctx, way, square, ctx_size)
                place = slots[item](come, origin(step) * 2 + core)
                arrive(item, place, ctx_sems, (way - 1, step, item))
                source = outs[item].at[place]
                if square and (steps[step][0] % 2 == 0) == (way == 1):
                    send(
                        item,
                        source,
                        place,
                        (ctx ^ (3 - way), pair * 2 + core),
                        ctx_sems,
                        (2, step, item),
                        functools.partial(present, step),
                    )
                to_core(item, source, come, way, step)

    def collect_far(step):
        for item in range(arity):
            place = slots[item](ctx ^ 3, origin(step) * 2 + core)
            arrive(item, place, ctx_sems, (2, step, item))
            to_core(item, outs[item].at[place], ctx ^ 3, 3, step)

    locals_ = []
    for item in range(arity):
        copy = pltpu.make_async_copy(sources[item], outs[item].at[homes[item]], local_sem.at[item])
        copy.start()
        locals_.append(copy)
    when(None, lambda: spread(0))
    flows = []
    count = len(steps)
    for turn in range(1, count + 4):
        if turn < count:
            when(present(turn), functools.partial(spread, turn))
        if turn == count:
            for item in range(swaps):
                flow = Exchange(
                    swap_sources[item],
                    swap_outs[item],
                    refs[7 + 3 * item : 9 + 3 * item],
                    refs[9 + 3 * item],
                    pair_count,
                )
                flow.start()
                flows.append(flow)
        if 0 <= turn - 2 < count:
            when(present(turn - 2), functools.partial(collect, turn - 2))
        if square and 0 <= turn - 4 < count:
            when(present(turn - 4), functools.partial(collect_far, turn - 4))

    def from_core(step):
        for way in (0, *ways):
            come = ctx_source(ctx, way, square, ctx_size) if way else ctx
            for item in range(arity):
                arrive(item, slots[item](come, origin(step) * 2 + 1 - core), core_sems, (way, step, item))

    for step in range(count):
        when(present(step), functools.partial(from_core, step))
    for flow in flows:
        flow.finish()
    for copy in locals_:
        copy.wait()
    for condition, *which in started:
        when(condition(), functools.partial(sent, *which))


def gather(pieces, slots, collective_id, name, swaps=(), with_ctx=True):
    ctx_size, shard_count = lax.axis_size("ctx"), lax.axis_size("fsdp")
    pair_count = shard_count // 2
    arity = len(pieces)
    dma = pltpu.SemaphoreType.DMA
    moved = sum(piece.size for piece in pieces) * 2
    steps = 2 * pair_count - 1
    return pl.pallas_call(
        functools.partial(gather_kernel, arity, ctx_size, pair_count, slots, len(swaps), with_ctx),
        in_specs=[pl.BlockSpec(memory_space=pltpu.VMEM)] * (arity + len(swaps)),
        out_specs=[pl.BlockSpec(memory_space=pl.ANY)] * (arity + len(swaps)),
        out_shape=[
            jax.ShapeDtypeStruct(
                ((ctx_size if with_ctx else 1) * shard_count,) + piece.shape, piece.dtype
            )
            for piece in pieces
        ]
        + [jax.ShapeDtypeStruct(swap.shape, swap.dtype) for swap in swaps],
        scratch_shapes=[dma((2, pair_count - 1, arity))] * 2
        + [dma((ctx_size - 1, steps, arity))] * 2
        + [dma((ctx_size, steps, arity))] * 2
        + [dma((arity,))]
        + [dma((shard_count - 1,)), dma((shard_count - 1,)), dma] * len(swaps),
        compiler_params=pltpu.CompilerParams(collective_id=collective_id, has_side_effects=True),
        cost_estimate=pl.CostEstimate(
            flops=0, bytes_accessed=moved * ctx_size * shard_count * 4, transcendentals=0
        ),
        name=name,
    )(*pieces, *swaps)


class LineScatter:
    def __init__(self, source, out, half, above, below, sems, where, pair_count):
        self.source, self.out, self.half, self.rooms = source, out, half, {1: above, -1: below}
        self.core_sems, self.line_sems = sems[0:2], {1: sems[2:4], -1: sems[4:6]}
        self.ctx, self.pair, self.core = where
        self.count = pair_count
        self.order = []
        for turn in range(pair_count - 1):
            self.order += [(pair_count - 1 - turn, 1), (turn, -1)]

    def copy(self, source, target, device, sems, at):
        return pltpu.make_async_remote_copy(
            src_ref=source,
            dst_ref=target,
            send_sem=sems[0].at[at],
            recv_sem=sems[1].at[at],
            device_id=device,
            device_id_type=MESH_ID,
        )

    def here(self):
        return (self.ctx, self.pair * 2 + self.core)

    def core_copy(self, pair):
        return self.copy(
            self.source.at[pair * 2 + 1 - self.core],
            self.half.at[pair],
            (self.ctx, self.pair * 2 + 1 - self.core),
            self.core_sems,
            pair,
        )

    def line_copy(self, pair, way):
        return self.copy(
            self.half.at[pair],
            self.rooms[way].at[pair],
            (self.ctx, (self.pair + way) * 2 + self.core),
            self.line_sems[way],
            pair,
        )

    def line_room(self, pair, way):
        room = self.rooms[way].at[pair]
        return self.copy(room, room, self.here(), self.line_sems[way], pair)

    def add(self, pair, value):
        half = self.half.at[pair]
        half[...] = (half[...].astype(jnp.float32) + value.astype(jnp.float32)).astype(half.dtype)

    def beyond(self, pair, way):
        return pair > self.pair if way == 1 else pair < self.pair

    def behind(self, way):
        return self.pair > 0 if way == 1 else self.pair < self.count - 1

    def start(self):
        done = []
        for pair, _ in self.order:
            if pair not in done:
                done.append(pair)
                self.core_copy(pair).start()
        self.folds = done

    def fold(self):
        for pair in self.folds:
            self.copy(
                self.half.at[pair], self.half.at[pair], self.here(), self.core_sems, pair
            ).wait_recv()
            self.add(pair, self.source[pair * 2 + self.core])

    def advance(self, turn):
        pair, way = self.order[turn]

        @pl.when(self.beyond(pair, way))
        def pass_on():
            @pl.when(self.behind(way))
            def join():
                self.line_room(pair, way).wait_recv()
                self.add(pair, self.rooms[way][pair])

            self.line_copy(pair, way).start()

    def finish(self):
        for pair in range(self.count):

            @pl.when(self.pair == pair)
            def close(pair=pair):
                self.out[...] = self.half[pair].astype(jnp.float32)
                for way in (1, -1):

                    @pl.when(self.behind(way))
                    def join(way=way):
                        self.line_room(pair, way).wait_recv()
                        self.out[...] += self.rooms[way][pair].astype(jnp.float32)

        for pair in range(self.count):
            self.core_copy(pair).wait_send()
        for pair, way in self.order:

            @pl.when(self.beyond(pair, way))
            def sent(pair=pair, way=way):
                self.line_copy(pair, way).wait_send()


def scatter_kernel(arity, ctx_size, pair_count, slot, spread_ctx, lines, *refs):
    sources, refs = refs[:arity], refs[arity:]
    line_sources, refs = refs[:lines], refs[lines:]
    outs, refs = refs[:arity], refs[arity:]
    line_outs, refs = refs[:lines], refs[lines:]
    halves, relays, asides, ends, finals = (refs[i * arity : (i + 1) * arity] for i in range(5))
    sems = refs[5 * arity : 5 * arity + 10]
    core_sems, relay_sems, ctx_sems, pair_sems, last_sems = (sems[2 * i : 2 * i + 2] for i in range(5))
    square, ways = peers_of(ctx_size)
    ctx, pair, core = greet(ctx_size, pair_count, True, False)
    order = list(range(1, pair_count)) + [0]
    started = []
    flows = []
    for item in range(lines):
        at = 5 * arity + 10 + 9 * item
        flows.append(
            LineScatter(
                line_sources[item],
                line_outs[item],
                *refs[at : at + 3],
                refs[at + 3 : at + 9],
                (ctx, pair, core),
                pair_count,
            )
        )

    def send(source, target, device, pair_of_sems, at):
        copy = pltpu.make_async_remote_copy(
            src_ref=source,
            dst_ref=target,
            send_sem=pair_of_sems[0].at[at],
            recv_sem=pair_of_sems[1].at[at],
            device_id=device,
            device_id_type=MESH_ID,
        )
        copy.start()
        started.append(copy)

    def arrive(target, pair_of_sems, at):
        pltpu.make_async_remote_copy(
            src_ref=target,
            dst_ref=target,
            send_sem=pair_of_sems[0].at[at],
            recv_sem=pair_of_sems[1].at[at],
            device_id=(ctx, pair * 2 + core),
            device_id_type=MESH_ID,
        ).wait_recv()

    def toward(step):
        return lax.rem(pair + step, pair_count)

    def target_ctx(way):
        return ctx_target(ctx, way, square, ctx_size) if way else ctx

    def f32(value):
        return value.astype(jnp.float32)

    far_first = [3, 1, 2, 0] if square else list(ways) + [0]
    for step in order:
        for way in far_first:
            for item in range(arity):
                send(
                    sources[item].at[slot(target_ctx(way), toward(step) * 2 + 1 - core)],
                    halves[item].at[way, step],
                    (ctx, pair * 2 + 1 - core),
                    core_sems,
                    (way, step, item),
                )

    def fold_core(step):
        for way in far_first:
            for item in range(arity):
                half = halves[item].at[way, step]
                arrive(half, core_sems, (way, step, item))
                mine = sources[item][slot(target_ctx(way), toward(step) * 2 + core)]
                half[...] = (f32(mine) + f32(half[...])).astype(half.dtype)
                if square and way == 3:
                    there = ctx ^ (1 if step % 2 == 0 else 2)
                    send(
                        half,
                        relays[item].at[step],
                        (there, pair * 2 + core),
                        relay_sems,
                        (step, item),
                    )

    def fold_relay(step):
        for item in range(arity):
            if square:
                relay = relays[item].at[step]
                arrive(relay, relay_sems, (step, item))
                half = halves[item].at[2 if step % 2 == 0 else 1, step]
                half[...] = (f32(half[...]) + f32(relay[...])).astype(half.dtype)
            for way in ways:
                if square and way == 3:
                    continue
                send(
                    halves[item].at[way, step],
                    asides[item].at[way - 1, step],
                    (target_ctx(way), pair * 2 + core),
                    ctx_sems,
                    (way - 1, step, item),
                )

    def fold_ctx(step):
        for item in range(arity):
            half = halves[item].at[0, step]
            total = f32(half[...])
            for way in ways:
                if square and way == 3:
                    continue
                aside = asides[item].at[way - 1, step]
                arrive(aside, ctx_sems, (way - 1, step, item))
                total = total + f32(aside[...])
            if step:
                half[...] = total.astype(half.dtype)
                send(
                    half,
                    ends[item].at[step - 1],
                    (ctx, toward(step) * 2 + core),
                    pair_sems,
                    (step - 1, item),
                )
            else:
                for other in range(1, pair_count):
                    end = ends[item].at[other - 1]
                    arrive(end, pair_sems, (other - 1, item))
                    total = total + f32(end[...])
                if spread_ctx:
                    finals[item][...] = total.astype(finals[item].dtype)
                else:
                    outs[item][...] = total.astype(outs[item].dtype)

    for flow in flows:
        flow.start()
    turns = 2 * (pair_count - 1)
    for turn in range(pair_count + 2):
        if turn < pair_count:
            fold_core(order[turn])
        if 1 <= turn <= pair_count:
            fold_relay(order[turn - 1])
        for flow in flows:
            if turn == pair_count - 1:
                flow.fold()
                for part in range(2):
                    flow.advance(part)
        if turn >= 2:
            fold_ctx(order[turn - 2])
    for flow in flows:
        for part in range(2, turns):
            flow.advance(part)
    if spread_ctx:
        for item in range(arity):
            for way in ways:
                send(
                    finals[item],
                    outs[item].at[ctx],
                    (target_ctx(way), pair * 2 + core),
                    last_sems,
                    (way - 1, item),
                )
            outs[item][ctx] = finals[item][...]
        for item in range(arity):
            for way in ways:
                arrive(outs[item].at[ctx_source(ctx, way, square, ctx_size)], last_sems, (way - 1, item))
    for flow in flows:
        flow.finish()
    for copy in started:
        copy.wait_send()


def scatter(terms, slot, collective_id, name, spread_ctx=False, out_dtype=None, lines=()):
    ctx_size, shard_count = lax.axis_size("ctx"), lax.axis_size("fsdp")
    pair_count = shard_count // 2
    arity = len(terms)
    dma = pltpu.SemaphoreType.DMA
    lead = (ctx_size,) if spread_ctx else ()
    asides = 2 if ctx_size == 4 else ctx_size - 1

    def room(*extent):
        return [pltpu.VMEM(extent + term.shape[1:], term.dtype) for term in terms]

    moved = sum(term.size * term.dtype.itemsize for term in terms)
    return pl.pallas_call(
        functools.partial(scatter_kernel, arity, ctx_size, pair_count, slot, spread_ctx, len(lines)),
        in_specs=[pl.BlockSpec(memory_space=pltpu.VMEM)] * (arity + len(lines)),
        out_specs=[pl.BlockSpec(memory_space=pltpu.VMEM)] * (arity + len(lines)),
        out_shape=[
            jax.ShapeDtypeStruct(lead + term.shape[1:], out_dtype or term.dtype) for term in terms
        ]
        + [jax.ShapeDtypeStruct(line.shape[1:], jnp.float32) for line in lines],
        scratch_shapes=room(ctx_size, pair_count)
        + room(pair_count)
        + room(asides, pair_count)
        + room(pair_count - 1)
        + room()
        + [dma((ctx_size, pair_count, arity))] * 2
        + [dma((pair_count, arity))] * 2
        + [dma((ctx_size - 1, pair_count, arity))] * 2
        + [dma((pair_count - 1, arity))] * 2
        + [dma((ctx_size - 1, arity))] * 2
        + [
            scratch
            for line in lines
            for scratch in [pltpu.VMEM((pair_count,) + line.shape[1:], line.dtype)] * 3
            + [dma((pair_count,))] * 6
        ],
        compiler_params=pltpu.CompilerParams(
            collective_id=collective_id, has_side_effects=True, vmem_limit_bytes=60 * 2**20
        ),
        cost_estimate=pl.CostEstimate(flops=0, bytes_accessed=moved * 16, transcendentals=0),
        name=name,
    )(*terms, *lines)

def pack_kernel(columns, gate_ref, up_ref, out_ref):
    width = out_ref.shape[2] // 2
    cut = out_ref.shape[1]
    for there in range(out_ref.shape[0]):
        for side, ref in enumerate((gate_ref, up_ref)):
            at = side * width
            out_ref[there, :, at + width - HD : at + width] = jnp.zeros((cut, HD), out_ref.dtype)
            out_ref[there, :, at : at + columns] = ref[:, there * columns : (there + 1) * columns]


def pack(gate, up, shard_count, columns, width):
    return pl.pallas_call(
        functools.partial(pack_kernel, columns),
        in_specs=[pl.BlockSpec(memory_space=pltpu.VMEM)] * 2,
        out_specs=pl.BlockSpec(memory_space=pltpu.VMEM),
        out_shape=jax.ShapeDtypeStruct((shard_count, gate.shape[0], 2 * width), gate.dtype),
        name="pack",
    )(gate, up)


def unpack_kernel(columns, in_ref, gate_ref, up_ref):
    width = in_ref.shape[3] // 2
    for there in range(in_ref.shape[1]):
        for side, ref in enumerate((gate_ref, up_ref)):
            part = in_ref[0, there, :, side * width : side * width + columns]
            ref[0, :, there * columns : (there + 1) * columns] = part.astype(jnp.float32)


def unpack(rows, columns):
    ctx_size, shard_count, cut, _ = rows.shape
    out = jax.ShapeDtypeStruct((ctx_size, cut, shard_count * columns), jnp.float32)
    return pl.pallas_call(
        functools.partial(unpack_kernel, columns),
        grid=(ctx_size,),
        in_specs=[pl.BlockSpec((1,) + rows.shape[1:], lambda c: (c, 0, 0, 0))],
        out_specs=[pl.BlockSpec((1, cut, shard_count * columns), lambda c: (c, 0, 0))] * 2,
        out_shape=[out, out],
        name="unpack",
    )(rows)


def shards(
    layer_input,
    block_order,
    first_gain,
    w_qkv,
    b_qkv,
    w_o,
    second_gain,
    w_gate,
    w_up,
    w_down,
    cotangent,
):
    ctx_size = lax.axis_size("ctx")
    shard_count = lax.axis_size("fsdp")
    own_ctx = lax.axis_index("ctx")
    own_shard = lax.axis_index("fsdp")
    rows_here = layer_input.shape[0]
    slots = layer_input.shape[1]
    block_rows = rows_here * shard_count
    kv_width = KVH * HD
    cut = D // (ctx_size * shard_count)
    columns = FF // shard_count
    first_row = (own_ctx * shard_count + own_shard) * rows_here
    own_pos = block_positions(block_order, first_row, rows_here, block_rows, ctx_size)
    cosine_table, sine_table = rope_tables(own_pos.reshape(-1))
    query_scale = HD ** (-0.5)

    def by_rows(ctx, shard):
        return shard * ctx_size + ctx

    def by_tokens(ctx, shard):
        return ctx * shard_count + shard

    def own_cut(weight):
        return lax.dynamic_slice_in_dim(weight, own_ctx * cut, cut, 0)

    def mix_features(values):
        shaped = values.reshape(-1, shard_count, ctx_size, cut)
        return shaped.transpose(0, 2, 1, 3).reshape(-1, D)

    def unmix_features(values):
        shaped = values.reshape(-1, ctx_size, shard_count, cut)
        return shaped.transpose(0, 2, 1, 3).reshape(-1, D)

    small = jnp.concatenate([b_qkv, first_gain, second_gain]).reshape(ctx_size, -1)
    small_width = small.shape[1]
    small = lax.dynamic_slice_in_dim(small, own_ctx, 1, 0)
    small = jnp.pad(small, ((0, 0), (0, 16 * HD - small_width))).reshape(16, HD)
    width = -(-columns // HD) * HD
    w_qkv_all, small_all, gate_up_cut = gather(
        [own_cut(w_qkv), small],
        [by_rows, by_rows],
        1,
        "gather_weights",
        swaps=[pack(own_cut(w_gate), own_cut(w_up), shard_count, columns, width)],
    )
    w_qkv_all = w_qkv_all.reshape(D, QKV)
    small_all = small_all.reshape(shard_count, ctx_size, -1)[:, :, :small_width]
    small_all = small_all.reshape(shard_count, -1).astype(jnp.float32)
    bias_width = QKV // shard_count
    gain_width = D // shard_count
    bias_all = small_all[:, :bias_width].reshape(-1)
    gain_one = small_all[:, bias_width : bias_width + gain_width].reshape(-1)
    gain_two = small_all[:, bias_width + gain_width :].reshape(-1)

    gate_up_cols = lax.all_gather(
        gate_up_cut.reshape(shard_count * cut, 2 * width), "ctx", axis=0, tiled=True
    )
    down_padded = jnp.pad(w_down, ((0, width - columns), (0, 0)))
    cotangent_all = lax.all_gather(cotangent.reshape(-1, D), "fsdp", axis=0, tiled=True)

    inputs = layer_input.reshape(-1, D).astype(jnp.float32)
    unit_one, scale_one, normed = normalize(inputs, gain_one)
    normed_one = normed.astype(jnp.bfloat16)
    projected = jnp.dot(normed_one, w_qkv_all, preferred_element_type=jnp.float32) + bias_all
    query_raw = projected[:, : H * HD].reshape(-1, H, HD)
    key_raw = projected[:, H * HD : H * HD + kv_width].reshape(-1, KVH, HD)
    value_raw = projected[:, H * HD + kv_width :]
    query_tokens = (
        (rotate(query_raw, cosine_table, sine_table) * query_scale)
        .astype(jnp.bfloat16)
        .reshape(-1, H * HD)
    )
    key_tokens = (
        rotate(key_raw, cosine_table, sine_table).astype(jnp.bfloat16).reshape(-1, kv_width)
    )
    own_kv = jnp.stack([key_tokens, value_raw.astype(jnp.bfloat16)], 1)
    own_kv = own_kv.reshape(rows_here, 2, SEQS, 2, KVH, HD).transpose(0, 2, 4, 1, 3, 5)
    own_kv = own_kv.reshape(rows_here, SEQS * KVH * 4 * HD)
    all_kv, w_o_all = gather([own_kv, own_cut(w_o)], [by_tokens, by_rows], 2, "gather_keys")
    w_o_all = w_o_all.reshape(D, D)
    all_kv = all_kv.reshape(-1, SEQS * KVH * 4 * HD)
    queries = to_groups(query_tokens, rows_here)
    scalars = jnp.concatenate(
        [block_order.reshape(-1), jnp.stack([own_ctx, own_shard]).astype(jnp.int32)]
    )
    attended_grouped, stats = attend_forward(
        scalars, queries, all_kv, ctx_size, block_rows, rows_here
    )
    attended_low = from_groups(attended_grouped, rows_here).astype(jnp.bfloat16)
    middle = inputs + jnp.dot(attended_low, w_o_all, preferred_element_type=jnp.float32)
    unit_two, scale_two, normed = normalize(middle, gain_two)
    normed_two = mix_features(normed.astype(jnp.bfloat16))

    (tokens_all,) = gather(
        [normed_two], [lambda ctx, shard: shard], 6, "gather_tokens", with_ctx=False
    )
    tokens_all = tokens_all.reshape(-1, D)
    gate_up_part = jnp.dot(tokens_all, gate_up_cols, preferred_element_type=jnp.float32)
    gate_part, up_part = gate_up_part[:, :width], gate_up_part[:, width:]
    sigmoid_gate = jax.nn.sigmoid(gate_part)
    activated = gate_part * sigmoid_gate
    hidden = (activated * up_part).astype(jnp.bfloat16)
    grad_hidden = lax.dot_general(
        cotangent_all, down_padded, CONTRACT_LAST, preferred_element_type=jnp.float32
    )
    grad_gate = grad_hidden * up_part * sigmoid_gate * (1.0 + gate_part * (1.0 - sigmoid_gate))
    grad_gate_up = jnp.concatenate([grad_gate, grad_hidden * activated], -1).astype(jnp.bfloat16)
    grad_tokens = lax.dot_general(
        grad_gate_up, gate_up_cols, CONTRACT_LAST, preferred_element_type=jnp.float32
    )
    grad_normed_two = lax.psum_scatter(
        grad_tokens.astype(jnp.bfloat16), "fsdp", scatter_dimension=0, tiled=True
    )
    down_terms = lax.dot_general(
        hidden, cotangent_all, CONTRACT_FIRST, preferred_element_type=jnp.float32
    ).astype(jnp.bfloat16)
    gate_up_terms = lax.dot_general(
        tokens_all, grad_gate_up, CONTRACT_FIRST, preferred_element_type=jnp.float32
    ).astype(jnp.bfloat16)
    mixed_terms = jnp.dot(hidden, down_padded, preferred_element_type=jnp.float32).astype(jnp.bfloat16)
    down_rows = lax.psum(down_terms, "ctx")
    gate_up_rows = lax.psum_scatter(gate_up_terms, "ctx", scatter_dimension=0, tiled=True)
    gate_up_rows = exchange(
        gate_up_rows.reshape(shard_count, cut, 2 * width), 5, "exchange_rows"
    )
    gate_up_rows = lax.all_gather(gate_up_rows, "ctx", axis=0, tiled=False)

    grad_normed_two, down_terms, gate_up_terms, mixed_terms = lax.optimization_barrier(
        (grad_normed_two, down_terms, gate_up_terms, mixed_terms)
    )
    grad_normed_two = unmix_features(grad_normed_two.astype(jnp.float32))
    grad_middle_norm, grad_gain_two = norm_back(grad_normed_two, unit_two, scale_two, gain_two)
    grad_middle = cotangent.reshape(-1, D).astype(jnp.float32) + grad_middle_norm
    grad_branch_one = grad_middle.astype(jnp.bfloat16)
    grad_attended = lax.dot_general(
        grad_branch_one, w_o_all, CONTRACT_LAST, preferred_element_type=jnp.float32
    ).astype(jnp.bfloat16)
    o_terms = lax.dot_general(
        attended_low, grad_branch_one, CONTRACT_FIRST, preferred_element_type=jnp.float32
    ).astype(jnp.bfloat16)
    grad_queries, grad_kv_full = attend_backward(
        scalars,
        queries,
        to_groups(grad_attended, rows_here),
        attended_grouped,
        stats,
        all_kv,
        ctx_size,
        block_rows,
        rows_here,
    )
    (grad_kv,) = scatter(
        [grad_kv_full.reshape(-1, rows_here, SEQS * KVH * 4 * HD)],
        by_tokens,
        3,
        "scatter_keys",
        out_dtype=jnp.float32,
    )
    grad_kv_low = narrowed(grad_kv).reshape(rows_here, SEQS, KVH, 2, 2, HD)
    grad_kv_low = grad_kv_low.transpose(0, 3, 1, 4, 2, 5).reshape(-1, 2 * kv_width)
    grad_query_tokens = from_groups(narrowed(grad_queries), rows_here) * query_scale
    grad_query_raw = rotate_back(
        grad_query_tokens.reshape(-1, H, HD), cosine_table, sine_table
    ).reshape(-1, H * HD)
    grad_key_raw = rotate_back(
        grad_kv_low[:, :kv_width].reshape(-1, KVH, HD), cosine_table, sine_table
    ).reshape(-1, kv_width)
    grad_projected = jnp.concatenate(
        [grad_query_raw, grad_key_raw, grad_kv_low[:, kv_width:]], -1
    ).astype(jnp.bfloat16)
    grad_bias = jnp.sum(grad_projected, 0, dtype=jnp.float32)
    grad_normed_one = lax.dot_general(
        grad_projected, w_qkv_all, CONTRACT_LAST, preferred_element_type=jnp.float32
    )
    grad_input_norm, grad_gain_one = norm_back(grad_normed_one, unit_one, scale_one, gain_one)
    grad_input = (grad_middle + grad_input_norm).reshape(rows_here, slots, D)
    qkv_terms = lax.dot_general(
        normed_one, grad_projected, CONTRACT_FIRST, preferred_element_type=jnp.float32
    ).astype(jnp.bfloat16)
    small_terms = jnp.concatenate(
        [
            part.reshape(shard_count, -1)
            for part in (grad_gain_one, grad_gain_two, grad_bias[:QK], grad_bias[QK:])
        ],
        1,
    )
    small_terms = small_terms.reshape(ctx_size * shard_count, small_width)
    small_terms = jnp.pad(small_terms, ((0, 0), (0, 8 * HD - small_width)))
    qkv_rows, o_rows, small_rows, mixed_rows = scatter(
        [
            qkv_terms.reshape(-1, cut, QKV),
            o_terms.reshape(-1, cut, D),
            small_terms.reshape(-1, 8, HD),
        ],
        by_rows,
        4,
        "scatter_weights",
        spread_ctx=True,
        lines=[mixed_terms.reshape(shard_count, -1, D)],
    )
    mixed_out = middle + mixed_rows
    output = mixed_out.astype(jnp.bfloat16).reshape(rows_here, slots, D)
    small_rows = small_rows.reshape(ctx_size, -1)[:, :small_width].reshape(-1)
    bias_start = 2 * gain_width
    value_start = bias_start + QK // shard_count

    gate_rows, up_rows = unpack(gate_up_rows, columns)
    return (
        output,
        grad_input,
        small_rows[:gain_width],
        qkv_rows.reshape(-1, QKV).astype(jnp.float32),
        small_rows[bias_start:value_start],
        small_rows[value_start:],
        o_rows.reshape(-1, D).astype(jnp.float32),
        small_rows[gain_width:bias_start],
        gate_rows.reshape(-1, FF),
        up_rows.reshape(-1, FF),
        down_rows[:columns].astype(jnp.float32),
    )


def solution(mesh):
    in_specs = (
        P(("ctx", "fsdp"), None, None),
        P(),
        P("fsdp"),
        P("fsdp", None),
        P("fsdp"),
        P("fsdp", None),
        P("fsdp"),
        P("fsdp", None),
        P("fsdp", None),
        P("fsdp", None),
        P(("ctx", "fsdp"), None, None),
    )
    out_specs = (
        P(("ctx", "fsdp"), None, None),
        P(("ctx", "fsdp"), None, None),
        P("fsdp"),
        P("fsdp", None),
        P("fsdp"),
        P("fsdp"),
        P("fsdp", None),
        P("fsdp"),
        P("fsdp", None),
        P("fsdp", None),
        P("fsdp", None),
    )
    return jax.shard_map(shards, mesh=mesh, in_specs=in_specs, out_specs=out_specs, check_vma=False)
```

```python
import functools

import jax
import jax.numpy as jnp
from jax import lax
from jax.experimental import pallas as pl
from jax.experimental.pallas import tpu as pltpu
from jax.sharding import PartitionSpec as P

D = 1536
H = 12
KVH = 2
HD = 128
FF = 8960
SEQS = 2
QKV = 2048
QK = 1792


EPS = 1e-06
THETA = 1000000.0
NEG_FILL = -1e30
MESH_ID = pl.DeviceIdType.MESH
CONTRACT_LAST = (((1,), (1,)), ((), ()))
CONTRACT_FIRST = (((0,), (0,)), ((), ()))


def narrowed(values):
    return lax.optimization_barrier(values.astype(jnp.bfloat16)).astype(jnp.float32)


def block_positions(block_order, first_row, row_count, block_rows, ctx_size):
    row_index = first_row + jnp.arange(row_count, dtype=jnp.int32)
    slot_index = jnp.arange(2 * SEQS, dtype=jnp.int32)
    entries = (slot_index // SEQS)[None, :] * ctx_size + (row_index // block_rows)[:, None]
    tiled = jnp.tile(block_order, (2, 1))
    entry_ids = jnp.arange(2 * ctx_size, dtype=jnp.int32)
    picked = jnp.sum(
        jnp.where(entries[:, :, None] == entry_ids[None, None, :], tiled[None, :, :], 0), -1
    )
    return picked * block_rows + (row_index % block_rows)[:, None]


def to_groups(tokens, row_count):
    shaped = tokens.reshape(row_count, 2, SEQS, KVH, H // KVH, HD)
    return shaped.transpose(2, 1, 3, 4, 0, 5).reshape(SEQS, 2, KVH, H // KVH * row_count, HD)


def from_groups(grouped, row_count):
    shaped = grouped.reshape(SEQS, 2, KVH, H // KVH, row_count, HD).transpose(4, 1, 0, 2, 3, 5)
    return shaped.reshape(row_count * 2 * SEQS, H * HD)


def rope_tables(positions):
    half_width = HD // 2
    frequency = THETA ** (-jnp.arange(half_width, dtype=jnp.float32) * 2.0 / HD)
    angles = positions.astype(jnp.float32)[:, None] * frequency[None, :]
    cosine_table = jnp.concatenate([jnp.cos(angles), jnp.cos(angles)], -1)[:, None, :]
    sine_table = jnp.concatenate([jnp.sin(angles), jnp.sin(angles)], -1)[:, None, :]
    return (cosine_table, sine_table)


def rotate(head_values, cosine_table, sine_table):
    half_width = HD // 2
    turned = jnp.concatenate([-head_values[..., half_width:], head_values[..., :half_width]], -1)
    return head_values * cosine_table + turned * sine_table


def rotate_back(grad_values, cosine_table, sine_table):
    half_width = HD // 2
    moved = grad_values * sine_table
    return grad_values * cosine_table + jnp.concatenate(
        [moved[..., half_width:], -moved[..., :half_width]], -1
    )


def normalize(values, gain):
    scale = lax.rsqrt(jnp.mean(values * values, -1, keepdims=True) + EPS)
    unit = values * scale
    return (unit, scale, unit * gain)


def norm_back(grad_out, unit, scale, gain):
    grad_unit = grad_out * gain
    inner = jnp.mean(grad_unit * unit, -1, keepdims=True)
    return (scale * (grad_unit - unit * inner), jnp.sum(grad_out * unit, 0))


def attend_forward_kernel(ctx_size, block_rows, rows_here, scalars, q_ref, kv_ref, out_ref, stat_ref, best_ref, total_ref, accum_ref):
    seq = pl.program_id(0)
    blocks = 2 * ctx_size
    own_ctx = scalars[SEQS * blocks]
    own_shard = scalars[SEQS * blocks + 1]
    lanes = q_ref.shape[3]
    best_ref[...] = jnp.full(best_ref.shape, NEG_FILL, jnp.float32)
    total_ref[...] = jnp.zeros(total_ref.shape, jnp.float32)
    accum_ref[...] = jnp.zeros(accum_ref.shape, jnp.float32)

    def step(key_ctx, half_key, half):
        order_key = scalars[seq * blocks + half_key * ctx_size + key_ctx]
        order_query = scalars[seq * blocks + half * ctx_size + own_ctx]

        def work(masked):
            rows = pl.ds(pl.multiple_of(key_ctx * block_rows, block_rows), block_rows)
            keys = kv_ref[rows, half_key * 2 * HD : half_key * 2 * HD + HD]
            values = kv_ref[rows, half_key * 2 * HD + HD : half_key * 2 * HD + 2 * HD]
            scores = lax.dot_general(
                keys, q_ref[0, half, 0], CONTRACT_LAST, preferred_element_type=jnp.float32
            )
            if masked:
                row = lax.broadcasted_iota(jnp.int32, (block_rows, lanes), 0)
                lane = lax.broadcasted_iota(jnp.int32, (block_rows, lanes), 1)
                scores = jnp.where(
                    row <= own_shard * rows_here + lax.rem(lane, rows_here), scores, NEG_FILL
                )
            best = best_ref[half]
            fresh = jnp.maximum(best, jnp.max(scores, 0, keepdims=True))
            decay = jnp.exp(best - fresh)
            weights = jnp.exp(scores - fresh)
            total_ref[half] = total_ref[half] * decay + jnp.sum(weights, 0, keepdims=True)
            accum_ref[half] = accum_ref[half] * decay + lax.dot_general(
                values,
                weights.astype(jnp.bfloat16),
                CONTRACT_FIRST,
                preferred_element_type=jnp.float32,
            )
            best_ref[half] = fresh

        @pl.when(order_key < order_query)
        def full():
            work(False)

        @pl.when(order_key == order_query)
        def diagonal():
            work(True)

    @pl.loop(0, ctx_size)
    def sweep(key_ctx):
        for half_key in range(2):
            for half in range(2):
                step(key_ctx, half_key, half)

    for half in range(2):
        totals = total_ref[half]
        out_ref[0, half, 0] = (accum_ref[half] / totals).T
        stat_ref[0, half, 0] = best_ref[half] + jnp.log(totals)


def attend_forward(scalars, queries, all_kv, ctx_size, block_rows, rows_here):
    lanes = queries.shape[3]
    kernel = functools.partial(attend_forward_kernel, ctx_size, block_rows, rows_here)
    group = pl.BlockSpec((1, 2, 1, lanes, HD), lambda s, n, _: (s, 0, n, 0, 0))
    stat = pl.BlockSpec((1, 2, 1, 1, lanes), lambda s, n, _: (s, 0, n, 0, 0))
    return pl.pallas_call(
        kernel,
        grid_spec=pltpu.PrefetchScalarGridSpec(
            num_scalar_prefetch=1,
            grid=(SEQS, KVH),
            in_specs=[
                group,
                pl.BlockSpec((all_kv.shape[0], 4 * HD), lambda s, n, _: (0, s * KVH + n)),
            ],
            out_specs=[group, stat],
            scratch_shapes=[
                pltpu.VMEM((2, 1, lanes), jnp.float32),
                pltpu.VMEM((2, 1, lanes), jnp.float32),
                pltpu.VMEM((2, HD, lanes), jnp.float32),
            ],
        ),
        out_shape=(
            jax.ShapeDtypeStruct(queries.shape, jnp.float32),
            jax.ShapeDtypeStruct((SEQS, 2, KVH, 1, lanes), jnp.float32),
        ),
        compiler_params=pltpu.CompilerParams(vmem_limit_bytes=56 * 2**20),
        name="attend_forward",
    )(scalars, queries, all_kv)


def attend_backward_kernel(ctx_size, block_rows, rows_here, scalars, q_ref, go_ref, att_ref, stat_ref, kv_ref, gq_ref, gkv_ref, delta_ref, gq_acc, gk_acc, gv_acc):
    seq = pl.program_id(0)
    blocks = 2 * ctx_size
    own_ctx = scalars[SEQS * blocks]
    own_shard = scalars[SEQS * blocks + 1]
    lanes = q_ref.shape[3]
    gq_acc[...] = jnp.zeros(gq_acc.shape, jnp.float32)
    for half in range(2):
        product = go_ref[0, half, 0].astype(jnp.float32) * att_ref[0, half, 0]
        delta_ref[half] = jnp.sum(product.T, 0, keepdims=True)

    def step(key_ctx, half_key, half):
        order_key = scalars[seq * blocks + half_key * ctx_size + key_ctx]
        order_query = scalars[seq * blocks + half * ctx_size + own_ctx]

        def work(masked):
            rows = pl.ds(pl.multiple_of(key_ctx * block_rows, block_rows), block_rows)
            keys = kv_ref[rows, half_key * 2 * HD : half_key * 2 * HD + HD]
            values = kv_ref[rows, half_key * 2 * HD + HD : half_key * 2 * HD + 2 * HD]
            queries = q_ref[0, half, 0]
            grad_out = go_ref[0, half, 0]
            scores = lax.dot_general(
                keys, queries, CONTRACT_LAST, preferred_element_type=jnp.float32
            )
            probs = jnp.exp(scores - stat_ref[0, half, 0])
            if masked:
                row = lax.broadcasted_iota(jnp.int32, (block_rows, lanes), 0)
                lane = lax.broadcasted_iota(jnp.int32, (block_rows, lanes), 1)
                probs = jnp.where(
                    row <= own_shard * rows_here + lax.rem(lane, rows_here), probs, 0.0
                )
            grad_probs = lax.dot_general(
                values, grad_out, CONTRACT_LAST, preferred_element_type=jnp.float32
            )
            grad_scores = (probs * (grad_probs - delta_ref[half])).astype(jnp.bfloat16)
            gv_acc[...] += jnp.dot(
                probs.astype(jnp.bfloat16), grad_out, preferred_element_type=jnp.float32
            )
            gk_acc[...] += jnp.dot(grad_scores, queries, preferred_element_type=jnp.float32)
            gq_acc[half] += lax.dot_general(
                keys, grad_scores, CONTRACT_FIRST, preferred_element_type=jnp.float32
            )

        @pl.when(order_key < order_query)
        def full():
            work(False)

        @pl.when(order_key == order_query)
        def diagonal():
            work(True)

    @pl.loop(0, ctx_size)
    def sweep(key_ctx):
        rows = pl.ds(pl.multiple_of(key_ctx * block_rows, block_rows), block_rows)
        for half_key in range(2):
            gk_acc[...] = jnp.zeros(gk_acc.shape, jnp.float32)
            gv_acc[...] = jnp.zeros(gv_acc.shape, jnp.float32)
            for half in range(2):
                step(key_ctx, half_key, half)
            at = half_key * 2 * HD
            gkv_ref[rows, at : at + HD] = gk_acc[...].astype(jnp.bfloat16)
            gkv_ref[rows, at + HD : at + 2 * HD] = gv_acc[...].astype(jnp.bfloat16)

    for half in range(2):
        gq_ref[0, half, 0] = gq_acc[half].T


def attend_backward(scalars, queries, grad_out, attended, stats, all_kv, ctx_size, block_rows, rows_here):
    lanes = queries.shape[3]
    kernel = functools.partial(attend_backward_kernel, ctx_size, block_rows, rows_here)
    group = pl.BlockSpec((1, 2, 1, lanes, HD), lambda s, n, _: (s, 0, n, 0, 0))
    stat = pl.BlockSpec((1, 2, 1, 1, lanes), lambda s, n, _: (s, 0, n, 0, 0))
    full = pl.BlockSpec((all_kv.shape[0], 4 * HD), lambda s, n, _: (0, s * KVH + n))
    return pl.pallas_call(
        kernel,
        grid_spec=pltpu.PrefetchScalarGridSpec(
            num_scalar_prefetch=1,
            grid=(SEQS, KVH),
            in_specs=[group, group, group, stat, full],
            out_specs=[group, full],
            scratch_shapes=[
                pltpu.VMEM((2, 1, lanes), jnp.float32),
                pltpu.VMEM((2, HD, lanes), jnp.float32),
                pltpu.VMEM((block_rows, HD), jnp.float32),
                pltpu.VMEM((block_rows, HD), jnp.float32),
            ],
        ),
        out_shape=(
            jax.ShapeDtypeStruct(queries.shape, jnp.float32),
            jax.ShapeDtypeStruct(all_kv.shape, jnp.bfloat16),
        ),
        compiler_params=pltpu.CompilerParams(vmem_limit_bytes=56 * 2**20),
        name="attend_backward",
    )(scalars, queries, grad_out, attended, stats, all_kv)


def peers_of(ctx_size):
    return ctx_size == 4, range(1, ctx_size)


def ctx_target(position, way, square, ctx_size):
    return position ^ way if square else lax.rem(position + way, ctx_size)


def ctx_source(position, way, square, ctx_size):
    return position ^ way if square else lax.rem(position + ctx_size - way, ctx_size)


def greet(ctx_size, pair_count, with_ctx, all_shards):
    ctx = lax.axis_index("ctx")
    shard = lax.axis_index("fsdp")
    pair, core = shard // 2, shard % 2
    barrier = pltpu.get_barrier_semaphore()
    partners = [(ctx, pair * 2 + 1 - core)]
    for step in range(1, pair_count):
        there = lax.rem(pair + step, pair_count) * 2
        partners.append((ctx, there + core))
        if all_shards:
            partners.append((ctx, there + 1 - core))
    if with_ctx:
        for way in range(1, ctx_size):
            partners.append((lax.rem(ctx + way, ctx_size), shard))
    for partner in partners:
        pl.semaphore_signal(barrier, inc=1, device_id=partner, device_id_type=MESH_ID)
    pl.semaphore_wait(barrier, len(partners))
    return ctx, pair, core


class Exchange:
    def __init__(self, source, out, sems, own_sem, pair_count):
        self.source, self.out, self.sems, self.own_sem = source, out, sems, own_sem
        self.shard_count = 2 * pair_count

    def start(self):
        ctx, shard = lax.axis_index("ctx"), lax.axis_index("fsdp")
        self.own = pltpu.make_async_copy(self.source.at[shard], self.out.at[shard], self.own_sem)
        self.own.start()
        self.copies = []
        for step in range(1, self.shard_count):
            there = lax.rem(shard + step, self.shard_count)
            copy = pltpu.make_async_remote_copy(
                src_ref=self.source.at[there],
                dst_ref=self.out.at[shard],
                send_sem=self.sems[0].at[step - 1],
                recv_sem=self.sems[1].at[step - 1],
                device_id=(ctx, there),
                device_id_type=MESH_ID,
            )
            copy.start()
            self.copies.append(copy)

    def finish(self):
        ctx, shard = lax.axis_index("ctx"), lax.axis_index("fsdp")
        for step in range(1, self.shard_count):
            come = lax.rem(shard + self.shard_count - step, self.shard_count)
            pltpu.make_async_remote_copy(
                src_ref=self.out.at[come],
                dst_ref=self.out.at[come],
                send_sem=self.sems[0].at[step - 1],
                recv_sem=self.sems[1].at[step - 1],
                device_id=(ctx, shard),
                device_id_type=MESH_ID,
            ).wait_recv()
        self.own.wait()
        for copy in self.copies:
            copy.wait_send()


def exchange_kernel(pair_count, source, out, send_sem, recv_sem, own_sem):
    greet(1, pair_count, False, True)
    flow = Exchange(source, out, (send_sem, recv_sem), own_sem, pair_count)
    flow.start()
    flow.finish()


def exchange(pieces, collective_id):
    shard_count = lax.axis_size("fsdp")
    dma = pltpu.SemaphoreType.DMA
    return pl.pallas_call(
        functools.partial(exchange_kernel, shard_count // 2),
        in_specs=[pl.BlockSpec(memory_space=pltpu.VMEM)],
        out_specs=pl.BlockSpec(memory_space=pl.ANY),
        out_shape=jax.ShapeDtypeStruct(pieces.shape, pieces.dtype),
        scratch_shapes=[dma((shard_count - 1,))] * 2 + [dma],
        compiler_params=pltpu.CompilerParams(collective_id=collective_id, has_side_effects=True),
        cost_estimate=pl.CostEstimate(
            flops=0, bytes_accessed=pieces.size * 64, transcendentals=0
        ),
    )(pieces)


def gather_kernel(arity, ctx_size, pair_count, slots, swaps, with_ctx, *refs):
    sources, refs = refs[:arity], refs[arity:]
    swap_sources, refs = refs[:swaps], refs[swaps:]
    outs, refs = refs[:arity], refs[arity:]
    swap_outs, refs = refs[:swaps], refs[swaps:]
    pair_sems, ctx_sems, core_sems = refs[0:2], refs[2:4], refs[4:6]
    local_sem = refs[6]
    square, ways = peers_of(ctx_size) if with_ctx else (False, ())
    near = [way for way in ways if not (square and way == 3)]
    ctx, pair, core = greet(ctx_size, pair_count, with_ctx, swaps > 0)
    homes = [place(ctx, pair * 2 + core) for place in slots]
    started = []
    steps = [(0, 1)] + [(far, way) for far in range(1, pair_count) for way in (1, -1)]

    def present(step):
        far, way = steps[step]
        if far == 0:
            return None
        return pair >= far if way == 1 else pair + far < pair_count

    def origin(step):
        far, way = steps[step]
        return pair - far * way

    def when(condition, work):
        if condition is None:
            work()
        else:
            pl.when(condition)(work)

    def send(item, source, place, target, sems, at, condition):
        copy = pltpu.make_async_remote_copy(
            src_ref=source,
            dst_ref=outs[item].at[place],
            send_sem=sems[0].at[at],
            recv_sem=sems[1].at[at],
            device_id=target,
            device_id_type=MESH_ID,
        )
        copy.start()
        started.append((condition, item, sems, at))

    def sent(item, sems, at):
        pltpu.make_async_remote_copy(
            src_ref=outs[item].at[0],
            dst_ref=outs[item].at[0],
            send_sem=sems[0].at[at],
            recv_sem=sems[1].at[at],
            device_id=(ctx, pair * 2 + core),
            device_id_type=MESH_ID,
        ).wait_send()

    def arrive(item, place, sems, at):
        pltpu.make_async_remote_copy(
            src_ref=outs[item].at[place],
            dst_ref=outs[item].at[place],
            send_sem=sems[0].at[at],
            recv_sem=sems[1].at[at],
            device_id=(ctx, pair * 2 + core),
            device_id_type=MESH_ID,
        ).wait_recv()

    def pass_on(step, item, source, place):
        far, way = steps[step]
        for side in (1, -1) if far == 0 else (way,):

            def further(side=side):
                return pair + 1 < pair_count if side == 1 else pair >= 1

            def both(further=further):
                return further() if far == 0 else jnp.logical_and(further(), present(step))

            def work(side=side, both=both):
                send(
                    item,
                    source,
                    place,
                    (ctx, (pair + side) * 2 + core),
                    pair_sems,
                    ((side + 1) // 2, far, item),
                    both,
                )

            if far + 1 < pair_count:
                pl.when(further())(work)

    def to_core(item, source, from_ctx, way, step):
        send(
            item,
            source,
            slots[item](from_ctx, origin(step) * 2 + core),
            (ctx, pair * 2 + 1 - core),
            core_sems,
            (way, step, item),
            functools.partial(present, step),
        )

    def spread(step):
        for item in range(arity):
            place = slots[item](ctx, origin(step) * 2 + core)
            source = sources[item]
            if step:
                far, way = steps[step]
                arrive(item, place, pair_sems, ((way + 1) // 2, far - 1, item))
                source = outs[item].at[place]
            pass_on(step, item, source, place)
            for way in near:
                there = ctx_target(ctx, way, square, ctx_size)
                send(
                    item,
                    source,
                    place,
                    (there, pair * 2 + core),
                    ctx_sems,
                    (way - 1, step, item),
                    functools.partial(present, step),
                )
            to_core(item, source, ctx, 0, step)

    def collect(step):
        for way in near:
            for item in range(arity):
                come = ctx_source(ctx, way, square, ctx_size)
                place = slots[item](come, origin(step) * 2 + core)
                arrive(item, place, ctx_sems, (way - 1, step, item))
                source = outs[item].at[place]
                if square and (steps[step][0] % 2 == 0) == (way == 1):
                    send(
                        item,
                        source,
                        place,
                        (ctx ^ (3 - way), pair * 2 + core),
                        ctx_sems,
                        (2, step, item),
                        functools.partial(present, step),
                    )
                to_core(item, source, come, way, step)

    def collect_far(step):
        for item in range(arity):
            place = slots[item](ctx ^ 3, origin(step) * 2 + core)
            arrive(item, place, ctx_sems, (2, step, item))
            to_core(item, outs[item].at[place], ctx ^ 3, 3, step)

    locals_ = []
    for item in range(arity):
        copy = pltpu.make_async_copy(sources[item], outs[item].at[homes[item]], local_sem.at[item])
        copy.start()
        locals_.append(copy)
    when(None, lambda: spread(0))
    flows = []
    count = len(steps)
    for turn in range(1, count + 4):
        if turn < count:
            when(present(turn), functools.partial(spread, turn))
        if turn == count:
            for item in range(swaps):
                flow = Exchange(
                    swap_sources[item],
                    swap_outs[item],
                    refs[7 + 3 * item : 9 + 3 * item],
                    refs[9 + 3 * item],
                    pair_count,
                )
                flow.start()
                flows.append(flow)
        if 0 <= turn - 2 < count:
            when(present(turn - 2), functools.partial(collect, turn - 2))
        if square and 0 <= turn - 4 < count:
            when(present(turn - 4), functools.partial(collect_far, turn - 4))

    def from_core(step):
        for way in (0, *ways):
            come = ctx_source(ctx, way, square, ctx_size) if way else ctx
            for item in range(arity):
                arrive(item, slots[item](come, origin(step) * 2 + 1 - core), core_sems, (way, step, item))

    for step in range(count):
        when(present(step), functools.partial(from_core, step))
    for flow in flows:
        flow.finish()
    for copy in locals_:
        copy.wait()
    for condition, *which in started:
        when(condition(), functools.partial(sent, *which))


def gather(pieces, slots, collective_id, swaps=(), with_ctx=True):
    ctx_size, shard_count = lax.axis_size("ctx"), lax.axis_size("fsdp")
    pair_count = shard_count // 2
    arity = len(pieces)
    dma = pltpu.SemaphoreType.DMA
    moved = sum(piece.size for piece in pieces) * 2
    steps = 2 * pair_count - 1
    return pl.pallas_call(
        functools.partial(gather_kernel, arity, ctx_size, pair_count, slots, len(swaps), with_ctx),
        in_specs=[pl.BlockSpec(memory_space=pltpu.VMEM)] * (arity + len(swaps)),
        out_specs=[pl.BlockSpec(memory_space=pl.ANY)] * (arity + len(swaps)),
        out_shape=[
            jax.ShapeDtypeStruct(
                ((ctx_size if with_ctx else 1) * shard_count,) + piece.shape, piece.dtype
            )
            for piece in pieces
        ]
        + [jax.ShapeDtypeStruct(swap.shape, swap.dtype) for swap in swaps],
        scratch_shapes=[dma((2, pair_count - 1, arity))] * 2
        + [dma((ctx_size - 1, steps, arity))] * 2
        + [dma((ctx_size, steps, arity))] * 2
        + [dma((arity,))]
        + [dma((shard_count - 1,)), dma((shard_count - 1,)), dma] * len(swaps),
        compiler_params=pltpu.CompilerParams(collective_id=collective_id, has_side_effects=True),
        cost_estimate=pl.CostEstimate(
            flops=0, bytes_accessed=moved * ctx_size * shard_count * 4, transcendentals=0
        ),
    )(*pieces, *swaps)


class LineScatter:
    def __init__(self, source, out, half, above, below, sems, where, counts, last):
        pair_count, self.ctx_size = counts
        self.source, self.out, self.half, self.rooms = source, out, half, {1: above, -1: below}
        self.last = last
        self.core_sems, self.line_sems = sems[0:2], {1: sems[2:4], -1: sems[4:6]}
        self.ctx, self.pair, self.core = where
        self.count = pair_count
        self.order = []
        for turn in range(pair_count - 1):
            self.order += [(pair_count - 1 - turn, 1), (turn, -1)]

    def copy(self, source, target, device, sems, at):
        return pltpu.make_async_remote_copy(
            src_ref=source,
            dst_ref=target,
            send_sem=sems[0].at[at],
            recv_sem=sems[1].at[at],
            device_id=device,
            device_id_type=MESH_ID,
        )

    def here(self):
        return (self.ctx, self.pair * 2 + self.core)

    def core_copy(self, pair):
        return self.copy(
            self.source.at[pair * 2 + 1 - self.core],
            self.half.at[pair],
            (self.ctx, self.pair * 2 + 1 - self.core),
            self.core_sems,
            pair,
        )

    def line_copy(self, pair, way):
        return self.copy(
            self.half.at[pair],
            self.rooms[way].at[pair],
            (self.ctx, (self.pair + way) * 2 + self.core),
            self.line_sems[way],
            pair,
        )

    def line_room(self, pair, way):
        room = self.rooms[way].at[pair]
        return self.copy(room, room, self.here(), self.line_sems[way], pair)

    def add(self, pair, value):
        half = self.half.at[pair]
        half[...] = (half[...].astype(jnp.float32) + value.astype(jnp.float32)).astype(half.dtype)

    def beyond(self, pair, way):
        return pair > self.pair if way == 1 else pair < self.pair

    def behind(self, way):
        return self.pair > 0 if way == 1 else self.pair < self.count - 1

    def start(self):
        done = []
        for pair, _ in self.order:
            if pair not in done:
                done.append(pair)
                self.core_copy(pair).start()
        self.folds = done

    def fold(self):
        for pair in self.folds:
            self.copy(
                self.half.at[pair], self.half.at[pair], self.here(), self.core_sems, pair
            ).wait_recv()
            self.add(pair, self.source[pair * 2 + self.core])

    def advance(self, turn):
        pair, way = self.order[turn]

        @pl.when(self.beyond(pair, way))
        def pass_on():
            @pl.when(self.behind(way))
            def join():
                self.line_room(pair, way).wait_recv()
                self.add(pair, self.rooms[way][pair])

            self.line_copy(pair, way).start()

    def over_ctx(self, terms, room, landing, *sems):
        shard = self.pair * 2 + self.core
        copies = []

        def send(source, target, way, sems):
            there = lax.rem(self.ctx + way, self.ctx_size)
            copies.append(self.copy(source(there), target, (there, shard), sems, way - 1))
            copies[-1].start()

        def arrive(target, way, sems):
            self.copy(target, target, self.here(), sems, way - 1).wait_recv()

        terms[...] = self.out[...].astype(terms.dtype)
        for way in range(1, self.ctx_size):
            send(lambda there: terms.at[there], room.at[way - 1], way, sems[0:2])
        total = self.out[self.ctx]
        for way in range(1, self.ctx_size):
            arrive(room.at[way - 1], way, sems[0:2])
            total = total + room[way - 1].astype(jnp.float32)
        landing[self.ctx] = total.astype(landing.dtype)
        for way in range(1, self.ctx_size):
            send(lambda there: landing.at[self.ctx], landing.at[self.ctx], way, sems[2:4])
        for way in range(1, self.ctx_size):
            come = lax.rem(self.ctx + self.ctx_size - way, self.ctx_size)
            arrive(landing.at[come], way, sems[2:4])
        self.out[...] = landing[...].astype(jnp.float32)
        for copy in copies:
            copy.wait_send()

    def finish(self):
        for pair in range(self.count):

            @pl.when(self.pair == pair)
            def close(pair=pair):
                self.out[...] = self.half[pair].astype(jnp.float32)
                for way in (1, -1):

                    @pl.when(self.behind(way))
                    def join(way=way):
                        self.line_room(pair, way).wait_recv()
                        self.out[...] += self.rooms[way][pair].astype(jnp.float32)

        if self.last:
            self.over_ctx(*self.last)
        for pair in range(self.count):
            self.core_copy(pair).wait_send()
        for pair, way in self.order:

            @pl.when(self.beyond(pair, way))
            def sent(pair=pair, way=way):
                self.line_copy(pair, way).wait_send()


def scatter_kernel(arity, ctx_size, pair_count, slot, spread_ctx, lines, *refs):
    sources, refs = refs[:arity], refs[arity:]
    line_sources, refs = refs[:lines], refs[lines:]
    outs, refs = refs[:arity], refs[arity:]
    line_outs, refs = refs[:lines], refs[lines:]
    halves, relays, asides, ends, finals = (refs[i * arity : (i + 1) * arity] for i in range(5))
    sems = refs[5 * arity : 5 * arity + 10]
    core_sems, relay_sems, ctx_sems, pair_sems, last_sems = (sems[2 * i : 2 * i + 2] for i in range(5))
    square, ways = peers_of(ctx_size)
    ctx, pair, core = greet(ctx_size, pair_count, True, False)
    order = list(range(1, pair_count)) + [0]
    started = []
    flows = []
    for item in range(lines):
        at = 5 * arity + 10 + 16 * item
        spread = len(line_sources[item].shape) == 4
        flows.append(
            LineScatter(
                line_sources[item],
                line_outs[item],
                *refs[at : at + 3],
                refs[at + 3 : at + 9],
                (ctx, pair, core),
                (pair_count, ctx_size),
                refs[at + 9 : at + 16] if spread else (),
            )
        )

    def send(source, target, device, pair_of_sems, at):
        copy = pltpu.make_async_remote_copy(
            src_ref=source,
            dst_ref=target,
            send_sem=pair_of_sems[0].at[at],
            recv_sem=pair_of_sems[1].at[at],
            device_id=device,
            device_id_type=MESH_ID,
        )
        copy.start()
        started.append(copy)

    def arrive(target, pair_of_sems, at):
        pltpu.make_async_remote_copy(
            src_ref=target,
            dst_ref=target,
            send_sem=pair_of_sems[0].at[at],
            recv_sem=pair_of_sems[1].at[at],
            device_id=(ctx, pair * 2 + core),
            device_id_type=MESH_ID,
        ).wait_recv()

    def toward(step):
        return lax.rem(pair + step, pair_count)

    def target_ctx(way):
        return ctx_target(ctx, way, square, ctx_size) if way else ctx

    def f32(value):
        return value.astype(jnp.float32)

    far_first = [3, 1, 2, 0] if square else list(ways) + [0]
    for step in order:
        for way in far_first:
            for item in range(arity):
                send(
                    sources[item].at[slot(target_ctx(way), toward(step) * 2 + 1 - core)],
                    halves[item].at[way, step],
                    (ctx, pair * 2 + 1 - core),
                    core_sems,
                    (way, step, item),
                )

    def fold_core(step):
        for way in far_first:
            for item in range(arity):
                half = halves[item].at[way, step]
                arrive(half, core_sems, (way, step, item))
                mine = sources[item][slot(target_ctx(way), toward(step) * 2 + core)]
                half[...] = (f32(mine) + f32(half[...])).astype(half.dtype)
                if square and way == 3:
                    there = ctx ^ (1 if step % 2 == 0 else 2)
                    send(
                        half,
                        relays[item].at[step],
                        (there, pair * 2 + core),
                        relay_sems,
                        (step, item),
                    )

    def fold_relay(step):
        for item in range(arity):
            if square:
                relay = relays[item].at[step]
                arrive(relay, relay_sems, (step, item))
                half = halves[item].at[2 if step % 2 == 0 else 1, step]
                half[...] = (f32(half[...]) + f32(relay[...])).astype(half.dtype)
            for way in ways:
                if square and way == 3:
                    continue
                send(
                    halves[item].at[way, step],
                    asides[item].at[way - 1, step],
                    (target_ctx(way), pair * 2 + core),
                    ctx_sems,
                    (way - 1, step, item),
                )

    def fold_ctx(step):
        for item in range(arity):
            half = halves[item].at[0, step]
            total = f32(half[...])
            for way in ways:
                if square and way == 3:
                    continue
                aside = asides[item].at[way - 1, step]
                arrive(aside, ctx_sems, (way - 1, step, item))
                total = total + f32(aside[...])
            if step:
                half[...] = total.astype(half.dtype)
                send(
                    half,
                    ends[item].at[step - 1],
                    (ctx, toward(step) * 2 + core),
                    pair_sems,
                    (step - 1, item),
                )
            else:
                for other in range(1, pair_count):
                    end = ends[item].at[other - 1]
                    arrive(end, pair_sems, (other - 1, item))
                    total = total + f32(end[...])
                if spread_ctx:
                    finals[item][...] = total.astype(finals[item].dtype)
                else:
                    outs[item][...] = total.astype(outs[item].dtype)

    for flow in flows:
        flow.start()
    turns = 2 * (pair_count - 1)
    for turn in range(pair_count + 2):
        if turn < pair_count:
            fold_core(order[turn])
        if 1 <= turn <= pair_count:
            fold_relay(order[turn - 1])
        for flow in flows:
            if turn == pair_count - 1:
                flow.fold()
                for part in range(2):
                    flow.advance(part)
        if turn >= 2:
            fold_ctx(order[turn - 2])
    for flow in flows:
        for part in range(2, turns):
            flow.advance(part)
    if spread_ctx:
        for item in range(arity):
            for way in ways:
                send(
                    finals[item],
                    outs[item].at[ctx],
                    (target_ctx(way), pair * 2 + core),
                    last_sems,
                    (way - 1, item),
                )
            outs[item][ctx] = finals[item][...]
        for item in range(arity):
            for way in ways:
                arrive(outs[item].at[ctx_source(ctx, way, square, ctx_size)], last_sems, (way - 1, item))
    for flow in flows:
        flow.finish()
    for copy in started:
        copy.wait_send()


def scatter(terms, slot, collective_id, spread_ctx=False, out_dtype=None, lines=()):
    ctx_size, shard_count = lax.axis_size("ctx"), lax.axis_size("fsdp")
    pair_count = shard_count // 2
    arity = len(terms)
    dma = pltpu.SemaphoreType.DMA
    lead = (ctx_size,) if spread_ctx else ()
    asides = 2 if ctx_size == 4 else ctx_size - 1

    def room(*extent):
        return [pltpu.VMEM(extent + term.shape[1:], term.dtype) for term in terms]

    def line_room(line):
        if len(line.shape) == 3:
            return [pltpu.VMEM((8, HD), line.dtype)] * 3 + [dma((1,))] * 4
        cut = line.shape[2:]
        rooms = [pltpu.VMEM((count,) + cut, line.dtype) for count in (ctx_size, ctx_size - 1, ctx_size)]
        return rooms + [dma((ctx_size - 1,))] * 4

    moved = sum(term.size * term.dtype.itemsize for term in terms)
    return pl.pallas_call(
        functools.partial(scatter_kernel, arity, ctx_size, pair_count, slot, spread_ctx, len(lines)),
        in_specs=[pl.BlockSpec(memory_space=pltpu.VMEM)] * (arity + len(lines)),
        out_specs=[pl.BlockSpec(memory_space=pltpu.VMEM)] * (arity + len(lines)),
        out_shape=[
            jax.ShapeDtypeStruct(lead + term.shape[1:], out_dtype or term.dtype) for term in terms
        ]
        + [jax.ShapeDtypeStruct(line.shape[1:], jnp.float32) for line in lines],
        scratch_shapes=room(ctx_size, pair_count)
        + room(pair_count)
        + room(asides, pair_count)
        + room(pair_count - 1)
        + room()
        + [dma((ctx_size, pair_count, arity))] * 2
        + [dma((pair_count, arity))] * 2
        + [dma((ctx_size - 1, pair_count, arity))] * 2
        + [dma((pair_count - 1, arity))] * 2
        + [dma((ctx_size - 1, arity))] * 2
        + [
            scratch
            for line in lines
            for scratch in [pltpu.VMEM((pair_count,) + line.shape[1:], line.dtype)] * 3
            + [dma((pair_count,))] * 6
            + line_room(line)
        ],
        compiler_params=pltpu.CompilerParams(
            collective_id=collective_id, has_side_effects=True, vmem_limit_bytes=63 * 2**20
        ),
        cost_estimate=pl.CostEstimate(flops=0, bytes_accessed=moved * 16, transcendentals=0),
    )(*terms, *lines)


def pack_kernel(columns, gate_ref, up_ref, out_ref):
    width = out_ref.shape[2] // 2
    cut = out_ref.shape[1]
    for there in range(out_ref.shape[0]):
        for side, ref in enumerate((gate_ref, up_ref)):
            at = side * width
            out_ref[there, :, at + width - HD : at + width] = jnp.zeros((cut, HD), out_ref.dtype)
            out_ref[there, :, at : at + columns] = ref[:, there * columns : (there + 1) * columns]


def pack(gate, up, shard_count, columns, width):
    return pl.pallas_call(
        functools.partial(pack_kernel, columns),
        in_specs=[pl.BlockSpec(memory_space=pltpu.VMEM)] * 2,
        out_specs=pl.BlockSpec(memory_space=pltpu.VMEM),
        out_shape=jax.ShapeDtypeStruct((shard_count, gate.shape[0], 2 * width), gate.dtype),
        name="pack",
    )(gate, up)


def unpack_kernel(columns, in_ref, gate_ref, up_ref):
    width = in_ref.shape[3] // 2
    for there in range(in_ref.shape[1]):
        for side, ref in enumerate((gate_ref, up_ref)):
            part = in_ref[0, there, :, side * width : side * width + columns]
            ref[0, :, there * columns : (there + 1) * columns] = part.astype(jnp.float32)


def unpack(rows, columns):
    ctx_size, shard_count, cut, _ = rows.shape
    out = jax.ShapeDtypeStruct((ctx_size, cut, shard_count * columns), jnp.float32)
    return pl.pallas_call(
        functools.partial(unpack_kernel, columns),
        grid=(ctx_size,),
        in_specs=[pl.BlockSpec((1,) + rows.shape[1:], lambda c: (c, 0, 0, 0))],
        out_specs=[pl.BlockSpec((1, cut, shard_count * columns), lambda c: (c, 0, 0))] * 2,
        out_shape=[out, out],
        name="unpack",
    )(rows)


def shards(
    layer_input,
    block_order,
    first_gain,
    w_qkv,
    b_qkv,
    w_o,
    second_gain,
    w_gate,
    w_up,
    w_down,
    cotangent,
):
    ctx_size = lax.axis_size("ctx")
    shard_count = lax.axis_size("fsdp")
    own_ctx = lax.axis_index("ctx")
    own_shard = lax.axis_index("fsdp")
    rows_here = layer_input.shape[0]
    slots = layer_input.shape[1]
    block_rows = rows_here * shard_count
    kv_width = KVH * HD
    cut = D // (ctx_size * shard_count)
    columns = FF // shard_count
    first_row = (own_ctx * shard_count + own_shard) * rows_here
    own_pos = block_positions(block_order, first_row, rows_here, block_rows, ctx_size)
    cosine_table, sine_table = rope_tables(own_pos.reshape(-1))
    query_scale = HD ** (-0.5)

    def by_rows(ctx, shard):
        return shard * ctx_size + ctx

    def by_tokens(ctx, shard):
        return ctx * shard_count + shard

    def own_cut(weight):
        return lax.dynamic_slice_in_dim(weight, own_ctx * cut, cut, 0)

    def mix_features(values):
        shaped = values.reshape(-1, shard_count, ctx_size, cut)
        return shaped.transpose(0, 2, 1, 3).reshape(-1, D)

    def unmix_features(values):
        shaped = values.reshape(-1, ctx_size, shard_count, cut)
        return shaped.transpose(0, 2, 1, 3).reshape(-1, D)

    small = jnp.concatenate([b_qkv, first_gain, second_gain]).reshape(ctx_size, -1)
    small_width = small.shape[1]
    small = lax.dynamic_slice_in_dim(small, own_ctx, 1, 0)
    small = jnp.pad(small, ((0, 0), (0, 16 * HD - small_width))).reshape(16, HD)
    width = -(-columns // HD) * HD
    w_qkv_all, w_o_all, small_all, gate_up_cut = gather(
        [own_cut(w_qkv), own_cut(w_o), small],
        [by_rows, by_rows, by_rows],
        1,
        swaps=[pack(own_cut(w_gate), own_cut(w_up), shard_count, columns, width)],
    )
    w_qkv_all = w_qkv_all.reshape(D, QKV)
    w_o_all = w_o_all.reshape(D, D)
    small_all = small_all.reshape(shard_count, ctx_size, -1)[:, :, :small_width]
    small_all = small_all.reshape(shard_count, -1).astype(jnp.float32)
    bias_width = QKV // shard_count
    gain_width = D // shard_count
    bias_all = small_all[:, :bias_width].reshape(-1)
    gain_one = small_all[:, bias_width : bias_width + gain_width].reshape(-1)
    gain_two = small_all[:, bias_width + gain_width :].reshape(-1)

    gate_up_cols = lax.all_gather(
        gate_up_cut.reshape(shard_count * cut, 2 * width), "ctx", axis=0, tiled=True
    )
    down_padded = jnp.pad(w_down, ((0, width - columns), (0, 0)))
    cotangent_all = lax.all_gather(cotangent.reshape(-1, D), "fsdp", axis=0, tiled=True)

    inputs = layer_input.reshape(-1, D).astype(jnp.float32)
    unit_one, scale_one, normed = normalize(inputs, gain_one)
    normed_one = normed.astype(jnp.bfloat16)
    projected = jnp.dot(normed_one, w_qkv_all, preferred_element_type=jnp.float32) + bias_all
    query_raw = projected[:, : H * HD].reshape(-1, H, HD)
    key_raw = projected[:, H * HD : H * HD + kv_width].reshape(-1, KVH, HD)
    value_raw = projected[:, H * HD + kv_width :]
    query_tokens = (
        (rotate(query_raw, cosine_table, sine_table) * query_scale)
        .astype(jnp.bfloat16)
        .reshape(-1, H * HD)
    )
    key_tokens = (
        rotate(key_raw, cosine_table, sine_table).astype(jnp.bfloat16).reshape(-1, kv_width)
    )
    own_kv = jnp.stack([key_tokens, value_raw.astype(jnp.bfloat16)], 1)
    own_kv = own_kv.reshape(rows_here, 2, SEQS, 2, KVH, HD).transpose(0, 2, 4, 1, 3, 5)
    own_kv = own_kv.reshape(rows_here, SEQS * KVH * 4 * HD)
    (all_kv,) = gather([own_kv], [by_tokens], 2)
    all_kv = all_kv.reshape(-1, SEQS * KVH * 4 * HD)
    queries = to_groups(query_tokens, rows_here)
    scalars = jnp.concatenate(
        [block_order.reshape(-1), jnp.stack([own_ctx, own_shard]).astype(jnp.int32)]
    )
    attended_grouped, stats = attend_forward(
        scalars, queries, all_kv, ctx_size, block_rows, rows_here
    )
    attended_low = from_groups(attended_grouped, rows_here).astype(jnp.bfloat16)
    middle = inputs + jnp.dot(attended_low, w_o_all, preferred_element_type=jnp.float32)
    unit_two, scale_two, normed = normalize(middle, gain_two)
    normed_two = mix_features(normed.astype(jnp.bfloat16))

    (tokens_all,) = gather([normed_two], [lambda ctx, shard: shard], 6, with_ctx=False)
    tokens_all = tokens_all.reshape(-1, D)
    gate_up_part = jnp.dot(tokens_all, gate_up_cols, preferred_element_type=jnp.float32)
    gate_part, up_part = gate_up_part[:, :width], gate_up_part[:, width:]
    sigmoid_gate = jax.nn.sigmoid(gate_part)
    activated = gate_part * sigmoid_gate
    hidden = (activated * up_part).astype(jnp.bfloat16)
    grad_hidden = lax.dot_general(
        cotangent_all, down_padded, CONTRACT_LAST, preferred_element_type=jnp.float32
    )
    grad_gate = grad_hidden * up_part * sigmoid_gate * (1.0 + gate_part * (1.0 - sigmoid_gate))
    grad_gate_up = jnp.concatenate([grad_gate, grad_hidden * activated], -1).astype(jnp.bfloat16)
    grad_tokens = lax.dot_general(
        grad_gate_up, gate_up_cols, CONTRACT_LAST, preferred_element_type=jnp.float32
    )
    grad_normed_two = lax.psum_scatter(
        grad_tokens.astype(jnp.bfloat16), "fsdp", scatter_dimension=0, tiled=True
    )
    down_terms = lax.dot_general(
        hidden, cotangent_all, CONTRACT_FIRST, preferred_element_type=jnp.float32
    ).astype(jnp.bfloat16)
    gate_up_terms = lax.dot_general(
        tokens_all, grad_gate_up, CONTRACT_FIRST, preferred_element_type=jnp.float32
    ).astype(jnp.bfloat16)
    mixed_terms = jnp.dot(hidden, down_padded, preferred_element_type=jnp.float32).astype(jnp.bfloat16)
    down_rows = lax.psum(down_terms, "ctx")
    gate_up_rows = lax.psum_scatter(gate_up_terms, "ctx", scatter_dimension=0, tiled=True)
    grad_normed_two, down_terms, gate_up_terms, mixed_terms = lax.optimization_barrier(
        (grad_normed_two, down_terms, gate_up_terms, mixed_terms)
    )
    grad_normed_two = unmix_features(grad_normed_two.astype(jnp.float32))
    grad_middle_norm, grad_gain_two = norm_back(grad_normed_two, unit_two, scale_two, gain_two)
    grad_middle = cotangent.reshape(-1, D).astype(jnp.float32) + grad_middle_norm
    grad_branch_one = grad_middle.astype(jnp.bfloat16)
    grad_attended = lax.dot_general(
        grad_branch_one, w_o_all, CONTRACT_LAST, preferred_element_type=jnp.float32
    ).astype(jnp.bfloat16)
    o_terms = lax.dot_general(
        attended_low, grad_branch_one, CONTRACT_FIRST, preferred_element_type=jnp.float32
    ).astype(jnp.bfloat16)
    grad_queries, grad_kv_full = attend_backward(
        scalars,
        queries,
        to_groups(grad_attended, rows_here),
        attended_grouped,
        stats,
        all_kv,
        ctx_size,
        block_rows,
        rows_here,
    )
    grad_kv, mixed_rows = scatter(
        [grad_kv_full.reshape(-1, rows_here, SEQS * KVH * 4 * HD)],
        by_tokens,
        3,
        out_dtype=jnp.float32,
        lines=[mixed_terms.reshape(shard_count, -1, D)],
    )
    gate_up_rows, grad_kv = lax.optimization_barrier((gate_up_rows, grad_kv))
    gate_up_rows = exchange(gate_up_rows.reshape(shard_count, cut, 2 * width), 5)
    gate_up_rows = lax.all_gather(gate_up_rows, "ctx", axis=0, tiled=False)
    mixed_out = middle + mixed_rows
    output = mixed_out.astype(jnp.bfloat16).reshape(rows_here, slots, D)
    grad_kv_low = narrowed(grad_kv).reshape(rows_here, SEQS, KVH, 2, 2, HD)
    grad_kv_low = grad_kv_low.transpose(0, 3, 1, 4, 2, 5).reshape(-1, 2 * kv_width)
    grad_query_tokens = from_groups(narrowed(grad_queries), rows_here) * query_scale
    grad_query_raw = rotate_back(
        grad_query_tokens.reshape(-1, H, HD), cosine_table, sine_table
    ).reshape(-1, H * HD)
    grad_key_raw = rotate_back(
        grad_kv_low[:, :kv_width].reshape(-1, KVH, HD), cosine_table, sine_table
    ).reshape(-1, kv_width)
    grad_projected = jnp.concatenate(
        [grad_query_raw, grad_key_raw, grad_kv_low[:, kv_width:]], -1
    ).astype(jnp.bfloat16)
    grad_bias = jnp.sum(grad_projected, 0, dtype=jnp.float32)
    grad_normed_one = lax.dot_general(
        grad_projected, w_qkv_all, CONTRACT_LAST, preferred_element_type=jnp.float32
    )
    grad_input_norm, grad_gain_one = norm_back(grad_normed_one, unit_one, scale_one, gain_one)
    grad_input = (grad_middle + grad_input_norm).reshape(rows_here, slots, D)
    qkv_terms = lax.dot_general(
        normed_one, grad_projected, CONTRACT_FIRST, preferred_element_type=jnp.float32
    ).astype(jnp.bfloat16)
    small_terms = jnp.concatenate(
        [
            part.reshape(shard_count, -1)
            for part in (grad_gain_one, grad_gain_two, grad_bias[:QK], grad_bias[QK:])
        ],
        1,
    )
    small_terms = small_terms.reshape(ctx_size * shard_count, small_width)
    small_terms = jnp.pad(small_terms, ((0, 0), (0, 8 * HD - small_width)))
    qkv_rows, small_rows, o_rows = scatter(
        [
            qkv_terms.reshape(-1, cut, QKV),
            small_terms.reshape(-1, 8, HD),
        ],
        by_rows,
        4,
        spread_ctx=True,
        lines=[o_terms.reshape(shard_count, ctx_size, cut, D)],
    )
    small_rows = small_rows.reshape(ctx_size, -1)[:, :small_width].reshape(-1)
    bias_start = 2 * gain_width
    value_start = bias_start + QK // shard_count

    gate_rows, up_rows = unpack(gate_up_rows, columns)
    return (
        output,
        grad_input,
        small_rows[:gain_width],
        qkv_rows.reshape(-1, QKV).astype(jnp.float32),
        small_rows[bias_start:value_start],
        small_rows[value_start:],
        o_rows.reshape(-1, D),
        small_rows[gain_width:bias_start],
        gate_rows.reshape(-1, FF),
        up_rows.reshape(-1, FF),
        down_rows[:columns].astype(jnp.float32),
    )


def solution(mesh):
    in_specs = (
        P(("ctx", "fsdp"), None, None),
        P(),
        P("fsdp"),
        P("fsdp", None),
        P("fsdp"),
        P("fsdp", None),
        P("fsdp"),
        P("fsdp", None),
        P("fsdp", None),
        P("fsdp", None),
        P(("ctx", "fsdp"), None, None),
    )
    out_specs = (
        P(("ctx", "fsdp"), None, None),
        P(("ctx", "fsdp"), None, None),
        P("fsdp"),
        P("fsdp", None),
        P("fsdp"),
        P("fsdp"),
        P("fsdp", None),
        P("fsdp"),
        P("fsdp", None),
        P("fsdp", None),
        P("fsdp", None),
    )
    return jax.shard_map(shards, mesh=mesh, in_specs=in_specs, out_specs=out_specs, check_vma=False)
```

```python
import functools

import jax
import jax.numpy as jnp
from jax import lax
from jax.experimental import pallas as pl
from jax.experimental.pallas import tpu as pltpu
from jax.sharding import PartitionSpec as P

D = 1536
H = 12
KVH = 2
HD = 128
FF = 8960
SEQS = 2
QKV = 2048
QK = 1792


EPS = 1e-06
THETA = 1000000.0
NEG_FILL = -1e30
MESH_ID = pl.DeviceIdType.MESH
CONTRACT_LAST = (((1,), (1,)), ((), ()))
CONTRACT_FIRST = (((0,), (0,)), ((), ()))


def narrowed(values):
    return lax.optimization_barrier(values.astype(jnp.bfloat16)).astype(jnp.float32)


def block_positions(block_order, first_row, row_count, block_rows, ctx_size):
    row_index = first_row + jnp.arange(row_count, dtype=jnp.int32)
    slot_index = jnp.arange(2 * SEQS, dtype=jnp.int32)
    entries = (slot_index // SEQS)[None, :] * ctx_size + (row_index // block_rows)[:, None]
    tiled = jnp.tile(block_order, (2, 1))
    entry_ids = jnp.arange(2 * ctx_size, dtype=jnp.int32)
    picked = jnp.sum(
        jnp.where(entries[:, :, None] == entry_ids[None, None, :], tiled[None, :, :], 0), -1
    )
    return picked * block_rows + (row_index % block_rows)[:, None]


def to_groups(tokens, row_count):
    shaped = tokens.reshape(row_count, 2, SEQS, KVH, H // KVH, HD)
    return shaped.transpose(2, 1, 3, 4, 0, 5).reshape(SEQS, 2, KVH, H // KVH * row_count, HD)


def from_groups(grouped, row_count):
    shaped = grouped.reshape(SEQS, 2, KVH, H // KVH, row_count, HD).transpose(4, 1, 0, 2, 3, 5)
    return shaped.reshape(row_count * 2 * SEQS, H * HD)


def rope_tables(positions):
    half_width = HD // 2
    frequency = THETA ** (-jnp.arange(half_width, dtype=jnp.float32) * 2.0 / HD)
    angles = positions.astype(jnp.float32)[:, None] * frequency[None, :]
    cosine_table = jnp.concatenate([jnp.cos(angles), jnp.cos(angles)], -1)[:, None, :]
    sine_table = jnp.concatenate([jnp.sin(angles), jnp.sin(angles)], -1)[:, None, :]
    return (cosine_table, sine_table)


def rotate(head_values, cosine_table, sine_table):
    half_width = HD // 2
    turned = jnp.concatenate([-head_values[..., half_width:], head_values[..., :half_width]], -1)
    return head_values * cosine_table + turned * sine_table


def rotate_back(grad_values, cosine_table, sine_table):
    half_width = HD // 2
    moved = grad_values * sine_table
    return grad_values * cosine_table + jnp.concatenate(
        [moved[..., half_width:], -moved[..., :half_width]], -1
    )


def normalize(values, gain):
    scale = lax.rsqrt(jnp.mean(values * values, -1, keepdims=True) + EPS)
    unit = values * scale
    return (unit, scale, unit * gain)


def norm_back(grad_out, unit, scale, gain):
    grad_unit = grad_out * gain
    inner = jnp.mean(grad_unit * unit, -1, keepdims=True)
    return (scale * (grad_unit - unit * inner), jnp.sum(grad_out * unit, 0))


def attend_forward_kernel(ctx_size, block_rows, rows_here, scalars, q_ref, kv_ref, out_ref, stat_ref, best_ref, total_ref, accum_ref):
    seq = pl.program_id(0)
    blocks = 2 * ctx_size
    own_ctx = scalars[SEQS * blocks]
    own_shard = scalars[SEQS * blocks + 1]
    lanes = q_ref.shape[3]
    best_ref[...] = jnp.full(best_ref.shape, NEG_FILL, jnp.float32)
    total_ref[...] = jnp.zeros(total_ref.shape, jnp.float32)
    accum_ref[...] = jnp.zeros(accum_ref.shape, jnp.float32)

    def step(key_ctx, half_key, half):
        order_key = scalars[seq * blocks + half_key * ctx_size + key_ctx]
        order_query = scalars[seq * blocks + half * ctx_size + own_ctx]

        def work(masked):
            rows = pl.ds(pl.multiple_of(key_ctx * block_rows, block_rows), block_rows)
            keys = kv_ref[rows, half_key * 2 * HD : half_key * 2 * HD + HD]
            values = kv_ref[rows, half_key * 2 * HD + HD : half_key * 2 * HD + 2 * HD]
            scores = lax.dot_general(
                keys, q_ref[0, half, 0], CONTRACT_LAST, preferred_element_type=jnp.float32
            )
            if masked:
                row = lax.broadcasted_iota(jnp.int32, (block_rows, lanes), 0)
                lane = lax.broadcasted_iota(jnp.int32, (block_rows, lanes), 1)
                scores = jnp.where(
                    row <= own_shard * rows_here + lax.rem(lane, rows_here), scores, NEG_FILL
                )
            best = best_ref[half]
            fresh = jnp.maximum(best, jnp.max(scores, 0, keepdims=True))
            decay = jnp.exp(best - fresh)
            weights = jnp.exp(scores - fresh)
            total_ref[half] = total_ref[half] * decay + jnp.sum(weights, 0, keepdims=True)
            accum_ref[half] = accum_ref[half] * decay + lax.dot_general(
                values,
                weights.astype(jnp.bfloat16),
                CONTRACT_FIRST,
                preferred_element_type=jnp.float32,
            )
            best_ref[half] = fresh

        @pl.when(order_key < order_query)
        def full():
            work(False)

        @pl.when(order_key == order_query)
        def diagonal():
            work(True)

    @pl.loop(0, ctx_size)
    def sweep(key_ctx):
        for half_key in range(2):
            for half in range(2):
                step(key_ctx, half_key, half)

    for half in range(2):
        totals = total_ref[half]
        out_ref[0, half, 0] = (accum_ref[half] / totals).T
        stat_ref[0, half, 0] = best_ref[half] + jnp.log(totals)


def attend_forward(scalars, queries, all_kv, ctx_size, block_rows, rows_here):
    lanes = queries.shape[3]
    kernel = functools.partial(attend_forward_kernel, ctx_size, block_rows, rows_here)
    group = pl.BlockSpec((1, 2, 1, lanes, HD), lambda s, n, _: (s, 0, n, 0, 0))
    stat = pl.BlockSpec((1, 2, 1, 1, lanes), lambda s, n, _: (s, 0, n, 0, 0))
    return pl.pallas_call(
        kernel,
        grid_spec=pltpu.PrefetchScalarGridSpec(
            num_scalar_prefetch=1,
            grid=(SEQS, KVH),
            in_specs=[
                group,
                pl.BlockSpec((all_kv.shape[0], 4 * HD), lambda s, n, _: (0, s * KVH + n)),
            ],
            out_specs=[group, stat],
            scratch_shapes=[
                pltpu.VMEM((2, 1, lanes), jnp.float32),
                pltpu.VMEM((2, 1, lanes), jnp.float32),
                pltpu.VMEM((2, HD, lanes), jnp.float32),
            ],
        ),
        out_shape=(
            jax.ShapeDtypeStruct(queries.shape, jnp.float32),
            jax.ShapeDtypeStruct((SEQS, 2, KVH, 1, lanes), jnp.float32),
        ),
        compiler_params=pltpu.CompilerParams(vmem_limit_bytes=56 * 2**20),
        name="attend_forward",
    )(scalars, queries, all_kv)


def attend_backward_kernel(ctx_size, block_rows, rows_here, scalars, q_ref, go_ref, att_ref, stat_ref, kv_ref, gq_ref, gkv_ref, delta_ref, gq_acc, gk_acc, gv_acc):
    seq = pl.program_id(0)
    blocks = 2 * ctx_size
    own_ctx = scalars[SEQS * blocks]
    own_shard = scalars[SEQS * blocks + 1]
    lanes = q_ref.shape[3]
    gq_acc[...] = jnp.zeros(gq_acc.shape, jnp.float32)
    for half in range(2):
        product = go_ref[0, half, 0].astype(jnp.float32) * att_ref[0, half, 0]
        delta_ref[half] = jnp.sum(product.T, 0, keepdims=True)

    def step(key_ctx, half_key, half):
        order_key = scalars[seq * blocks + half_key * ctx_size + key_ctx]
        order_query = scalars[seq * blocks + half * ctx_size + own_ctx]

        def work(masked):
            rows = pl.ds(pl.multiple_of(key_ctx * block_rows, block_rows), block_rows)
            keys = kv_ref[rows, half_key * 2 * HD : half_key * 2 * HD + HD]
            values = kv_ref[rows, half_key * 2 * HD + HD : half_key * 2 * HD + 2 * HD]
            queries = q_ref[0, half, 0]
            grad_out = go_ref[0, half, 0]
            scores = lax.dot_general(
                keys, queries, CONTRACT_LAST, preferred_element_type=jnp.float32
            )
            probs = jnp.exp(scores - stat_ref[0, half, 0])
            if masked:
                row = lax.broadcasted_iota(jnp.int32, (block_rows, lanes), 0)
                lane = lax.broadcasted_iota(jnp.int32, (block_rows, lanes), 1)
                probs = jnp.where(
                    row <= own_shard * rows_here + lax.rem(lane, rows_here), probs, 0.0
                )
            grad_probs = lax.dot_general(
                values, grad_out, CONTRACT_LAST, preferred_element_type=jnp.float32
            )
            grad_scores = (probs * (grad_probs - delta_ref[half])).astype(jnp.bfloat16)
            gv_acc[...] += jnp.dot(
                probs.astype(jnp.bfloat16), grad_out, preferred_element_type=jnp.float32
            )
            gk_acc[...] += jnp.dot(grad_scores, queries, preferred_element_type=jnp.float32)
            gq_acc[half] += lax.dot_general(
                keys, grad_scores, CONTRACT_FIRST, preferred_element_type=jnp.float32
            )

        @pl.when(order_key < order_query)
        def full():
            work(False)

        @pl.when(order_key == order_query)
        def diagonal():
            work(True)

    @pl.loop(0, ctx_size)
    def sweep(key_ctx):
        rows = pl.ds(pl.multiple_of(key_ctx * block_rows, block_rows), block_rows)
        for half_key in range(2):
            gk_acc[...] = jnp.zeros(gk_acc.shape, jnp.float32)
            gv_acc[...] = jnp.zeros(gv_acc.shape, jnp.float32)
            for half in range(2):
                step(key_ctx, half_key, half)
            at = half_key * 2 * HD
            gkv_ref[rows, at : at + HD] = gk_acc[...].astype(jnp.bfloat16)
            gkv_ref[rows, at + HD : at + 2 * HD] = gv_acc[...].astype(jnp.bfloat16)

    for half in range(2):
        gq_ref[0, half, 0] = gq_acc[half].T


def attend_backward(scalars, queries, grad_out, attended, stats, all_kv, ctx_size, block_rows, rows_here):
    lanes = queries.shape[3]
    kernel = functools.partial(attend_backward_kernel, ctx_size, block_rows, rows_here)
    group = pl.BlockSpec((1, 2, 1, lanes, HD), lambda s, n, _: (s, 0, n, 0, 0))
    stat = pl.BlockSpec((1, 2, 1, 1, lanes), lambda s, n, _: (s, 0, n, 0, 0))
    full = pl.BlockSpec((all_kv.shape[0], 4 * HD), lambda s, n, _: (0, s * KVH + n))
    return pl.pallas_call(
        kernel,
        grid_spec=pltpu.PrefetchScalarGridSpec(
            num_scalar_prefetch=1,
            grid=(SEQS, KVH),
            in_specs=[group, group, group, stat, full],
            out_specs=[group, full],
            scratch_shapes=[
                pltpu.VMEM((2, 1, lanes), jnp.float32),
                pltpu.VMEM((2, HD, lanes), jnp.float32),
                pltpu.VMEM((block_rows, HD), jnp.float32),
                pltpu.VMEM((block_rows, HD), jnp.float32),
            ],
        ),
        out_shape=(
            jax.ShapeDtypeStruct(queries.shape, jnp.float32),
            jax.ShapeDtypeStruct(all_kv.shape, jnp.bfloat16),
        ),
        compiler_params=pltpu.CompilerParams(vmem_limit_bytes=56 * 2**20),
        name="attend_backward",
    )(scalars, queries, grad_out, attended, stats, all_kv)


def peers_of(ctx_size):
    return ctx_size == 4, range(1, ctx_size)


def ctx_target(position, way, square, ctx_size):
    return position ^ way if square else lax.rem(position + way, ctx_size)


def ctx_source(position, way, square, ctx_size):
    return position ^ way if square else lax.rem(position + ctx_size - way, ctx_size)


def greet(ctx_size, pair_count, with_ctx, all_shards):
    ctx = lax.axis_index("ctx")
    shard = lax.axis_index("fsdp")
    pair, core = shard // 2, shard % 2
    barrier = pltpu.get_barrier_semaphore()
    partners = [(ctx, pair * 2 + 1 - core)]
    for step in range(1, pair_count):
        there = lax.rem(pair + step, pair_count) * 2
        partners.append((ctx, there + core))
        if all_shards:
            partners.append((ctx, there + 1 - core))
    if with_ctx:
        for way in range(1, ctx_size):
            partners.append((lax.rem(ctx + way, ctx_size), shard))
    for partner in partners:
        pl.semaphore_signal(barrier, inc=1, device_id=partner, device_id_type=MESH_ID)
    pl.semaphore_wait(barrier, len(partners))
    return ctx, pair, core


class Exchange:
    def __init__(self, source, out, sems, own_sem, pair_count):
        self.source, self.out, self.sems, self.own_sem = source, out, sems, own_sem
        self.shard_count = 2 * pair_count

    def start(self):
        ctx, shard = lax.axis_index("ctx"), lax.axis_index("fsdp")
        self.own = pltpu.make_async_copy(self.source.at[shard], self.out.at[shard], self.own_sem)
        self.own.start()
        self.copies = []
        for step in range(1, self.shard_count):
            there = lax.rem(shard + step, self.shard_count)
            copy = pltpu.make_async_remote_copy(
                src_ref=self.source.at[there],
                dst_ref=self.out.at[shard],
                send_sem=self.sems[0].at[step - 1],
                recv_sem=self.sems[1].at[step - 1],
                device_id=(ctx, there),
                device_id_type=MESH_ID,
            )
            copy.start()
            self.copies.append(copy)

    def finish(self):
        ctx, shard = lax.axis_index("ctx"), lax.axis_index("fsdp")
        for step in range(1, self.shard_count):
            come = lax.rem(shard + self.shard_count - step, self.shard_count)
            pltpu.make_async_remote_copy(
                src_ref=self.out.at[come],
                dst_ref=self.out.at[come],
                send_sem=self.sems[0].at[step - 1],
                recv_sem=self.sems[1].at[step - 1],
                device_id=(ctx, shard),
                device_id_type=MESH_ID,
            ).wait_recv()
        self.own.wait()
        for copy in self.copies:
            copy.wait_send()


def exchange_kernel(pair_count, source, out, send_sem, recv_sem, own_sem):
    greet(1, pair_count, False, True)
    flow = Exchange(source, out, (send_sem, recv_sem), own_sem, pair_count)
    flow.start()
    flow.finish()


def exchange(pieces, collective_id):
    shard_count = lax.axis_size("fsdp")
    dma = pltpu.SemaphoreType.DMA
    return pl.pallas_call(
        functools.partial(exchange_kernel, shard_count // 2),
        in_specs=[pl.BlockSpec(memory_space=pltpu.VMEM)],
        out_specs=pl.BlockSpec(memory_space=pl.ANY),
        out_shape=jax.ShapeDtypeStruct(pieces.shape, pieces.dtype),
        scratch_shapes=[dma((shard_count - 1,))] * 2 + [dma],
        compiler_params=pltpu.CompilerParams(collective_id=collective_id, has_side_effects=True),
        cost_estimate=pl.CostEstimate(
            flops=0, bytes_accessed=pieces.size * 64, transcendentals=0
        ),
    )(pieces)


def gather_kernel(arity, ctx_size, pair_count, slots, swaps, wide, *refs):
    sources, refs = refs[:arity], refs[arity:]
    swap_sources, refs = refs[:swaps], refs[swaps:]
    outs, refs = refs[:arity], refs[arity:]
    swap_outs, refs = refs[:swaps], refs[swaps:]
    pair_sems, ctx_sems, core_sems = refs[0:2], refs[2:4], refs[4:6]
    local_sem = refs[6]
    square, ways = peers_of(ctx_size) if wide else (False, ())
    narrow = [item for item in range(arity) if item not in wide]
    near = [way for way in ways if not (square and way == 3)]
    ctx, pair, core = greet(ctx_size, pair_count, len(wide) > 0, swaps > 0)
    homes = [place(ctx, pair * 2 + core) for place in slots]
    started = []
    steps = [(0, 1)] + [(far, way) for far in range(1, pair_count) for way in (1, -1)]

    def present(step):
        far, way = steps[step]
        if far == 0:
            return None
        return pair >= far if way == 1 else pair + far < pair_count

    def origin(step):
        far, way = steps[step]
        return pair - far * way

    def when(condition, work):
        if condition is None:
            work()
        else:
            pl.when(condition)(work)

    def send(item, source, place, target, sems, at, condition):
        copy = pltpu.make_async_remote_copy(
            src_ref=source,
            dst_ref=outs[item].at[place],
            send_sem=sems[0].at[at],
            recv_sem=sems[1].at[at],
            device_id=target,
            device_id_type=MESH_ID,
        )
        copy.start()
        started.append((condition, item, sems, at))

    def sent(item, sems, at):
        pltpu.make_async_remote_copy(
            src_ref=outs[item].at[0],
            dst_ref=outs[item].at[0],
            send_sem=sems[0].at[at],
            recv_sem=sems[1].at[at],
            device_id=(ctx, pair * 2 + core),
            device_id_type=MESH_ID,
        ).wait_send()

    def arrive(item, place, sems, at):
        pltpu.make_async_remote_copy(
            src_ref=outs[item].at[place],
            dst_ref=outs[item].at[place],
            send_sem=sems[0].at[at],
            recv_sem=sems[1].at[at],
            device_id=(ctx, pair * 2 + core),
            device_id_type=MESH_ID,
        ).wait_recv()

    def pass_on(step, item, source, place):
        far, way = steps[step]
        for side in (1, -1) if far == 0 else (way,):

            def further(side=side):
                return pair + 1 < pair_count if side == 1 else pair >= 1

            def both(further=further):
                return further() if far == 0 else jnp.logical_and(further(), present(step))

            def work(side=side, both=both):
                send(
                    item,
                    source,
                    place,
                    (ctx, (pair + side) * 2 + core),
                    pair_sems,
                    ((side + 1) // 2, far, item),
                    both,
                )

            if far + 1 < pair_count:
                pl.when(further())(work)

    def to_core(item, source, from_ctx, way, step):
        send(
            item,
            source,
            slots[item](from_ctx, origin(step) * 2 + core),
            (ctx, pair * 2 + 1 - core),
            core_sems,
            (way, step, item),
            functools.partial(present, step),
        )

    def spread(step, items):
        for item in items:
            place = slots[item](ctx, origin(step) * 2 + core)
            source = sources[item]
            if step:
                far, way = steps[step]
                arrive(item, place, pair_sems, ((way + 1) // 2, far - 1, item))
                source = outs[item].at[place]
            pass_on(step, item, source, place)
            for way in near if item in wide else ():
                there = ctx_target(ctx, way, square, ctx_size)
                send(
                    item,
                    source,
                    place,
                    (there, pair * 2 + core),
                    ctx_sems,
                    (way - 1, step, item),
                    functools.partial(present, step),
                )
            to_core(item, source, ctx, 0, step)

    def collect(step):
        for way in near:
            for item in wide:
                come = ctx_source(ctx, way, square, ctx_size)
                place = slots[item](come, origin(step) * 2 + core)
                arrive(item, place, ctx_sems, (way - 1, step, item))
                source = outs[item].at[place]
                if square and (steps[step][0] % 2 == 0) == (way == 1):
                    send(
                        item,
                        source,
                        place,
                        (ctx ^ (3 - way), pair * 2 + core),
                        ctx_sems,
                        (2, step, item),
                        functools.partial(present, step),
                    )
                to_core(item, source, come, way, step)

    def collect_far(step):
        for item in wide:
            place = slots[item](ctx ^ 3, origin(step) * 2 + core)
            arrive(item, place, ctx_sems, (2, step, item))
            to_core(item, outs[item].at[place], ctx ^ 3, 3, step)

    locals_ = []
    for item in range(arity):
        copy = pltpu.make_async_copy(sources[item], outs[item].at[homes[item]], local_sem.at[item])
        copy.start()
        locals_.append(copy)
    spread(0, wide)
    flows = []
    count = len(steps)
    for turn in range(1, count + 4):
        if turn < count:
            when(present(turn), functools.partial(spread, turn, wide))
        if turn == count:
            spread(0, narrow)
            for item in range(swaps):
                flow = Exchange(
                    swap_sources[item],
                    swap_outs[item],
                    refs[7 + 3 * item : 9 + 3 * item],
                    refs[9 + 3 * item],
                    pair_count,
                )
                flow.start()
                flows.append(flow)
        if 0 <= turn - 2 < count:
            when(present(turn - 2), functools.partial(collect, turn - 2))
        if square and 0 <= turn - 4 < count:
            when(present(turn - 4), functools.partial(collect_far, turn - 4))

    for turn in range(1, count):
        when(present(turn), functools.partial(spread, turn, narrow))

    def from_core(step):
        for way in (0, *ways):
            come = ctx_source(ctx, way, square, ctx_size) if way else ctx
            for item in wide if way else range(arity):
                arrive(item, slots[item](come, origin(step) * 2 + 1 - core), core_sems, (way, step, item))

    for step in range(count):
        when(present(step), functools.partial(from_core, step))
    for flow in flows:
        flow.finish()
    for copy in locals_:
        copy.wait()
    for condition, *which in started:
        when(condition(), functools.partial(sent, *which))


def gather(pieces, slots, collective_id, swaps=(), wide=None):
    ctx_size, shard_count = lax.axis_size("ctx"), lax.axis_size("fsdp")
    pair_count = shard_count // 2
    arity = len(pieces)
    wide = range(arity) if wide is None else wide
    dma = pltpu.SemaphoreType.DMA
    moved = sum(piece.size for piece in pieces) * 2
    steps = 2 * pair_count - 1
    return pl.pallas_call(
        functools.partial(gather_kernel, arity, ctx_size, pair_count, slots, len(swaps), wide),
        in_specs=[pl.BlockSpec(memory_space=pltpu.VMEM)] * (arity + len(swaps)),
        out_specs=[pl.BlockSpec(memory_space=pl.ANY)] * (arity + len(swaps)),
        out_shape=[
            jax.ShapeDtypeStruct(
                ((ctx_size if item in wide else 1) * shard_count,) + piece.shape, piece.dtype
            )
            for item, piece in enumerate(pieces)
        ]
        + [jax.ShapeDtypeStruct(swap.shape, swap.dtype) for swap in swaps],
        scratch_shapes=[dma((2, pair_count - 1, arity))] * 2
        + [dma((ctx_size - 1, steps, arity))] * 2
        + [dma((ctx_size, steps, arity))] * 2
        + [dma((arity,))]
        + [dma((shard_count - 1,)), dma((shard_count - 1,)), dma] * len(swaps),
        compiler_params=pltpu.CompilerParams(collective_id=collective_id, has_side_effects=True),
        cost_estimate=pl.CostEstimate(
            flops=0, bytes_accessed=moved * ctx_size * shard_count * 4, transcendentals=0
        ),
    )(*pieces, *swaps)


class LineScatter:
    def __init__(self, source, out, half, room, sems, where, counts, last):
        self.count, self.ctx_size = counts
        self.source, self.out, self.half, self.room = source, out, half, room
        self.last = last
        self.core_sems, self.pair_sems = sems[0:2], sems[2:4]
        self.ctx, self.pair, self.core = where
        self.order = [*range(1, self.count), 0]

    def copy(self, source, target, device, sems, at):
        return pltpu.make_async_remote_copy(
            src_ref=source,
            dst_ref=target,
            send_sem=sems[0].at[at],
            recv_sem=sems[1].at[at],
            device_id=device,
            device_id_type=MESH_ID,
        )

    def here(self):
        return (self.ctx, self.pair * 2 + self.core)

    def toward(self, step):
        return lax.rem(self.pair + step, self.count)

    def start(self):
        self.copies = []
        for step in self.order:
            self.copies.append(
                self.copy(
                    self.source.at[self.toward(step) * 2 + 1 - self.core],
                    self.half.at[step],
                    (self.ctx, self.pair * 2 + 1 - self.core),
                    self.core_sems,
                    step,
                )
            )
            self.copies[-1].start()

    def fold(self, step):
        half = self.half.at[step]
        self.copy(half, half, self.here(), self.core_sems, step).wait_recv()
        mine = self.source[self.toward(step) * 2 + self.core].astype(jnp.float32)
        total = mine + half[...].astype(jnp.float32)
        if step == 0:
            self.out[...] = total
            return
        half[...] = total.astype(half.dtype)
        self.copies.append(
            self.copy(
                half,
                self.room.at[step - 1],
                (self.ctx, self.toward(step) * 2 + self.core),
                self.pair_sems,
                step - 1,
            )
        )
        self.copies[-1].start()

    def over_ctx(self, terms, room, landing, *sems):
        shard = self.pair * 2 + self.core
        copies = []

        def send(source, target, way, sems):
            there = lax.rem(self.ctx + way, self.ctx_size)
            copies.append(self.copy(source(there), target, (there, shard), sems, way - 1))
            copies[-1].start()

        def arrive(target, way, sems):
            self.copy(target, target, self.here(), sems, way - 1).wait_recv()

        terms[...] = self.out[...].astype(terms.dtype)
        for way in range(1, self.ctx_size):
            send(lambda there: terms.at[there], room.at[way - 1], way, sems[0:2])
        total = self.out[self.ctx]
        for way in range(1, self.ctx_size):
            arrive(room.at[way - 1], way, sems[0:2])
            total = total + room[way - 1].astype(jnp.float32)
        landing[self.ctx] = total.astype(landing.dtype)
        for way in range(1, self.ctx_size):
            send(lambda there: landing.at[self.ctx], landing.at[self.ctx], way, sems[2:4])
        for way in range(1, self.ctx_size):
            come = lax.rem(self.ctx + self.ctx_size - way, self.ctx_size)
            arrive(landing.at[come], way, sems[2:4])
        self.out[...] = landing[...].astype(jnp.float32)
        for copy in copies:
            copy.wait_send()

    def finish(self):
        for step in range(1, self.count):
            room = self.room.at[step - 1]
            self.copy(room, room, self.here(), self.pair_sems, step - 1).wait_recv()
            self.out[...] += room[...].astype(jnp.float32)
        if self.last:
            self.over_ctx(*self.last)
        for copy in self.copies:
            copy.wait_send()


def scatter_kernel(arity, ctx_size, pair_count, slot, spread_ctx, lines, *refs):
    sources, refs = refs[:arity], refs[arity:]
    line_sources, refs = refs[:lines], refs[lines:]
    outs, refs = refs[:arity], refs[arity:]
    line_outs, refs = refs[:lines], refs[lines:]
    halves, relays, asides, ends, finals = (refs[i * arity : (i + 1) * arity] for i in range(5))
    sems = refs[5 * arity : 5 * arity + 10]
    core_sems, relay_sems, ctx_sems, pair_sems, last_sems = (sems[2 * i : 2 * i + 2] for i in range(5))
    square, ways = peers_of(ctx_size)
    ctx, pair, core = greet(ctx_size, pair_count, True, False)
    order = list(range(1, pair_count)) + [0]
    started = []
    flows = []
    for item in range(lines):
        at = 5 * arity + 10 + 13 * item
        spread = len(line_sources[item].shape) == 4
        flows.append(
            LineScatter(
                line_sources[item],
                line_outs[item],
                *refs[at : at + 2],
                refs[at + 2 : at + 6],
                (ctx, pair, core),
                (pair_count, ctx_size),
                refs[at + 6 : at + 13] if spread else (),
            )
        )

    def send(source, target, device, pair_of_sems, at):
        copy = pltpu.make_async_remote_copy(
            src_ref=source,
            dst_ref=target,
            send_sem=pair_of_sems[0].at[at],
            recv_sem=pair_of_sems[1].at[at],
            device_id=device,
            device_id_type=MESH_ID,
        )
        copy.start()
        started.append(copy)

    def arrive(target, pair_of_sems, at):
        pltpu.make_async_remote_copy(
            src_ref=target,
            dst_ref=target,
            send_sem=pair_of_sems[0].at[at],
            recv_sem=pair_of_sems[1].at[at],
            device_id=(ctx, pair * 2 + core),
            device_id_type=MESH_ID,
        ).wait_recv()

    def toward(step):
        return lax.rem(pair + step, pair_count)

    def target_ctx(way):
        return ctx_target(ctx, way, square, ctx_size) if way else ctx

    def f32(value):
        return value.astype(jnp.float32)

    far_first = [3, 1, 2, 0] if square else list(ways) + [0]
    for step in order:
        for way in far_first:
            for item in range(arity):
                send(
                    sources[item].at[slot(target_ctx(way), toward(step) * 2 + 1 - core)],
                    halves[item].at[way, step],
                    (ctx, pair * 2 + 1 - core),
                    core_sems,
                    (way, step, item),
                )

    def fold_core(step):
        for way in far_first:
            for item in range(arity):
                half = halves[item].at[way, step]
                arrive(half, core_sems, (way, step, item))
                mine = sources[item][slot(target_ctx(way), toward(step) * 2 + core)]
                half[...] = (f32(mine) + f32(half[...])).astype(half.dtype)
                if square and way == 3:
                    there = ctx ^ (1 if step % 2 == 0 else 2)
                    send(
                        half,
                        relays[item].at[step],
                        (there, pair * 2 + core),
                        relay_sems,
                        (step, item),
                    )

    def fold_relay(step):
        for item in range(arity):
            if square:
                relay = relays[item].at[step]
                arrive(relay, relay_sems, (step, item))
                half = halves[item].at[2 if step % 2 == 0 else 1, step]
                half[...] = (f32(half[...]) + f32(relay[...])).astype(half.dtype)
            for way in ways:
                if square and way == 3:
                    continue
                send(
                    halves[item].at[way, step],
                    asides[item].at[way - 1, step],
                    (target_ctx(way), pair * 2 + core),
                    ctx_sems,
                    (way - 1, step, item),
                )

    def fold_ctx(step):
        for item in range(arity):
            half = halves[item].at[0, step]
            total = f32(half[...])
            for way in ways:
                if square and way == 3:
                    continue
                aside = asides[item].at[way - 1, step]
                arrive(aside, ctx_sems, (way - 1, step, item))
                total = total + f32(aside[...])
            if step:
                half[...] = total.astype(half.dtype)
                send(
                    half,
                    ends[item].at[step - 1],
                    (ctx, toward(step) * 2 + core),
                    pair_sems,
                    (step - 1, item),
                )
            else:
                for other in range(1, pair_count):
                    end = ends[item].at[other - 1]
                    arrive(end, pair_sems, (other - 1, item))
                    total = total + f32(end[...])
                if spread_ctx:
                    finals[item][...] = total.astype(finals[item].dtype)
                else:
                    outs[item][...] = total.astype(outs[item].dtype)

    for flow in flows:
        flow.start()
    for turn in range(pair_count + 2):
        if turn < pair_count:
            fold_core(order[turn])
        if 1 <= turn <= pair_count:
            fold_relay(order[turn - 1])
            for flow in flows:
                flow.fold(order[turn - 1])
        if turn >= 2:
            fold_ctx(order[turn - 2])
    if spread_ctx:
        for item in range(arity):
            for way in ways:
                send(
                    finals[item],
                    outs[item].at[ctx],
                    (target_ctx(way), pair * 2 + core),
                    last_sems,
                    (way - 1, item),
                )
            outs[item][ctx] = finals[item][...]
        for item in range(arity):
            for way in ways:
                arrive(outs[item].at[ctx_source(ctx, way, square, ctx_size)], last_sems, (way - 1, item))
    for flow in flows:
        flow.finish()
    for copy in started:
        copy.wait_send()


def scatter(terms, slot, collective_id, spread_ctx=False, out_dtype=None, lines=()):
    ctx_size, shard_count = lax.axis_size("ctx"), lax.axis_size("fsdp")
    pair_count = shard_count // 2
    arity = len(terms)
    dma = pltpu.SemaphoreType.DMA
    lead = (ctx_size,) if spread_ctx else ()
    asides = 2 if ctx_size == 4 else ctx_size - 1

    def room(*extent):
        return [pltpu.VMEM(extent + term.shape[1:], term.dtype) for term in terms]

    def line_room(line):
        if len(line.shape) == 3:
            return [pltpu.VMEM((8, HD), line.dtype)] * 3 + [dma((1,))] * 4
        cut = line.shape[2:]
        rooms = [pltpu.VMEM((count,) + cut, line.dtype) for count in (ctx_size, ctx_size - 1, ctx_size)]
        return rooms + [dma((ctx_size - 1,))] * 4

    moved = sum(term.size * term.dtype.itemsize for term in terms)
    return pl.pallas_call(
        functools.partial(scatter_kernel, arity, ctx_size, pair_count, slot, spread_ctx, len(lines)),
        in_specs=[pl.BlockSpec(memory_space=pltpu.VMEM)] * (arity + len(lines)),
        out_specs=[pl.BlockSpec(memory_space=pltpu.VMEM)] * (arity + len(lines)),
        out_shape=[
            jax.ShapeDtypeStruct(lead + term.shape[1:], out_dtype or term.dtype) for term in terms
        ]
        + [jax.ShapeDtypeStruct(line.shape[1:], jnp.float32) for line in lines],
        scratch_shapes=room(ctx_size, pair_count)
        + room(pair_count)
        + room(asides, pair_count)
        + room(pair_count - 1)
        + room()
        + [dma((ctx_size, pair_count, arity))] * 2
        + [dma((pair_count, arity))] * 2
        + [dma((ctx_size - 1, pair_count, arity))] * 2
        + [dma((pair_count - 1, arity))] * 2
        + [dma((ctx_size - 1, arity))] * 2
        + [
            scratch
            for line in lines
            for scratch in [
                pltpu.VMEM((pair_count,) + line.shape[1:], line.dtype),
                pltpu.VMEM((pair_count - 1,) + line.shape[1:], line.dtype),
            ]
            + [dma((pair_count,))] * 4
            + line_room(line)
        ],
        compiler_params=pltpu.CompilerParams(
            collective_id=collective_id, has_side_effects=True, vmem_limit_bytes=63 * 2**20
        ),
        cost_estimate=pl.CostEstimate(flops=0, bytes_accessed=moved * 16, transcendentals=0),
    )(*terms, *lines)


def pack_kernel(columns, gate_ref, up_ref, out_ref):
    width = out_ref.shape[2] // 2
    cut = out_ref.shape[1]
    for there in range(out_ref.shape[0]):
        for side, ref in enumerate((gate_ref, up_ref)):
            at = side * width
            out_ref[there, :, at + width - HD : at + width] = jnp.zeros((cut, HD), out_ref.dtype)
            out_ref[there, :, at : at + columns] = ref[:, there * columns : (there + 1) * columns]


def pack(gate, up, shard_count, columns, width):
    return pl.pallas_call(
        functools.partial(pack_kernel, columns),
        in_specs=[pl.BlockSpec(memory_space=pltpu.VMEM)] * 2,
        out_specs=pl.BlockSpec(memory_space=pltpu.VMEM),
        out_shape=jax.ShapeDtypeStruct((shard_count, gate.shape[0], 2 * width), gate.dtype),
        name="pack",
    )(gate, up)


def unpack_kernel(columns, in_ref, gate_ref, up_ref):
    width = in_ref.shape[3] // 2
    for there in range(in_ref.shape[1]):
        for side, ref in enumerate((gate_ref, up_ref)):
            part = in_ref[0, there, :, side * width : side * width + columns]
            ref[0, :, there * columns : (there + 1) * columns] = part.astype(jnp.float32)


def unpack(rows, columns):
    ctx_size, shard_count, cut, _ = rows.shape
    out = jax.ShapeDtypeStruct((ctx_size, cut, shard_count * columns), jnp.float32)
    return pl.pallas_call(
        functools.partial(unpack_kernel, columns),
        grid=(ctx_size,),
        in_specs=[pl.BlockSpec((1,) + rows.shape[1:], lambda c: (c, 0, 0, 0))],
        out_specs=[pl.BlockSpec((1, cut, shard_count * columns), lambda c: (c, 0, 0))] * 2,
        out_shape=[out, out],
        name="unpack",
    )(rows)


def shards(
    layer_input,
    block_order,
    first_gain,
    w_qkv,
    b_qkv,
    w_o,
    second_gain,
    w_gate,
    w_up,
    w_down,
    cotangent,
):
    ctx_size = lax.axis_size("ctx")
    shard_count = lax.axis_size("fsdp")
    own_ctx = lax.axis_index("ctx")
    own_shard = lax.axis_index("fsdp")
    rows_here = layer_input.shape[0]
    slots = layer_input.shape[1]
    block_rows = rows_here * shard_count
    kv_width = KVH * HD
    cut = D // (ctx_size * shard_count)
    columns = FF // shard_count
    first_row = (own_ctx * shard_count + own_shard) * rows_here
    own_pos = block_positions(block_order, first_row, rows_here, block_rows, ctx_size)
    cosine_table, sine_table = rope_tables(own_pos.reshape(-1))
    query_scale = HD ** (-0.5)

    def by_rows(ctx, shard):
        return shard * ctx_size + ctx

    def by_tokens(ctx, shard):
        return ctx * shard_count + shard

    def own_cut(weight):
        return lax.dynamic_slice_in_dim(weight, own_ctx * cut, cut, 0)

    def mix_features(values):
        shaped = values.reshape(-1, shard_count, ctx_size, cut)
        return shaped.transpose(0, 2, 1, 3).reshape(-1, D)

    def unmix_features(values):
        shaped = values.reshape(-1, ctx_size, shard_count, cut)
        return shaped.transpose(0, 2, 1, 3).reshape(-1, D)

    small = jnp.concatenate([b_qkv, first_gain, second_gain]).reshape(ctx_size, -1)
    small_width = small.shape[1]
    small = lax.dynamic_slice_in_dim(small, own_ctx, 1, 0)
    small = jnp.pad(small, ((0, 0), (0, 16 * HD - small_width))).reshape(16, HD)
    width = -(-columns // HD) * HD
    w_qkv_all, w_o_all, small_all, gate_up_cut = gather(
        [own_cut(w_qkv), own_cut(w_o), small],
        [by_rows, by_rows, by_rows],
        1,
        swaps=[pack(own_cut(w_gate), own_cut(w_up), shard_count, columns, width)],
    )
    w_qkv_all = w_qkv_all.reshape(D, QKV)
    w_o_all = w_o_all.reshape(D, D)
    small_all = small_all.reshape(shard_count, ctx_size, -1)[:, :, :small_width]
    small_all = small_all.reshape(shard_count, -1).astype(jnp.float32)
    bias_width = QKV // shard_count
    gain_width = D // shard_count
    bias_all = small_all[:, :bias_width].reshape(-1)
    gain_one = small_all[:, bias_width : bias_width + gain_width].reshape(-1)
    gain_two = small_all[:, bias_width + gain_width :].reshape(-1)

    gate_up_cols = lax.all_gather(
        gate_up_cut.reshape(shard_count * cut, 2 * width), "ctx", axis=0, tiled=True
    )
    down_padded = jnp.pad(w_down, ((0, width - columns), (0, 0)))

    inputs = layer_input.reshape(-1, D).astype(jnp.float32)
    unit_one, scale_one, normed = normalize(inputs, gain_one)
    normed_one = normed.astype(jnp.bfloat16)
    projected = jnp.dot(normed_one, w_qkv_all, preferred_element_type=jnp.float32) + bias_all
    query_raw = projected[:, : H * HD].reshape(-1, H, HD)
    key_raw = projected[:, H * HD : H * HD + kv_width].reshape(-1, KVH, HD)
    value_raw = projected[:, H * HD + kv_width :]
    query_tokens = (
        (rotate(query_raw, cosine_table, sine_table) * query_scale)
        .astype(jnp.bfloat16)
        .reshape(-1, H * HD)
    )
    key_tokens = (
        rotate(key_raw, cosine_table, sine_table).astype(jnp.bfloat16).reshape(-1, kv_width)
    )
    own_kv = jnp.stack([key_tokens, value_raw.astype(jnp.bfloat16)], 1)
    own_kv = own_kv.reshape(rows_here, 2, SEQS, 2, KVH, HD).transpose(0, 2, 4, 1, 3, 5)
    own_kv = own_kv.reshape(rows_here, SEQS * KVH * 4 * HD)
    all_kv, cotangent_all = gather(
        [own_kv, cotangent.reshape(-1, D)], [by_tokens, lambda ctx, shard: shard], 2, wide=(0,)
    )
    cotangent_all = cotangent_all.reshape(-1, D)
    all_kv = all_kv.reshape(-1, SEQS * KVH * 4 * HD)
    queries = to_groups(query_tokens, rows_here)
    scalars = jnp.concatenate(
        [block_order.reshape(-1), jnp.stack([own_ctx, own_shard]).astype(jnp.int32)]
    )
    attended_grouped, stats = attend_forward(
        scalars, queries, all_kv, ctx_size, block_rows, rows_here
    )
    attended_low = from_groups(attended_grouped, rows_here).astype(jnp.bfloat16)
    middle = inputs + jnp.dot(attended_low, w_o_all, preferred_element_type=jnp.float32)
    unit_two, scale_two, normed = normalize(middle, gain_two)
    normed_two = mix_features(normed.astype(jnp.bfloat16))

    (tokens_all,) = gather([normed_two], [lambda ctx, shard: shard], 6, wide=())
    tokens_all = tokens_all.reshape(-1, D)
    gate_up_part = jnp.dot(tokens_all, gate_up_cols, preferred_element_type=jnp.float32)
    gate_part, up_part = gate_up_part[:, :width], gate_up_part[:, width:]
    sigmoid_gate = jax.nn.sigmoid(gate_part)
    activated = gate_part * sigmoid_gate
    hidden = (activated * up_part).astype(jnp.bfloat16)
    grad_hidden = lax.dot_general(
        cotangent_all, down_padded, CONTRACT_LAST, preferred_element_type=jnp.float32
    )
    grad_gate = grad_hidden * up_part * sigmoid_gate * (1.0 + gate_part * (1.0 - sigmoid_gate))
    grad_gate_up = jnp.concatenate([grad_gate, grad_hidden * activated], -1).astype(jnp.bfloat16)
    grad_tokens = lax.dot_general(
        grad_gate_up, gate_up_cols, CONTRACT_LAST, preferred_element_type=jnp.float32
    )
    grad_normed_two = lax.psum_scatter(
        grad_tokens.astype(jnp.bfloat16), "fsdp", scatter_dimension=0, tiled=True
    )
    down_terms = lax.dot_general(
        hidden, cotangent_all, CONTRACT_FIRST, preferred_element_type=jnp.float32
    ).astype(jnp.bfloat16)
    gate_up_terms = lax.dot_general(
        tokens_all, grad_gate_up, CONTRACT_FIRST, preferred_element_type=jnp.float32
    ).astype(jnp.bfloat16)
    mixed_terms = jnp.dot(hidden, down_padded, preferred_element_type=jnp.float32).astype(jnp.bfloat16)
    down_rows = lax.psum(down_terms, "ctx")
    gate_up_rows = lax.psum_scatter(gate_up_terms, "ctx", scatter_dimension=0, tiled=True)
    grad_normed_two, down_terms, gate_up_terms, mixed_terms = lax.optimization_barrier(
        (grad_normed_two, down_terms, gate_up_terms, mixed_terms)
    )
    grad_normed_two = unmix_features(grad_normed_two.astype(jnp.float32))
    grad_middle_norm, grad_gain_two = norm_back(grad_normed_two, unit_two, scale_two, gain_two)
    grad_middle = cotangent.reshape(-1, D).astype(jnp.float32) + grad_middle_norm
    grad_branch_one = grad_middle.astype(jnp.bfloat16)
    grad_attended = lax.dot_general(
        grad_branch_one, w_o_all, CONTRACT_LAST, preferred_element_type=jnp.float32
    ).astype(jnp.bfloat16)
    o_terms = lax.dot_general(
        attended_low, grad_branch_one, CONTRACT_FIRST, preferred_element_type=jnp.float32
    ).astype(jnp.bfloat16)
    grad_queries, grad_kv_full = attend_backward(
        scalars,
        queries,
        to_groups(grad_attended, rows_here),
        attended_grouped,
        stats,
        all_kv,
        ctx_size,
        block_rows,
        rows_here,
    )
    grad_kv, mixed_rows = scatter(
        [grad_kv_full.reshape(-1, rows_here, SEQS * KVH * 4 * HD)],
        by_tokens,
        3,
        out_dtype=jnp.float32,
        lines=[mixed_terms.reshape(shard_count, -1, D)],
    )
    gate_up_rows, grad_kv = lax.optimization_barrier((gate_up_rows, grad_kv))
    gate_up_rows = exchange(gate_up_rows.reshape(shard_count, cut, 2 * width), 5)
    gate_up_rows = lax.all_gather(gate_up_rows, "ctx", axis=0, tiled=False)
    mixed_out = middle + mixed_rows
    output = mixed_out.astype(jnp.bfloat16).reshape(rows_here, slots, D)
    grad_kv_low = narrowed(grad_kv).reshape(rows_here, SEQS, KVH, 2, 2, HD)
    grad_kv_low = grad_kv_low.transpose(0, 3, 1, 4, 2, 5).reshape(-1, 2 * kv_width)
    grad_query_tokens = from_groups(narrowed(grad_queries), rows_here) * query_scale
    grad_query_raw = rotate_back(
        grad_query_tokens.reshape(-1, H, HD), cosine_table, sine_table
    ).reshape(-1, H * HD)
    grad_key_raw = rotate_back(
        grad_kv_low[:, :kv_width].reshape(-1, KVH, HD), cosine_table, sine_table
    ).reshape(-1, kv_width)
    grad_projected = jnp.concatenate(
        [grad_query_raw, grad_key_raw, grad_kv_low[:, kv_width:]], -1
    ).astype(jnp.bfloat16)
    grad_bias = jnp.sum(grad_projected, 0, dtype=jnp.float32)
    grad_normed_one = lax.dot_general(
        grad_projected, w_qkv_all, CONTRACT_LAST, preferred_element_type=jnp.float32
    )
    grad_input_norm, grad_gain_one = norm_back(grad_normed_one, unit_one, scale_one, gain_one)
    grad_input = (grad_middle + grad_input_norm).reshape(rows_here, slots, D)
    qkv_terms = lax.dot_general(
        normed_one, grad_projected, CONTRACT_FIRST, preferred_element_type=jnp.float32
    ).astype(jnp.bfloat16)
    small_terms = jnp.concatenate(
        [
            part.reshape(shard_count, -1)
            for part in (grad_gain_one, grad_gain_two, grad_bias[:QK], grad_bias[QK:])
        ],
        1,
    )
    small_terms = small_terms.reshape(ctx_size * shard_count, small_width)
    small_terms = jnp.pad(small_terms, ((0, 0), (0, 8 * HD - small_width)))
    qkv_rows, small_rows, o_rows = scatter(
        [
            qkv_terms.reshape(-1, cut, QKV),
            small_terms.reshape(-1, 8, HD),
        ],
        by_rows,
        4,
        spread_ctx=True,
        lines=[o_terms.reshape(shard_count, ctx_size, cut, D)],
    )
    small_rows = small_rows.reshape(ctx_size, -1)[:, :small_width].reshape(-1)
    bias_start = 2 * gain_width
    value_start = bias_start + QK // shard_count

    gate_rows, up_rows = unpack(gate_up_rows, columns)
    return (
        output,
        grad_input,
        small_rows[:gain_width],
        qkv_rows.reshape(-1, QKV).astype(jnp.float32),
        small_rows[bias_start:value_start],
        small_rows[value_start:],
        o_rows.reshape(-1, D),
        small_rows[gain_width:bias_start],
        gate_rows.reshape(-1, FF),
        up_rows.reshape(-1, FF),
        down_rows[:columns].astype(jnp.float32),
    )


def solution(mesh):
    in_specs = (
        P(("ctx", "fsdp"), None, None),
        P(),
        P("fsdp"),
        P("fsdp", None),
        P("fsdp"),
        P("fsdp", None),
        P("fsdp"),
        P("fsdp", None),
        P("fsdp", None),
        P("fsdp", None),
        P(("ctx", "fsdp"), None, None),
    )
    out_specs = (
        P(("ctx", "fsdp"), None, None),
        P(("ctx", "fsdp"), None, None),
        P("fsdp"),
        P("fsdp", None),
        P("fsdp"),
        P("fsdp"),
        P("fsdp", None),
        P("fsdp"),
        P("fsdp", None),
        P("fsdp", None),
        P("fsdp", None),
    )
    return jax.shard_map(shards, mesh=mesh, in_specs=in_specs, out_specs=out_specs, check_vma=False)
```

```python
import functools

import jax
import jax.numpy as jnp
from jax import lax
from jax.experimental import pallas as pl
from jax.experimental.pallas import tpu as pltpu
from jax.sharding import PartitionSpec as P

D = 1536
H = 12
KVH = 2
HD = 128
FF = 8960
SEQS = 2
QKV = 2048
QK = 1792


EPS = 1e-06
THETA = 1000000.0
NEG_FILL = -1e30
MESH_ID = pl.DeviceIdType.MESH
CONTRACT_LAST = (((1,), (1,)), ((), ()))
CONTRACT_FIRST = (((0,), (0,)), ((), ()))


def narrowed(values):
    return lax.optimization_barrier(values.astype(jnp.bfloat16)).astype(jnp.float32)


def block_positions(block_order, first_row, row_count, block_rows, ctx_size):
    row_index = first_row + jnp.arange(row_count, dtype=jnp.int32)
    slot_index = jnp.arange(2 * SEQS, dtype=jnp.int32)
    entries = (slot_index // SEQS)[None, :] * ctx_size + (row_index // block_rows)[:, None]
    tiled = jnp.tile(block_order, (2, 1))
    entry_ids = jnp.arange(2 * ctx_size, dtype=jnp.int32)
    picked = jnp.sum(
        jnp.where(entries[:, :, None] == entry_ids[None, None, :], tiled[None, :, :], 0), -1
    )
    return picked * block_rows + (row_index % block_rows)[:, None]


def to_groups(tokens, row_count):
    shaped = tokens.reshape(row_count, 2, SEQS, KVH, H // KVH, HD)
    return shaped.transpose(2, 1, 3, 4, 0, 5).reshape(SEQS, 2, KVH, H // KVH * row_count, HD)


def from_groups(grouped, row_count):
    shaped = grouped.reshape(SEQS, 2, KVH, H // KVH, row_count, HD).transpose(4, 1, 0, 2, 3, 5)
    return shaped.reshape(row_count * 2 * SEQS, H * HD)


def rope_tables(positions):
    half_width = HD // 2
    frequency = THETA ** (-jnp.arange(half_width, dtype=jnp.float32) * 2.0 / HD)
    angles = positions.astype(jnp.float32)[:, None] * frequency[None, :]
    cosine_table = jnp.concatenate([jnp.cos(angles), jnp.cos(angles)], -1)[:, None, :]
    sine_table = jnp.concatenate([jnp.sin(angles), jnp.sin(angles)], -1)[:, None, :]
    return (cosine_table, sine_table)


def rotate(head_values, cosine_table, sine_table):
    half_width = HD // 2
    turned = jnp.concatenate([-head_values[..., half_width:], head_values[..., :half_width]], -1)
    return head_values * cosine_table + turned * sine_table


def rotate_back(grad_values, cosine_table, sine_table):
    half_width = HD // 2
    moved = grad_values * sine_table
    return grad_values * cosine_table + jnp.concatenate(
        [moved[..., half_width:], -moved[..., :half_width]], -1
    )


def normalize(values, gain):
    scale = lax.rsqrt(jnp.mean(values * values, -1, keepdims=True) + EPS)
    unit = values * scale
    return (unit, scale, unit * gain)


def norm_back(grad_out, unit, scale, gain):
    grad_unit = grad_out * gain
    inner = jnp.mean(grad_unit * unit, -1, keepdims=True)
    return (scale * (grad_unit - unit * inner), jnp.sum(grad_out * unit, 0))


def attend_forward_kernel(ctx_size, block_rows, rows_here, scalars, q_ref, kv_ref, out_ref, stat_ref, best_ref, total_ref, accum_ref):
    seq = pl.program_id(0)
    blocks = 2 * ctx_size
    own_ctx = scalars[SEQS * blocks]
    own_shard = scalars[SEQS * blocks + 1]
    lanes = q_ref.shape[3]
    best_ref[...] = jnp.full(best_ref.shape, NEG_FILL, jnp.float32)
    total_ref[...] = jnp.zeros(total_ref.shape, jnp.float32)
    accum_ref[...] = jnp.zeros(accum_ref.shape, jnp.float32)

    def step(key_ctx, half_key, half):
        order_key = scalars[seq * blocks + half_key * ctx_size + key_ctx]
        order_query = scalars[seq * blocks + half * ctx_size + own_ctx]

        def work(masked):
            rows = pl.ds(pl.multiple_of(key_ctx * block_rows, block_rows), block_rows)
            keys = kv_ref[rows, half_key * 2 * HD : half_key * 2 * HD + HD]
            values = kv_ref[rows, half_key * 2 * HD + HD : half_key * 2 * HD + 2 * HD]
            scores = lax.dot_general(
                keys, q_ref[0, half, 0], CONTRACT_LAST, preferred_element_type=jnp.float32
            )
            if masked:
                row = lax.broadcasted_iota(jnp.int32, (block_rows, lanes), 0)
                lane = lax.broadcasted_iota(jnp.int32, (block_rows, lanes), 1)
                scores = jnp.where(
                    row <= own_shard * rows_here + lax.rem(lane, rows_here), scores, NEG_FILL
                )
            best = best_ref[half]
            fresh = jnp.maximum(best, jnp.max(scores, 0, keepdims=True))
            decay = jnp.exp(best - fresh)
            weights = jnp.exp(scores - fresh)
            total_ref[half] = total_ref[half] * decay + jnp.sum(weights, 0, keepdims=True)
            accum_ref[half] = accum_ref[half] * decay + lax.dot_general(
                values,
                weights.astype(jnp.bfloat16),
                CONTRACT_FIRST,
                preferred_element_type=jnp.float32,
            )
            best_ref[half] = fresh

        @pl.when(order_key < order_query)
        def full():
            work(False)

        @pl.when(order_key == order_query)
        def diagonal():
            work(True)

    @pl.loop(0, ctx_size)
    def sweep(key_ctx):
        for half_key in range(2):
            for half in range(2):
                step(key_ctx, half_key, half)

    for half in range(2):
        totals = total_ref[half]
        out_ref[0, half, 0] = (accum_ref[half] / totals).T
        stat_ref[0, half, 0] = best_ref[half] + jnp.log(totals)


def attend_forward(scalars, queries, all_kv, ctx_size, block_rows, rows_here):
    lanes = queries.shape[3]
    kernel = functools.partial(attend_forward_kernel, ctx_size, block_rows, rows_here)
    group = pl.BlockSpec((1, 2, 1, lanes, HD), lambda s, n, _: (s, 0, n, 0, 0))
    stat = pl.BlockSpec((1, 2, 1, 1, lanes), lambda s, n, _: (s, 0, n, 0, 0))
    return pl.pallas_call(
        kernel,
        grid_spec=pltpu.PrefetchScalarGridSpec(
            num_scalar_prefetch=1,
            grid=(SEQS, KVH),
            in_specs=[
                group,
                pl.BlockSpec((all_kv.shape[0], 4 * HD), lambda s, n, _: (0, s * KVH + n)),
            ],
            out_specs=[group, stat],
            scratch_shapes=[
                pltpu.VMEM((2, 1, lanes), jnp.float32),
                pltpu.VMEM((2, 1, lanes), jnp.float32),
                pltpu.VMEM((2, HD, lanes), jnp.float32),
            ],
        ),
        out_shape=(
            jax.ShapeDtypeStruct(queries.shape, jnp.float32),
            jax.ShapeDtypeStruct((SEQS, 2, KVH, 1, lanes), jnp.float32),
        ),
        compiler_params=pltpu.CompilerParams(vmem_limit_bytes=56 * 2**20),
        name="attend_forward",
    )(scalars, queries, all_kv)


def attend_backward_kernel(ctx_size, block_rows, rows_here, scalars, q_ref, go_ref, att_ref, stat_ref, kv_ref, gq_ref, gkv_ref, delta_ref, gq_acc, gk_acc, gv_acc):
    seq = pl.program_id(0)
    blocks = 2 * ctx_size
    own_ctx = scalars[SEQS * blocks]
    own_shard = scalars[SEQS * blocks + 1]
    lanes = q_ref.shape[3]
    gq_acc[...] = jnp.zeros(gq_acc.shape, jnp.float32)
    for half in range(2):
        product = go_ref[0, half, 0].astype(jnp.float32) * att_ref[0, half, 0]
        delta_ref[half] = jnp.sum(product.T, 0, keepdims=True)

    def step(key_ctx, half_key, half):
        order_key = scalars[seq * blocks + half_key * ctx_size + key_ctx]
        order_query = scalars[seq * blocks + half * ctx_size + own_ctx]

        def work(masked):
            rows = pl.ds(pl.multiple_of(key_ctx * block_rows, block_rows), block_rows)
            keys = kv_ref[rows, half_key * 2 * HD : half_key * 2 * HD + HD]
            values = kv_ref[rows, half_key * 2 * HD + HD : half_key * 2 * HD + 2 * HD]
            queries = q_ref[0, half, 0]
            grad_out = go_ref[0, half, 0]
            scores = lax.dot_general(
                keys, queries, CONTRACT_LAST, preferred_element_type=jnp.float32
            )
            probs = jnp.exp(scores - stat_ref[0, half, 0])
            if masked:
                row = lax.broadcasted_iota(jnp.int32, (block_rows, lanes), 0)
                lane = lax.broadcasted_iota(jnp.int32, (block_rows, lanes), 1)
                probs = jnp.where(
                    row <= own_shard * rows_here + lax.rem(lane, rows_here), probs, 0.0
                )
            grad_probs = lax.dot_general(
                values, grad_out, CONTRACT_LAST, preferred_element_type=jnp.float32
            )
            grad_scores = (probs * (grad_probs - delta_ref[half])).astype(jnp.bfloat16)
            gv_acc[...] += jnp.dot(
                probs.astype(jnp.bfloat16), grad_out, preferred_element_type=jnp.float32
            )
            gk_acc[...] += jnp.dot(grad_scores, queries, preferred_element_type=jnp.float32)
            gq_acc[half] += lax.dot_general(
                keys, grad_scores, CONTRACT_FIRST, preferred_element_type=jnp.float32
            )

        @pl.when(order_key < order_query)
        def full():
            work(False)

        @pl.when(order_key == order_query)
        def diagonal():
            work(True)

    @pl.loop(0, ctx_size)
    def sweep(key_ctx):
        rows = pl.ds(pl.multiple_of(key_ctx * block_rows, block_rows), block_rows)
        for half_key in range(2):
            gk_acc[...] = jnp.zeros(gk_acc.shape, jnp.float32)
            gv_acc[...] = jnp.zeros(gv_acc.shape, jnp.float32)
            for half in range(2):
                step(key_ctx, half_key, half)
            at = half_key * 2 * HD
            gkv_ref[rows, at : at + HD] = gk_acc[...].astype(jnp.bfloat16)
            gkv_ref[rows, at + HD : at + 2 * HD] = gv_acc[...].astype(jnp.bfloat16)

    for half in range(2):
        gq_ref[0, half, 0] = gq_acc[half].T


def attend_backward(scalars, queries, grad_out, attended, stats, all_kv, ctx_size, block_rows, rows_here):
    lanes = queries.shape[3]
    kernel = functools.partial(attend_backward_kernel, ctx_size, block_rows, rows_here)
    group = pl.BlockSpec((1, 2, 1, lanes, HD), lambda s, n, _: (s, 0, n, 0, 0))
    stat = pl.BlockSpec((1, 2, 1, 1, lanes), lambda s, n, _: (s, 0, n, 0, 0))
    full = pl.BlockSpec((all_kv.shape[0], 4 * HD), lambda s, n, _: (0, s * KVH + n))
    return pl.pallas_call(
        kernel,
        grid_spec=pltpu.PrefetchScalarGridSpec(
            num_scalar_prefetch=1,
            grid=(SEQS, KVH),
            in_specs=[group, group, group, stat, full],
            out_specs=[group, full],
            scratch_shapes=[
                pltpu.VMEM((2, 1, lanes), jnp.float32),
                pltpu.VMEM((2, HD, lanes), jnp.float32),
                pltpu.VMEM((block_rows, HD), jnp.float32),
                pltpu.VMEM((block_rows, HD), jnp.float32),
            ],
        ),
        out_shape=(
            jax.ShapeDtypeStruct(queries.shape, jnp.float32),
            jax.ShapeDtypeStruct(all_kv.shape, jnp.bfloat16),
        ),
        compiler_params=pltpu.CompilerParams(vmem_limit_bytes=56 * 2**20),
        name="attend_backward",
    )(scalars, queries, grad_out, attended, stats, all_kv)


def peers_of(ctx_size):
    return ctx_size == 4, range(1, ctx_size)


def ctx_target(position, way, square, ctx_size):
    return position ^ way if square else lax.rem(position + way, ctx_size)


def ctx_source(position, way, square, ctx_size):
    return position ^ way if square else lax.rem(position + ctx_size - way, ctx_size)


def greet(ctx_size, pair_count, with_ctx, all_shards):
    ctx = lax.axis_index("ctx")
    shard = lax.axis_index("fsdp")
    pair, core = shard // 2, shard % 2
    barrier = pltpu.get_barrier_semaphore()
    partners = [(ctx, pair * 2 + 1 - core)]
    for step in range(1, pair_count):
        there = lax.rem(pair + step, pair_count) * 2
        partners.append((ctx, there + core))
        if all_shards:
            partners.append((ctx, there + 1 - core))
    if with_ctx:
        for way in range(1, ctx_size):
            partners.append((lax.rem(ctx + way, ctx_size), shard))
    for partner in partners:
        pl.semaphore_signal(barrier, inc=1, device_id=partner, device_id_type=MESH_ID)
    pl.semaphore_wait(barrier, len(partners))
    return ctx, pair, core


class Exchange:
    def __init__(self, source, out, sems, own_sem, pair_count):
        self.source, self.out, self.sems, self.own_sem = source, out, sems, own_sem
        self.shard_count = 2 * pair_count

    def start(self):
        ctx, shard = lax.axis_index("ctx"), lax.axis_index("fsdp")
        self.own = pltpu.make_async_copy(self.source.at[shard], self.out.at[shard], self.own_sem)
        self.own.start()
        self.copies = []
        for step in range(1, self.shard_count):
            there = lax.rem(shard + step, self.shard_count)
            copy = pltpu.make_async_remote_copy(
                src_ref=self.source.at[there],
                dst_ref=self.out.at[shard],
                send_sem=self.sems[0].at[step - 1],
                recv_sem=self.sems[1].at[step - 1],
                device_id=(ctx, there),
                device_id_type=MESH_ID,
            )
            copy.start()
            self.copies.append(copy)

    def finish(self):
        ctx, shard = lax.axis_index("ctx"), lax.axis_index("fsdp")
        for step in range(1, self.shard_count):
            come = lax.rem(shard + self.shard_count - step, self.shard_count)
            pltpu.make_async_remote_copy(
                src_ref=self.out.at[come],
                dst_ref=self.out.at[come],
                send_sem=self.sems[0].at[step - 1],
                recv_sem=self.sems[1].at[step - 1],
                device_id=(ctx, shard),
                device_id_type=MESH_ID,
            ).wait_recv()
        self.own.wait()
        for copy in self.copies:
            copy.wait_send()


def exchange_kernel(pair_count, source, out, send_sem, recv_sem, own_sem):
    greet(1, pair_count, False, True)
    flow = Exchange(source, out, (send_sem, recv_sem), own_sem, pair_count)
    flow.start()
    flow.finish()


def exchange(pieces, collective_id):
    shard_count = lax.axis_size("fsdp")
    dma = pltpu.SemaphoreType.DMA
    return pl.pallas_call(
        functools.partial(exchange_kernel, shard_count // 2),
        in_specs=[pl.BlockSpec(memory_space=pltpu.VMEM)],
        out_specs=pl.BlockSpec(memory_space=pl.ANY),
        out_shape=jax.ShapeDtypeStruct(pieces.shape, pieces.dtype),
        scratch_shapes=[dma((shard_count - 1,))] * 2 + [dma],
        compiler_params=pltpu.CompilerParams(collective_id=collective_id, has_side_effects=True),
        cost_estimate=pl.CostEstimate(
            flops=0, bytes_accessed=pieces.size * 64, transcendentals=0
        ),
    )(pieces)


def gather_kernel(arity, ctx_size, pair_count, slots, swaps, wide, *refs):
    sources, refs = refs[:arity], refs[arity:]
    swap_sources, refs = refs[:swaps], refs[swaps:]
    outs, refs = refs[:arity], refs[arity:]
    swap_outs, refs = refs[:swaps], refs[swaps:]
    pair_sems, ctx_sems, core_sems = refs[0:2], refs[2:4], refs[4:6]
    local_sem = refs[6]
    square, ways = peers_of(ctx_size) if wide else (False, ())
    narrow = [item for item in range(arity) if item not in wide]
    near = [way for way in ways if not (square and way == 3)]
    ctx, pair, core = greet(ctx_size, pair_count, len(wide) > 0, swaps > 0)
    homes = [place(ctx, pair * 2 + core) for place in slots]
    started = []
    steps = [(0, 1)] + [(far, way) for far in range(1, pair_count) for way in (1, -1)]

    def present(step):
        far, way = steps[step]
        if far == 0:
            return None
        return pair >= far if way == 1 else pair + far < pair_count

    def origin(step):
        far, way = steps[step]
        return pair - far * way

    def when(condition, work):
        if condition is None:
            work()
        else:
            pl.when(condition)(work)

    def send(item, source, place, target, sems, at, condition):
        copy = pltpu.make_async_remote_copy(
            src_ref=source,
            dst_ref=outs[item].at[place],
            send_sem=sems[0].at[at],
            recv_sem=sems[1].at[at],
            device_id=target,
            device_id_type=MESH_ID,
        )
        copy.start()
        started.append((condition, item, sems, at))

    def sent(item, sems, at):
        pltpu.make_async_remote_copy(
            src_ref=outs[item].at[0],
            dst_ref=outs[item].at[0],
            send_sem=sems[0].at[at],
            recv_sem=sems[1].at[at],
            device_id=(ctx, pair * 2 + core),
            device_id_type=MESH_ID,
        ).wait_send()

    def arrive(item, place, sems, at):
        pltpu.make_async_remote_copy(
            src_ref=outs[item].at[place],
            dst_ref=outs[item].at[place],
            send_sem=sems[0].at[at],
            recv_sem=sems[1].at[at],
            device_id=(ctx, pair * 2 + core),
            device_id_type=MESH_ID,
        ).wait_recv()

    def pass_on(step, item, source, place):
        far, way = steps[step]
        for side in (1, -1) if far == 0 else (way,):

            def further(side=side):
                return pair + 1 < pair_count if side == 1 else pair >= 1

            def both(further=further):
                return further() if far == 0 else jnp.logical_and(further(), present(step))

            def work(side=side, both=both):
                send(
                    item,
                    source,
                    place,
                    (ctx, (pair + side) * 2 + core),
                    pair_sems,
                    ((side + 1) // 2, far, item),
                    both,
                )

            if far + 1 < pair_count:
                pl.when(further())(work)

    def to_core(item, source, from_ctx, way, step):
        send(
            item,
            source,
            slots[item](from_ctx, origin(step) * 2 + core),
            (ctx, pair * 2 + 1 - core),
            core_sems,
            (way, step, item),
            functools.partial(present, step),
        )

    def spread(step, items):
        for item in items:
            place = slots[item](ctx, origin(step) * 2 + core)
            source = sources[item]
            if step:
                far, way = steps[step]
                arrive(item, place, pair_sems, ((way + 1) // 2, far - 1, item))
                source = outs[item].at[place]
            pass_on(step, item, source, place)
            for way in near if item in wide else ():
                there = ctx_target(ctx, way, square, ctx_size)
                send(
                    item,
                    source,
                    place,
                    (there, pair * 2 + core),
                    ctx_sems,
                    (way - 1, step, item),
                    functools.partial(present, step),
                )
            to_core(item, source, ctx, 0, step)

    def collect(step):
        for way in near:
            for item in wide:
                come = ctx_source(ctx, way, square, ctx_size)
                place = slots[item](come, origin(step) * 2 + core)
                arrive(item, place, ctx_sems, (way - 1, step, item))
                source = outs[item].at[place]
                if square and (steps[step][0] % 2 == 0) == (way == 1):
                    send(
                        item,
                        source,
                        place,
                        (ctx ^ (3 - way), pair * 2 + core),
                        ctx_sems,
                        (2, step, item),
                        functools.partial(present, step),
                    )
                to_core(item, source, come, way, step)

    def collect_far(step):
        for item in wide:
            place = slots[item](ctx ^ 3, origin(step) * 2 + core)
            arrive(item, place, ctx_sems, (2, step, item))
            to_core(item, outs[item].at[place], ctx ^ 3, 3, step)

    locals_ = []
    for item in range(arity):
        copy = pltpu.make_async_copy(sources[item], outs[item].at[homes[item]], local_sem.at[item])
        copy.start()
        locals_.append(copy)
    spread(0, wide)
    flows = []
    count = len(steps)
    for turn in range(1, count + 4):
        if turn < count:
            when(present(turn), functools.partial(spread, turn, wide))
        if turn == count:
            spread(0, narrow)
            for item in range(swaps):
                flow = Exchange(
                    swap_sources[item],
                    swap_outs[item],
                    refs[7 + 3 * item : 9 + 3 * item],
                    refs[9 + 3 * item],
                    pair_count,
                )
                flow.start()
                flows.append(flow)
        if 0 <= turn - 2 < count:
            when(present(turn - 2), functools.partial(collect, turn - 2))
        if square and 0 <= turn - 4 < count:
            when(present(turn - 4), functools.partial(collect_far, turn - 4))

    for turn in range(1, count):
        when(present(turn), functools.partial(spread, turn, narrow))

    def from_core(step):
        for way in (0, *ways):
            come = ctx_source(ctx, way, square, ctx_size) if way else ctx
            for item in wide if way else range(arity):
                arrive(item, slots[item](come, origin(step) * 2 + 1 - core), core_sems, (way, step, item))

    for step in range(count):
        when(present(step), functools.partial(from_core, step))
    for flow in flows:
        flow.finish()
    for copy in locals_:
        copy.wait()
    for condition, *which in started:
        when(condition(), functools.partial(sent, *which))


def gather(pieces, slots, collective_id, swaps=(), wide=None):
    ctx_size, shard_count = lax.axis_size("ctx"), lax.axis_size("fsdp")
    pair_count = shard_count // 2
    arity = len(pieces)
    wide = range(arity) if wide is None else wide
    dma = pltpu.SemaphoreType.DMA
    moved = sum(piece.size for piece in pieces) * 2
    steps = 2 * pair_count - 1
    return pl.pallas_call(
        functools.partial(gather_kernel, arity, ctx_size, pair_count, slots, len(swaps), wide),
        in_specs=[pl.BlockSpec(memory_space=pltpu.VMEM)] * (arity + len(swaps)),
        out_specs=[pl.BlockSpec(memory_space=pl.ANY)] * (arity + len(swaps)),
        out_shape=[
            jax.ShapeDtypeStruct(
                ((ctx_size if item in wide else 1) * shard_count,) + piece.shape, piece.dtype
            )
            for item, piece in enumerate(pieces)
        ]
        + [jax.ShapeDtypeStruct(swap.shape, swap.dtype) for swap in swaps],
        scratch_shapes=[dma((2, pair_count - 1, arity))] * 2
        + [dma((ctx_size - 1, steps, arity))] * 2
        + [dma((ctx_size, steps, arity))] * 2
        + [dma((arity,))]
        + [dma((shard_count - 1,)), dma((shard_count - 1,)), dma] * len(swaps),
        compiler_params=pltpu.CompilerParams(collective_id=collective_id, has_side_effects=True),
        cost_estimate=pl.CostEstimate(
            flops=0, bytes_accessed=moved * ctx_size * shard_count * 4, transcendentals=0
        ),
    )(*pieces, *swaps)


class LineScatter:
    def __init__(self, source, out, half, room, sems, where, counts, last):
        self.count, self.ctx_size = counts
        self.source, self.out, self.half, self.room = source, out, half, room
        self.last = last
        self.core_sems, self.pair_sems = sems[0:2], sems[2:4]
        self.ctx, self.pair, self.core = where
        self.order = [*range(1, self.count), 0]

    def copy(self, source, target, device, sems, at):
        return pltpu.make_async_remote_copy(
            src_ref=source,
            dst_ref=target,
            send_sem=sems[0].at[at],
            recv_sem=sems[1].at[at],
            device_id=device,
            device_id_type=MESH_ID,
        )

    def here(self):
        return (self.ctx, self.pair * 2 + self.core)

    def toward(self, step):
        return lax.rem(self.pair + step, self.count)

    def start(self):
        self.copies = []
        for step in self.order:
            self.copies.append(
                self.copy(
                    self.source.at[self.toward(step) * 2 + 1 - self.core],
                    self.half.at[step],
                    (self.ctx, self.pair * 2 + 1 - self.core),
                    self.core_sems,
                    step,
                )
            )
            self.copies[-1].start()

    def fold(self, step):
        half = self.half.at[step]
        self.copy(half, half, self.here(), self.core_sems, step).wait_recv()
        mine = self.source[self.toward(step) * 2 + self.core].astype(jnp.float32)
        total = mine + half[...].astype(jnp.float32)
        if step == 0:
            self.out[...] = total
            return
        half[...] = total.astype(half.dtype)
        self.copies.append(
            self.copy(
                half,
                self.room.at[step - 1],
                (self.ctx, self.toward(step) * 2 + self.core),
                self.pair_sems,
                step - 1,
            )
        )
        self.copies[-1].start()

    def over_ctx(self, terms, room, landing, *sems):
        shard = self.pair * 2 + self.core
        copies = []

        def send(source, target, way, sems):
            there = lax.rem(self.ctx + way, self.ctx_size)
            copies.append(self.copy(source(there), target, (there, shard), sems, way - 1))
            copies[-1].start()

        def arrive(target, way, sems):
            self.copy(target, target, self.here(), sems, way - 1).wait_recv()

        terms[...] = self.out[...].astype(terms.dtype)
        for way in range(1, self.ctx_size):
            send(lambda there: terms.at[there], room.at[way - 1], way, sems[0:2])
        total = self.out[self.ctx]
        for way in range(1, self.ctx_size):
            arrive(room.at[way - 1], way, sems[0:2])
            total = total + room[way - 1].astype(jnp.float32)
        landing[self.ctx] = total.astype(landing.dtype)
        for way in range(1, self.ctx_size):
            send(lambda there: landing.at[self.ctx], landing.at[self.ctx], way, sems[2:4])
        for way in range(1, self.ctx_size):
            come = lax.rem(self.ctx + self.ctx_size - way, self.ctx_size)
            arrive(landing.at[come], way, sems[2:4])
        self.out[...] = landing[...].astype(jnp.float32)
        for copy in copies:
            copy.wait_send()

    def finish(self):
        for step in range(1, self.count):
            room = self.room.at[step - 1]
            self.copy(room, room, self.here(), self.pair_sems, step - 1).wait_recv()
            self.out[...] += room[...].astype(jnp.float32)
        if self.last:
            self.over_ctx(*self.last)
        for copy in self.copies:
            copy.wait_send()


def scatter_kernel(arity, ctx_size, pair_count, slot, spread_ctx, lines, *refs):
    sources, refs = refs[:arity], refs[arity:]
    line_sources, refs = refs[:lines], refs[lines:]
    outs, refs = refs[:arity], refs[arity:]
    line_outs, refs = refs[:lines], refs[lines:]
    halves, relays, asides, ends, finals = (refs[i * arity : (i + 1) * arity] for i in range(5))
    sems = refs[5 * arity : 5 * arity + 10]
    core_sems, relay_sems, ctx_sems, pair_sems, last_sems = (sems[2 * i : 2 * i + 2] for i in range(5))
    square, ways = peers_of(ctx_size)
    ctx, pair, core = greet(ctx_size, pair_count, True, False)
    order = list(range(1, pair_count)) + [0]
    started = []
    flows = []
    for item in range(lines):
        at = 5 * arity + 10 + 13 * item
        spread = len(line_sources[item].shape) == 4
        flows.append(
            LineScatter(
                line_sources[item],
                line_outs[item],
                *refs[at : at + 2],
                refs[at + 2 : at + 6],
                (ctx, pair, core),
                (pair_count, ctx_size),
                refs[at + 6 : at + 13] if spread else (),
            )
        )

    def send(source, target, device, pair_of_sems, at):
        copy = pltpu.make_async_remote_copy(
            src_ref=source,
            dst_ref=target,
            send_sem=pair_of_sems[0].at[at],
            recv_sem=pair_of_sems[1].at[at],
            device_id=device,
            device_id_type=MESH_ID,
        )
        copy.start()
        started.append(copy)

    def arrive(target, pair_of_sems, at):
        pltpu.make_async_remote_copy(
            src_ref=target,
            dst_ref=target,
            send_sem=pair_of_sems[0].at[at],
            recv_sem=pair_of_sems[1].at[at],
            device_id=(ctx, pair * 2 + core),
            device_id_type=MESH_ID,
        ).wait_recv()

    def toward(step):
        return lax.rem(pair + step, pair_count)

    def target_ctx(way):
        return ctx_target(ctx, way, square, ctx_size) if way else ctx

    def f32(value):
        return value.astype(jnp.float32)

    far_first = [3, 1, 2, 0] if square else list(ways) + [0]
    for step in order:
        for way in far_first:
            for item in range(arity):
                send(
                    sources[item].at[slot(target_ctx(way), toward(step) * 2 + 1 - core)],
                    halves[item].at[way, step],
                    (ctx, pair * 2 + 1 - core),
                    core_sems,
                    (way, step, item),
                )

    def fold_core(step):
        for way in far_first:
            for item in range(arity):
                half = halves[item].at[way, step]
                arrive(half, core_sems, (way, step, item))
                mine = sources[item][slot(target_ctx(way), toward(step) * 2 + core)]
                half[...] = (f32(mine) + f32(half[...])).astype(half.dtype)
                if square and way == 3:
                    there = ctx ^ (1 if step % 2 == 0 else 2)
                    send(
                        half,
                        relays[item].at[step],
                        (there, pair * 2 + core),
                        relay_sems,
                        (step, item),
                    )

    def fold_relay(step):
        for item in range(arity):
            if square:
                relay = relays[item].at[step]
                arrive(relay, relay_sems, (step, item))
                half = halves[item].at[2 if step % 2 == 0 else 1, step]
                half[...] = (f32(half[...]) + f32(relay[...])).astype(half.dtype)
            for way in ways:
                if square and way == 3:
                    continue
                send(
                    halves[item].at[way, step],
                    asides[item].at[way - 1, step],
                    (target_ctx(way), pair * 2 + core),
                    ctx_sems,
                    (way - 1, step, item),
                )

    def fold_ctx(step):
        for item in range(arity):
            half = halves[item].at[0, step]
            total = f32(half[...])
            for way in ways:
                if square and way == 3:
                    continue
                aside = asides[item].at[way - 1, step]
                arrive(aside, ctx_sems, (way - 1, step, item))
                total = total + f32(aside[...])
            if step:
                half[...] = total.astype(half.dtype)
                send(
                    half,
                    ends[item].at[step - 1],
                    (ctx, toward(step) * 2 + core),
                    pair_sems,
                    (step - 1, item),
                )
            else:
                for other in range(1, pair_count):
                    end = ends[item].at[other - 1]
                    arrive(end, pair_sems, (other - 1, item))
                    total = total + f32(end[...])
                if spread_ctx:
                    finals[item][...] = total.astype(finals[item].dtype)
                else:
                    outs[item][...] = total.astype(outs[item].dtype)

    for flow in flows:
        flow.start()
    for turn in range(pair_count + 2):
        if turn < pair_count:
            fold_core(order[turn])
        if 1 <= turn <= pair_count:
            fold_relay(order[turn - 1])
            for flow in flows:
                flow.fold(order[turn - 1])
        if turn >= 2:
            fold_ctx(order[turn - 2])
    if spread_ctx:
        for item in range(arity):
            for way in ways:
                send(
                    finals[item],
                    outs[item].at[ctx],
                    (target_ctx(way), pair * 2 + core),
                    last_sems,
                    (way - 1, item),
                )
            outs[item][ctx] = finals[item][...]
        for item in range(arity):
            for way in ways:
                arrive(outs[item].at[ctx_source(ctx, way, square, ctx_size)], last_sems, (way - 1, item))
    for flow in flows:
        flow.finish()
    for copy in started:
        copy.wait_send()


def scatter(terms, slot, collective_id, spread_ctx=False, out_dtype=None, lines=()):
    ctx_size, shard_count = lax.axis_size("ctx"), lax.axis_size("fsdp")
    pair_count = shard_count // 2
    arity = len(terms)
    dma = pltpu.SemaphoreType.DMA
    lead = (ctx_size,) if spread_ctx else ()
    asides = 2 if ctx_size == 4 else ctx_size - 1

    def room(*extent):
        return [pltpu.VMEM(extent + term.shape[1:], term.dtype) for term in terms]

    def line_room(line):
        if len(line.shape) == 3:
            return [pltpu.VMEM((8, HD), line.dtype)] * 3 + [dma((1,))] * 4
        cut = line.shape[2:]
        rooms = [pltpu.VMEM((count,) + cut, line.dtype) for count in (ctx_size, ctx_size - 1, ctx_size)]
        return rooms + [dma((ctx_size - 1,))] * 4

    moved = sum(term.size * term.dtype.itemsize for term in terms)
    return pl.pallas_call(
        functools.partial(scatter_kernel, arity, ctx_size, pair_count, slot, spread_ctx, len(lines)),
        in_specs=[pl.BlockSpec(memory_space=pltpu.VMEM)] * (arity + len(lines)),
        out_specs=[pl.BlockSpec(memory_space=pltpu.VMEM)] * (arity + len(lines)),
        out_shape=[
            jax.ShapeDtypeStruct(lead + term.shape[1:], out_dtype or term.dtype) for term in terms
        ]
        + [jax.ShapeDtypeStruct(line.shape[1:], jnp.float32) for line in lines],
        scratch_shapes=room(ctx_size, pair_count)
        + room(pair_count)
        + room(asides, pair_count)
        + room(pair_count - 1)
        + room()
        + [dma((ctx_size, pair_count, arity))] * 2
        + [dma((pair_count, arity))] * 2
        + [dma((ctx_size - 1, pair_count, arity))] * 2
        + [dma((pair_count - 1, arity))] * 2
        + [dma((ctx_size - 1, arity))] * 2
        + [
            scratch
            for line in lines
            for scratch in [
                pltpu.VMEM((pair_count,) + line.shape[1:], line.dtype),
                pltpu.VMEM((pair_count - 1,) + line.shape[1:], line.dtype),
            ]
            + [dma((pair_count,))] * 4
            + line_room(line)
        ],
        compiler_params=pltpu.CompilerParams(
            collective_id=collective_id, has_side_effects=True, vmem_limit_bytes=63 * 2**20
        ),
        cost_estimate=pl.CostEstimate(flops=0, bytes_accessed=moved * 16, transcendentals=0),
    )(*terms, *lines)


def line_sum_kernel(pair_count, source, out, half, room, *sems):
    where = greet(1, pair_count, False, False)
    flow = LineScatter(source, out, half, room, sems, where, (pair_count, 1), ())
    flow.start()
    for step in flow.order:
        flow.fold(step)
    flow.finish()


def line_sum(terms, collective_id):
    pair_count = lax.axis_size("fsdp") // 2
    extent = terms.shape[1:]
    dma = pltpu.SemaphoreType.DMA((pair_count,))
    return pl.pallas_call(
        functools.partial(line_sum_kernel, pair_count),
        in_specs=[pl.BlockSpec(memory_space=pltpu.VMEM)],
        out_specs=pl.BlockSpec(memory_space=pltpu.VMEM),
        out_shape=jax.ShapeDtypeStruct(extent, jnp.float32),
        scratch_shapes=[
            pltpu.VMEM((pair_count,) + extent, terms.dtype),
            pltpu.VMEM((pair_count - 1,) + extent, terms.dtype),
        ]
        + [dma] * 4,
        compiler_params=pltpu.CompilerParams(
            collective_id=collective_id, has_side_effects=True, vmem_limit_bytes=63 * 2**20
        ),
        cost_estimate=pl.CostEstimate(flops=0, bytes_accessed=terms.size * 16, transcendentals=0),
    )(terms)


def pack_kernel(columns, gate_ref, up_ref, out_ref):
    width = out_ref.shape[2] // 2
    cut = out_ref.shape[1]
    for there in range(out_ref.shape[0]):
        for side, ref in enumerate((gate_ref, up_ref)):
            at = side * width
            out_ref[there, :, at + width - HD : at + width] = jnp.zeros((cut, HD), out_ref.dtype)
            out_ref[there, :, at : at + columns] = ref[:, there * columns : (there + 1) * columns]


def pack(gate, up, shard_count, columns, width):
    return pl.pallas_call(
        functools.partial(pack_kernel, columns),
        in_specs=[pl.BlockSpec(memory_space=pltpu.VMEM)] * 2,
        out_specs=pl.BlockSpec(memory_space=pltpu.VMEM),
        out_shape=jax.ShapeDtypeStruct((shard_count, gate.shape[0], 2 * width), gate.dtype),
        name="pack",
    )(gate, up)


def unpack_kernel(columns, in_ref, gate_ref, up_ref):
    width = in_ref.shape[3] // 2
    for there in range(in_ref.shape[1]):
        for side, ref in enumerate((gate_ref, up_ref)):
            part = in_ref[0, there, :, side * width : side * width + columns]
            ref[0, :, there * columns : (there + 1) * columns] = part.astype(jnp.float32)


def unpack(rows, columns):
    ctx_size, shard_count, cut, _ = rows.shape
    out = jax.ShapeDtypeStruct((ctx_size, cut, shard_count * columns), jnp.float32)
    return pl.pallas_call(
        functools.partial(unpack_kernel, columns),
        grid=(ctx_size,),
        in_specs=[pl.BlockSpec((1,) + rows.shape[1:], lambda c: (c, 0, 0, 0))],
        out_specs=[pl.BlockSpec((1, cut, shard_count * columns), lambda c: (c, 0, 0))] * 2,
        out_shape=[out, out],
        name="unpack",
    )(rows)


def shards(
    layer_input,
    block_order,
    first_gain,
    w_qkv,
    b_qkv,
    w_o,
    second_gain,
    w_gate,
    w_up,
    w_down,
    cotangent,
):
    ctx_size = lax.axis_size("ctx")
    shard_count = lax.axis_size("fsdp")
    own_ctx = lax.axis_index("ctx")
    own_shard = lax.axis_index("fsdp")
    rows_here = layer_input.shape[0]
    slots = layer_input.shape[1]
    block_rows = rows_here * shard_count
    kv_width = KVH * HD
    cut = D // (ctx_size * shard_count)
    columns = FF // shard_count
    first_row = (own_ctx * shard_count + own_shard) * rows_here
    own_pos = block_positions(block_order, first_row, rows_here, block_rows, ctx_size)
    cosine_table, sine_table = rope_tables(own_pos.reshape(-1))
    query_scale = HD ** (-0.5)

    def by_rows(ctx, shard):
        return shard * ctx_size + ctx

    def by_tokens(ctx, shard):
        return ctx * shard_count + shard

    def own_cut(weight):
        return lax.dynamic_slice_in_dim(weight, own_ctx * cut, cut, 0)

    def mix_features(values):
        shaped = values.reshape(-1, shard_count, ctx_size, cut)
        return shaped.transpose(0, 2, 1, 3).reshape(-1, D)

    def unmix_features(values):
        shaped = values.reshape(-1, ctx_size, shard_count, cut)
        return shaped.transpose(0, 2, 1, 3).reshape(-1, D)

    small = jnp.concatenate([b_qkv, first_gain, second_gain]).reshape(ctx_size, -1)
    small_width = small.shape[1]
    small = lax.dynamic_slice_in_dim(small, own_ctx, 1, 0)
    small = jnp.pad(small, ((0, 0), (0, 16 * HD - small_width))).reshape(16, HD)
    width = -(-columns // HD) * HD
    w_qkv_all, w_o_all, small_all = gather(
        [own_cut(w_qkv), own_cut(w_o), small], [by_rows, by_rows, by_rows], 1
    )
    cotangent_all = lax.all_gather(cotangent.reshape(-1, D), "fsdp", axis=0, tiled=True)
    w_qkv_all = w_qkv_all.reshape(D, QKV)
    w_o_all = w_o_all.reshape(D, D)
    small_all = small_all.reshape(shard_count, ctx_size, -1)[:, :, :small_width]
    small_all = small_all.reshape(shard_count, -1).astype(jnp.float32)
    bias_width = QKV // shard_count
    gain_width = D // shard_count
    bias_all = small_all[:, :bias_width].reshape(-1)
    gain_one = small_all[:, bias_width : bias_width + gain_width].reshape(-1)
    gain_two = small_all[:, bias_width + gain_width :].reshape(-1)

    down_padded = jnp.pad(w_down, ((0, width - columns), (0, 0)))

    inputs = layer_input.reshape(-1, D).astype(jnp.float32)
    unit_one, scale_one, normed = normalize(inputs, gain_one)
    normed_one = normed.astype(jnp.bfloat16)
    projected = jnp.dot(normed_one, w_qkv_all, preferred_element_type=jnp.float32) + bias_all
    query_raw = projected[:, : H * HD].reshape(-1, H, HD)
    key_raw = projected[:, H * HD : H * HD + kv_width].reshape(-1, KVH, HD)
    value_raw = projected[:, H * HD + kv_width :]
    query_tokens = (
        (rotate(query_raw, cosine_table, sine_table) * query_scale)
        .astype(jnp.bfloat16)
        .reshape(-1, H * HD)
    )
    key_tokens = (
        rotate(key_raw, cosine_table, sine_table).astype(jnp.bfloat16).reshape(-1, kv_width)
    )
    own_kv = jnp.stack([key_tokens, value_raw.astype(jnp.bfloat16)], 1)
    own_kv = own_kv.reshape(rows_here, 2, SEQS, 2, KVH, HD).transpose(0, 2, 4, 1, 3, 5)
    own_kv = own_kv.reshape(rows_here, SEQS * KVH * 4 * HD)
    all_kv, gate_up_cut = gather(
        [own_kv],
        [by_tokens],
        2,
        swaps=[pack(own_cut(w_gate), own_cut(w_up), shard_count, columns, width)],
    )
    gate_up_cols = lax.all_gather(
        gate_up_cut.reshape(shard_count * cut, 2 * width), "ctx", axis=0, tiled=True
    )
    all_kv = all_kv.reshape(-1, SEQS * KVH * 4 * HD)
    queries = to_groups(query_tokens, rows_here)
    scalars = jnp.concatenate(
        [block_order.reshape(-1), jnp.stack([own_ctx, own_shard]).astype(jnp.int32)]
    )
    attended_grouped, stats = attend_forward(
        scalars, queries, all_kv, ctx_size, block_rows, rows_here
    )
    attended_low = from_groups(attended_grouped, rows_here).astype(jnp.bfloat16)
    middle = inputs + jnp.dot(attended_low, w_o_all, preferred_element_type=jnp.float32)
    unit_two, scale_two, normed = normalize(middle, gain_two)
    normed_two = mix_features(normed.astype(jnp.bfloat16))

    (tokens_all,) = gather([normed_two], [lambda ctx, shard: shard], 6, wide=())
    tokens_all = tokens_all.reshape(-1, D)
    gate_up_part = jnp.dot(tokens_all, gate_up_cols, preferred_element_type=jnp.float32)
    gate_part, up_part = gate_up_part[:, :width], gate_up_part[:, width:]
    sigmoid_gate = jax.nn.sigmoid(gate_part)
    activated = gate_part * sigmoid_gate
    hidden = (activated * up_part).astype(jnp.bfloat16)
    grad_hidden = lax.dot_general(
        cotangent_all, down_padded, CONTRACT_LAST, preferred_element_type=jnp.float32
    )
    grad_gate = grad_hidden * up_part * sigmoid_gate * (1.0 + gate_part * (1.0 - sigmoid_gate))
    grad_gate_up = jnp.concatenate([grad_gate, grad_hidden * activated], -1).astype(jnp.bfloat16)
    down_terms = lax.dot_general(
        hidden, cotangent_all, CONTRACT_FIRST, preferred_element_type=jnp.float32
    ).astype(jnp.bfloat16)
    down_rows = lax.psum(down_terms, "ctx")
    grad_gate_up, hidden, down_terms = lax.optimization_barrier(
        (grad_gate_up, hidden, down_terms)
    )
    gate_up_terms = lax.dot_general(
        tokens_all, grad_gate_up, CONTRACT_FIRST, preferred_element_type=jnp.float32
    ).astype(jnp.bfloat16)
    gate_up_rows = lax.psum_scatter(gate_up_terms, "ctx", scatter_dimension=0, tiled=True)
    grad_gate_up, hidden, gate_up_terms = lax.optimization_barrier(
        (grad_gate_up, hidden, gate_up_terms)
    )
    grad_tokens = lax.dot_general(
        grad_gate_up, gate_up_cols, CONTRACT_LAST, preferred_element_type=jnp.float32
    ).astype(jnp.bfloat16)
    grad_normed_two = line_sum(grad_tokens.reshape(shard_count, -1, D), 7)
    mixed_terms = jnp.dot(hidden, down_padded, preferred_element_type=jnp.float32).astype(jnp.bfloat16)
    grad_normed_two = unmix_features(grad_normed_two)
    grad_middle_norm, grad_gain_two = norm_back(grad_normed_two, unit_two, scale_two, gain_two)
    grad_middle = cotangent.reshape(-1, D).astype(jnp.float32) + grad_middle_norm
    grad_branch_one = grad_middle.astype(jnp.bfloat16)
    grad_attended = lax.dot_general(
        grad_branch_one, w_o_all, CONTRACT_LAST, preferred_element_type=jnp.float32
    ).astype(jnp.bfloat16)
    o_terms = lax.dot_general(
        attended_low, grad_branch_one, CONTRACT_FIRST, preferred_element_type=jnp.float32
    ).astype(jnp.bfloat16)
    grad_queries, grad_kv_full = attend_backward(
        scalars,
        queries,
        to_groups(grad_attended, rows_here),
        attended_grouped,
        stats,
        all_kv,
        ctx_size,
        block_rows,
        rows_here,
    )
    grad_kv, mixed_rows = scatter(
        [grad_kv_full.reshape(-1, rows_here, SEQS * KVH * 4 * HD)],
        by_tokens,
        3,
        out_dtype=jnp.float32,
        lines=[mixed_terms.reshape(shard_count, -1, D)],
    )
    gate_up_rows, grad_kv = lax.optimization_barrier((gate_up_rows, grad_kv))
    gate_up_rows = exchange(gate_up_rows.reshape(shard_count, cut, 2 * width), 5)
    gate_up_rows = lax.all_gather(gate_up_rows, "ctx", axis=0, tiled=False)
    mixed_out = middle + mixed_rows
    output = mixed_out.astype(jnp.bfloat16).reshape(rows_here, slots, D)
    grad_kv_low = narrowed(grad_kv).reshape(rows_here, SEQS, KVH, 2, 2, HD)
    grad_kv_low = grad_kv_low.transpose(0, 3, 1, 4, 2, 5).reshape(-1, 2 * kv_width)
    grad_query_tokens = from_groups(narrowed(grad_queries), rows_here) * query_scale
    grad_query_raw = rotate_back(
        grad_query_tokens.reshape(-1, H, HD), cosine_table, sine_table
    ).reshape(-1, H * HD)
    grad_key_raw = rotate_back(
        grad_kv_low[:, :kv_width].reshape(-1, KVH, HD), cosine_table, sine_table
    ).reshape(-1, kv_width)
    grad_projected = jnp.concatenate(
        [grad_query_raw, grad_key_raw, grad_kv_low[:, kv_width:]], -1
    ).astype(jnp.bfloat16)
    grad_bias = jnp.sum(grad_projected, 0, dtype=jnp.float32)
    grad_normed_one = lax.dot_general(
        grad_projected, w_qkv_all, CONTRACT_LAST, preferred_element_type=jnp.float32
    )
    grad_input_norm, grad_gain_one = norm_back(grad_normed_one, unit_one, scale_one, gain_one)
    grad_input = (grad_middle + grad_input_norm).reshape(rows_here, slots, D)
    qkv_terms = lax.dot_general(
        normed_one, grad_projected, CONTRACT_FIRST, preferred_element_type=jnp.float32
    ).astype(jnp.bfloat16)
    small_terms = jnp.concatenate(
        [
            part.reshape(shard_count, -1)
            for part in (grad_gain_one, grad_gain_two, grad_bias[:QK], grad_bias[QK:])
        ],
        1,
    )
    small_terms = small_terms.reshape(ctx_size * shard_count, small_width)
    small_terms = jnp.pad(small_terms, ((0, 0), (0, 8 * HD - small_width)))
    small_rows, qkv_rows, o_rows = scatter(
        [
            small_terms.reshape(-1, 8, HD),
        ],
        by_rows,
        4,
        spread_ctx=True,
        lines=[
            qkv_terms.reshape(shard_count, ctx_size, cut, QKV),
            o_terms.reshape(shard_count, ctx_size, cut, D),
        ],
    )
    small_rows = small_rows.reshape(ctx_size, -1)[:, :small_width].reshape(-1)
    bias_start = 2 * gain_width
    value_start = bias_start + QK // shard_count

    gate_rows, up_rows = unpack(gate_up_rows, columns)
    return (
        output,
        grad_input,
        small_rows[:gain_width],
        qkv_rows.reshape(-1, QKV),
        small_rows[bias_start:value_start],
        small_rows[value_start:],
        o_rows.reshape(-1, D),
        small_rows[gain_width:bias_start],
        gate_rows.reshape(-1, FF),
        up_rows.reshape(-1, FF),
        down_rows[:columns].astype(jnp.float32),
    )


def solution(mesh):
    in_specs = (
        P(("ctx", "fsdp"), None, None),
        P(),
        P("fsdp"),
        P("fsdp", None),
        P("fsdp"),
        P("fsdp", None),
        P("fsdp"),
        P("fsdp", None),
        P("fsdp", None),
        P("fsdp", None),
        P(("ctx", "fsdp"), None, None),
    )
    out_specs = (
        P(("ctx", "fsdp"), None, None),
        P(("ctx", "fsdp"), None, None),
        P("fsdp"),
        P("fsdp", None),
        P("fsdp"),
        P("fsdp"),
        P("fsdp", None),
        P("fsdp"),
        P("fsdp", None),
        P("fsdp", None),
        P("fsdp", None),
    )
    return jax.shard_map(shards, mesh=mesh, in_specs=in_specs, out_specs=out_specs, check_vma=False)
```

```python
import functools

import jax
import jax.numpy as jnp
from jax import lax
from jax.experimental import pallas as pl
from jax.experimental.pallas import tpu as pltpu
from jax.sharding import PartitionSpec as P

D = 1536
H = 12
KVH = 2
HD = 128
FF = 8960
SEQS = 2
QKV = 2048
QK = 1792


EPS = 1e-06
THETA = 1000000.0
NEG_FILL = -1e30
MESH_ID = pl.DeviceIdType.MESH
CONTRACT_LAST = (((1,), (1,)), ((), ()))
CONTRACT_FIRST = (((0,), (0,)), ((), ()))


def narrowed(values):
    return lax.optimization_barrier(values.astype(jnp.bfloat16)).astype(jnp.float32)


def block_positions(block_order, first_row, row_count, block_rows, ctx_size):
    row_index = first_row + jnp.arange(row_count, dtype=jnp.int32)
    slot_index = jnp.arange(2 * SEQS, dtype=jnp.int32)
    entries = (slot_index // SEQS)[None, :] * ctx_size + (row_index // block_rows)[:, None]
    tiled = jnp.tile(block_order, (2, 1))
    entry_ids = jnp.arange(2 * ctx_size, dtype=jnp.int32)
    picked = jnp.sum(
        jnp.where(entries[:, :, None] == entry_ids[None, None, :], tiled[None, :, :], 0), -1
    )
    return picked * block_rows + (row_index % block_rows)[:, None]


def to_groups(tokens, row_count):
    shaped = tokens.reshape(row_count, 2, SEQS, KVH, H // KVH, HD)
    return shaped.transpose(2, 1, 3, 4, 0, 5).reshape(SEQS, 2, KVH, H // KVH * row_count, HD)


def from_groups(grouped, row_count):
    shaped = grouped.reshape(SEQS, 2, KVH, H // KVH, row_count, HD).transpose(4, 1, 0, 2, 3, 5)
    return shaped.reshape(row_count * 2 * SEQS, H * HD)


def rope_tables(positions):
    half_width = HD // 2
    frequency = THETA ** (-jnp.arange(half_width, dtype=jnp.float32) * 2.0 / HD)
    angles = positions.astype(jnp.float32)[:, None] * frequency[None, :]
    cosine_table = jnp.concatenate([jnp.cos(angles), jnp.cos(angles)], -1)[:, None, :]
    sine_table = jnp.concatenate([jnp.sin(angles), jnp.sin(angles)], -1)[:, None, :]
    return (cosine_table, sine_table)


def rotate(head_values, cosine_table, sine_table):
    half_width = HD // 2
    turned = jnp.concatenate([-head_values[..., half_width:], head_values[..., :half_width]], -1)
    return head_values * cosine_table + turned * sine_table


def rotate_back(grad_values, cosine_table, sine_table):
    half_width = HD // 2
    moved = grad_values * sine_table
    return grad_values * cosine_table + jnp.concatenate(
        [moved[..., half_width:], -moved[..., :half_width]], -1
    )


def normalize(values, gain):
    scale = lax.rsqrt(jnp.mean(values * values, -1, keepdims=True) + EPS)
    unit = values * scale
    return (unit, scale, unit * gain)


def norm_back(grad_out, unit, scale, gain):
    grad_unit = grad_out * gain
    inner = jnp.mean(grad_unit * unit, -1, keepdims=True)
    return (scale * (grad_unit - unit * inner), jnp.sum(grad_out * unit, 0))


def attend_forward_kernel(ctx_size, block_rows, rows_here, scalars, q_ref, kv_ref, out_ref, stat_ref, best_ref, total_ref, accum_ref):
    seq = pl.program_id(0)
    blocks = 2 * ctx_size
    own_ctx = scalars[SEQS * blocks]
    own_shard = scalars[SEQS * blocks + 1]
    lanes = q_ref.shape[3]
    best_ref[...] = jnp.full(best_ref.shape, NEG_FILL, jnp.float32)
    total_ref[...] = jnp.zeros(total_ref.shape, jnp.float32)
    accum_ref[...] = jnp.zeros(accum_ref.shape, jnp.float32)

    def step(key_ctx, half_key, half):
        order_key = scalars[seq * blocks + half_key * ctx_size + key_ctx]
        order_query = scalars[seq * blocks + half * ctx_size + own_ctx]

        def work(masked):
            rows = pl.ds(pl.multiple_of(key_ctx * block_rows, block_rows), block_rows)
            keys = kv_ref[rows, half_key * 2 * HD : half_key * 2 * HD + HD]
            values = kv_ref[rows, half_key * 2 * HD + HD : half_key * 2 * HD + 2 * HD]
            scores = lax.dot_general(
                keys, q_ref[0, half, 0], CONTRACT_LAST, preferred_element_type=jnp.float32
            )
            if masked:
                row = lax.broadcasted_iota(jnp.int32, (block_rows, lanes), 0)
                lane = lax.broadcasted_iota(jnp.int32, (block_rows, lanes), 1)
                scores = jnp.where(
                    row <= own_shard * rows_here + lax.rem(lane, rows_here), scores, NEG_FILL
                )
            best = best_ref[half]
            fresh = jnp.maximum(best, jnp.max(scores, 0, keepdims=True))
            decay = jnp.exp(best - fresh)
            weights = jnp.exp(scores - fresh)
            total_ref[half] = total_ref[half] * decay + jnp.sum(weights, 0, keepdims=True)
            accum_ref[half] = accum_ref[half] * decay + lax.dot_general(
                values,
                weights.astype(jnp.bfloat16),
                CONTRACT_FIRST,
                preferred_element_type=jnp.float32,
            )
            best_ref[half] = fresh

        @pl.when(order_key < order_query)
        def full():
            work(False)

        @pl.when(order_key == order_query)
        def diagonal():
            work(True)

    @pl.loop(0, ctx_size)
    def sweep(key_ctx):
        for half_key in range(2):
            for half in range(2):
                step(key_ctx, half_key, half)

    for half in range(2):
        totals = total_ref[half]
        out_ref[0, half, 0] = (accum_ref[half] / totals).T
        stat_ref[0, half, 0] = best_ref[half] + jnp.log(totals)


def attend_forward(scalars, queries, all_kv, ctx_size, block_rows, rows_here):
    lanes = queries.shape[3]
    kernel = functools.partial(attend_forward_kernel, ctx_size, block_rows, rows_here)
    group = pl.BlockSpec((1, 2, 1, lanes, HD), lambda s, n, _: (s, 0, n, 0, 0))
    stat = pl.BlockSpec((1, 2, 1, 1, lanes), lambda s, n, _: (s, 0, n, 0, 0))
    return pl.pallas_call(
        kernel,
        grid_spec=pltpu.PrefetchScalarGridSpec(
            num_scalar_prefetch=1,
            grid=(SEQS, KVH),
            in_specs=[
                group,
                pl.BlockSpec((all_kv.shape[0], 4 * HD), lambda s, n, _: (0, s * KVH + n)),
            ],
            out_specs=[group, stat],
            scratch_shapes=[
                pltpu.VMEM((2, 1, lanes), jnp.float32),
                pltpu.VMEM((2, 1, lanes), jnp.float32),
                pltpu.VMEM((2, HD, lanes), jnp.float32),
            ],
        ),
        out_shape=(
            jax.ShapeDtypeStruct(queries.shape, jnp.float32),
            jax.ShapeDtypeStruct((SEQS, 2, KVH, 1, lanes), jnp.float32),
        ),
        compiler_params=pltpu.CompilerParams(vmem_limit_bytes=56 * 2**20),
        name="attend_forward",
    )(scalars, queries, all_kv)


def attend_backward_kernel(ctx_size, block_rows, rows_here, scalars, q_ref, go_ref, att_ref, stat_ref, kv_ref, gq_ref, gkv_ref, delta_ref, gq_acc, gk_acc, gv_acc):
    seq = pl.program_id(0)
    blocks = 2 * ctx_size
    own_ctx = scalars[SEQS * blocks]
    own_shard = scalars[SEQS * blocks + 1]
    lanes = q_ref.shape[3]
    gq_acc[...] = jnp.zeros(gq_acc.shape, jnp.float32)
    for half in range(2):
        product = go_ref[0, half, 0].astype(jnp.float32) * att_ref[0, half, 0]
        delta_ref[half] = jnp.sum(product.T, 0, keepdims=True)

    def step(key_ctx, half_key, half):
        order_key = scalars[seq * blocks + half_key * ctx_size + key_ctx]
        order_query = scalars[seq * blocks + half * ctx_size + own_ctx]

        def work(masked):
            rows = pl.ds(pl.multiple_of(key_ctx * block_rows, block_rows), block_rows)
            keys = kv_ref[rows, half_key * 2 * HD : half_key * 2 * HD + HD]
            values = kv_ref[rows, half_key * 2 * HD + HD : half_key * 2 * HD + 2 * HD]
            queries = q_ref[0, half, 0]
            grad_out = go_ref[0, half, 0]
            scores = lax.dot_general(
                keys, queries, CONTRACT_LAST, preferred_element_type=jnp.float32
            )
            probs = jnp.exp(scores - stat_ref[0, half, 0])
            if masked:
                row = lax.broadcasted_iota(jnp.int32, (block_rows, lanes), 0)
                lane = lax.broadcasted_iota(jnp.int32, (block_rows, lanes), 1)
                probs = jnp.where(
                    row <= own_shard * rows_here + lax.rem(lane, rows_here), probs, 0.0
                )
            grad_probs = lax.dot_general(
                values, grad_out, CONTRACT_LAST, preferred_element_type=jnp.float32
            )
            grad_scores = (probs * (grad_probs - delta_ref[half])).astype(jnp.bfloat16)
            gv_acc[...] += jnp.dot(
                probs.astype(jnp.bfloat16), grad_out, preferred_element_type=jnp.float32
            )
            gk_acc[...] += jnp.dot(grad_scores, queries, preferred_element_type=jnp.float32)
            gq_acc[half] += lax.dot_general(
                keys, grad_scores, CONTRACT_FIRST, preferred_element_type=jnp.float32
            )

        @pl.when(order_key < order_query)
        def full():
            work(False)

        @pl.when(order_key == order_query)
        def diagonal():
            work(True)

    @pl.loop(0, ctx_size)
    def sweep(key_ctx):
        rows = pl.ds(pl.multiple_of(key_ctx * block_rows, block_rows), block_rows)
        for half_key in range(2):
            gk_acc[...] = jnp.zeros(gk_acc.shape, jnp.float32)
            gv_acc[...] = jnp.zeros(gv_acc.shape, jnp.float32)
            for half in range(2):
                step(key_ctx, half_key, half)
            at = half_key * 2 * HD
            gkv_ref[rows, at : at + HD] = gk_acc[...].astype(jnp.bfloat16)
            gkv_ref[rows, at + HD : at + 2 * HD] = gv_acc[...].astype(jnp.bfloat16)

    for half in range(2):
        gq_ref[0, half, 0] = gq_acc[half].T


def attend_backward(scalars, queries, grad_out, attended, stats, all_kv, ctx_size, block_rows, rows_here):
    lanes = queries.shape[3]
    kernel = functools.partial(attend_backward_kernel, ctx_size, block_rows, rows_here)
    group = pl.BlockSpec((1, 2, 1, lanes, HD), lambda s, n, _: (s, 0, n, 0, 0))
    stat = pl.BlockSpec((1, 2, 1, 1, lanes), lambda s, n, _: (s, 0, n, 0, 0))
    full = pl.BlockSpec((all_kv.shape[0], 4 * HD), lambda s, n, _: (0, s * KVH + n))
    return pl.pallas_call(
        kernel,
        grid_spec=pltpu.PrefetchScalarGridSpec(
            num_scalar_prefetch=1,
            grid=(SEQS, KVH),
            in_specs=[group, group, group, stat, full],
            out_specs=[group, full],
            scratch_shapes=[
                pltpu.VMEM((2, 1, lanes), jnp.float32),
                pltpu.VMEM((2, HD, lanes), jnp.float32),
                pltpu.VMEM((block_rows, HD), jnp.float32),
                pltpu.VMEM((block_rows, HD), jnp.float32),
            ],
        ),
        out_shape=(
            jax.ShapeDtypeStruct(queries.shape, jnp.float32),
            jax.ShapeDtypeStruct(all_kv.shape, jnp.bfloat16),
        ),
        compiler_params=pltpu.CompilerParams(vmem_limit_bytes=56 * 2**20),
        name="attend_backward",
    )(scalars, queries, grad_out, attended, stats, all_kv)


def peers_of(ctx_size):
    return ctx_size == 4, range(1, ctx_size)


def ctx_target(position, way, square, ctx_size):
    return position ^ way if square else lax.rem(position + way, ctx_size)


def ctx_source(position, way, square, ctx_size):
    return position ^ way if square else lax.rem(position + ctx_size - way, ctx_size)


def greet(ctx_size, pair_count, with_ctx, all_shards):
    ctx = lax.axis_index("ctx")
    shard = lax.axis_index("fsdp")
    pair, core = shard // 2, shard % 2
    barrier = pltpu.get_barrier_semaphore()
    partners = [(ctx, pair * 2 + 1 - core)]
    for step in range(1, pair_count):
        there = lax.rem(pair + step, pair_count) * 2
        partners.append((ctx, there + core))
        if all_shards:
            partners.append((ctx, there + 1 - core))
    if with_ctx:
        for way in range(1, ctx_size):
            partners.append((lax.rem(ctx + way, ctx_size), shard))
    for partner in partners:
        pl.semaphore_signal(barrier, inc=1, device_id=partner, device_id_type=MESH_ID)
    pl.semaphore_wait(barrier, len(partners))
    return ctx, pair, core


class Exchange:
    def __init__(self, source, out, sems, own_sem, pair_count):
        self.source, self.out, self.sems, self.own_sem = source, out, sems, own_sem
        self.shard_count = 2 * pair_count

    def start(self):
        ctx, shard = lax.axis_index("ctx"), lax.axis_index("fsdp")
        self.own = pltpu.make_async_copy(self.source.at[shard], self.out.at[shard], self.own_sem)
        self.own.start()
        self.copies = []
        for step in range(1, self.shard_count):
            there = lax.rem(shard + step, self.shard_count)
            copy = pltpu.make_async_remote_copy(
                src_ref=self.source.at[there],
                dst_ref=self.out.at[shard],
                send_sem=self.sems[0].at[step - 1],
                recv_sem=self.sems[1].at[step - 1],
                device_id=(ctx, there),
                device_id_type=MESH_ID,
            )
            copy.start()
            self.copies.append(copy)

    def finish(self):
        ctx, shard = lax.axis_index("ctx"), lax.axis_index("fsdp")
        for step in range(1, self.shard_count):
            come = lax.rem(shard + self.shard_count - step, self.shard_count)
            pltpu.make_async_remote_copy(
                src_ref=self.out.at[come],
                dst_ref=self.out.at[come],
                send_sem=self.sems[0].at[step - 1],
                recv_sem=self.sems[1].at[step - 1],
                device_id=(ctx, shard),
                device_id_type=MESH_ID,
            ).wait_recv()
        self.own.wait()
        for copy in self.copies:
            copy.wait_send()


def exchange_kernel(pair_count, source, out, send_sem, recv_sem, own_sem):
    greet(1, pair_count, False, True)
    flow = Exchange(source, out, (send_sem, recv_sem), own_sem, pair_count)
    flow.start()
    flow.finish()


def exchange(pieces, collective_id):
    shard_count = lax.axis_size("fsdp")
    dma = pltpu.SemaphoreType.DMA
    return pl.pallas_call(
        functools.partial(exchange_kernel, shard_count // 2),
        in_specs=[pl.BlockSpec(memory_space=pltpu.VMEM)],
        out_specs=pl.BlockSpec(memory_space=pl.ANY),
        out_shape=jax.ShapeDtypeStruct(pieces.shape, pieces.dtype),
        scratch_shapes=[dma((shard_count - 1,))] * 2 + [dma],
        compiler_params=pltpu.CompilerParams(collective_id=collective_id, has_side_effects=True),
        cost_estimate=pl.CostEstimate(
            flops=0, bytes_accessed=pieces.size * 64, transcendentals=0
        ),
    )(pieces)


def gather_kernel(arity, ctx_size, pair_count, slots, swaps, wide, *refs):
    sources, refs = refs[:arity], refs[arity:]
    swap_sources, refs = refs[:swaps], refs[swaps:]
    outs, refs = refs[:arity], refs[arity:]
    swap_outs, refs = refs[:swaps], refs[swaps:]
    pair_sems, ctx_sems, core_sems = refs[0:2], refs[2:4], refs[4:6]
    local_sem = refs[6]
    square, ways = peers_of(ctx_size) if wide else (False, ())
    narrow = [item for item in range(arity) if item not in wide]
    near = [way for way in ways if not (square and way == 3)]
    ctx, pair, core = greet(ctx_size, pair_count, len(wide) > 0, swaps > 0)
    homes = [place(ctx, pair * 2 + core) for place in slots]
    started = []
    steps = [(0, 1)] + [(far, way) for far in range(1, pair_count) for way in (1, -1)]

    def present(step):
        far, way = steps[step]
        if far == 0:
            return None
        return pair >= far if way == 1 else pair + far < pair_count

    def origin(step):
        far, way = steps[step]
        return pair - far * way

    def when(condition, work):
        if condition is None:
            work()
        else:
            pl.when(condition)(work)

    def send(item, source, place, target, sems, at, condition):
        copy = pltpu.make_async_remote_copy(
            src_ref=source,
            dst_ref=outs[item].at[place],
            send_sem=sems[0].at[at],
            recv_sem=sems[1].at[at],
            device_id=target,
            device_id_type=MESH_ID,
        )
        copy.start()
        started.append((condition, item, sems, at))

    def sent(item, sems, at):
        pltpu.make_async_remote_copy(
            src_ref=outs[item].at[0],
            dst_ref=outs[item].at[0],
            send_sem=sems[0].at[at],
            recv_sem=sems[1].at[at],
            device_id=(ctx, pair * 2 + core),
            device_id_type=MESH_ID,
        ).wait_send()

    def arrive(item, place, sems, at):
        pltpu.make_async_remote_copy(
            src_ref=outs[item].at[place],
            dst_ref=outs[item].at[place],
            send_sem=sems[0].at[at],
            recv_sem=sems[1].at[at],
            device_id=(ctx, pair * 2 + core),
            device_id_type=MESH_ID,
        ).wait_recv()

    def pass_on(step, item, source, place):
        far, way = steps[step]
        for side in (1, -1) if far == 0 else (way,):

            def further(side=side):
                return pair + 1 < pair_count if side == 1 else pair >= 1

            def both(further=further):
                return further() if far == 0 else jnp.logical_and(further(), present(step))

            def work(side=side, both=both):
                send(
                    item,
                    source,
                    place,
                    (ctx, (pair + side) * 2 + core),
                    pair_sems,
                    ((side + 1) // 2, far, item),
                    both,
                )

            if far + 1 < pair_count:
                pl.when(further())(work)

    def to_core(item, source, from_ctx, way, step):
        send(
            item,
            source,
            slots[item](from_ctx, origin(step) * 2 + core),
            (ctx, pair * 2 + 1 - core),
            core_sems,
            (way, step, item),
            functools.partial(present, step),
        )

    def spread(step, items):
        for item in items:
            place = slots[item](ctx, origin(step) * 2 + core)
            source = sources[item]
            if step:
                far, way = steps[step]
                arrive(item, place, pair_sems, ((way + 1) // 2, far - 1, item))
                source = outs[item].at[place]
            pass_on(step, item, source, place)
            for way in near if item in wide else ():
                there = ctx_target(ctx, way, square, ctx_size)
                send(
                    item,
                    source,
                    place,
                    (there, pair * 2 + core),
                    ctx_sems,
                    (way - 1, step, item),
                    functools.partial(present, step),
                )
            to_core(item, source, ctx, 0, step)

    def collect(step):
        for way in near:
            for item in wide:
                come = ctx_source(ctx, way, square, ctx_size)
                place = slots[item](come, origin(step) * 2 + core)
                arrive(item, place, ctx_sems, (way - 1, step, item))
                source = outs[item].at[place]
                if square and (steps[step][0] % 2 == 0) == (way == 1):
                    send(
                        item,
                        source,
                        place,
                        (ctx ^ (3 - way), pair * 2 + core),
                        ctx_sems,
                        (2, step, item),
                        functools.partial(present, step),
                    )
                to_core(item, source, come, way, step)

    def collect_far(step):
        for item in wide:
            place = slots[item](ctx ^ 3, origin(step) * 2 + core)
            arrive(item, place, ctx_sems, (2, step, item))
            to_core(item, outs[item].at[place], ctx ^ 3, 3, step)

    locals_ = []
    for item in range(arity):
        copy = pltpu.make_async_copy(sources[item], outs[item].at[homes[item]], local_sem.at[item])
        copy.start()
        locals_.append(copy)
    spread(0, wide)
    flows = []
    count = len(steps)
    for turn in range(1, count + 4):
        if turn < count:
            when(present(turn), functools.partial(spread, turn, wide))
        if turn == count:
            spread(0, narrow)
            for item in range(swaps):
                flow = Exchange(
                    swap_sources[item],
                    swap_outs[item],
                    refs[7 + 3 * item : 9 + 3 * item],
                    refs[9 + 3 * item],
                    pair_count,
                )
                flow.start()
                flows.append(flow)
        if 0 <= turn - 2 < count:
            when(present(turn - 2), functools.partial(collect, turn - 2))
        if square and 0 <= turn - 4 < count:
            when(present(turn - 4), functools.partial(collect_far, turn - 4))

    for turn in range(1, count):
        when(present(turn), functools.partial(spread, turn, narrow))

    def from_core(step):
        for way in (0, *ways):
            come = ctx_source(ctx, way, square, ctx_size) if way else ctx
            for item in wide if way else range(arity):
                arrive(item, slots[item](come, origin(step) * 2 + 1 - core), core_sems, (way, step, item))

    for step in range(count):
        when(present(step), functools.partial(from_core, step))
    for flow in flows:
        flow.finish()
    for copy in locals_:
        copy.wait()
    for condition, *which in started:
        when(condition(), functools.partial(sent, *which))


def gather(pieces, slots, collective_id, swaps=(), wide=None):
    ctx_size, shard_count = lax.axis_size("ctx"), lax.axis_size("fsdp")
    pair_count = shard_count // 2
    arity = len(pieces)
    wide = range(arity) if wide is None else wide
    dma = pltpu.SemaphoreType.DMA
    moved = sum(piece.size for piece in pieces) * 2
    steps = 2 * pair_count - 1
    return pl.pallas_call(
        functools.partial(gather_kernel, arity, ctx_size, pair_count, slots, len(swaps), wide),
        in_specs=[pl.BlockSpec(memory_space=pltpu.VMEM)] * (arity + len(swaps)),
        out_specs=[pl.BlockSpec(memory_space=pl.ANY)] * (arity + len(swaps)),
        out_shape=[
            jax.ShapeDtypeStruct(
                ((ctx_size if item in wide else 1) * shard_count,) + piece.shape, piece.dtype
            )
            for item, piece in enumerate(pieces)
        ]
        + [jax.ShapeDtypeStruct(swap.shape, swap.dtype) for swap in swaps],
        scratch_shapes=[dma((2, pair_count - 1, arity))] * 2
        + [dma((ctx_size - 1, steps, arity))] * 2
        + [dma((ctx_size, steps, arity))] * 2
        + [dma((arity,))]
        + [dma((shard_count - 1,)), dma((shard_count - 1,)), dma] * len(swaps),
        compiler_params=pltpu.CompilerParams(collective_id=collective_id, has_side_effects=True),
        cost_estimate=pl.CostEstimate(
            flops=0, bytes_accessed=moved * ctx_size * shard_count * 4, transcendentals=0
        ),
    )(*pieces, *swaps)


class LineScatter:
    def __init__(self, source, out, half, room, sems, where, counts, last):
        self.count, self.ctx_size = counts
        self.source, self.out, self.half, self.room = source, out, half, room
        self.last = last
        self.core_sems, self.pair_sems = sems[0:2], sems[2:4]
        self.ctx, self.pair, self.core = where
        self.order = [*range(1, self.count), 0]

    def copy(self, source, target, device, sems, at):
        return pltpu.make_async_remote_copy(
            src_ref=source,
            dst_ref=target,
            send_sem=sems[0].at[at],
            recv_sem=sems[1].at[at],
            device_id=device,
            device_id_type=MESH_ID,
        )

    def here(self):
        return (self.ctx, self.pair * 2 + self.core)

    def toward(self, step):
        return lax.rem(self.pair + step, self.count)

    def start(self):
        self.copies = []
        for step in self.order:
            self.copies.append(
                self.copy(
                    self.source.at[self.toward(step) * 2 + 1 - self.core],
                    self.half.at[step],
                    (self.ctx, self.pair * 2 + 1 - self.core),
                    self.core_sems,
                    step,
                )
            )
            self.copies[-1].start()

    def fold(self, step):
        half = self.half.at[step]
        self.copy(half, half, self.here(), self.core_sems, step).wait_recv()
        mine = self.source[self.toward(step) * 2 + self.core].astype(jnp.float32)
        total = mine + half[...].astype(jnp.float32)
        if step == 0:
            self.out[...] = total
            return
        half[...] = total.astype(half.dtype)
        self.copies.append(
            self.copy(
                half,
                self.room.at[step - 1],
                (self.ctx, self.toward(step) * 2 + self.core),
                self.pair_sems,
                step - 1,
            )
        )
        self.copies[-1].start()

    def over_ctx(self, terms, room, landing, *sems):
        shard = self.pair * 2 + self.core
        copies = []

        def send(source, target, way, sems):
            there = lax.rem(self.ctx + way, self.ctx_size)
            copies.append(self.copy(source(there), target, (there, shard), sems, way - 1))
            copies[-1].start()

        def arrive(target, way, sems):
            self.copy(target, target, self.here(), sems, way - 1).wait_recv()

        terms[...] = self.out[...].astype(terms.dtype)
        for way in range(1, self.ctx_size):
            send(lambda there: terms.at[there], room.at[way - 1], way, sems[0:2])
        total = self.out[self.ctx]
        for way in range(1, self.ctx_size):
            arrive(room.at[way - 1], way, sems[0:2])
            total = total + room[way - 1].astype(jnp.float32)
        landing[self.ctx] = total.astype(landing.dtype)
        for way in range(1, self.ctx_size):
            send(lambda there: landing.at[self.ctx], landing.at[self.ctx], way, sems[2:4])
        for way in range(1, self.ctx_size):
            come = lax.rem(self.ctx + self.ctx_size - way, self.ctx_size)
            arrive(landing.at[come], way, sems[2:4])
        self.out[...] = landing[...].astype(jnp.float32)
        for copy in copies:
            copy.wait_send()

    def finish(self):
        for step in range(1, self.count):
            room = self.room.at[step - 1]
            self.copy(room, room, self.here(), self.pair_sems, step - 1).wait_recv()
            self.out[...] += room[...].astype(jnp.float32)
        if self.last:
            self.over_ctx(*self.last)
        for copy in self.copies:
            copy.wait_send()


def scatter_kernel(arity, ctx_size, pair_count, slot, spread_ctx, lines, *refs):
    sources, refs = refs[:arity], refs[arity:]
    line_sources, refs = refs[:lines], refs[lines:]
    outs, refs = refs[:arity], refs[arity:]
    line_outs, refs = refs[:lines], refs[lines:]
    halves, relays, asides, ends, finals = (refs[i * arity : (i + 1) * arity] for i in range(5))
    sems = refs[5 * arity : 5 * arity + 10]
    core_sems, relay_sems, ctx_sems, pair_sems, last_sems = (sems[2 * i : 2 * i + 2] for i in range(5))
    square, ways = peers_of(ctx_size)
    ctx, pair, core = greet(ctx_size, pair_count, True, False)
    order = list(range(1, pair_count)) + [0]
    started = []
    flows = []
    for item in range(lines):
        at = 5 * arity + 10 + 13 * item
        spread = len(line_sources[item].shape) == 4
        flows.append(
            LineScatter(
                line_sources[item],
                line_outs[item],
                *refs[at : at + 2],
                refs[at + 2 : at + 6],
                (ctx, pair, core),
                (pair_count, ctx_size),
                refs[at + 6 : at + 13] if spread else (),
            )
        )

    def send(source, target, device, pair_of_sems, at):
        copy = pltpu.make_async_remote_copy(
            src_ref=source,
            dst_ref=target,
            send_sem=pair_of_sems[0].at[at],
            recv_sem=pair_of_sems[1].at[at],
            device_id=device,
            device_id_type=MESH_ID,
        )
        copy.start()
        started.append(copy)

    def arrive(target, pair_of_sems, at):
        pltpu.make_async_remote_copy(
            src_ref=target,
            dst_ref=target,
            send_sem=pair_of_sems[0].at[at],
            recv_sem=pair_of_sems[1].at[at],
            device_id=(ctx, pair * 2 + core),
            device_id_type=MESH_ID,
        ).wait_recv()

    def toward(step):
        return lax.rem(pair + step, pair_count)

    def target_ctx(way):
        return ctx_target(ctx, way, square, ctx_size) if way else ctx

    def f32(value):
        return value.astype(jnp.float32)

    far_first = [3, 1, 2, 0] if square else list(ways) + [0]
    for step in order:
        for way in far_first:
            for item in range(arity):
                send(
                    sources[item].at[slot(target_ctx(way), toward(step) * 2 + 1 - core)],
                    halves[item].at[way, step],
                    (ctx, pair * 2 + 1 - core),
                    core_sems,
                    (way, step, item),
                )

    def fold_core(step):
        for way in far_first:
            for item in range(arity):
                half = halves[item].at[way, step]
                arrive(half, core_sems, (way, step, item))
                mine = sources[item][slot(target_ctx(way), toward(step) * 2 + core)]
                half[...] = (f32(mine) + f32(half[...])).astype(half.dtype)
                if square and way == 3:
                    there = ctx ^ (1 if step % 2 == 0 else 2)
                    send(
                        half,
                        relays[item].at[step],
                        (there, pair * 2 + core),
                        relay_sems,
                        (step, item),
                    )

    def fold_relay(step):
        for item in range(arity):
            if square:
                relay = relays[item].at[step]
                arrive(relay, relay_sems, (step, item))
                half = halves[item].at[2 if step % 2 == 0 else 1, step]
                half[...] = (f32(half[...]) + f32(relay[...])).astype(half.dtype)
            for way in ways:
                if square and way == 3:
                    continue
                send(
                    halves[item].at[way, step],
                    asides[item].at[way - 1, step],
                    (target_ctx(way), pair * 2 + core),
                    ctx_sems,
                    (way - 1, step, item),
                )

    def fold_ctx(step):
        for item in range(arity):
            half = halves[item].at[0, step]
            total = f32(half[...])
            for way in ways:
                if square and way == 3:
                    continue
                aside = asides[item].at[way - 1, step]
                arrive(aside, ctx_sems, (way - 1, step, item))
                total = total + f32(aside[...])
            if step:
                half[...] = total.astype(half.dtype)
                send(
                    half,
                    ends[item].at[step - 1],
                    (ctx, toward(step) * 2 + core),
                    pair_sems,
                    (step - 1, item),
                )
            else:
                for other in range(1, pair_count):
                    end = ends[item].at[other - 1]
                    arrive(end, pair_sems, (other - 1, item))
                    total = total + f32(end[...])
                if spread_ctx:
                    finals[item][...] = total.astype(finals[item].dtype)
                else:
                    outs[item][...] = total.astype(outs[item].dtype)

    for flow in flows:
        flow.start()
    for turn in range(pair_count + 2):
        if turn < pair_count:
            fold_core(order[turn])
        if 1 <= turn <= pair_count:
            fold_relay(order[turn - 1])
            for flow in flows:
                flow.fold(order[turn - 1])
        if turn >= 2:
            fold_ctx(order[turn - 2])
    if spread_ctx:
        for item in range(arity):
            for way in ways:
                send(
                    finals[item],
                    outs[item].at[ctx],
                    (target_ctx(way), pair * 2 + core),
                    last_sems,
                    (way - 1, item),
                )
            outs[item][ctx] = finals[item][...]
        for item in range(arity):
            for way in ways:
                arrive(outs[item].at[ctx_source(ctx, way, square, ctx_size)], last_sems, (way - 1, item))
    for flow in flows:
        flow.finish()
    for copy in started:
        copy.wait_send()


def scatter(terms, slot, collective_id, spread_ctx=False, out_dtype=None, lines=()):
    ctx_size, shard_count = lax.axis_size("ctx"), lax.axis_size("fsdp")
    pair_count = shard_count // 2
    arity = len(terms)
    dma = pltpu.SemaphoreType.DMA
    lead = (ctx_size,) if spread_ctx else ()
    asides = 2 if ctx_size == 4 else ctx_size - 1

    def room(*extent):
        return [pltpu.VMEM(extent + term.shape[1:], term.dtype) for term in terms]

    def line_room(line):
        if len(line.shape) == 3:
            return [pltpu.VMEM((8, HD), line.dtype)] * 3 + [dma((1,))] * 4
        cut = line.shape[2:]
        rooms = [pltpu.VMEM((count,) + cut, line.dtype) for count in (ctx_size, ctx_size - 1, ctx_size)]
        return rooms + [dma((ctx_size - 1,))] * 4

    moved = sum(term.size * term.dtype.itemsize for term in terms)
    return pl.pallas_call(
        functools.partial(scatter_kernel, arity, ctx_size, pair_count, slot, spread_ctx, len(lines)),
        in_specs=[pl.BlockSpec(memory_space=pltpu.VMEM)] * (arity + len(lines)),
        out_specs=[pl.BlockSpec(memory_space=pltpu.VMEM)] * (arity + len(lines)),
        out_shape=[
            jax.ShapeDtypeStruct(lead + term.shape[1:], out_dtype or term.dtype) for term in terms
        ]
        + [jax.ShapeDtypeStruct(line.shape[1:], jnp.float32) for line in lines],
        scratch_shapes=room(ctx_size, pair_count)
        + room(pair_count)
        + room(asides, pair_count)
        + room(pair_count - 1)
        + room()
        + [dma((ctx_size, pair_count, arity))] * 2
        + [dma((pair_count, arity))] * 2
        + [dma((ctx_size - 1, pair_count, arity))] * 2
        + [dma((pair_count - 1, arity))] * 2
        + [dma((ctx_size - 1, arity))] * 2
        + [
            scratch
            for line in lines
            for scratch in [
                pltpu.VMEM((pair_count,) + line.shape[1:], line.dtype),
                pltpu.VMEM((pair_count - 1,) + line.shape[1:], line.dtype),
            ]
            + [dma((pair_count,))] * 4
            + line_room(line)
        ],
        compiler_params=pltpu.CompilerParams(
            collective_id=collective_id, has_side_effects=True, vmem_limit_bytes=63 * 2**20
        ),
        cost_estimate=pl.CostEstimate(flops=0, bytes_accessed=moved * 16, transcendentals=0),
    )(*terms, *lines)


def pack_kernel(columns, gate_ref, up_ref, out_ref):
    width = out_ref.shape[2] // 2
    cut = out_ref.shape[1]
    for there in range(out_ref.shape[0]):
        for side, ref in enumerate((gate_ref, up_ref)):
            at = side * width
            out_ref[there, :, at + width - HD : at + width] = jnp.zeros((cut, HD), out_ref.dtype)
            out_ref[there, :, at : at + columns] = ref[:, there * columns : (there + 1) * columns]


def pack(gate, up, shard_count, columns, width):
    return pl.pallas_call(
        functools.partial(pack_kernel, columns),
        in_specs=[pl.BlockSpec(memory_space=pltpu.VMEM)] * 2,
        out_specs=pl.BlockSpec(memory_space=pltpu.VMEM),
        out_shape=jax.ShapeDtypeStruct((shard_count, gate.shape[0], 2 * width), gate.dtype),
        name="pack",
    )(gate, up)


def unpack_kernel(columns, in_ref, gate_ref, up_ref):
    width = in_ref.shape[3] // 2
    for there in range(in_ref.shape[1]):
        for side, ref in enumerate((gate_ref, up_ref)):
            part = in_ref[0, there, :, side * width : side * width + columns]
            ref[0, :, there * columns : (there + 1) * columns] = part.astype(jnp.float32)


def unpack(rows, columns):
    ctx_size, shard_count, cut, _ = rows.shape
    out = jax.ShapeDtypeStruct((ctx_size, cut, shard_count * columns), jnp.float32)
    return pl.pallas_call(
        functools.partial(unpack_kernel, columns),
        grid=(ctx_size,),
        in_specs=[pl.BlockSpec((1,) + rows.shape[1:], lambda c: (c, 0, 0, 0))],
        out_specs=[pl.BlockSpec((1, cut, shard_count * columns), lambda c: (c, 0, 0))] * 2,
        out_shape=[out, out],
        name="unpack",
    )(rows)


def shards(
    layer_input,
    block_order,
    first_gain,
    w_qkv,
    b_qkv,
    w_o,
    second_gain,
    w_gate,
    w_up,
    w_down,
    cotangent,
):
    ctx_size = lax.axis_size("ctx")
    shard_count = lax.axis_size("fsdp")
    own_ctx = lax.axis_index("ctx")
    own_shard = lax.axis_index("fsdp")
    rows_here = layer_input.shape[0]
    slots = layer_input.shape[1]
    block_rows = rows_here * shard_count
    kv_width = KVH * HD
    cut = D // (ctx_size * shard_count)
    columns = FF // shard_count
    first_row = (own_ctx * shard_count + own_shard) * rows_here
    own_pos = block_positions(block_order, first_row, rows_here, block_rows, ctx_size)
    cosine_table, sine_table = rope_tables(own_pos.reshape(-1))
    query_scale = HD ** (-0.5)

    def by_rows(ctx, shard):
        return shard * ctx_size + ctx

    def by_tokens(ctx, shard):
        return ctx * shard_count + shard

    def own_cut(weight):
        return lax.dynamic_slice_in_dim(weight, own_ctx * cut, cut, 0)

    def mix_features(values):
        shaped = values.reshape(-1, shard_count, ctx_size, cut)
        return shaped.transpose(0, 2, 1, 3).reshape(-1, D)

    def unmix_features(values):
        shaped = values.reshape(-1, ctx_size, shard_count, cut)
        return shaped.transpose(0, 2, 1, 3).reshape(-1, D)

    small = jnp.concatenate([b_qkv, first_gain, second_gain]).reshape(ctx_size, -1)
    small_width = small.shape[1]
    small = lax.dynamic_slice_in_dim(small, own_ctx, 1, 0)
    small = jnp.pad(small, ((0, 0), (0, 16 * HD - small_width))).reshape(16, HD)
    width = -(-columns // HD) * HD
    w_qkv_all, w_o_all, small_all, cotangent_all = gather(
        [own_cut(w_qkv), own_cut(w_o), small, cotangent.reshape(-1, D)],
        [by_rows, by_rows, by_rows, lambda ctx, shard: shard],
        1,
        wide=(0, 1, 2),
    )
    cotangent_all = cotangent_all.reshape(-1, D)
    w_qkv_all = w_qkv_all.reshape(D, QKV)
    w_o_all = w_o_all.reshape(D, D)
    small_all = small_all.reshape(shard_count, ctx_size, -1)[:, :, :small_width]
    small_all = small_all.reshape(shard_count, -1).astype(jnp.float32)
    bias_width = QKV // shard_count
    gain_width = D // shard_count
    bias_all = small_all[:, :bias_width].reshape(-1)
    gain_one = small_all[:, bias_width : bias_width + gain_width].reshape(-1)
    gain_two = small_all[:, bias_width + gain_width :].reshape(-1)

    down_padded = jnp.pad(w_down, ((0, width - columns), (0, 0)))

    inputs = layer_input.reshape(-1, D).astype(jnp.float32)
    unit_one, scale_one, normed = normalize(inputs, gain_one)
    normed_one = normed.astype(jnp.bfloat16)
    projected = jnp.dot(normed_one, w_qkv_all, preferred_element_type=jnp.float32) + bias_all
    query_raw = projected[:, : H * HD].reshape(-1, H, HD)
    key_raw = projected[:, H * HD : H * HD + kv_width].reshape(-1, KVH, HD)
    value_raw = projected[:, H * HD + kv_width :]
    query_tokens = (
        (rotate(query_raw, cosine_table, sine_table) * query_scale)
        .astype(jnp.bfloat16)
        .reshape(-1, H * HD)
    )
    key_tokens = (
        rotate(key_raw, cosine_table, sine_table).astype(jnp.bfloat16).reshape(-1, kv_width)
    )
    own_kv = jnp.stack([key_tokens, value_raw.astype(jnp.bfloat16)], 1)
    own_kv = own_kv.reshape(rows_here, 2, SEQS, 2, KVH, HD).transpose(0, 2, 4, 1, 3, 5)
    own_kv = own_kv.reshape(rows_here, SEQS * KVH * 4 * HD)
    all_kv, gate_up_cut = gather(
        [own_kv],
        [by_tokens],
        2,
        swaps=[pack(own_cut(w_gate), own_cut(w_up), shard_count, columns, width)],
    )
    gate_up_cols = lax.all_gather(
        gate_up_cut.reshape(shard_count * cut, 2 * width), "ctx", axis=0, tiled=True
    )
    all_kv = all_kv.reshape(-1, SEQS * KVH * 4 * HD)
    queries = to_groups(query_tokens, rows_here)
    scalars = jnp.concatenate(
        [block_order.reshape(-1), jnp.stack([own_ctx, own_shard]).astype(jnp.int32)]
    )
    attended_grouped, stats = attend_forward(
        scalars, queries, all_kv, ctx_size, block_rows, rows_here
    )
    attended_low = from_groups(attended_grouped, rows_here).astype(jnp.bfloat16)
    middle = inputs + jnp.dot(attended_low, w_o_all, preferred_element_type=jnp.float32)
    unit_two, scale_two, normed = normalize(middle, gain_two)
    normed_two = mix_features(normed.astype(jnp.bfloat16))

    (tokens_all,) = gather([normed_two], [lambda ctx, shard: shard], 6, wide=())
    tokens_all = tokens_all.reshape(-1, D)
    gate_up_part = jnp.dot(tokens_all, gate_up_cols, preferred_element_type=jnp.float32)
    gate_part, up_part = gate_up_part[:, :width], gate_up_part[:, width:]
    sigmoid_gate = jax.nn.sigmoid(gate_part)
    activated = gate_part * sigmoid_gate
    hidden = (activated * up_part).astype(jnp.bfloat16)
    grad_hidden = lax.dot_general(
        cotangent_all, down_padded, CONTRACT_LAST, preferred_element_type=jnp.float32
    )
    grad_gate = grad_hidden * up_part * sigmoid_gate * (1.0 + gate_part * (1.0 - sigmoid_gate))
    grad_gate_up = jnp.concatenate([grad_gate, grad_hidden * activated], -1).astype(jnp.bfloat16)
    grad_tokens = lax.dot_general(
        grad_gate_up, gate_up_cols, CONTRACT_LAST, preferred_element_type=jnp.float32
    ).astype(jnp.bfloat16)
    grad_normed_two = lax.psum_scatter(
        grad_tokens, "fsdp", scatter_dimension=0, tiled=True
    ).astype(jnp.float32)
    grad_gate_up, hidden, grad_tokens = lax.optimization_barrier(
        (grad_gate_up, hidden, grad_tokens)
    )
    gate_up_terms = lax.dot_general(
        tokens_all, grad_gate_up, CONTRACT_FIRST, preferred_element_type=jnp.float32
    ).astype(jnp.bfloat16)
    gate_up_rows = lax.psum_scatter(gate_up_terms, "ctx", scatter_dimension=0, tiled=True)
    down_terms = lax.dot_general(
        hidden, cotangent_all, CONTRACT_FIRST, preferred_element_type=jnp.float32
    ).astype(jnp.bfloat16)
    down_rows = lax.psum(down_terms, "ctx")
    mixed_terms = jnp.dot(hidden, down_padded, preferred_element_type=jnp.float32).astype(jnp.bfloat16)
    grad_normed_two, down_terms, gate_up_terms, mixed_terms = lax.optimization_barrier(
        (grad_normed_two, down_terms, gate_up_terms, mixed_terms)
    )
    grad_normed_two = unmix_features(grad_normed_two)
    grad_middle_norm, grad_gain_two = norm_back(grad_normed_two, unit_two, scale_two, gain_two)
    grad_middle = cotangent.reshape(-1, D).astype(jnp.float32) + grad_middle_norm
    grad_branch_one = grad_middle.astype(jnp.bfloat16)
    grad_attended = lax.dot_general(
        grad_branch_one, w_o_all, CONTRACT_LAST, preferred_element_type=jnp.float32
    ).astype(jnp.bfloat16)
    o_terms = lax.dot_general(
        attended_low, grad_branch_one, CONTRACT_FIRST, preferred_element_type=jnp.float32
    ).astype(jnp.bfloat16)
    grad_queries, grad_kv_full = attend_backward(
        scalars,
        queries,
        to_groups(grad_attended, rows_here),
        attended_grouped,
        stats,
        all_kv,
        ctx_size,
        block_rows,
        rows_here,
    )
    (grad_kv,) = scatter(
        [grad_kv_full.reshape(-1, rows_here, SEQS * KVH * 4 * HD)],
        by_tokens,
        3,
        out_dtype=jnp.float32,
    )
    gate_up_rows, grad_kv = lax.optimization_barrier((gate_up_rows, grad_kv))
    gate_up_rows = exchange(gate_up_rows.reshape(shard_count, cut, 2 * width), 5)
    gate_up_rows = lax.all_gather(gate_up_rows, "ctx", axis=0, tiled=False)
    grad_kv_low = narrowed(grad_kv).reshape(rows_here, SEQS, KVH, 2, 2, HD)
    grad_kv_low = grad_kv_low.transpose(0, 3, 1, 4, 2, 5).reshape(-1, 2 * kv_width)
    grad_query_tokens = from_groups(narrowed(grad_queries), rows_here) * query_scale
    grad_query_raw = rotate_back(
        grad_query_tokens.reshape(-1, H, HD), cosine_table, sine_table
    ).reshape(-1, H * HD)
    grad_key_raw = rotate_back(
        grad_kv_low[:, :kv_width].reshape(-1, KVH, HD), cosine_table, sine_table
    ).reshape(-1, kv_width)
    grad_projected = jnp.concatenate(
        [grad_query_raw, grad_key_raw, grad_kv_low[:, kv_width:]], -1
    ).astype(jnp.bfloat16)
    grad_bias = jnp.sum(grad_projected, 0, dtype=jnp.float32)
    grad_normed_one = lax.dot_general(
        grad_projected, w_qkv_all, CONTRACT_LAST, preferred_element_type=jnp.float32
    )
    grad_input_norm, grad_gain_one = norm_back(grad_normed_one, unit_one, scale_one, gain_one)
    grad_input = (grad_middle + grad_input_norm).reshape(rows_here, slots, D)
    qkv_terms = lax.dot_general(
        normed_one, grad_projected, CONTRACT_FIRST, preferred_element_type=jnp.float32
    ).astype(jnp.bfloat16)
    small_terms = jnp.concatenate(
        [
            part.reshape(shard_count, -1)
            for part in (grad_gain_one, grad_gain_two, grad_bias[:QK], grad_bias[QK:])
        ],
        1,
    )
    small_terms = small_terms.reshape(ctx_size * shard_count, small_width)
    small_terms = jnp.pad(small_terms, ((0, 0), (0, 8 * HD - small_width)))
    qkv_rows, small_rows, o_rows, mixed_rows = scatter(
        [
            qkv_terms.reshape(-1, cut, QKV),
            small_terms.reshape(-1, 8, HD),
        ],
        by_rows,
        4,
        spread_ctx=True,
        lines=[
            o_terms.reshape(shard_count, ctx_size, cut, D),
            mixed_terms.reshape(shard_count, -1, D),
        ],
    )
    mixed_out = middle + mixed_rows
    output = mixed_out.astype(jnp.bfloat16).reshape(rows_here, slots, D)
    small_rows = small_rows.reshape(ctx_size, -1)[:, :small_width].reshape(-1)
    bias_start = 2 * gain_width
    value_start = bias_start + QK // shard_count

    gate_rows, up_rows = unpack(gate_up_rows, columns)
    return (
        output,
        grad_input,
        small_rows[:gain_width],
        qkv_rows.reshape(-1, QKV).astype(jnp.float32),
        small_rows[bias_start:value_start],
        small_rows[value_start:],
        o_rows.reshape(-1, D),
        small_rows[gain_width:bias_start],
        gate_rows.reshape(-1, FF),
        up_rows.reshape(-1, FF),
        down_rows[:columns].astype(jnp.float32),
    )


def solution(mesh):
    in_specs = (
        P(("ctx", "fsdp"), None, None),
        P(),
        P("fsdp"),
        P("fsdp", None),
        P("fsdp"),
        P("fsdp", None),
        P("fsdp"),
        P("fsdp", None),
        P("fsdp", None),
        P("fsdp", None),
        P(("ctx", "fsdp"), None, None),
    )
    out_specs = (
        P(("ctx", "fsdp"), None, None),
        P(("ctx", "fsdp"), None, None),
        P("fsdp"),
        P("fsdp", None),
        P("fsdp"),
        P("fsdp"),
        P("fsdp", None),
        P("fsdp"),
        P("fsdp", None),
        P("fsdp", None),
        P("fsdp", None),
    )
    return jax.shard_map(shards, mesh=mesh, in_specs=in_specs, out_specs=out_specs, check_vma=False)
```

```python
import functools

import jax
import jax.numpy as jnp
from jax import lax
from jax.experimental import pallas as pl
from jax.experimental.pallas import tpu as pltpu
from jax.sharding import PartitionSpec as P

D = 1536
H = 12
KVH = 2
HD = 128
FF = 8960
SEQS = 2
QKV = 2048
QK = 1792


EPS = 1e-06
THETA = 1000000.0
NEG_FILL = -1e30
MESH_ID = pl.DeviceIdType.MESH
CONTRACT_LAST = (((1,), (1,)), ((), ()))
CONTRACT_FIRST = (((0,), (0,)), ((), ()))


def by_slot(tokens):
    return tokens.transpose(1, 0, 2).reshape(-1, tokens.shape[2])


def from_slot(tokens, row_count):
    return tokens.reshape(2 * SEQS, row_count, -1).transpose(1, 0, 2)


def to_groups(tokens, row_count):
    shaped = tokens.reshape(2, SEQS, row_count, KVH, H // KVH, HD)
    return shaped.transpose(1, 0, 3, 4, 2, 5).reshape(SEQS, 2, KVH, H // KVH * row_count, HD)


def from_groups(grouped, row_count):
    shaped = grouped.reshape(SEQS, 2, KVH, H // KVH, row_count, HD).transpose(1, 0, 4, 2, 3, 5)
    return shaped.reshape(row_count * 2 * SEQS, H * HD)


def turn_tables(block_order, own_ctx, ctx_size, block_rows, first_row, row_count):
    half_width = HD // 2
    frequency = THETA ** (-jnp.arange(half_width, dtype=jnp.float32) * 2.0 / HD)
    frequency = jnp.tile(frequency, 2)[None, :]
    order = lax.dynamic_index_in_dim(block_order.reshape(SEQS, 2, ctx_size), own_ctx, 2, False)
    start = (order.T.reshape(-1) * block_rows + first_row).astype(jnp.float32)
    far = start[:, None] * frequency
    near = jnp.arange(row_count, dtype=jnp.float32)[:, None] * frequency
    far_cos, far_sin = jnp.cos(far)[:, None, :], jnp.sin(far)[:, None, :]
    near_cos, near_sin = jnp.cos(near)[None], jnp.sin(near)[None]
    sign = jnp.where(jnp.arange(HD) < half_width, -1.0, 1.0).astype(jnp.float32)
    cosine = far_cos * near_cos - far_sin * near_sin
    sine = (far_sin * near_cos + far_cos * near_sin) * sign
    return cosine.reshape(-1, HD), sine.reshape(-1, HD)


def normalize(values, gain):
    scale = lax.rsqrt(jnp.mean(values * values, -1, keepdims=True) + EPS)
    unit = values * scale
    return (unit, scale, unit * gain)


def norm_back(grad_out, unit, scale, gain):
    grad_unit = grad_out * gain
    inner = jnp.mean(grad_unit * unit, -1, keepdims=True)
    return (scale * (grad_unit - unit * inner), jnp.sum(grad_out * unit, 0))


def attend_forward_kernel(ctx_size, block_rows, rows_here, scalars, q_ref, kv_ref, out_ref, stat_ref, best_ref, total_ref, accum_ref):
    seq = pl.program_id(0)
    blocks = 2 * ctx_size
    own_ctx = scalars[SEQS * blocks]
    own_shard = scalars[SEQS * blocks + 1]
    lanes = q_ref.shape[3]
    best_ref[...] = jnp.full(best_ref.shape, NEG_FILL, jnp.float32)
    total_ref[...] = jnp.zeros(total_ref.shape, jnp.float32)
    accum_ref[...] = jnp.zeros(accum_ref.shape, jnp.float32)

    def step(key_ctx, half_key, half):
        order_key = scalars[seq * blocks + half_key * ctx_size + key_ctx]
        order_query = scalars[seq * blocks + half * ctx_size + own_ctx]

        def work(masked):
            rows = pl.ds(pl.multiple_of(key_ctx * block_rows, block_rows), block_rows)
            keys = kv_ref[rows, half_key * 2 * HD : half_key * 2 * HD + HD]
            values = kv_ref[rows, half_key * 2 * HD + HD : half_key * 2 * HD + 2 * HD]
            scores = lax.dot_general(
                keys, q_ref[0, half, 0], CONTRACT_LAST, preferred_element_type=jnp.float32
            )
            if masked:
                row = lax.broadcasted_iota(jnp.int32, (block_rows, lanes), 0)
                lane = lax.broadcasted_iota(jnp.int32, (block_rows, lanes), 1)
                scores = jnp.where(
                    row <= own_shard * rows_here + lax.rem(lane, rows_here), scores, NEG_FILL
                )
            best = best_ref[half]
            fresh = jnp.maximum(best, jnp.max(scores, 0, keepdims=True))
            decay = jnp.exp(best - fresh)
            weights = jnp.exp(scores - fresh)
            total_ref[half] = total_ref[half] * decay + jnp.sum(weights, 0, keepdims=True)
            accum_ref[half] = accum_ref[half] * decay + lax.dot_general(
                values,
                weights.astype(jnp.bfloat16),
                CONTRACT_FIRST,
                preferred_element_type=jnp.float32,
            )
            best_ref[half] = fresh

        @pl.when(order_key < order_query)
        def full():
            work(False)

        @pl.when(order_key == order_query)
        def diagonal():
            work(True)

    @pl.loop(0, ctx_size)
    def sweep(key_ctx):
        for half_key in range(2):
            for half in range(2):
                step(key_ctx, half_key, half)

    for half in range(2):
        totals = total_ref[half]
        out_ref[0, half, 0] = (accum_ref[half] / totals).T
        stat_ref[0, half, 0] = best_ref[half] + jnp.log(totals)


def attend_forward(scalars, queries, all_kv, ctx_size, block_rows, rows_here):
    lanes = queries.shape[3]
    kernel = functools.partial(attend_forward_kernel, ctx_size, block_rows, rows_here)
    group = pl.BlockSpec((1, 2, 1, lanes, HD), lambda s, n, _: (s, 0, n, 0, 0))
    stat = pl.BlockSpec((1, 2, 1, 1, lanes), lambda s, n, _: (s, 0, n, 0, 0))
    return pl.pallas_call(
        kernel,
        grid_spec=pltpu.PrefetchScalarGridSpec(
            num_scalar_prefetch=1,
            grid=(SEQS, KVH),
            in_specs=[
                group,
                pl.BlockSpec((all_kv.shape[0], 4 * HD), lambda s, n, _: (0, s * KVH + n)),
            ],
            out_specs=[group, stat],
            scratch_shapes=[
                pltpu.VMEM((2, 1, lanes), jnp.float32),
                pltpu.VMEM((2, 1, lanes), jnp.float32),
                pltpu.VMEM((2, HD, lanes), jnp.float32),
            ],
        ),
        out_shape=(
            jax.ShapeDtypeStruct(queries.shape, jnp.float32),
            jax.ShapeDtypeStruct((SEQS, 2, KVH, 1, lanes), jnp.float32),
        ),
        compiler_params=pltpu.CompilerParams(vmem_limit_bytes=56 * 2**20),
        name="attend_forward",
    )(scalars, queries, all_kv)


def attend_backward_kernel(ctx_size, block_rows, rows_here, scalars, q_ref, go_ref, att_ref, stat_ref, kv_ref, gq_ref, gkv_ref, delta_ref, gq_acc, gk_acc, gv_acc):
    seq = pl.program_id(0)
    blocks = 2 * ctx_size
    own_ctx = scalars[SEQS * blocks]
    own_shard = scalars[SEQS * blocks + 1]
    lanes = q_ref.shape[3]
    gq_acc[...] = jnp.zeros(gq_acc.shape, jnp.float32)
    for half in range(2):
        product = go_ref[0, half, 0].astype(jnp.float32) * att_ref[0, half, 0]
        delta_ref[half] = jnp.sum(product.T, 0, keepdims=True)

    def step(key_ctx, half_key, half):
        order_key = scalars[seq * blocks + half_key * ctx_size + key_ctx]
        order_query = scalars[seq * blocks + half * ctx_size + own_ctx]

        def work(masked):
            rows = pl.ds(pl.multiple_of(key_ctx * block_rows, block_rows), block_rows)
            keys = kv_ref[rows, half_key * 2 * HD : half_key * 2 * HD + HD]
            values = kv_ref[rows, half_key * 2 * HD + HD : half_key * 2 * HD + 2 * HD]
            queries = q_ref[0, half, 0]
            grad_out = go_ref[0, half, 0]
            scores = lax.dot_general(
                keys, queries, CONTRACT_LAST, preferred_element_type=jnp.float32
            )
            probs = jnp.exp(scores - stat_ref[0, half, 0])
            if masked:
                row = lax.broadcasted_iota(jnp.int32, (block_rows, lanes), 0)
                lane = lax.broadcasted_iota(jnp.int32, (block_rows, lanes), 1)
                probs = jnp.where(
                    row <= own_shard * rows_here + lax.rem(lane, rows_here), probs, 0.0
                )
            grad_probs = lax.dot_general(
                values, grad_out, CONTRACT_LAST, preferred_element_type=jnp.float32
            )
            grad_scores = (probs * (grad_probs - delta_ref[half])).astype(jnp.bfloat16)
            gv_acc[...] += jnp.dot(
                probs.astype(jnp.bfloat16), grad_out, preferred_element_type=jnp.float32
            )
            gk_acc[...] += jnp.dot(grad_scores, queries, preferred_element_type=jnp.float32)
            gq_acc[half] += lax.dot_general(
                keys, grad_scores, CONTRACT_FIRST, preferred_element_type=jnp.float32
            )

        @pl.when(order_key < order_query)
        def full():
            work(False)

        @pl.when(order_key == order_query)
        def diagonal():
            work(True)

    @pl.loop(0, ctx_size)
    def sweep(key_ctx):
        rows = pl.ds(pl.multiple_of(key_ctx * block_rows, block_rows), block_rows)
        for half_key in range(2):
            gk_acc[...] = jnp.zeros(gk_acc.shape, jnp.float32)
            gv_acc[...] = jnp.zeros(gv_acc.shape, jnp.float32)
            for half in range(2):
                step(key_ctx, half_key, half)
            at = half_key * 2 * HD
            gkv_ref[rows, at : at + HD] = gk_acc[...].astype(jnp.bfloat16)
            gkv_ref[rows, at + HD : at + 2 * HD] = gv_acc[...].astype(jnp.bfloat16)

    for half in range(2):
        gq_ref[0, half, 0] = gq_acc[half].T


def attend_backward(scalars, queries, grad_out, attended, stats, all_kv, ctx_size, block_rows, rows_here):
    lanes = queries.shape[3]
    kernel = functools.partial(attend_backward_kernel, ctx_size, block_rows, rows_here)
    group = pl.BlockSpec((1, 2, 1, lanes, HD), lambda s, n, _: (s, 0, n, 0, 0))
    stat = pl.BlockSpec((1, 2, 1, 1, lanes), lambda s, n, _: (s, 0, n, 0, 0))
    full = pl.BlockSpec((all_kv.shape[0], 4 * HD), lambda s, n, _: (0, s * KVH + n))
    return pl.pallas_call(
        kernel,
        grid_spec=pltpu.PrefetchScalarGridSpec(
            num_scalar_prefetch=1,
            grid=(SEQS, KVH),
            in_specs=[group, group, group, stat, full],
            out_specs=[group, full],
            scratch_shapes=[
                pltpu.VMEM((2, 1, lanes), jnp.float32),
                pltpu.VMEM((2, HD, lanes), jnp.float32),
                pltpu.VMEM((block_rows, HD), jnp.float32),
                pltpu.VMEM((block_rows, HD), jnp.float32),
            ],
        ),
        out_shape=(
            jax.ShapeDtypeStruct(queries.shape, jnp.float32),
            jax.ShapeDtypeStruct(all_kv.shape, jnp.bfloat16),
        ),
        compiler_params=pltpu.CompilerParams(vmem_limit_bytes=56 * 2**20),
        name="attend_backward",
    )(scalars, queries, grad_out, attended, stats, all_kv)


def peers_of(ctx_size):
    return ctx_size == 4, range(1, ctx_size)


def ctx_target(position, way, square, ctx_size):
    return position ^ way if square else lax.rem(position + way, ctx_size)


def ctx_source(position, way, square, ctx_size):
    return position ^ way if square else lax.rem(position + ctx_size - way, ctx_size)


def greet(ctx_size, pair_count, with_ctx, all_shards):
    ctx = lax.axis_index("ctx")
    shard = lax.axis_index("fsdp")
    pair, core = shard // 2, shard % 2
    barrier = pltpu.get_barrier_semaphore()
    partners = [(ctx, pair * 2 + 1 - core)]
    for step in range(1, pair_count):
        there = lax.rem(pair + step, pair_count) * 2
        partners.append((ctx, there + core))
        if all_shards:
            partners.append((ctx, there + 1 - core))
    if with_ctx:
        for way in range(1, ctx_size):
            partners.append((lax.rem(ctx + way, ctx_size), shard))
    for partner in partners:
        pl.semaphore_signal(barrier, inc=1, device_id=partner, device_id_type=MESH_ID)
    pl.semaphore_wait(barrier, len(partners))
    return ctx, pair, core


class Exchange:
    def __init__(self, source, out, sems, own_sem, pair_count):
        self.source, self.out, self.sems, self.own_sem = source, out, sems, own_sem
        self.shard_count = 2 * pair_count

    def start(self):
        ctx, shard = lax.axis_index("ctx"), lax.axis_index("fsdp")
        self.own = pltpu.make_async_copy(self.source.at[shard], self.out.at[shard], self.own_sem)
        self.own.start()
        self.copies = []
        for step in range(1, self.shard_count):
            there = lax.rem(shard + step, self.shard_count)
            copy = pltpu.make_async_remote_copy(
                src_ref=self.source.at[there],
                dst_ref=self.out.at[shard],
                send_sem=self.sems[0].at[step - 1],
                recv_sem=self.sems[1].at[step - 1],
                device_id=(ctx, there),
                device_id_type=MESH_ID,
            )
            copy.start()
            self.copies.append(copy)

    def finish(self):
        ctx, shard = lax.axis_index("ctx"), lax.axis_index("fsdp")
        for step in range(1, self.shard_count):
            come = lax.rem(shard + self.shard_count - step, self.shard_count)
            pltpu.make_async_remote_copy(
                src_ref=self.out.at[come],
                dst_ref=self.out.at[come],
                send_sem=self.sems[0].at[step - 1],
                recv_sem=self.sems[1].at[step - 1],
                device_id=(ctx, shard),
                device_id_type=MESH_ID,
            ).wait_recv()
        self.own.wait()
        for copy in self.copies:
            copy.wait_send()


def exchange_kernel(pair_count, source, out, send_sem, recv_sem, own_sem):
    greet(1, pair_count, False, True)
    flow = Exchange(source, out, (send_sem, recv_sem), own_sem, pair_count)
    flow.start()
    flow.finish()


def exchange(pieces, collective_id):
    shard_count = lax.axis_size("fsdp")
    dma = pltpu.SemaphoreType.DMA
    return pl.pallas_call(
        functools.partial(exchange_kernel, shard_count // 2),
        in_specs=[pl.BlockSpec(memory_space=pltpu.VMEM)],
        out_specs=pl.BlockSpec(memory_space=pl.ANY),
        out_shape=jax.ShapeDtypeStruct(pieces.shape, pieces.dtype),
        scratch_shapes=[dma((shard_count - 1,))] * 2 + [dma],
        compiler_params=pltpu.CompilerParams(collective_id=collective_id, has_side_effects=True),
        cost_estimate=pl.CostEstimate(
            flops=0, bytes_accessed=pieces.size * 64, transcendentals=0
        ),
    )(pieces)


def gather_kernel(arity, ctx_size, pair_count, slots, swaps, wide, *refs):
    sources, refs = refs[:arity], refs[arity:]
    swap_sources, refs = refs[:swaps], refs[swaps:]
    outs, refs = refs[:arity], refs[arity:]
    swap_outs, refs = refs[:swaps], refs[swaps:]
    pair_sems, ctx_sems, core_sems = refs[0:2], refs[2:4], refs[4:6]
    local_sem = refs[6]
    square, ways = peers_of(ctx_size) if wide else (False, ())
    narrow = [item for item in range(arity) if item not in wide]
    near = [way for way in ways if not (square and way == 3)]
    ctx, pair, core = greet(ctx_size, pair_count, len(wide) > 0, swaps > 0)
    homes = [place(ctx, pair * 2 + core) for place in slots]
    started = []
    steps = [(0, 1)] + [(far, way) for far in range(1, pair_count) for way in (1, -1)]

    def present(step):
        far, way = steps[step]
        if far == 0:
            return None
        return pair >= far if way == 1 else pair + far < pair_count

    def origin(step):
        far, way = steps[step]
        return pair - far * way

    def when(condition, work):
        if condition is None:
            work()
        else:
            pl.when(condition)(work)

    def send(item, source, place, target, sems, at, condition):
        copy = pltpu.make_async_remote_copy(
            src_ref=source,
            dst_ref=outs[item].at[place],
            send_sem=sems[0].at[at],
            recv_sem=sems[1].at[at],
            device_id=target,
            device_id_type=MESH_ID,
        )
        copy.start()
        started.append((condition, item, sems, at))

    def sent(item, sems, at):
        pltpu.make_async_remote_copy(
            src_ref=outs[item].at[0],
            dst_ref=outs[item].at[0],
            send_sem=sems[0].at[at],
            recv_sem=sems[1].at[at],
            device_id=(ctx, pair * 2 + core),
            device_id_type=MESH_ID,
        ).wait_send()

    def arrive(item, place, sems, at):
        pltpu.make_async_remote_copy(
            src_ref=outs[item].at[place],
            dst_ref=outs[item].at[place],
            send_sem=sems[0].at[at],
            recv_sem=sems[1].at[at],
            device_id=(ctx, pair * 2 + core),
            device_id_type=MESH_ID,
        ).wait_recv()

    def pass_on(step, item, source, place):
        far, way = steps[step]
        for side in (1, -1) if far == 0 else (way,):

            def further(side=side):
                return pair + 1 < pair_count if side == 1 else pair >= 1

            def both(further=further):
                return further() if far == 0 else jnp.logical_and(further(), present(step))

            def work(side=side, both=both):
                send(
                    item,
                    source,
                    place,
                    (ctx, (pair + side) * 2 + core),
                    pair_sems,
                    ((side + 1) // 2, far, item),
                    both,
                )

            if far + 1 < pair_count:
                pl.when(further())(work)

    def to_core(item, source, from_ctx, way, step):
        send(
            item,
            source,
            slots[item](from_ctx, origin(step) * 2 + core),
            (ctx, pair * 2 + 1 - core),
            core_sems,
            (way, step, item),
            functools.partial(present, step),
        )

    def spread(step, items):
        for item in items:
            place = slots[item](ctx, origin(step) * 2 + core)
            source = sources[item]
            if step:
                far, way = steps[step]
                arrive(item, place, pair_sems, ((way + 1) // 2, far - 1, item))
                source = outs[item].at[place]
            pass_on(step, item, source, place)
            for way in near if item in wide else ():
                there = ctx_target(ctx, way, square, ctx_size)
                send(
                    item,
                    source,
                    place,
                    (there, pair * 2 + core),
                    ctx_sems,
                    (way - 1, step, item),
                    functools.partial(present, step),
                )
            to_core(item, source, ctx, 0, step)

    def collect(step):
        for way in near:
            for item in wide:
                come = ctx_source(ctx, way, square, ctx_size)
                place = slots[item](come, origin(step) * 2 + core)
                arrive(item, place, ctx_sems, (way - 1, step, item))
                source = outs[item].at[place]
                if square and (steps[step][0] % 2 == 0) == (way == 1):
                    send(
                        item,
                        source,
                        place,
                        (ctx ^ (3 - way), pair * 2 + core),
                        ctx_sems,
                        (2, step, item),
                        functools.partial(present, step),
                    )
                to_core(item, source, come, way, step)

    def collect_far(step):
        for item in wide:
            place = slots[item](ctx ^ 3, origin(step) * 2 + core)
            arrive(item, place, ctx_sems, (2, step, item))
            to_core(item, outs[item].at[place], ctx ^ 3, 3, step)

    def straight_core(item, source, place, step):
        sibling = (ctx, pair * 2 + 1 - core)
        send(item, source, place, sibling, core_sems, (0, step, item), lambda: None)

    def go_straight(item):
        for step in range(1, pair_count):
            there = lax.rem(pair + step, pair_count) * 2 + core
            at = (0, step - 1, item)
            send(item, sources[item], homes[item], (ctx, there), pair_sems, at, lambda: None)
        straight_core(item, sources[item], homes[item], 0)

    locals_ = []
    for item in range(arity):
        copy = pltpu.make_async_copy(sources[item], outs[item].at[homes[item]], local_sem.at[item])
        copy.start()
        locals_.append(copy)
    spread(0, wide or range(arity))
    flows = []
    count = len(steps)
    for turn in range(1, count + 4):
        if turn < count:
            when(present(turn), functools.partial(spread, turn, wide or range(arity)))
        if turn == count:
            for item in narrow if wide else ():
                go_straight(item)
            for item in range(swaps):
                flow = Exchange(
                    swap_sources[item],
                    swap_outs[item],
                    refs[7 + 3 * item : 9 + 3 * item],
                    refs[9 + 3 * item],
                    pair_count,
                )
                flow.start()
                flows.append(flow)
        if 0 <= turn - 2 < count:
            when(present(turn - 2), functools.partial(collect, turn - 2))
        if square and 0 <= turn - 4 < count:
            when(present(turn - 4), functools.partial(collect_far, turn - 4))

    for item in narrow if wide else ():
        for step in range(1, pair_count):
            come = lax.rem(pair + pair_count - step, pair_count)
            place = slots[item](ctx, come * 2 + core)
            arrive(item, place, pair_sems, (0, step - 1, item))
            straight_core(item, outs[item].at[place], place, step)
    for item in narrow if wide else ():
        for step in range(pair_count):
            come = lax.rem(pair + pair_count - step, pair_count)
            arrive(item, slots[item](ctx, come * 2 + 1 - core), core_sems, (0, step, item))

    def from_core(step):
        for way in (0, *ways):
            come = ctx_source(ctx, way, square, ctx_size) if way else ctx
            for item in wide or range(arity):
                arrive(item, slots[item](come, origin(step) * 2 + 1 - core), core_sems, (way, step, item))

    for step in range(count):
        when(present(step), functools.partial(from_core, step))
    for flow in flows:
        flow.finish()
    for copy in locals_:
        copy.wait()
    for condition, *which in started:
        when(condition(), functools.partial(sent, *which))


def gather(pieces, slots, collective_id, swaps=(), wide=None):
    ctx_size, shard_count = lax.axis_size("ctx"), lax.axis_size("fsdp")
    pair_count = shard_count // 2
    arity = len(pieces)
    wide = range(arity) if wide is None else wide
    dma = pltpu.SemaphoreType.DMA
    moved = sum(piece.size for piece in pieces) * 2
    steps = 2 * pair_count - 1
    return pl.pallas_call(
        functools.partial(gather_kernel, arity, ctx_size, pair_count, slots, len(swaps), wide),
        in_specs=[pl.BlockSpec(memory_space=pltpu.VMEM)] * (arity + len(swaps)),
        out_specs=[pl.BlockSpec(memory_space=pl.ANY)] * (arity + len(swaps)),
        out_shape=[
            jax.ShapeDtypeStruct(
                ((ctx_size if item in wide else 1) * shard_count,) + piece.shape, piece.dtype
            )
            for item, piece in enumerate(pieces)
        ]
        + [jax.ShapeDtypeStruct(swap.shape, swap.dtype) for swap in swaps],
        scratch_shapes=[dma((2, pair_count - 1, arity))] * 2
        + [dma((ctx_size - 1, steps, arity))] * 2
        + [dma((ctx_size, steps, arity))] * 2
        + [dma((arity,))]
        + [dma((shard_count - 1,)), dma((shard_count - 1,)), dma] * len(swaps),
        compiler_params=pltpu.CompilerParams(collective_id=collective_id, has_side_effects=True),
        cost_estimate=pl.CostEstimate(
            flops=0, bytes_accessed=moved * ctx_size * shard_count * 4, transcendentals=0
        ),
    )(*pieces, *swaps)


class LineScatter:
    def __init__(self, source, out, half, room, sems, where, counts, last):
        self.count, self.ctx_size = counts
        self.source, self.out, self.half, self.room = source, out, half, room
        self.last = last
        self.core_sems, self.pair_sems = sems[0:2], sems[2:4]
        self.ctx, self.pair, self.core = where
        self.order = [*range(1, self.count), 0]

    def copy(self, source, target, device, sems, at):
        return pltpu.make_async_remote_copy(
            src_ref=source,
            dst_ref=target,
            send_sem=sems[0].at[at],
            recv_sem=sems[1].at[at],
            device_id=device,
            device_id_type=MESH_ID,
        )

    def here(self):
        return (self.ctx, self.pair * 2 + self.core)

    def toward(self, step):
        return lax.rem(self.pair + step, self.count)

    def start(self):
        self.copies = []
        for step in self.order:
            self.copies.append(
                self.copy(
                    self.source.at[self.toward(step) * 2 + 1 - self.core],
                    self.half.at[step],
                    (self.ctx, self.pair * 2 + 1 - self.core),
                    self.core_sems,
                    step,
                )
            )
            self.copies[-1].start()

    def fold(self, step):
        half = self.half.at[step]
        self.copy(half, half, self.here(), self.core_sems, step).wait_recv()
        mine = self.source[self.toward(step) * 2 + self.core].astype(jnp.float32)
        total = mine + half[...].astype(jnp.float32)
        if step == 0:
            self.out[...] = total
            return
        half[...] = total.astype(half.dtype)
        self.copies.append(
            self.copy(
                half,
                self.room.at[step - 1],
                (self.ctx, self.toward(step) * 2 + self.core),
                self.pair_sems,
                step - 1,
            )
        )
        self.copies[-1].start()

    def over_ctx(self, terms, room, landing, *sems):
        shard = self.pair * 2 + self.core
        copies = []

        def send(source, target, way, sems):
            there = lax.rem(self.ctx + way, self.ctx_size)
            copies.append(self.copy(source(there), target, (there, shard), sems, way - 1))
            copies[-1].start()

        def arrive(target, way, sems):
            self.copy(target, target, self.here(), sems, way - 1).wait_recv()

        terms[...] = self.out[...].astype(terms.dtype)
        for way in range(1, self.ctx_size):
            send(lambda there: terms.at[there], room.at[way - 1], way, sems[0:2])
        total = self.out[self.ctx]
        for way in range(1, self.ctx_size):
            arrive(room.at[way - 1], way, sems[0:2])
            total = total + room[way - 1].astype(jnp.float32)
        landing[self.ctx] = total.astype(landing.dtype)
        for way in range(1, self.ctx_size):
            send(lambda there: landing.at[self.ctx], landing.at[self.ctx], way, sems[2:4])
        for way in range(1, self.ctx_size):
            come = lax.rem(self.ctx + self.ctx_size - way, self.ctx_size)
            arrive(landing.at[come], way, sems[2:4])
        self.out[...] = landing[...].astype(jnp.float32)
        for copy in copies:
            copy.wait_send()

    def finish(self):
        for step in range(1, self.count):
            room = self.room.at[step - 1]
            self.copy(room, room, self.here(), self.pair_sems, step - 1).wait_recv()
            self.out[...] += room[...].astype(jnp.float32)
        if self.last:
            self.over_ctx(*self.last)
        for copy in self.copies:
            copy.wait_send()


def scatter_kernel(arity, ctx_size, pair_count, slot, spread_ctx, lines, *refs):
    sources, refs = refs[:arity], refs[arity:]
    line_sources, refs = refs[:lines], refs[lines:]
    outs, refs = refs[:arity], refs[arity:]
    line_outs, refs = refs[:lines], refs[lines:]
    halves, relays, asides, ends, finals = (refs[i * arity : (i + 1) * arity] for i in range(5))
    sems = refs[5 * arity : 5 * arity + 10]
    core_sems, relay_sems, ctx_sems, pair_sems, last_sems = (sems[2 * i : 2 * i + 2] for i in range(5))
    square, ways = peers_of(ctx_size)
    ctx, pair, core = greet(ctx_size, pair_count, True, False)
    order = list(range(1, pair_count)) + [0]
    started = []
    flows = []
    for item in range(lines):
        at = 5 * arity + 10 + 13 * item
        spread = len(line_sources[item].shape) == 4
        flows.append(
            LineScatter(
                line_sources[item],
                line_outs[item],
                *refs[at : at + 2],
                refs[at + 2 : at + 6],
                (ctx, pair, core),
                (pair_count, ctx_size),
                refs[at + 6 : at + 13] if spread else (),
            )
        )

    def send(source, target, device, pair_of_sems, at):
        copy = pltpu.make_async_remote_copy(
            src_ref=source,
            dst_ref=target,
            send_sem=pair_of_sems[0].at[at],
            recv_sem=pair_of_sems[1].at[at],
            device_id=device,
            device_id_type=MESH_ID,
        )
        copy.start()
        started.append(copy)

    def arrive(target, pair_of_sems, at):
        pltpu.make_async_remote_copy(
            src_ref=target,
            dst_ref=target,
            send_sem=pair_of_sems[0].at[at],
            recv_sem=pair_of_sems[1].at[at],
            device_id=(ctx, pair * 2 + core),
            device_id_type=MESH_ID,
        ).wait_recv()

    def toward(step):
        return lax.rem(pair + step, pair_count)

    def target_ctx(way):
        return ctx_target(ctx, way, square, ctx_size) if way else ctx

    def f32(value):
        return value.astype(jnp.float32)

    far_first = [3, 1, 2, 0] if square else list(ways) + [0]
    for step in order:
        for way in far_first:
            for item in range(arity):
                send(
                    sources[item].at[slot(target_ctx(way), toward(step) * 2 + 1 - core)],
                    halves[item].at[way, step],
                    (ctx, pair * 2 + 1 - core),
                    core_sems,
                    (way, step, item),
                )

    def fold_core(step):
        for way in far_first:
            for item in range(arity):
                half = halves[item].at[way, step]
                arrive(half, core_sems, (way, step, item))
                mine = sources[item][slot(target_ctx(way), toward(step) * 2 + core)]
                half[...] = (f32(mine) + f32(half[...])).astype(half.dtype)
                if square and way == 3:
                    there = ctx ^ (1 if step % 2 == 0 else 2)
                    send(
                        half,
                        relays[item].at[step],
                        (there, pair * 2 + core),
                        relay_sems,
                        (step, item),
                    )

    def fold_relay(step):
        for item in range(arity):
            if square:
                relay = relays[item].at[step]
                arrive(relay, relay_sems, (step, item))
                half = halves[item].at[2 if step % 2 == 0 else 1, step]
                half[...] = (f32(half[...]) + f32(relay[...])).astype(half.dtype)
            for way in ways:
                if square and way == 3:
                    continue
                send(
                    halves[item].at[way, step],
                    asides[item].at[way - 1, step],
                    (target_ctx(way), pair * 2 + core),
                    ctx_sems,
                    (way - 1, step, item),
                )

    def fold_ctx(step):
        for item in range(arity):
            half = halves[item].at[0, step]
            total = f32(half[...])
            for way in ways:
                if square and way == 3:
                    continue
                aside = asides[item].at[way - 1, step]
                arrive(aside, ctx_sems, (way - 1, step, item))
                total = total + f32(aside[...])
            if step:
                half[...] = total.astype(half.dtype)
                send(
                    half,
                    ends[item].at[step - 1],
                    (ctx, toward(step) * 2 + core),
                    pair_sems,
                    (step - 1, item),
                )
            else:
                for other in range(1, pair_count):
                    end = ends[item].at[other - 1]
                    arrive(end, pair_sems, (other - 1, item))
                    total = total + f32(end[...])
                if spread_ctx:
                    finals[item][...] = total.astype(finals[item].dtype)
                else:
                    outs[item][...] = total.astype(outs[item].dtype)

    for flow in flows:
        flow.start()
    for turn in range(pair_count + 2):
        if turn < pair_count:
            fold_core(order[turn])
        if 1 <= turn <= pair_count:
            fold_relay(order[turn - 1])
            for flow in flows:
                flow.fold(order[turn - 1])
        if turn >= 2:
            fold_ctx(order[turn - 2])
    if spread_ctx:
        for item in range(arity):
            for way in ways:
                send(
                    finals[item],
                    outs[item].at[ctx],
                    (target_ctx(way), pair * 2 + core),
                    last_sems,
                    (way - 1, item),
                )
            outs[item][ctx] = finals[item][...]
        for item in range(arity):
            for way in ways:
                arrive(outs[item].at[ctx_source(ctx, way, square, ctx_size)], last_sems, (way - 1, item))
    for flow in flows:
        flow.finish()
    for copy in started:
        copy.wait_send()


def scatter(terms, slot, collective_id, spread_ctx=False, out_dtype=None, lines=()):
    ctx_size, shard_count = lax.axis_size("ctx"), lax.axis_size("fsdp")
    pair_count = shard_count // 2
    arity = len(terms)
    dma = pltpu.SemaphoreType.DMA
    lead = (ctx_size,) if spread_ctx else ()
    asides = 2 if ctx_size == 4 else ctx_size - 1

    def room(*extent):
        return [pltpu.VMEM(extent + term.shape[1:], term.dtype) for term in terms]

    def line_room(line):
        if len(line.shape) == 3:
            return [pltpu.VMEM((8, HD), line.dtype)] * 3 + [dma((1,))] * 4
        cut = line.shape[2:]
        rooms = [pltpu.VMEM((count,) + cut, line.dtype) for count in (ctx_size, ctx_size - 1, ctx_size)]
        return rooms + [dma((ctx_size - 1,))] * 4

    moved = sum(term.size * term.dtype.itemsize for term in terms)
    return pl.pallas_call(
        functools.partial(scatter_kernel, arity, ctx_size, pair_count, slot, spread_ctx, len(lines)),
        in_specs=[pl.BlockSpec(memory_space=pltpu.VMEM)] * (arity + len(lines)),
        out_specs=[pl.BlockSpec(memory_space=pltpu.VMEM)] * (arity + len(lines)),
        out_shape=[
            jax.ShapeDtypeStruct(lead + term.shape[1:], out_dtype or term.dtype) for term in terms
        ]
        + [jax.ShapeDtypeStruct(line.shape[1:], jnp.float32) for line in lines],
        scratch_shapes=room(ctx_size, pair_count)
        + room(pair_count)
        + room(asides, pair_count)
        + room(pair_count - 1)
        + room()
        + [dma((ctx_size, pair_count, arity))] * 2
        + [dma((pair_count, arity))] * 2
        + [dma((ctx_size - 1, pair_count, arity))] * 2
        + [dma((pair_count - 1, arity))] * 2
        + [dma((ctx_size - 1, arity))] * 2
        + [
            scratch
            for line in lines
            for scratch in [
                pltpu.VMEM((pair_count,) + line.shape[1:], line.dtype),
                pltpu.VMEM((pair_count - 1,) + line.shape[1:], line.dtype),
            ]
            + [dma((pair_count,))] * 4
            + line_room(line)
        ],
        compiler_params=pltpu.CompilerParams(
            collective_id=collective_id, has_side_effects=True, vmem_limit_bytes=63 * 2**20
        ),
        cost_estimate=pl.CostEstimate(flops=0, bytes_accessed=moved * 16, transcendentals=0),
    )(*terms, *lines)


def turned(values, cosine, signed_sine):
    return values * cosine + pltpu.roll(values, HD // 2, 1) * signed_sine


def turned_back(grads, cosine, signed_sine):
    return grads * cosine + pltpu.roll(grads * signed_sine, HD // 2, 1)


def slot_of(index):
    return index % SEQS, index // SEQS


def key_column(index, group, part):
    seq, half = slot_of(index)
    return (((seq * KVH + group) * 2 + half) * 2 + part) * HD


def project_kernel(rows, x_ref, gain_ref, w_hbm, bias_ref, cos_ref, sin_ref, normed_ref, q_ref, kv_ref, w_ref, q_acc, sems):
    wide = w_ref.shape[2]
    copies = []
    for part in range(w_ref.shape[0]):
        copy = pltpu.make_async_copy(
            w_hbm.at[:, part * wide : (part + 1) * wide], w_ref.at[part], sems.at[part]
        )
        copy.start()
        copies.append(copy)
    values = x_ref[...].astype(jnp.float32)
    scale = lax.rsqrt(jnp.mean(values * values, -1, keepdims=True) + EPS)
    normed = (values * scale * gain_ref[...]).astype(jnp.bfloat16)
    normed_ref[...] = normed
    cosine, sine = cos_ref[...], sin_ref[...]
    for part, copy in enumerate(copies):
        copy.wait()
        columns = jnp.dot(normed, w_ref[part], preferred_element_type=jnp.float32)
        columns = columns + bias_ref[:, part * wide : (part + 1) * wide]
        for index in range(wide // HD):
            head = part * (wide // HD) + index
            piece = columns[:, index * HD : (index + 1) * HD]
            if head < H + KVH:
                piece = turned(piece, cosine, sine)
            if head < H:
                piece = piece * (HD**-0.5)
            for slot in range(2 * SEQS):
                seq, half = slot_of(slot)
                own = piece[slot * rows : (slot + 1) * rows]
                if head < H:
                    group, member = head // (H // KVH), head % (H // KVH)
                    q_acc[seq, half, group, member * rows : (member + 1) * rows] = own
                else:
                    group, kind = (head - H) % KVH, (head - H) // KVH
                    at = key_column(slot, group, kind)
                    kv_ref[:, at : at + HD] = own.astype(jnp.bfloat16)
    q_ref[...] = q_acc[...].astype(jnp.bfloat16)


def project(tokens, gain, weight, bias, cosine, signed_sine, rows):
    vmem = pl.BlockSpec(memory_space=pltpu.VMEM)
    parts = 8
    grouped = (SEQS, 2, KVH, H // KVH * rows, HD)
    return pl.pallas_call(
        functools.partial(project_kernel, rows),
        in_specs=[vmem, vmem, pl.BlockSpec(memory_space=pl.ANY), vmem, vmem, vmem],
        out_specs=[vmem, vmem, vmem],
        out_shape=[
            jax.ShapeDtypeStruct(tokens.shape, jnp.bfloat16),
            jax.ShapeDtypeStruct(grouped, jnp.bfloat16),
            jax.ShapeDtypeStruct((rows, SEQS * KVH * 4 * HD), jnp.bfloat16),
        ],
        scratch_shapes=[
            pltpu.VMEM((parts, D, QKV // parts), jnp.bfloat16),
            pltpu.VMEM(grouped, jnp.float32),
            pltpu.SemaphoreType.DMA((parts,)),
        ],
        compiler_params=pltpu.CompilerParams(vmem_limit_bytes=40 * 2**20),
        cost_estimate=pl.CostEstimate(
            flops=2 * tokens.shape[0] * D * QKV, bytes_accessed=2 * D * QKV, transcendentals=0
        ),
        name="project",
    )(tokens, gain.reshape(1, -1), weight, bias.reshape(1, -1), cosine, signed_sine)


def unproject_kernel(rows, gq_ref, gkv_ref, cos_ref, sin_ref, w_hbm, x_ref, gain_ref, past_ref, gp_ref, gi_ref, gg_ref, gb_ref, w_ref, gp_acc, sem):
    copy = pltpu.make_async_copy(w_hbm, w_ref, sem)
    copy.start()
    cosine, sine = cos_ref[...], sin_ref[...]

    def rounded(values):
        return values.astype(jnp.bfloat16).astype(jnp.float32)

    for head in range(H + 2 * KVH):
        for slot in range(2 * SEQS):
            seq, half = slot_of(slot)
            at = slice(slot * rows, (slot + 1) * rows)
            if head < H:
                group, member = head // (H // KVH), head % (H // KVH)
                grad = gq_ref[seq, half, group, member * rows : (member + 1) * rows]
                grad = rounded(grad) * (HD**-0.5)
            else:
                group, kind = (head - H) % KVH, (head - H) // KVH
                column = key_column(slot, group, kind)
                grad = rounded(gkv_ref[:, column : column + HD])
            if head < H + KVH:
                grad = turned_back(grad, cosine[at], sine[at])
            gp_acc[at, head * HD : (head + 1) * HD] = grad
    low = gp_acc[...].astype(jnp.bfloat16)
    gp_ref[...] = low
    gb_ref[...] = jnp.sum(low.astype(jnp.float32), 0, keepdims=True)
    values = x_ref[...].astype(jnp.float32)
    scale = lax.rsqrt(jnp.mean(values * values, -1, keepdims=True) + EPS)
    unit = values * scale
    copy.wait()
    grad_normed = lax.dot_general(low, w_ref[...], CONTRACT_LAST, preferred_element_type=jnp.float32)
    gg_ref[...] = jnp.sum(grad_normed * unit, 0, keepdims=True)
    grad_unit = grad_normed * gain_ref[...]
    inner = jnp.mean(grad_unit * unit, -1, keepdims=True)
    gi_ref[...] = past_ref[...] + scale * (grad_unit - unit * inner)


def unproject(grad_queries, grad_kv, cosine, signed_sine, weight, tokens, gain, past, rows):
    vmem = pl.BlockSpec(memory_space=pltpu.VMEM)
    return pl.pallas_call(
        functools.partial(unproject_kernel, rows),
        in_specs=[vmem, vmem, vmem, vmem, pl.BlockSpec(memory_space=pl.ANY), vmem, vmem, vmem],
        out_specs=[vmem] * 4,
        out_shape=[
            jax.ShapeDtypeStruct((tokens.shape[0], QKV), jnp.bfloat16),
            jax.ShapeDtypeStruct(tokens.shape, jnp.float32),
            jax.ShapeDtypeStruct((1, D), jnp.float32),
            jax.ShapeDtypeStruct((1, QKV), jnp.float32),
        ],
        scratch_shapes=[
            pltpu.VMEM((D, QKV), jnp.bfloat16),
            pltpu.VMEM((tokens.shape[0], QKV), jnp.float32),
            pltpu.SemaphoreType.DMA,
        ],
        compiler_params=pltpu.CompilerParams(vmem_limit_bytes=40 * 2**20),
        cost_estimate=pl.CostEstimate(
            flops=2 * tokens.shape[0] * D * QKV, bytes_accessed=2 * D * QKV, transcendentals=0
        ),
        name="unproject",
    )(grad_queries, grad_kv, cosine, signed_sine, weight, tokens, gain.reshape(1, -1), past)


def pack_kernel(columns, gate_ref, up_ref, out_ref):
    width = out_ref.shape[2] // 2
    cut = out_ref.shape[1]
    for there in range(out_ref.shape[0]):
        for side, ref in enumerate((gate_ref, up_ref)):
            at = side * width
            out_ref[there, :, at + width - HD : at + width] = jnp.zeros((cut, HD), out_ref.dtype)
            out_ref[there, :, at : at + columns] = ref[:, there * columns : (there + 1) * columns]


def pack(gate, up, shard_count, columns, width):
    return pl.pallas_call(
        functools.partial(pack_kernel, columns),
        in_specs=[pl.BlockSpec(memory_space=pltpu.VMEM)] * 2,
        out_specs=pl.BlockSpec(memory_space=pltpu.VMEM),
        out_shape=jax.ShapeDtypeStruct((shard_count, gate.shape[0], 2 * width), gate.dtype),
        name="pack",
    )(gate, up)


def unpack_kernel(columns, in_ref, gate_ref, up_ref):
    width = in_ref.shape[3] // 2
    for there in range(in_ref.shape[1]):
        for side, ref in enumerate((gate_ref, up_ref)):
            part = in_ref[0, there, :, side * width : side * width + columns]
            ref[0, :, there * columns : (there + 1) * columns] = part.astype(jnp.float32)


def unpack(rows, columns):
    ctx_size, shard_count, cut, _ = rows.shape
    out = jax.ShapeDtypeStruct((ctx_size, cut, shard_count * columns), jnp.float32)
    return pl.pallas_call(
        functools.partial(unpack_kernel, columns),
        grid=(ctx_size,),
        in_specs=[pl.BlockSpec((1,) + rows.shape[1:], lambda c: (c, 0, 0, 0))],
        out_specs=[pl.BlockSpec((1, cut, shard_count * columns), lambda c: (c, 0, 0))] * 2,
        out_shape=[out, out],
        name="unpack",
    )(rows)


def shards(
    layer_input,
    block_order,
    first_gain,
    w_qkv,
    b_qkv,
    w_o,
    second_gain,
    w_gate,
    w_up,
    w_down,
    cotangent,
):
    ctx_size = lax.axis_size("ctx")
    shard_count = lax.axis_size("fsdp")
    own_ctx = lax.axis_index("ctx")
    own_shard = lax.axis_index("fsdp")
    rows_here = layer_input.shape[0]
    block_rows = rows_here * shard_count
    cut = D // (ctx_size * shard_count)
    columns = FF // shard_count
    cosine, signed_sine = turn_tables(
        block_order, own_ctx, ctx_size, block_rows, own_shard * rows_here, rows_here
    )
    tokens = by_slot(layer_input)
    grad_out = by_slot(cotangent)

    def by_rows(ctx, shard):
        return shard * ctx_size + ctx

    def by_tokens(ctx, shard):
        return ctx * shard_count + shard

    def own_cut(weight):
        return lax.dynamic_slice_in_dim(weight, own_ctx * cut, cut, 0)

    def mix_features(values):
        shaped = values.reshape(-1, shard_count, ctx_size, cut)
        return shaped.transpose(0, 2, 1, 3).reshape(-1, D)

    def unmix_features(values):
        shaped = values.reshape(-1, ctx_size, shard_count, cut)
        return shaped.transpose(0, 2, 1, 3).reshape(-1, D)

    small = jnp.concatenate([b_qkv, first_gain, second_gain]).reshape(ctx_size, -1)
    small_width = small.shape[1]
    small = lax.dynamic_slice_in_dim(small, own_ctx, 1, 0)
    small = jnp.pad(small, ((0, 0), (0, 16 * HD - small_width))).reshape(16, HD)
    width = -(-columns // HD) * HD
    w_qkv_all, w_o_all, small_all, cotangent_all = gather(
        [own_cut(w_qkv), own_cut(w_o), small, grad_out],
        [by_rows, by_rows, by_rows, lambda ctx, shard: shard],
        1,
        wide=(0, 1, 2),
    )
    cotangent_all = cotangent_all.reshape(-1, D)
    w_qkv_all = w_qkv_all.reshape(D, QKV)
    w_o_all = w_o_all.reshape(D, D)
    small_all = small_all.reshape(shard_count, ctx_size, -1)[:, :, :small_width]
    small_all = small_all.reshape(shard_count, -1).astype(jnp.float32)
    bias_width = QKV // shard_count
    gain_width = D // shard_count
    bias_all = small_all[:, :bias_width].reshape(-1)
    gain_one = small_all[:, bias_width : bias_width + gain_width].reshape(-1)
    gain_two = small_all[:, bias_width + gain_width :].reshape(-1)

    down_padded = jnp.pad(w_down, ((0, width - columns), (0, 0)))

    normed_one, queries, own_kv = project(
        tokens, gain_one, w_qkv_all, bias_all, cosine, signed_sine, rows_here
    )
    all_kv, gate_up_cut = gather(
        [own_kv],
        [by_tokens],
        2,
        swaps=[pack(own_cut(w_gate), own_cut(w_up), shard_count, columns, width)],
    )
    gate_up_cols = lax.all_gather(
        gate_up_cut.reshape(shard_count * cut, 2 * width), "ctx", axis=0, tiled=True
    )
    all_kv = all_kv.reshape(-1, SEQS * KVH * 4 * HD)
    scalars = jnp.concatenate(
        [block_order.reshape(-1), jnp.stack([own_ctx, own_shard]).astype(jnp.int32)]
    )
    attended_grouped, stats = attend_forward(
        scalars, queries, all_kv, ctx_size, block_rows, rows_here
    )
    attended_low = from_groups(attended_grouped, rows_here).astype(jnp.bfloat16)
    middle = tokens.astype(jnp.float32) + jnp.dot(attended_low, w_o_all, preferred_element_type=jnp.float32)
    unit_two, scale_two, normed = normalize(middle, gain_two)
    normed_two = mix_features(normed.astype(jnp.bfloat16))

    (tokens_all,) = gather([normed_two], [lambda ctx, shard: shard], 6, wide=())
    tokens_all = tokens_all.reshape(-1, D)
    gate_up_part = jnp.dot(tokens_all, gate_up_cols, preferred_element_type=jnp.float32)
    gate_part, up_part = gate_up_part[:, :width], gate_up_part[:, width:]
    sigmoid_gate = jax.nn.sigmoid(gate_part)
    activated = gate_part * sigmoid_gate
    hidden = (activated * up_part).astype(jnp.bfloat16)
    grad_hidden = lax.dot_general(
        cotangent_all, down_padded, CONTRACT_LAST, preferred_element_type=jnp.float32
    )
    grad_gate = grad_hidden * up_part * sigmoid_gate * (1.0 + gate_part * (1.0 - sigmoid_gate))
    grad_gate_up = jnp.concatenate([grad_gate, grad_hidden * activated], -1).astype(jnp.bfloat16)
    grad_tokens = lax.dot_general(
        grad_gate_up, gate_up_cols, CONTRACT_LAST, preferred_element_type=jnp.float32
    ).astype(jnp.bfloat16)
    grad_normed_two = lax.psum_scatter(
        grad_tokens, "fsdp", scatter_dimension=0, tiled=True
    ).astype(jnp.float32)
    grad_gate_up, hidden, grad_tokens = lax.optimization_barrier(
        (grad_gate_up, hidden, grad_tokens)
    )
    gate_up_terms = lax.dot_general(
        tokens_all, grad_gate_up, CONTRACT_FIRST, preferred_element_type=jnp.float32
    ).astype(jnp.bfloat16)
    gate_up_rows = lax.psum_scatter(gate_up_terms, "ctx", scatter_dimension=0, tiled=True)
    down_terms = lax.dot_general(
        hidden, cotangent_all, CONTRACT_FIRST, preferred_element_type=jnp.float32
    ).astype(jnp.bfloat16)
    down_rows = lax.psum(down_terms, "ctx")
    mixed_terms = jnp.dot(hidden, down_padded, preferred_element_type=jnp.float32).astype(jnp.bfloat16)
    grad_normed_two, down_terms, gate_up_terms, mixed_terms = lax.optimization_barrier(
        (grad_normed_two, down_terms, gate_up_terms, mixed_terms)
    )
    grad_normed_two = unmix_features(grad_normed_two)
    grad_middle_norm, grad_gain_two = norm_back(grad_normed_two, unit_two, scale_two, gain_two)
    grad_middle = grad_out.astype(jnp.float32) + grad_middle_norm
    grad_branch_one = grad_middle.astype(jnp.bfloat16)
    grad_attended = lax.dot_general(
        grad_branch_one, w_o_all, CONTRACT_LAST, preferred_element_type=jnp.float32
    ).astype(jnp.bfloat16)
    o_terms = lax.dot_general(
        attended_low, grad_branch_one, CONTRACT_FIRST, preferred_element_type=jnp.float32
    ).astype(jnp.bfloat16)
    grad_queries, grad_kv_full = attend_backward(
        scalars,
        queries,
        to_groups(grad_attended, rows_here),
        attended_grouped,
        stats,
        all_kv,
        ctx_size,
        block_rows,
        rows_here,
    )
    grad_kv, mixed_rows = scatter(
        [grad_kv_full.reshape(-1, rows_here, SEQS * KVH * 4 * HD)],
        by_tokens,
        3,
        out_dtype=jnp.float32,
        lines=[mixed_terms.reshape(shard_count, -1, D)],
    )
    gate_up_rows, grad_kv = lax.optimization_barrier((gate_up_rows, grad_kv))
    gate_up_rows = exchange(gate_up_rows.reshape(shard_count, cut, 2 * width), 5)
    gate_up_rows = lax.all_gather(gate_up_rows, "ctx", axis=0, tiled=False)
    grad_projected, grad_input, grad_gain_one, grad_bias = unproject(
        grad_queries,
        grad_kv,
        cosine,
        signed_sine,
        w_qkv_all,
        tokens,
        gain_one,
        grad_middle,
        rows_here,
    )
    grad_input = from_slot(grad_input, rows_here)
    grad_bias = grad_bias.reshape(-1)
    qkv_terms = lax.dot_general(
        normed_one, grad_projected, CONTRACT_FIRST, preferred_element_type=jnp.float32
    ).astype(jnp.bfloat16)
    small_terms = jnp.concatenate(
        [
            part.reshape(shard_count, -1)
            for part in (grad_gain_one, grad_gain_two, grad_bias[:QK], grad_bias[QK:])
        ],
        1,
    )
    small_terms = small_terms.reshape(ctx_size * shard_count, small_width)
    small_terms = jnp.pad(small_terms, ((0, 0), (0, 8 * HD - small_width)))
    qkv_rows, o_rows, small_rows = scatter(
        [
            qkv_terms.reshape(-1, cut, QKV),
            o_terms.reshape(-1, cut, D),
            small_terms.reshape(-1, 8, HD),
        ],
        by_rows,
        4,
        spread_ctx=True,
    )
    mixed_out = middle + mixed_rows
    output = from_slot(mixed_out.astype(jnp.bfloat16), rows_here)
    small_rows = small_rows.reshape(ctx_size, -1)[:, :small_width].reshape(-1)
    bias_start = 2 * gain_width
    value_start = bias_start + QK // shard_count

    gate_rows, up_rows = unpack(gate_up_rows, columns)
    return (
        output,
        grad_input,
        small_rows[:gain_width],
        qkv_rows.reshape(-1, QKV).astype(jnp.float32),
        small_rows[bias_start:value_start],
        small_rows[value_start:],
        o_rows.reshape(-1, D).astype(jnp.float32),
        small_rows[gain_width:bias_start],
        gate_rows.reshape(-1, FF),
        up_rows.reshape(-1, FF),
        down_rows[:columns].astype(jnp.float32),
    )


def solution(mesh):
    in_specs = (
        P(("ctx", "fsdp"), None, None),
        P(),
        P("fsdp"),
        P("fsdp", None),
        P("fsdp"),
        P("fsdp", None),
        P("fsdp"),
        P("fsdp", None),
        P("fsdp", None),
        P("fsdp", None),
        P(("ctx", "fsdp"), None, None),
    )
    out_specs = (
        P(("ctx", "fsdp"), None, None),
        P(("ctx", "fsdp"), None, None),
        P("fsdp"),
        P("fsdp", None),
        P("fsdp"),
        P("fsdp"),
        P("fsdp", None),
        P("fsdp"),
        P("fsdp", None),
        P("fsdp", None),
        P("fsdp", None),
    )
    return jax.shard_map(shards, mesh=mesh, in_specs=in_specs, out_specs=out_specs, check_vma=False)
```

```python
import functools

import jax
import jax.numpy as jnp
from jax import lax
from jax.experimental import pallas as pl
from jax.experimental.pallas import tpu as pltpu
from jax.sharding import PartitionSpec as P

D = 1536
H = 12
KVH = 2
HD = 128
FF = 8960
SEQS = 2
QKV = 2048
QK = 1792


EPS = 1e-06
THETA = 1000000.0
NEG_FILL = -1e30
MESH_ID = pl.DeviceIdType.MESH
CONTRACT_LAST = (((1,), (1,)), ((), ()))
CONTRACT_FIRST = (((0,), (0,)), ((), ()))


def by_slot(tokens):
    return tokens.transpose(1, 0, 2).reshape(-1, tokens.shape[2])


def from_slot(tokens, row_count):
    return tokens.reshape(2 * SEQS, row_count, -1).transpose(1, 0, 2)


def to_groups(tokens, row_count):
    shaped = tokens.reshape(2, SEQS, row_count, KVH, H // KVH, HD)
    return shaped.transpose(1, 0, 3, 4, 2, 5).reshape(SEQS, 2, KVH, H // KVH * row_count, HD)


def from_groups(grouped, row_count):
    shaped = grouped.reshape(SEQS, 2, KVH, H // KVH, row_count, HD).transpose(1, 0, 4, 2, 3, 5)
    return shaped.reshape(row_count * 2 * SEQS, H * HD)


def turn_tables(block_order, own_ctx, ctx_size, block_rows, first_row, row_count):
    half_width = HD // 2
    frequency = THETA ** (-jnp.arange(half_width, dtype=jnp.float32) * 2.0 / HD)
    frequency = jnp.tile(frequency, 2)[None, :]
    order = lax.dynamic_index_in_dim(block_order.reshape(SEQS, 2, ctx_size), own_ctx, 2, False)
    start = (order.T.reshape(-1) * block_rows + first_row).astype(jnp.float32)
    far = start[:, None] * frequency
    near = jnp.arange(row_count, dtype=jnp.float32)[:, None] * frequency
    far_cos, far_sin = jnp.cos(far)[:, None, :], jnp.sin(far)[:, None, :]
    near_cos, near_sin = jnp.cos(near)[None], jnp.sin(near)[None]
    sign = jnp.where(jnp.arange(HD) < half_width, -1.0, 1.0).astype(jnp.float32)
    cosine = far_cos * near_cos - far_sin * near_sin
    sine = (far_sin * near_cos + far_cos * near_sin) * sign
    return cosine.reshape(-1, HD), sine.reshape(-1, HD)


def normalize(values, gain):
    scale = lax.rsqrt(jnp.mean(values * values, -1, keepdims=True) + EPS)
    unit = values * scale
    return (unit, scale, unit * gain)


def norm_back(grad_out, unit, scale, gain):
    grad_unit = grad_out * gain
    inner = jnp.mean(grad_unit * unit, -1, keepdims=True)
    return (scale * (grad_unit - unit * inner), jnp.sum(grad_out * unit, 0))


def attend_forward_kernel(ctx_size, block_rows, rows_here, scalars, q_ref, kv_ref, out_ref, stat_ref, best_ref, total_ref, accum_ref):
    seq = pl.program_id(0)
    blocks = 2 * ctx_size
    own_ctx = scalars[SEQS * blocks]
    own_shard = scalars[SEQS * blocks + 1]
    lanes = q_ref.shape[3]
    best_ref[...] = jnp.full(best_ref.shape, NEG_FILL, jnp.float32)
    total_ref[...] = jnp.zeros(total_ref.shape, jnp.float32)
    accum_ref[...] = jnp.zeros(accum_ref.shape, jnp.float32)

    def step(key_ctx, half_key, half):
        order_key = scalars[seq * blocks + half_key * ctx_size + key_ctx]
        order_query = scalars[seq * blocks + half * ctx_size + own_ctx]

        def work(masked):
            rows = pl.ds(pl.multiple_of(key_ctx * block_rows, block_rows), block_rows)
            keys = kv_ref[rows, half_key * 2 * HD : half_key * 2 * HD + HD]
            values = kv_ref[rows, half_key * 2 * HD + HD : half_key * 2 * HD + 2 * HD]
            scores = lax.dot_general(
                keys, q_ref[0, half, 0], CONTRACT_LAST, preferred_element_type=jnp.float32
            )
            if masked:
                row = lax.broadcasted_iota(jnp.int32, (block_rows, lanes), 0)
                lane = lax.broadcasted_iota(jnp.int32, (block_rows, lanes), 1)
                scores = jnp.where(
                    row <= own_shard * rows_here + lax.rem(lane, rows_here), scores, NEG_FILL
                )
            best = best_ref[half]
            fresh = jnp.maximum(best, jnp.max(scores, 0, keepdims=True))
            decay = jnp.exp(best - fresh)
            weights = jnp.exp(scores - fresh)
            total_ref[half] = total_ref[half] * decay + jnp.sum(weights, 0, keepdims=True)
            accum_ref[half] = accum_ref[half] * decay + lax.dot_general(
                values,
                weights.astype(jnp.bfloat16),
                CONTRACT_FIRST,
                preferred_element_type=jnp.float32,
            )
            best_ref[half] = fresh

        @pl.when(order_key < order_query)
        def full():
            work(False)

        @pl.when(order_key == order_query)
        def diagonal():
            work(True)

    @pl.loop(0, ctx_size)
    def sweep(key_ctx):
        for half_key in range(2):
            for half in range(2):
                step(key_ctx, half_key, half)

    for half in range(2):
        totals = total_ref[half]
        out_ref[0, half, 0] = (accum_ref[half] / totals).T
        stat_ref[0, half, 0] = best_ref[half] + jnp.log(totals)


def attend_forward(scalars, queries, all_kv, ctx_size, block_rows, rows_here):
    lanes = queries.shape[3]
    kernel = functools.partial(attend_forward_kernel, ctx_size, block_rows, rows_here)
    group = pl.BlockSpec((1, 2, 1, lanes, HD), lambda s, n, _: (s, 0, n, 0, 0))
    stat = pl.BlockSpec((1, 2, 1, 1, lanes), lambda s, n, _: (s, 0, n, 0, 0))
    return pl.pallas_call(
        kernel,
        grid_spec=pltpu.PrefetchScalarGridSpec(
            num_scalar_prefetch=1,
            grid=(SEQS, KVH),
            in_specs=[
                group,
                pl.BlockSpec((all_kv.shape[0], 4 * HD), lambda s, n, _: (0, s * KVH + n)),
            ],
            out_specs=[group, stat],
            scratch_shapes=[
                pltpu.VMEM((2, 1, lanes), jnp.float32),
                pltpu.VMEM((2, 1, lanes), jnp.float32),
                pltpu.VMEM((2, HD, lanes), jnp.float32),
            ],
        ),
        out_shape=(
            jax.ShapeDtypeStruct(queries.shape, jnp.float32),
            jax.ShapeDtypeStruct((SEQS, 2, KVH, 1, lanes), jnp.float32),
        ),
        compiler_params=pltpu.CompilerParams(vmem_limit_bytes=56 * 2**20),
        name="attend_forward",
    )(scalars, queries, all_kv)


def attend_backward_kernel(ctx_size, block_rows, rows_here, scalars, q_ref, go_ref, att_ref, stat_ref, kv_ref, gq_ref, gkv_ref, delta_ref, gq_acc, gk_acc, gv_acc):
    seq = pl.program_id(0)
    blocks = 2 * ctx_size
    own_ctx = scalars[SEQS * blocks]
    own_shard = scalars[SEQS * blocks + 1]
    lanes = q_ref.shape[3]
    gq_acc[...] = jnp.zeros(gq_acc.shape, jnp.float32)
    for half in range(2):
        product = go_ref[0, half, 0].astype(jnp.float32) * att_ref[0, half, 0]
        delta_ref[half] = jnp.sum(product.T, 0, keepdims=True)

    def step(key_ctx, half_key, half):
        order_key = scalars[seq * blocks + half_key * ctx_size + key_ctx]
        order_query = scalars[seq * blocks + half * ctx_size + own_ctx]

        def work(masked):
            rows = pl.ds(pl.multiple_of(key_ctx * block_rows, block_rows), block_rows)
            keys = kv_ref[rows, half_key * 2 * HD : half_key * 2 * HD + HD]
            values = kv_ref[rows, half_key * 2 * HD + HD : half_key * 2 * HD + 2 * HD]
            queries = q_ref[0, half, 0]
            grad_out = go_ref[0, half, 0]
            scores = lax.dot_general(
                keys, queries, CONTRACT_LAST, preferred_element_type=jnp.float32
            )
            probs = jnp.exp(scores - stat_ref[0, half, 0])
            if masked:
                row = lax.broadcasted_iota(jnp.int32, (block_rows, lanes), 0)
                lane = lax.broadcasted_iota(jnp.int32, (block_rows, lanes), 1)
                probs = jnp.where(
                    row <= own_shard * rows_here + lax.rem(lane, rows_here), probs, 0.0
                )
            grad_probs = lax.dot_general(
                values, grad_out, CONTRACT_LAST, preferred_element_type=jnp.float32
            )
            grad_scores = (probs * (grad_probs - delta_ref[half])).astype(jnp.bfloat16)
            gv_acc[...] += jnp.dot(
                probs.astype(jnp.bfloat16), grad_out, preferred_element_type=jnp.float32
            )
            gk_acc[...] += jnp.dot(grad_scores, queries, preferred_element_type=jnp.float32)
            gq_acc[half] += lax.dot_general(
                keys, grad_scores, CONTRACT_FIRST, preferred_element_type=jnp.float32
            )

        @pl.when(order_key < order_query)
        def full():
            work(False)

        @pl.when(order_key == order_query)
        def diagonal():
            work(True)

    @pl.loop(0, ctx_size)
    def sweep(key_ctx):
        rows = pl.ds(pl.multiple_of(key_ctx * block_rows, block_rows), block_rows)
        for half_key in range(2):
            gk_acc[...] = jnp.zeros(gk_acc.shape, jnp.float32)
            gv_acc[...] = jnp.zeros(gv_acc.shape, jnp.float32)
            for half in range(2):
                step(key_ctx, half_key, half)
            at = half_key * 2 * HD
            gkv_ref[rows, at : at + HD] = gk_acc[...].astype(jnp.bfloat16)
            gkv_ref[rows, at + HD : at + 2 * HD] = gv_acc[...].astype(jnp.bfloat16)

    for half in range(2):
        gq_ref[0, half, 0] = gq_acc[half].T


def attend_backward(scalars, queries, grad_out, attended, stats, all_kv, ctx_size, block_rows, rows_here):
    lanes = queries.shape[3]
    kernel = functools.partial(attend_backward_kernel, ctx_size, block_rows, rows_here)
    group = pl.BlockSpec((1, 2, 1, lanes, HD), lambda s, n, _: (s, 0, n, 0, 0))
    stat = pl.BlockSpec((1, 2, 1, 1, lanes), lambda s, n, _: (s, 0, n, 0, 0))
    full = pl.BlockSpec((all_kv.shape[0], 4 * HD), lambda s, n, _: (0, s * KVH + n))
    return pl.pallas_call(
        kernel,
        grid_spec=pltpu.PrefetchScalarGridSpec(
            num_scalar_prefetch=1,
            grid=(SEQS, KVH),
            in_specs=[group, group, group, stat, full],
            out_specs=[group, full],
            scratch_shapes=[
                pltpu.VMEM((2, 1, lanes), jnp.float32),
                pltpu.VMEM((2, HD, lanes), jnp.float32),
                pltpu.VMEM((block_rows, HD), jnp.float32),
                pltpu.VMEM((block_rows, HD), jnp.float32),
            ],
        ),
        out_shape=(
            jax.ShapeDtypeStruct(queries.shape, jnp.float32),
            jax.ShapeDtypeStruct(all_kv.shape, jnp.bfloat16),
        ),
        compiler_params=pltpu.CompilerParams(vmem_limit_bytes=56 * 2**20),
        name="attend_backward",
    )(scalars, queries, grad_out, attended, stats, all_kv)


def peers_of(ctx_size):
    return ctx_size == 4, range(1, ctx_size)


def ctx_target(position, way, square, ctx_size):
    return position ^ way if square else lax.rem(position + way, ctx_size)


def ctx_source(position, way, square, ctx_size):
    return position ^ way if square else lax.rem(position + ctx_size - way, ctx_size)


def greet(ctx_size, pair_count, with_ctx, all_shards):
    ctx = lax.axis_index("ctx")
    shard = lax.axis_index("fsdp")
    pair, core = shard // 2, shard % 2
    barrier = pltpu.get_barrier_semaphore()
    partners = [(ctx, pair * 2 + 1 - core)]
    for step in range(1, pair_count):
        there = lax.rem(pair + step, pair_count) * 2
        partners.append((ctx, there + core))
        if all_shards:
            partners.append((ctx, there + 1 - core))
    if with_ctx:
        for way in range(1, ctx_size):
            partners.append((lax.rem(ctx + way, ctx_size), shard))
    for partner in partners:
        pl.semaphore_signal(barrier, inc=1, device_id=partner, device_id_type=MESH_ID)
    pl.semaphore_wait(barrier, len(partners))
    return ctx, pair, core


class Exchange:
    def __init__(self, source, out, sems, own_sem, pair_count):
        self.source, self.out, self.sems, self.own_sem = source, out, sems, own_sem
        self.shard_count = 2 * pair_count

    def start(self):
        ctx, shard = lax.axis_index("ctx"), lax.axis_index("fsdp")
        self.own = pltpu.make_async_copy(self.source.at[shard], self.out.at[shard], self.own_sem)
        self.own.start()
        self.copies = []
        for step in range(1, self.shard_count):
            there = lax.rem(shard + step, self.shard_count)
            copy = pltpu.make_async_remote_copy(
                src_ref=self.source.at[there],
                dst_ref=self.out.at[shard],
                send_sem=self.sems[0].at[step - 1],
                recv_sem=self.sems[1].at[step - 1],
                device_id=(ctx, there),
                device_id_type=MESH_ID,
            )
            copy.start()
            self.copies.append(copy)

    def finish(self):
        ctx, shard = lax.axis_index("ctx"), lax.axis_index("fsdp")
        for step in range(1, self.shard_count):
            come = lax.rem(shard + self.shard_count - step, self.shard_count)
            pltpu.make_async_remote_copy(
                src_ref=self.out.at[come],
                dst_ref=self.out.at[come],
                send_sem=self.sems[0].at[step - 1],
                recv_sem=self.sems[1].at[step - 1],
                device_id=(ctx, shard),
                device_id_type=MESH_ID,
            ).wait_recv()
        self.own.wait()
        for copy in self.copies:
            copy.wait_send()


def exchange_kernel(pair_count, source, out, send_sem, recv_sem, own_sem):
    greet(1, pair_count, False, True)
    flow = Exchange(source, out, (send_sem, recv_sem), own_sem, pair_count)
    flow.start()
    flow.finish()


def exchange(pieces, collective_id):
    shard_count = lax.axis_size("fsdp")
    dma = pltpu.SemaphoreType.DMA
    return pl.pallas_call(
        functools.partial(exchange_kernel, shard_count // 2),
        in_specs=[pl.BlockSpec(memory_space=pltpu.VMEM)],
        out_specs=pl.BlockSpec(memory_space=pl.ANY),
        out_shape=jax.ShapeDtypeStruct(pieces.shape, pieces.dtype),
        scratch_shapes=[dma((shard_count - 1,))] * 2 + [dma],
        compiler_params=pltpu.CompilerParams(collective_id=collective_id, has_side_effects=True),
        cost_estimate=pl.CostEstimate(
            flops=0, bytes_accessed=pieces.size * 64, transcendentals=0
        ),
    )(pieces)


def gather_kernel(arity, ctx_size, pair_count, slots, swaps, wide, *refs):
    sources, refs = refs[:arity], refs[arity:]
    swap_sources, refs = refs[:swaps], refs[swaps:]
    outs, refs = refs[:arity], refs[arity:]
    swap_outs, refs = refs[:swaps], refs[swaps:]
    pair_sems, ctx_sems, core_sems = refs[0:2], refs[2:4], refs[4:6]
    local_sem = refs[6]
    square, ways = peers_of(ctx_size) if wide else (False, ())
    narrow = [item for item in range(arity) if item not in wide]
    near = [way for way in ways if not (square and way == 3)]
    ctx, pair, core = greet(ctx_size, pair_count, len(wide) > 0, swaps > 0)
    homes = [place(ctx, pair * 2 + core) for place in slots]
    started = []
    steps = [(0, 1)] + [(far, way) for far in range(1, pair_count) for way in (1, -1)]

    def present(step):
        far, way = steps[step]
        if far == 0:
            return None
        return pair >= far if way == 1 else pair + far < pair_count

    def origin(step):
        far, way = steps[step]
        return pair - far * way

    def when(condition, work):
        if condition is None:
            work()
        else:
            pl.when(condition)(work)

    def send(item, source, place, target, sems, at, condition):
        copy = pltpu.make_async_remote_copy(
            src_ref=source,
            dst_ref=outs[item].at[place],
            send_sem=sems[0].at[at],
            recv_sem=sems[1].at[at],
            device_id=target,
            device_id_type=MESH_ID,
        )
        copy.start()
        started.append((condition, item, sems, at))

    def sent(item, sems, at):
        pltpu.make_async_remote_copy(
            src_ref=outs[item].at[0],
            dst_ref=outs[item].at[0],
            send_sem=sems[0].at[at],
            recv_sem=sems[1].at[at],
            device_id=(ctx, pair * 2 + core),
            device_id_type=MESH_ID,
        ).wait_send()

    def arrive(item, place, sems, at):
        pltpu.make_async_remote_copy(
            src_ref=outs[item].at[place],
            dst_ref=outs[item].at[place],
            send_sem=sems[0].at[at],
            recv_sem=sems[1].at[at],
            device_id=(ctx, pair * 2 + core),
            device_id_type=MESH_ID,
        ).wait_recv()

    def pass_on(step, item, source, place):
        far, way = steps[step]
        for side in (1, -1) if far == 0 else (way,):

            def further(side=side):
                return pair + 1 < pair_count if side == 1 else pair >= 1

            def both(further=further):
                return further() if far == 0 else jnp.logical_and(further(), present(step))

            def work(side=side, both=both):
                send(
                    item,
                    source,
                    place,
                    (ctx, (pair + side) * 2 + core),
                    pair_sems,
                    ((side + 1) // 2, far, item),
                    both,
                )

            if far + 1 < pair_count:
                pl.when(further())(work)

    def to_core(item, source, from_ctx, way, step):
        send(
            item,
            source,
            slots[item](from_ctx, origin(step) * 2 + core),
            (ctx, pair * 2 + 1 - core),
            core_sems,
            (way, step, item),
            functools.partial(present, step),
        )

    def spread(step, items):
        for item in items:
            place = slots[item](ctx, origin(step) * 2 + core)
            source = sources[item]
            if step:
                far, way = steps[step]
                arrive(item, place, pair_sems, ((way + 1) // 2, far - 1, item))
                source = outs[item].at[place]
            pass_on(step, item, source, place)
            for way in near if item in wide else ():
                there = ctx_target(ctx, way, square, ctx_size)
                send(
                    item,
                    source,
                    place,
                    (there, pair * 2 + core),
                    ctx_sems,
                    (way - 1, step, item),
                    functools.partial(present, step),
                )
            to_core(item, source, ctx, 0, step)

    def collect(step):
        for way in near:
            for item in wide:
                come = ctx_source(ctx, way, square, ctx_size)
                place = slots[item](come, origin(step) * 2 + core)
                arrive(item, place, ctx_sems, (way - 1, step, item))
                source = outs[item].at[place]
                if square and (steps[step][0] % 2 == 0) == (way == 1):
                    send(
                        item,
                        source,
                        place,
                        (ctx ^ (3 - way), pair * 2 + core),
                        ctx_sems,
                        (2, step, item),
                        functools.partial(present, step),
                    )
                to_core(item, source, come, way, step)

    def collect_far(step):
        for item in wide:
            place = slots[item](ctx ^ 3, origin(step) * 2 + core)
            arrive(item, place, ctx_sems, (2, step, item))
            to_core(item, outs[item].at[place], ctx ^ 3, 3, step)

    def straight_core(item, source, place, step):
        sibling = (ctx, pair * 2 + 1 - core)
        send(item, source, place, sibling, core_sems, (0, step, item), lambda: None)

    def go_straight(item):
        for step in range(1, pair_count):
            there = lax.rem(pair + step, pair_count) * 2 + core
            at = (0, step - 1, item)
            send(item, sources[item], homes[item], (ctx, there), pair_sems, at, lambda: None)
        straight_core(item, sources[item], homes[item], 0)

    locals_ = []
    for item in range(arity):
        copy = pltpu.make_async_copy(sources[item], outs[item].at[homes[item]], local_sem.at[item])
        copy.start()
        locals_.append(copy)
    spread(0, wide or range(arity))
    flows = []
    count = len(steps)
    for turn in range(1, count + 4):
        if turn < count:
            when(present(turn), functools.partial(spread, turn, wide or range(arity)))
        if turn == count:
            for item in narrow if wide else ():
                go_straight(item)
            for item in range(swaps):
                flow = Exchange(
                    swap_sources[item],
                    swap_outs[item],
                    refs[7 + 3 * item : 9 + 3 * item],
                    refs[9 + 3 * item],
                    pair_count,
                )
                flow.start()
                flows.append(flow)
        if 0 <= turn - 2 < count:
            when(present(turn - 2), functools.partial(collect, turn - 2))
        if square and 0 <= turn - 4 < count:
            when(present(turn - 4), functools.partial(collect_far, turn - 4))

    for item in narrow if wide else ():
        for step in range(1, pair_count):
            come = lax.rem(pair + pair_count - step, pair_count)
            place = slots[item](ctx, come * 2 + core)
            arrive(item, place, pair_sems, (0, step - 1, item))
            straight_core(item, outs[item].at[place], place, step)
    for item in narrow if wide else ():
        for step in range(pair_count):
            come = lax.rem(pair + pair_count - step, pair_count)
            arrive(item, slots[item](ctx, come * 2 + 1 - core), core_sems, (0, step, item))

    def from_core(step):
        for way in (0, *ways):
            come = ctx_source(ctx, way, square, ctx_size) if way else ctx
            for item in wide or range(arity):
                arrive(item, slots[item](come, origin(step) * 2 + 1 - core), core_sems, (way, step, item))

    for step in range(count):
        when(present(step), functools.partial(from_core, step))
    for flow in flows:
        flow.finish()
    for copy in locals_:
        copy.wait()
    for condition, *which in started:
        when(condition(), functools.partial(sent, *which))


def gather(pieces, slots, collective_id, swaps=(), wide=None):
    ctx_size, shard_count = lax.axis_size("ctx"), lax.axis_size("fsdp")
    pair_count = shard_count // 2
    arity = len(pieces)
    wide = range(arity) if wide is None else wide
    dma = pltpu.SemaphoreType.DMA
    moved = sum(piece.size for piece in pieces) * 2
    steps = 2 * pair_count - 1
    return pl.pallas_call(
        functools.partial(gather_kernel, arity, ctx_size, pair_count, slots, len(swaps), wide),
        in_specs=[pl.BlockSpec(memory_space=pltpu.VMEM)] * (arity + len(swaps)),
        out_specs=[pl.BlockSpec(memory_space=pl.ANY)] * (arity + len(swaps)),
        out_shape=[
            jax.ShapeDtypeStruct(
                ((ctx_size if item in wide else 1) * shard_count,) + piece.shape, piece.dtype
            )
            for item, piece in enumerate(pieces)
        ]
        + [jax.ShapeDtypeStruct(swap.shape, swap.dtype) for swap in swaps],
        scratch_shapes=[dma((2, pair_count - 1, arity))] * 2
        + [dma((ctx_size - 1, steps, arity))] * 2
        + [dma((ctx_size, steps, arity))] * 2
        + [dma((arity,))]
        + [dma((shard_count - 1,)), dma((shard_count - 1,)), dma] * len(swaps),
        compiler_params=pltpu.CompilerParams(collective_id=collective_id, has_side_effects=True),
        cost_estimate=pl.CostEstimate(
            flops=0, bytes_accessed=moved * ctx_size * shard_count * 4, transcendentals=0
        ),
    )(*pieces, *swaps)


class LineScatter:
    def __init__(self, source, out, half, room, sems, where, counts, last):
        self.count, self.ctx_size = counts
        self.source, self.out, self.half, self.room = source, out, half, room
        self.last = last
        self.core_sems, self.pair_sems = sems[0:2], sems[2:4]
        self.ctx, self.pair, self.core = where
        self.order = [*range(1, self.count), 0]

    def copy(self, source, target, device, sems, at):
        return pltpu.make_async_remote_copy(
            src_ref=source,
            dst_ref=target,
            send_sem=sems[0].at[at],
            recv_sem=sems[1].at[at],
            device_id=device,
            device_id_type=MESH_ID,
        )

    def here(self):
        return (self.ctx, self.pair * 2 + self.core)

    def toward(self, step):
        return lax.rem(self.pair + step, self.count)

    def start(self):
        self.copies = []
        for step in self.order:
            self.copies.append(
                self.copy(
                    self.source.at[self.toward(step) * 2 + 1 - self.core],
                    self.half.at[step],
                    (self.ctx, self.pair * 2 + 1 - self.core),
                    self.core_sems,
                    step,
                )
            )
            self.copies[-1].start()

    def fold(self, step):
        half = self.half.at[step]
        self.copy(half, half, self.here(), self.core_sems, step).wait_recv()
        mine = self.source[self.toward(step) * 2 + self.core].astype(jnp.float32)
        total = mine + half[...].astype(jnp.float32)
        if step == 0:
            self.out[...] = total
            return
        half[...] = total.astype(half.dtype)
        self.copies.append(
            self.copy(
                half,
                self.room.at[step - 1],
                (self.ctx, self.toward(step) * 2 + self.core),
                self.pair_sems,
                step - 1,
            )
        )
        self.copies[-1].start()

    def over_ctx(self, terms, room, landing, *sems):
        shard = self.pair * 2 + self.core
        copies = []

        def send(source, target, way, sems):
            there = lax.rem(self.ctx + way, self.ctx_size)
            copies.append(self.copy(source(there), target, (there, shard), sems, way - 1))
            copies[-1].start()

        def arrive(target, way, sems):
            self.copy(target, target, self.here(), sems, way - 1).wait_recv()

        terms[...] = self.out[...].astype(terms.dtype)
        for way in range(1, self.ctx_size):
            send(lambda there: terms.at[there], room.at[way - 1], way, sems[0:2])
        total = self.out[self.ctx]
        for way in range(1, self.ctx_size):
            arrive(room.at[way - 1], way, sems[0:2])
            total = total + room[way - 1].astype(jnp.float32)
        landing[self.ctx] = total.astype(landing.dtype)
        for way in range(1, self.ctx_size):
            send(lambda there: landing.at[self.ctx], landing.at[self.ctx], way, sems[2:4])
        for way in range(1, self.ctx_size):
            come = lax.rem(self.ctx + self.ctx_size - way, self.ctx_size)
            arrive(landing.at[come], way, sems[2:4])
        self.out[...] = landing[...].astype(jnp.float32)
        for copy in copies:
            copy.wait_send()

    def finish(self):
        for step in range(1, self.count):
            room = self.room.at[step - 1]
            self.copy(room, room, self.here(), self.pair_sems, step - 1).wait_recv()
            self.out[...] += room[...].astype(jnp.float32)
        if self.last:
            self.over_ctx(*self.last)
        for copy in self.copies:
            copy.wait_send()


def scatter_kernel(arity, ctx_size, pair_count, slot, spread_ctx, lines, *refs):
    sources, refs = refs[:arity], refs[arity:]
    line_sources, refs = refs[:lines], refs[lines:]
    outs, refs = refs[:arity], refs[arity:]
    line_outs, refs = refs[:lines], refs[lines:]
    halves, relays, asides, ends, finals = (refs[i * arity : (i + 1) * arity] for i in range(5))
    sems = refs[5 * arity : 5 * arity + 10]
    core_sems, relay_sems, ctx_sems, pair_sems, last_sems = (sems[2 * i : 2 * i + 2] for i in range(5))
    square, ways = peers_of(ctx_size)
    ctx, pair, core = greet(ctx_size, pair_count, True, False)
    order = list(range(1, pair_count)) + [0]
    started = []
    flows = []
    for item in range(lines):
        at = 5 * arity + 10 + 13 * item
        spread = len(line_sources[item].shape) == 4
        flows.append(
            LineScatter(
                line_sources[item],
                line_outs[item],
                *refs[at : at + 2],
                refs[at + 2 : at + 6],
                (ctx, pair, core),
                (pair_count, ctx_size),
                refs[at + 6 : at + 13] if spread else (),
            )
        )

    def send(source, target, device, pair_of_sems, at):
        copy = pltpu.make_async_remote_copy(
            src_ref=source,
            dst_ref=target,
            send_sem=pair_of_sems[0].at[at],
            recv_sem=pair_of_sems[1].at[at],
            device_id=device,
            device_id_type=MESH_ID,
        )
        copy.start()
        started.append(copy)

    def arrive(target, pair_of_sems, at):
        pltpu.make_async_remote_copy(
            src_ref=target,
            dst_ref=target,
            send_sem=pair_of_sems[0].at[at],
            recv_sem=pair_of_sems[1].at[at],
            device_id=(ctx, pair * 2 + core),
            device_id_type=MESH_ID,
        ).wait_recv()

    def toward(step):
        return lax.rem(pair + step, pair_count)

    def target_ctx(way):
        return ctx_target(ctx, way, square, ctx_size) if way else ctx

    def f32(value):
        return value.astype(jnp.float32)

    far_first = [3, 1, 2, 0] if square else list(ways) + [0]
    for step in order:
        for way in far_first:
            for item in range(arity):
                send(
                    sources[item].at[slot(target_ctx(way), toward(step) * 2 + 1 - core)],
                    halves[item].at[way, step],
                    (ctx, pair * 2 + 1 - core),
                    core_sems,
                    (way, step, item),
                )

    def fold_core(step):
        for way in far_first:
            for item in range(arity):
                half = halves[item].at[way, step]
                arrive(half, core_sems, (way, step, item))
                mine = sources[item][slot(target_ctx(way), toward(step) * 2 + core)]
                half[...] = (f32(mine) + f32(half[...])).astype(half.dtype)
                if square and way == 3:
                    there = ctx ^ (1 if step % 2 == 0 else 2)
                    send(
                        half,
                        relays[item].at[step],
                        (there, pair * 2 + core),
                        relay_sems,
                        (step, item),
                    )

    def fold_relay(step):
        for item in range(arity):
            if square:
                relay = relays[item].at[step]
                arrive(relay, relay_sems, (step, item))
                half = halves[item].at[2 if step % 2 == 0 else 1, step]
                half[...] = (f32(half[...]) + f32(relay[...])).astype(half.dtype)
            for way in ways:
                if square and way == 3:
                    continue
                send(
                    halves[item].at[way, step],
                    asides[item].at[way - 1, step],
                    (target_ctx(way), pair * 2 + core),
                    ctx_sems,
                    (way - 1, step, item),
                )

    def fold_ctx(step):
        for item in range(arity):
            half = halves[item].at[0, step]
            total = f32(half[...])
            for way in ways:
                if square and way == 3:
                    continue
                aside = asides[item].at[way - 1, step]
                arrive(aside, ctx_sems, (way - 1, step, item))
                total = total + f32(aside[...])
            if step:
                half[...] = total.astype(half.dtype)
                send(
                    half,
                    ends[item].at[step - 1],
                    (ctx, toward(step) * 2 + core),
                    pair_sems,
                    (step - 1, item),
                )
            else:
                for other in range(1, pair_count):
                    end = ends[item].at[other - 1]
                    arrive(end, pair_sems, (other - 1, item))
                    total = total + f32(end[...])
                if spread_ctx:
                    finals[item][...] = total.astype(finals[item].dtype)
                else:
                    outs[item][...] = total.astype(outs[item].dtype)

    for flow in flows:
        flow.start()
    for turn in range(pair_count + 2):
        if turn < pair_count:
            fold_core(order[turn])
        if 1 <= turn <= pair_count:
            fold_relay(order[turn - 1])
            for flow in flows:
                flow.fold(order[turn - 1])
        if turn >= 2:
            fold_ctx(order[turn - 2])
    if spread_ctx:
        for item in range(arity):
            for way in ways:
                send(
                    finals[item],
                    outs[item].at[ctx],
                    (target_ctx(way), pair * 2 + core),
                    last_sems,
                    (way - 1, item),
                )
            outs[item][ctx] = finals[item][...]
        for item in range(arity):
            for way in ways:
                arrive(outs[item].at[ctx_source(ctx, way, square, ctx_size)], last_sems, (way - 1, item))
    for flow in flows:
        flow.finish()
    for copy in started:
        copy.wait_send()


def scatter(terms, slot, collective_id, spread_ctx=False, out_dtype=None, lines=()):
    ctx_size, shard_count = lax.axis_size("ctx"), lax.axis_size("fsdp")
    pair_count = shard_count // 2
    arity = len(terms)
    dma = pltpu.SemaphoreType.DMA
    lead = (ctx_size,) if spread_ctx else ()
    asides = 2 if ctx_size == 4 else ctx_size - 1

    def room(*extent):
        return [pltpu.VMEM(extent + term.shape[1:], term.dtype) for term in terms]

    def line_room(line):
        if len(line.shape) == 3:
            return [pltpu.VMEM((8, HD), line.dtype)] * 3 + [dma((1,))] * 4
        cut = line.shape[2:]
        rooms = [pltpu.VMEM((count,) + cut, line.dtype) for count in (ctx_size, ctx_size - 1, ctx_size)]
        return rooms + [dma((ctx_size - 1,))] * 4

    moved = sum(term.size * term.dtype.itemsize for term in terms)
    return pl.pallas_call(
        functools.partial(scatter_kernel, arity, ctx_size, pair_count, slot, spread_ctx, len(lines)),
        in_specs=[pl.BlockSpec(memory_space=pltpu.VMEM)] * (arity + len(lines)),
        out_specs=[pl.BlockSpec(memory_space=pltpu.VMEM)] * (arity + len(lines)),
        out_shape=[
            jax.ShapeDtypeStruct(lead + term.shape[1:], out_dtype or term.dtype) for term in terms
        ]
        + [jax.ShapeDtypeStruct(line.shape[1:], jnp.float32) for line in lines],
        scratch_shapes=room(ctx_size, pair_count)
        + room(pair_count)
        + room(asides, pair_count)
        + room(pair_count - 1)
        + room()
        + [dma((ctx_size, pair_count, arity))] * 2
        + [dma((pair_count, arity))] * 2
        + [dma((ctx_size - 1, pair_count, arity))] * 2
        + [dma((pair_count - 1, arity))] * 2
        + [dma((ctx_size - 1, arity))] * 2
        + [
            scratch
            for line in lines
            for scratch in [
                pltpu.VMEM((pair_count,) + line.shape[1:], line.dtype),
                pltpu.VMEM((pair_count - 1,) + line.shape[1:], line.dtype),
            ]
            + [dma((pair_count,))] * 4
            + line_room(line)
        ],
        compiler_params=pltpu.CompilerParams(
            collective_id=collective_id, has_side_effects=True, vmem_limit_bytes=63 * 2**20
        ),
        cost_estimate=pl.CostEstimate(flops=0, bytes_accessed=moved * 16, transcendentals=0),
    )(*terms, *lines)


def line_sum_kernel(pair_count, source, out, half, room, *sems):
    where = greet(1, pair_count, False, False)
    flow = LineScatter(source, out, half, room, sems, where, (pair_count, 1), ())
    flow.start()
    for step in flow.order:
        flow.fold(step)
    flow.finish()


def line_sum(terms, collective_id):
    pair_count = lax.axis_size("fsdp") // 2
    extent = terms.shape[1:]
    dma = pltpu.SemaphoreType.DMA((pair_count,))
    return pl.pallas_call(
        functools.partial(line_sum_kernel, pair_count),
        in_specs=[pl.BlockSpec(memory_space=pltpu.VMEM)],
        out_specs=pl.BlockSpec(memory_space=pltpu.VMEM),
        out_shape=jax.ShapeDtypeStruct(extent, jnp.float32),
        scratch_shapes=[
            pltpu.VMEM((pair_count,) + extent, terms.dtype),
            pltpu.VMEM((pair_count - 1,) + extent, terms.dtype),
        ]
        + [dma] * 4,
        compiler_params=pltpu.CompilerParams(
            collective_id=collective_id, has_side_effects=True, vmem_limit_bytes=63 * 2**20
        ),
        cost_estimate=pl.CostEstimate(flops=0, bytes_accessed=terms.size * 16, transcendentals=0),
    )(terms)


def turned(values, cosine, signed_sine):
    return values * cosine + pltpu.roll(values, HD // 2, 1) * signed_sine


def turned_back(grads, cosine, signed_sine):
    return grads * cosine + pltpu.roll(grads * signed_sine, HD // 2, 1)


def slot_of(index):
    return index % SEQS, index // SEQS


def key_column(index, group, part):
    seq, half = slot_of(index)
    return (((seq * KVH + group) * 2 + half) * 2 + part) * HD


def project_kernel(rows, x_ref, gain_ref, w_hbm, bias_ref, cos_ref, sin_ref, normed_ref, q_ref, kv_ref, w_ref, q_acc, sems):
    wide = w_ref.shape[2]
    copies = []
    for part in range(w_ref.shape[0]):
        copy = pltpu.make_async_copy(
            w_hbm.at[:, part * wide : (part + 1) * wide], w_ref.at[part], sems.at[part]
        )
        copy.start()
        copies.append(copy)
    values = x_ref[...].astype(jnp.float32)
    scale = lax.rsqrt(jnp.mean(values * values, -1, keepdims=True) + EPS)
    normed = (values * scale * gain_ref[...]).astype(jnp.bfloat16)
    normed_ref[...] = normed
    cosine, sine = cos_ref[...], sin_ref[...]
    for part, copy in enumerate(copies):
        copy.wait()
        columns = jnp.dot(normed, w_ref[part], preferred_element_type=jnp.float32)
        columns = columns + bias_ref[:, part * wide : (part + 1) * wide]
        for index in range(wide // HD):
            head = part * (wide // HD) + index
            piece = columns[:, index * HD : (index + 1) * HD]
            if head < H + KVH:
                piece = turned(piece, cosine, sine)
            if head < H:
                piece = piece * (HD**-0.5)
            for slot in range(2 * SEQS):
                seq, half = slot_of(slot)
                own = piece[slot * rows : (slot + 1) * rows]
                if head < H:
                    group, member = head // (H // KVH), head % (H // KVH)
                    q_acc[seq, half, group, member * rows : (member + 1) * rows] = own
                else:
                    group, kind = (head - H) % KVH, (head - H) // KVH
                    at = key_column(slot, group, kind)
                    kv_ref[:, at : at + HD] = own.astype(jnp.bfloat16)
    q_ref[...] = q_acc[...].astype(jnp.bfloat16)


def project(tokens, gain, weight, bias, cosine, signed_sine, rows):
    vmem = pl.BlockSpec(memory_space=pltpu.VMEM)
    parts = 8
    grouped = (SEQS, 2, KVH, H // KVH * rows, HD)
    return pl.pallas_call(
        functools.partial(project_kernel, rows),
        in_specs=[vmem, vmem, pl.BlockSpec(memory_space=pl.ANY), vmem, vmem, vmem],
        out_specs=[vmem, vmem, vmem],
        out_shape=[
            jax.ShapeDtypeStruct(tokens.shape, jnp.bfloat16),
            jax.ShapeDtypeStruct(grouped, jnp.bfloat16),
            jax.ShapeDtypeStruct((rows, SEQS * KVH * 4 * HD), jnp.bfloat16),
        ],
        scratch_shapes=[
            pltpu.VMEM((parts, D, QKV // parts), jnp.bfloat16),
            pltpu.VMEM(grouped, jnp.float32),
            pltpu.SemaphoreType.DMA((parts,)),
        ],
        compiler_params=pltpu.CompilerParams(vmem_limit_bytes=40 * 2**20),
        cost_estimate=pl.CostEstimate(
            flops=2 * tokens.shape[0] * D * QKV, bytes_accessed=2 * D * QKV, transcendentals=0
        ),
        name="project",
    )(tokens, gain.reshape(1, -1), weight, bias.reshape(1, -1), cosine, signed_sine)


def unproject_kernel(rows, gq_ref, gkv_ref, cos_ref, sin_ref, w_hbm, x_ref, gain_ref, past_ref, gp_ref, gi_ref, gg_ref, gb_ref, w_ref, gp_acc, sem):
    copy = pltpu.make_async_copy(w_hbm, w_ref, sem)
    copy.start()
    cosine, sine = cos_ref[...], sin_ref[...]

    def rounded(values):
        return values.astype(jnp.bfloat16).astype(jnp.float32)

    for head in range(H + 2 * KVH):
        for slot in range(2 * SEQS):
            seq, half = slot_of(slot)
            at = slice(slot * rows, (slot + 1) * rows)
            if head < H:
                group, member = head // (H // KVH), head % (H // KVH)
                grad = gq_ref[seq, half, group, member * rows : (member + 1) * rows]
                grad = rounded(grad) * (HD**-0.5)
            else:
                group, kind = (head - H) % KVH, (head - H) // KVH
                column = key_column(slot, group, kind)
                grad = rounded(gkv_ref[:, column : column + HD])
            if head < H + KVH:
                grad = turned_back(grad, cosine[at], sine[at])
            gp_acc[at, head * HD : (head + 1) * HD] = grad
    low = gp_acc[...].astype(jnp.bfloat16)
    gp_ref[...] = low
    gb_ref[...] = jnp.sum(low.astype(jnp.float32), 0, keepdims=True)
    values = x_ref[...].astype(jnp.float32)
    scale = lax.rsqrt(jnp.mean(values * values, -1, keepdims=True) + EPS)
    unit = values * scale
    copy.wait()
    grad_normed = lax.dot_general(low, w_ref[...], CONTRACT_LAST, preferred_element_type=jnp.float32)
    gg_ref[...] = jnp.sum(grad_normed * unit, 0, keepdims=True)
    grad_unit = grad_normed * gain_ref[...]
    inner = jnp.mean(grad_unit * unit, -1, keepdims=True)
    gi_ref[...] = past_ref[...] + scale * (grad_unit - unit * inner)


def unproject(grad_queries, grad_kv, cosine, signed_sine, weight, tokens, gain, past, rows):
    vmem = pl.BlockSpec(memory_space=pltpu.VMEM)
    return pl.pallas_call(
        functools.partial(unproject_kernel, rows),
        in_specs=[vmem, vmem, vmem, vmem, pl.BlockSpec(memory_space=pl.ANY), vmem, vmem, vmem],
        out_specs=[vmem] * 4,
        out_shape=[
            jax.ShapeDtypeStruct((tokens.shape[0], QKV), jnp.bfloat16),
            jax.ShapeDtypeStruct(tokens.shape, jnp.float32),
            jax.ShapeDtypeStruct((1, D), jnp.float32),
            jax.ShapeDtypeStruct((1, QKV), jnp.float32),
        ],
        scratch_shapes=[
            pltpu.VMEM((D, QKV), jnp.bfloat16),
            pltpu.VMEM((tokens.shape[0], QKV), jnp.float32),
            pltpu.SemaphoreType.DMA,
        ],
        compiler_params=pltpu.CompilerParams(vmem_limit_bytes=40 * 2**20),
        cost_estimate=pl.CostEstimate(
            flops=2 * tokens.shape[0] * D * QKV, bytes_accessed=2 * D * QKV, transcendentals=0
        ),
        name="unproject",
    )(grad_queries, grad_kv, cosine, signed_sine, weight, tokens, gain.reshape(1, -1), past)


def pack_kernel(columns, gate_ref, up_ref, out_ref):
    width = out_ref.shape[2] // 2
    cut = out_ref.shape[1]
    for there in range(out_ref.shape[0]):
        for side, ref in enumerate((gate_ref, up_ref)):
            at = side * width
            out_ref[there, :, at + width - HD : at + width] = jnp.zeros((cut, HD), out_ref.dtype)
            out_ref[there, :, at : at + columns] = ref[:, there * columns : (there + 1) * columns]


def pack(gate, up, shard_count, columns, width):
    return pl.pallas_call(
        functools.partial(pack_kernel, columns),
        in_specs=[pl.BlockSpec(memory_space=pltpu.VMEM)] * 2,
        out_specs=pl.BlockSpec(memory_space=pltpu.VMEM),
        out_shape=jax.ShapeDtypeStruct((shard_count, gate.shape[0], 2 * width), gate.dtype),
        name="pack",
    )(gate, up)


def unpack_kernel(columns, in_ref, gate_ref, up_ref):
    width = in_ref.shape[3] // 2
    for there in range(in_ref.shape[1]):
        for side, ref in enumerate((gate_ref, up_ref)):
            part = in_ref[0, there, :, side * width : side * width + columns]
            ref[0, :, there * columns : (there + 1) * columns] = part.astype(jnp.float32)


def unpack(rows, columns):
    ctx_size, shard_count, cut, _ = rows.shape
    out = jax.ShapeDtypeStruct((ctx_size, cut, shard_count * columns), jnp.float32)
    return pl.pallas_call(
        functools.partial(unpack_kernel, columns),
        grid=(ctx_size,),
        in_specs=[pl.BlockSpec((1,) + rows.shape[1:], lambda c: (c, 0, 0, 0))],
        out_specs=[pl.BlockSpec((1, cut, shard_count * columns), lambda c: (c, 0, 0))] * 2,
        out_shape=[out, out],
        name="unpack",
    )(rows)


def shards(
    layer_input,
    block_order,
    first_gain,
    w_qkv,
    b_qkv,
    w_o,
    second_gain,
    w_gate,
    w_up,
    w_down,
    cotangent,
):
    ctx_size = lax.axis_size("ctx")
    shard_count = lax.axis_size("fsdp")
    own_ctx = lax.axis_index("ctx")
    own_shard = lax.axis_index("fsdp")
    rows_here = layer_input.shape[0]
    block_rows = rows_here * shard_count
    cut = D // (ctx_size * shard_count)
    columns = FF // shard_count
    cosine, signed_sine = turn_tables(
        block_order, own_ctx, ctx_size, block_rows, own_shard * rows_here, rows_here
    )
    tokens = by_slot(layer_input)
    grad_out = by_slot(cotangent)

    def by_rows(ctx, shard):
        return shard * ctx_size + ctx

    def by_tokens(ctx, shard):
        return ctx * shard_count + shard

    def own_cut(weight):
        return lax.dynamic_slice_in_dim(weight, own_ctx * cut, cut, 0)

    def mix_features(values):
        shaped = values.reshape(-1, shard_count, ctx_size, cut)
        return shaped.transpose(0, 2, 1, 3).reshape(-1, D)

    def unmix_features(values):
        shaped = values.reshape(-1, ctx_size, shard_count, cut)
        return shaped.transpose(0, 2, 1, 3).reshape(-1, D)

    small = jnp.concatenate([b_qkv, first_gain, second_gain]).reshape(ctx_size, -1)
    small_width = small.shape[1]
    small = lax.dynamic_slice_in_dim(small, own_ctx, 1, 0)
    small = jnp.pad(small, ((0, 0), (0, 16 * HD - small_width))).reshape(16, HD)
    width = -(-columns // HD) * HD
    w_qkv_all, small_all, gate_up_cut = gather(
        [own_cut(w_qkv), small],
        [by_rows, by_rows],
        1,
        swaps=[pack(own_cut(w_gate), own_cut(w_up), shard_count, columns, width)],
    )
    w_qkv_all = w_qkv_all.reshape(D, QKV)
    small_all = small_all.reshape(shard_count, ctx_size, -1)[:, :, :small_width]
    small_all = small_all.reshape(shard_count, -1).astype(jnp.float32)
    bias_width = QKV // shard_count
    gain_width = D // shard_count
    bias_all = small_all[:, :bias_width].reshape(-1)
    gain_one = small_all[:, bias_width : bias_width + gain_width].reshape(-1)
    gain_two = small_all[:, bias_width + gain_width :].reshape(-1)

    down_padded = jnp.pad(w_down, ((0, width - columns), (0, 0)))

    normed_one, queries, own_kv = project(
        tokens, gain_one, w_qkv_all, bias_all, cosine, signed_sine, rows_here
    )
    all_kv, w_o_all, cotangent_all = gather(
        [own_kv, own_cut(w_o), grad_out],
        [by_tokens, by_rows, lambda ctx, shard: shard],
        2,
        wide=(0, 1),
    )
    w_o_all = w_o_all.reshape(D, D)
    cotangent_all = cotangent_all.reshape(-1, D)
    gate_up_cut, all_kv = lax.optimization_barrier((gate_up_cut, all_kv))
    gate_up_cols = lax.all_gather(
        gate_up_cut.reshape(shard_count * cut, 2 * width), "ctx", axis=0, tiled=True
    )
    all_kv = all_kv.reshape(-1, SEQS * KVH * 4 * HD)
    scalars = jnp.concatenate(
        [block_order.reshape(-1), jnp.stack([own_ctx, own_shard]).astype(jnp.int32)]
    )
    attended_grouped, stats = attend_forward(
        scalars, queries, all_kv, ctx_size, block_rows, rows_here
    )
    attended_low = from_groups(attended_grouped, rows_here).astype(jnp.bfloat16)
    middle = tokens.astype(jnp.float32) + jnp.dot(attended_low, w_o_all, preferred_element_type=jnp.float32)
    unit_two, scale_two, normed = normalize(middle, gain_two)
    normed_two = mix_features(normed.astype(jnp.bfloat16))

    (tokens_all,) = gather([normed_two], [lambda ctx, shard: shard], 6, wide=())
    tokens_all = tokens_all.reshape(-1, D)
    gate_up_part = jnp.dot(tokens_all, gate_up_cols, preferred_element_type=jnp.float32)
    gate_part, up_part = gate_up_part[:, :width], gate_up_part[:, width:]
    sigmoid_gate = jax.nn.sigmoid(gate_part)
    activated = gate_part * sigmoid_gate
    hidden = (activated * up_part).astype(jnp.bfloat16)
    grad_hidden = lax.dot_general(
        cotangent_all, down_padded, CONTRACT_LAST, preferred_element_type=jnp.float32
    )
    grad_gate = grad_hidden * up_part * sigmoid_gate * (1.0 + gate_part * (1.0 - sigmoid_gate))
    grad_gate_up = jnp.concatenate([grad_gate, grad_hidden * activated], -1).astype(jnp.bfloat16)
    gate_up_terms = lax.dot_general(
        tokens_all, grad_gate_up, CONTRACT_FIRST, preferred_element_type=jnp.float32
    ).astype(jnp.bfloat16)
    gate_up_rows = lax.psum_scatter(gate_up_terms, "ctx", scatter_dimension=0, tiled=True)
    grad_gate_up, hidden, gate_up_terms = lax.optimization_barrier(
        (grad_gate_up, hidden, gate_up_terms)
    )
    grad_tokens = lax.dot_general(
        grad_gate_up, gate_up_cols, CONTRACT_LAST, preferred_element_type=jnp.float32
    ).astype(jnp.bfloat16)
    grad_normed_two = line_sum(grad_tokens.reshape(shard_count, -1, D), 7)
    grad_normed_two, hidden = lax.optimization_barrier((grad_normed_two, hidden))
    down_terms = lax.dot_general(
        hidden, cotangent_all, CONTRACT_FIRST, preferred_element_type=jnp.float32
    ).astype(jnp.bfloat16)
    down_rows = lax.psum(down_terms, "ctx")
    mixed_terms = jnp.dot(hidden, down_padded, preferred_element_type=jnp.float32).astype(jnp.bfloat16)
    grad_normed_two, down_terms, mixed_terms = lax.optimization_barrier(
        (grad_normed_two, down_terms, mixed_terms)
    )
    grad_normed_two = unmix_features(grad_normed_two)
    grad_middle_norm, grad_gain_two = norm_back(grad_normed_two, unit_two, scale_two, gain_two)
    grad_middle = grad_out.astype(jnp.float32) + grad_middle_norm
    grad_branch_one = grad_middle.astype(jnp.bfloat16)
    grad_attended = lax.dot_general(
        grad_branch_one, w_o_all, CONTRACT_LAST, preferred_element_type=jnp.float32
    ).astype(jnp.bfloat16)
    gate_up_rows, grad_attended = lax.optimization_barrier((gate_up_rows, grad_attended))
    gate_up_rows = exchange(gate_up_rows.reshape(shard_count, cut, 2 * width), 5)
    gate_up_rows, grad_attended = lax.optimization_barrier((gate_up_rows, grad_attended))
    gate_up_rows = lax.all_gather(gate_up_rows, "ctx", axis=0, tiled=False)
    o_terms = lax.dot_general(
        attended_low, grad_branch_one, CONTRACT_FIRST, preferred_element_type=jnp.float32
    ).astype(jnp.bfloat16)
    grad_queries, grad_kv_full = attend_backward(
        scalars,
        queries,
        to_groups(grad_attended, rows_here),
        attended_grouped,
        stats,
        all_kv,
        ctx_size,
        block_rows,
        rows_here,
    )
    grad_kv, mixed_rows = scatter(
        [grad_kv_full.reshape(-1, rows_here, SEQS * KVH * 4 * HD)],
        by_tokens,
        3,
        out_dtype=jnp.float32,
        lines=[mixed_terms.reshape(shard_count, -1, D)],
    )
    grad_projected, grad_input, grad_gain_one, grad_bias = unproject(
        grad_queries,
        grad_kv,
        cosine,
        signed_sine,
        w_qkv_all,
        tokens,
        gain_one,
        grad_middle,
        rows_here,
    )
    grad_input = from_slot(grad_input, rows_here)
    grad_bias = grad_bias.reshape(-1)
    qkv_terms = lax.dot_general(
        normed_one, grad_projected, CONTRACT_FIRST, preferred_element_type=jnp.float32
    ).astype(jnp.bfloat16)
    small_terms = jnp.concatenate(
        [
            part.reshape(shard_count, -1)
            for part in (grad_gain_one, grad_gain_two, grad_bias[:QK], grad_bias[QK:])
        ],
        1,
    )
    small_terms = small_terms.reshape(ctx_size * shard_count, small_width)
    small_terms = jnp.pad(small_terms, ((0, 0), (0, 8 * HD - small_width)))
    qkv_rows, o_rows, small_rows = scatter(
        [
            qkv_terms.reshape(-1, cut, QKV),
            o_terms.reshape(-1, cut, D),
            small_terms.reshape(-1, 8, HD),
        ],
        by_rows,
        4,
        spread_ctx=True,
    )
    mixed_out = middle + mixed_rows
    output = from_slot(mixed_out.astype(jnp.bfloat16), rows_here)
    small_rows = small_rows.reshape(ctx_size, -1)[:, :small_width].reshape(-1)
    bias_start = 2 * gain_width
    value_start = bias_start + QK // shard_count

    gate_rows, up_rows = unpack(gate_up_rows, columns)
    return (
        output,
        grad_input,
        small_rows[:gain_width],
        qkv_rows.reshape(-1, QKV).astype(jnp.float32),
        small_rows[bias_start:value_start],
        small_rows[value_start:],
        o_rows.reshape(-1, D).astype(jnp.float32),
        small_rows[gain_width:bias_start],
        gate_rows.reshape(-1, FF),
        up_rows.reshape(-1, FF),
        down_rows[:columns].astype(jnp.float32),
    )


def solution(mesh):
    in_specs = (
        P(("ctx", "fsdp"), None, None),
        P(),
        P("fsdp"),
        P("fsdp", None),
        P("fsdp"),
        P("fsdp", None),
        P("fsdp"),
        P("fsdp", None),
        P("fsdp", None),
        P("fsdp", None),
        P(("ctx", "fsdp"), None, None),
    )
    out_specs = (
        P(("ctx", "fsdp"), None, None),
        P(("ctx", "fsdp"), None, None),
        P("fsdp"),
        P("fsdp", None),
        P("fsdp"),
        P("fsdp"),
        P("fsdp", None),
        P("fsdp"),
        P("fsdp", None),
        P("fsdp", None),
        P("fsdp", None),
    )
    return jax.shard_map(shards, mesh=mesh, in_specs=in_specs, out_specs=out_specs, check_vma=False)
```

```python
import functools

import jax
import jax.numpy as jnp
from jax import lax
from jax.experimental import pallas as pl
from jax.experimental.pallas import tpu as pltpu
from jax.sharding import PartitionSpec as P

D = 1536
H = 12
KVH = 2
HD = 128
FF = 8960
SEQS = 2
QKV = 2048
QK = 1792


EPS = 1e-06
THETA = 1000000.0
NEG_FILL = -1e30
MESH_ID = pl.DeviceIdType.MESH
CONTRACT_LAST = (((1,), (1,)), ((), ()))
CONTRACT_FIRST = (((0,), (0,)), ((), ()))


def by_slot(tokens):
    return tokens.transpose(1, 0, 2).reshape(-1, tokens.shape[2])


def from_slot(tokens, row_count):
    return tokens.reshape(2 * SEQS, row_count, -1).transpose(1, 0, 2)


def to_groups(tokens, row_count):
    shaped = tokens.reshape(2, SEQS, row_count, KVH, H // KVH, HD)
    return shaped.transpose(1, 0, 3, 4, 2, 5).reshape(SEQS, 2, KVH, H // KVH * row_count, HD)


def from_groups(grouped, row_count):
    shaped = grouped.reshape(SEQS, 2, KVH, H // KVH, row_count, HD).transpose(1, 0, 4, 2, 3, 5)
    return shaped.reshape(row_count * 2 * SEQS, H * HD)


def turn_tables(block_order, own_ctx, ctx_size, block_rows, first_row, row_count):
    half_width = HD // 2
    frequency = THETA ** (-jnp.arange(half_width, dtype=jnp.float32) * 2.0 / HD)
    frequency = jnp.tile(frequency, 2)[None, :]
    order = lax.dynamic_index_in_dim(block_order.reshape(SEQS, 2, ctx_size), own_ctx, 2, False)
    start = (order.T.reshape(-1) * block_rows + first_row).astype(jnp.float32)
    far = start[:, None] * frequency
    near = jnp.arange(row_count, dtype=jnp.float32)[:, None] * frequency
    far_cos, far_sin = jnp.cos(far)[:, None, :], jnp.sin(far)[:, None, :]
    near_cos, near_sin = jnp.cos(near)[None], jnp.sin(near)[None]
    sign = jnp.where(jnp.arange(HD) < half_width, -1.0, 1.0).astype(jnp.float32)
    cosine = far_cos * near_cos - far_sin * near_sin
    sine = (far_sin * near_cos + far_cos * near_sin) * sign
    return cosine.reshape(-1, HD), sine.reshape(-1, HD)


def normalize(values, gain):
    scale = lax.rsqrt(jnp.mean(values * values, -1, keepdims=True) + EPS)
    unit = values * scale
    return (unit, scale, unit * gain)


def norm_back(grad_out, unit, scale, gain):
    grad_unit = grad_out * gain
    inner = jnp.mean(grad_unit * unit, -1, keepdims=True)
    return (scale * (grad_unit - unit * inner), jnp.sum(grad_out * unit, 0))


def hidden_rows(scores, own_shard, rows_here):
    row = lax.broadcasted_iota(jnp.int32, scores.shape, 0)
    lane = lax.broadcasted_iota(jnp.int32, scores.shape, 1)
    return row > own_shard * rows_here + lax.rem(lane, rows_here)


def key_part(group, half_key, part):
    at = ((group * 2 + half_key) * 2 + part) * HD
    return slice(at, at + HD)


def attend_forward_kernel(ctx_size, block_rows, rows_here, scalars, q_ref, kv_ref, out_ref, stat_ref, best_ref, total_ref, accum_ref):
    seq = pl.program_id(0)
    blocks = 2 * ctx_size
    own_ctx = scalars[SEQS * blocks]
    own_shard = scalars[SEQS * blocks + 1]
    groups = range(KVH)
    best_ref[...] = jnp.full(best_ref.shape, NEG_FILL, jnp.float32)
    total_ref[...] = jnp.zeros(total_ref.shape, jnp.float32)
    accum_ref[...] = jnp.zeros(accum_ref.shape, jnp.float32)

    def step(key_ctx, half_key, half):
        order_key = scalars[seq * blocks + half_key * ctx_size + key_ctx]
        order_query = scalars[seq * blocks + half * ctx_size + own_ctx]

        def work(masked):
            rows = pl.ds(pl.multiple_of(key_ctx * block_rows, block_rows), block_rows)
            scores = [
                lax.dot_general(
                    kv_ref[rows, key_part(group, half_key, 0)],
                    q_ref[0, half, group],
                    CONTRACT_LAST,
                    preferred_element_type=jnp.float32,
                )
                for group in groups
            ]
            if masked:
                hidden = hidden_rows(scores[0], own_shard, rows_here)
                scores = [jnp.where(hidden, NEG_FILL, score) for score in scores]
            best = [best_ref[half, group] for group in groups]
            fresh = [
                jnp.maximum(best[group], jnp.max(scores[group], 0, keepdims=True)) for group in groups
            ]
            weights = [jnp.exp(scores[group] - fresh[group]) for group in groups]
            decay = [jnp.exp(best[group] - fresh[group]) for group in groups]
            added = [
                lax.dot_general(
                    kv_ref[rows, key_part(group, half_key, 1)],
                    weights[group].astype(jnp.bfloat16),
                    CONTRACT_FIRST,
                    preferred_element_type=jnp.float32,
                )
                for group in groups
            ]
            for group in groups:
                total_ref[half, group] = total_ref[half, group] * decay[group] + jnp.sum(
                    weights[group], 0, keepdims=True
                )
                accum_ref[half, group] = accum_ref[half, group] * decay[group] + added[group]
                best_ref[half, group] = fresh[group]

        @pl.when(order_key < order_query)
        def full():
            work(False)

        @pl.when(order_key == order_query)
        def diagonal():
            work(True)

    @pl.loop(0, ctx_size)
    def sweep(key_ctx):
        for half_key in range(2):
            for half in range(2):
                step(key_ctx, half_key, half)

    for half in range(2):
        for group in groups:
            totals = total_ref[half, group]
            out_ref[0, half, group] = (accum_ref[half, group] / totals).T
            stat_ref[0, half, group] = best_ref[half, group] + jnp.log(totals)


def group_blocks(lanes, key_rows):
    group = pl.BlockSpec((1, 2, KVH, lanes, HD), lambda s, _: (s, 0, 0, 0, 0))
    stat = pl.BlockSpec((1, 2, KVH, 1, lanes), lambda s, _: (s, 0, 0, 0, 0))
    keys = pl.BlockSpec((key_rows, KVH * 4 * HD), lambda s, _: (0, s))
    return group, stat, keys


def attend_forward(scalars, queries, all_kv, ctx_size, block_rows, rows_here):
    lanes = queries.shape[3]
    kernel = functools.partial(attend_forward_kernel, ctx_size, block_rows, rows_here)
    group, stat, keys = group_blocks(lanes, all_kv.shape[0])
    return pl.pallas_call(
        kernel,
        grid_spec=pltpu.PrefetchScalarGridSpec(
            num_scalar_prefetch=1,
            grid=(SEQS,),
            in_specs=[group, keys],
            out_specs=[group, stat],
            scratch_shapes=[
                pltpu.VMEM((2, KVH, 1, lanes), jnp.float32),
                pltpu.VMEM((2, KVH, 1, lanes), jnp.float32),
                pltpu.VMEM((2, KVH, HD, lanes), jnp.float32),
            ],
        ),
        out_shape=(
            jax.ShapeDtypeStruct(queries.shape, jnp.float32),
            jax.ShapeDtypeStruct((SEQS, 2, KVH, 1, lanes), jnp.float32),
        ),
        compiler_params=pltpu.CompilerParams(vmem_limit_bytes=60 * 2**20),
        name="attend_forward",
    )(scalars, queries, all_kv)


def attend_backward_kernel(ctx_size, block_rows, rows_here, scalars, q_ref, go_ref, att_ref, stat_ref, kv_ref, gq_ref, gkv_ref, delta_ref, gq_acc, gk_acc, gv_acc):
    seq = pl.program_id(0)
    blocks = 2 * ctx_size
    own_ctx = scalars[SEQS * blocks]
    own_shard = scalars[SEQS * blocks + 1]
    groups = range(KVH)
    gq_acc[...] = jnp.zeros(gq_acc.shape, jnp.float32)
    for half in range(2):
        for group in groups:
            product = go_ref[0, half, group].astype(jnp.float32) * att_ref[0, half, group]
            delta_ref[half, group] = jnp.sum(product.T, 0, keepdims=True)

    def step(key_ctx, half_key, half):
        order_key = scalars[seq * blocks + half_key * ctx_size + key_ctx]
        order_query = scalars[seq * blocks + half * ctx_size + own_ctx]

        def work(masked):
            rows = pl.ds(pl.multiple_of(key_ctx * block_rows, block_rows), block_rows)
            keys = [kv_ref[rows, key_part(group, half_key, 0)] for group in groups]
            queries = [q_ref[0, half, group] for group in groups]
            grad_out = [go_ref[0, half, group] for group in groups]
            scores = [
                lax.dot_general(
                    keys[group], queries[group], CONTRACT_LAST, preferred_element_type=jnp.float32
                )
                for group in groups
            ]
            grad_probs = [
                lax.dot_general(
                    kv_ref[rows, key_part(group, half_key, 1)],
                    grad_out[group],
                    CONTRACT_LAST,
                    preferred_element_type=jnp.float32,
                )
                for group in groups
            ]
            probs = [jnp.exp(scores[group] - stat_ref[0, half, group]) for group in groups]
            if masked:
                hidden = hidden_rows(scores[0], own_shard, rows_here)
                probs = [jnp.where(hidden, 0.0, prob) for prob in probs]
            grad_scores = [
                (probs[group] * (grad_probs[group] - delta_ref[half, group])).astype(jnp.bfloat16)
                for group in groups
            ]
            for group in groups:
                gv_acc[group] += jnp.dot(
                    probs[group].astype(jnp.bfloat16),
                    grad_out[group],
                    preferred_element_type=jnp.float32,
                )
                gk_acc[group] += jnp.dot(
                    grad_scores[group], queries[group], preferred_element_type=jnp.float32
                )
                gq_acc[half, group] += lax.dot_general(
                    keys[group], grad_scores[group], CONTRACT_FIRST, preferred_element_type=jnp.float32
                )

        @pl.when(order_key < order_query)
        def full():
            work(False)

        @pl.when(order_key == order_query)
        def diagonal():
            work(True)

    @pl.loop(0, ctx_size)
    def sweep(key_ctx):
        rows = pl.ds(pl.multiple_of(key_ctx * block_rows, block_rows), block_rows)
        for half_key in range(2):
            gk_acc[...] = jnp.zeros(gk_acc.shape, jnp.float32)
            gv_acc[...] = jnp.zeros(gv_acc.shape, jnp.float32)
            for half in range(2):
                step(key_ctx, half_key, half)
            for group in groups:
                gkv_ref[rows, key_part(group, half_key, 0)] = gk_acc[group].astype(jnp.bfloat16)
                gkv_ref[rows, key_part(group, half_key, 1)] = gv_acc[group].astype(jnp.bfloat16)

    for half in range(2):
        for group in groups:
            gq_ref[0, half, group] = gq_acc[half, group].T


def attend_backward(scalars, queries, grad_out, attended, stats, all_kv, ctx_size, block_rows, rows_here):
    lanes = queries.shape[3]
    kernel = functools.partial(attend_backward_kernel, ctx_size, block_rows, rows_here)
    group, stat, keys = group_blocks(lanes, all_kv.shape[0])
    return pl.pallas_call(
        kernel,
        grid_spec=pltpu.PrefetchScalarGridSpec(
            num_scalar_prefetch=1,
            grid=(SEQS,),
            in_specs=[group, group, group, stat, keys],
            out_specs=[group, keys],
            scratch_shapes=[
                pltpu.VMEM((2, KVH, 1, lanes), jnp.float32),
                pltpu.VMEM((2, KVH, HD, lanes), jnp.float32),
                pltpu.VMEM((KVH, block_rows, HD), jnp.float32),
                pltpu.VMEM((KVH, block_rows, HD), jnp.float32),
            ],
        ),
        out_shape=(
            jax.ShapeDtypeStruct(queries.shape, jnp.float32),
            jax.ShapeDtypeStruct(all_kv.shape, jnp.bfloat16),
        ),
        compiler_params=pltpu.CompilerParams(vmem_limit_bytes=60 * 2**20),
        name="attend_backward",
    )(scalars, queries, grad_out, attended, stats, all_kv)


def peers_of(ctx_size):
    return ctx_size == 4, range(1, ctx_size)


def ctx_target(position, way, square, ctx_size):
    return position ^ way if square else lax.rem(position + way, ctx_size)


def ctx_source(position, way, square, ctx_size):
    return position ^ way if square else lax.rem(position + ctx_size - way, ctx_size)


def greet(ctx_size, pair_count, with_ctx, all_shards):
    ctx = lax.axis_index("ctx")
    shard = lax.axis_index("fsdp")
    pair, core = shard // 2, shard % 2
    barrier = pltpu.get_barrier_semaphore()
    partners = [(ctx, pair * 2 + 1 - core)]
    for step in range(1, pair_count):
        there = lax.rem(pair + step, pair_count) * 2
        partners.append((ctx, there + core))
        if all_shards:
            partners.append((ctx, there + 1 - core))
    if with_ctx:
        for way in range(1, ctx_size):
            partners.append((lax.rem(ctx + way, ctx_size), shard))
    for partner in partners:
        pl.semaphore_signal(barrier, inc=1, device_id=partner, device_id_type=MESH_ID)
    pl.semaphore_wait(barrier, len(partners))
    return ctx, pair, core


class Exchange:
    def __init__(self, source, out, sems, own_sem, pair_count):
        self.source, self.out, self.sems, self.own_sem = source, out, sems, own_sem
        self.shard_count = 2 * pair_count

    def start(self):
        ctx, shard = lax.axis_index("ctx"), lax.axis_index("fsdp")
        self.own = pltpu.make_async_copy(self.source.at[shard], self.out.at[shard], self.own_sem)
        self.own.start()
        self.copies = []
        for step in range(1, self.shard_count):
            there = lax.rem(shard + step, self.shard_count)
            copy = pltpu.make_async_remote_copy(
                src_ref=self.source.at[there],
                dst_ref=self.out.at[shard],
                send_sem=self.sems[0].at[step - 1],
                recv_sem=self.sems[1].at[step - 1],
                device_id=(ctx, there),
                device_id_type=MESH_ID,
            )
            copy.start()
            self.copies.append(copy)

    def finish(self):
        ctx, shard = lax.axis_index("ctx"), lax.axis_index("fsdp")
        for step in range(1, self.shard_count):
            come = lax.rem(shard + self.shard_count - step, self.shard_count)
            pltpu.make_async_remote_copy(
                src_ref=self.out.at[come],
                dst_ref=self.out.at[come],
                send_sem=self.sems[0].at[step - 1],
                recv_sem=self.sems[1].at[step - 1],
                device_id=(ctx, shard),
                device_id_type=MESH_ID,
            ).wait_recv()
        self.own.wait()
        for copy in self.copies:
            copy.wait_send()


def exchange_kernel(pair_count, source, out, send_sem, recv_sem, own_sem):
    greet(1, pair_count, False, True)
    flow = Exchange(source, out, (send_sem, recv_sem), own_sem, pair_count)
    flow.start()
    flow.finish()


def exchange(pieces, collective_id):
    shard_count = lax.axis_size("fsdp")
    dma = pltpu.SemaphoreType.DMA
    return pl.pallas_call(
        functools.partial(exchange_kernel, shard_count // 2),
        in_specs=[pl.BlockSpec(memory_space=pltpu.VMEM)],
        out_specs=pl.BlockSpec(memory_space=pl.ANY),
        out_shape=jax.ShapeDtypeStruct(pieces.shape, pieces.dtype),
        scratch_shapes=[dma((shard_count - 1,))] * 2 + [dma],
        compiler_params=pltpu.CompilerParams(collective_id=collective_id, has_side_effects=True),
        cost_estimate=pl.CostEstimate(
            flops=0, bytes_accessed=pieces.size * 64, transcendentals=0
        ),
    )(pieces)


def gather_kernel(arity, ctx_size, pair_count, slots, swaps, wide, *refs):
    sources, refs = refs[:arity], refs[arity:]
    swap_sources, refs = refs[:swaps], refs[swaps:]
    outs, refs = refs[:arity], refs[arity:]
    swap_outs, refs = refs[:swaps], refs[swaps:]
    pair_sems, ctx_sems, core_sems = refs[0:2], refs[2:4], refs[4:6]
    local_sem = refs[6]
    square, ways = peers_of(ctx_size) if wide else (False, ())
    narrow = [item for item in range(arity) if item not in wide]
    near = [way for way in ways if not (square and way == 3)]
    ctx, pair, core = greet(ctx_size, pair_count, len(wide) > 0, swaps > 0)
    homes = [place(ctx, pair * 2 + core) for place in slots]
    started = []
    steps = [(0, 1)] + [(far, way) for far in range(1, pair_count) for way in (1, -1)]

    def present(step):
        far, way = steps[step]
        if far == 0:
            return None
        return pair >= far if way == 1 else pair + far < pair_count

    def origin(step):
        far, way = steps[step]
        return pair - far * way

    def when(condition, work):
        if condition is None:
            work()
        else:
            pl.when(condition)(work)

    def send(item, source, place, target, sems, at, condition):
        copy = pltpu.make_async_remote_copy(
            src_ref=source,
            dst_ref=outs[item].at[place],
            send_sem=sems[0].at[at],
            recv_sem=sems[1].at[at],
            device_id=target,
            device_id_type=MESH_ID,
        )
        copy.start()
        started.append((condition, item, sems, at))

    def sent(item, sems, at):
        pltpu.make_async_remote_copy(
            src_ref=outs[item].at[0],
            dst_ref=outs[item].at[0],
            send_sem=sems[0].at[at],
            recv_sem=sems[1].at[at],
            device_id=(ctx, pair * 2 + core),
            device_id_type=MESH_ID,
        ).wait_send()

    def arrive(item, place, sems, at):
        pltpu.make_async_remote_copy(
            src_ref=outs[item].at[place],
            dst_ref=outs[item].at[place],
            send_sem=sems[0].at[at],
            recv_sem=sems[1].at[at],
            device_id=(ctx, pair * 2 + core),
            device_id_type=MESH_ID,
        ).wait_recv()

    def pass_on(step, item, source, place):
        far, way = steps[step]
        for side in (1, -1) if far == 0 else (way,):

            def further(side=side):
                return pair + 1 < pair_count if side == 1 else pair >= 1

            def both(further=further):
                return further() if far == 0 else jnp.logical_and(further(), present(step))

            def work(side=side, both=both):
                send(
                    item,
                    source,
                    place,
                    (ctx, (pair + side) * 2 + core),
                    pair_sems,
                    ((side + 1) // 2, far, item),
                    both,
                )

            if far + 1 < pair_count:
                pl.when(further())(work)

    def to_core(item, source, from_ctx, way, step):
        send(
            item,
            source,
            slots[item](from_ctx, origin(step) * 2 + core),
            (ctx, pair * 2 + 1 - core),
            core_sems,
            (way, step, item),
            functools.partial(present, step),
        )

    def spread(step, items):
        for item in items:
            place = slots[item](ctx, origin(step) * 2 + core)
            source = sources[item]
            if step:
                far, way = steps[step]
                arrive(item, place, pair_sems, ((way + 1) // 2, far - 1, item))
                source = outs[item].at[place]
            pass_on(step, item, source, place)
            for way in near if item in wide else ():
                there = ctx_target(ctx, way, square, ctx_size)
                send(
                    item,
                    source,
                    place,
                    (there, pair * 2 + core),
                    ctx_sems,
                    (way - 1, step, item),
                    functools.partial(present, step),
                )
            to_core(item, source, ctx, 0, step)

    def collect(step):
        for way in near:
            for item in wide:
                come = ctx_source(ctx, way, square, ctx_size)
                place = slots[item](come, origin(step) * 2 + core)
                arrive(item, place, ctx_sems, (way - 1, step, item))
                source = outs[item].at[place]
                if square and (steps[step][0] % 2 == 0) == (way == 1):
                    send(
                        item,
                        source,
                        place,
                        (ctx ^ (3 - way), pair * 2 + core),
                        ctx_sems,
                        (2, step, item),
                        functools.partial(present, step),
                    )
                to_core(item, source, come, way, step)

    def collect_far(step):
        for item in wide:
            place = slots[item](ctx ^ 3, origin(step) * 2 + core)
            arrive(item, place, ctx_sems, (2, step, item))
            to_core(item, outs[item].at[place], ctx ^ 3, 3, step)

    def straight_core(item, source, place, step):
        sibling = (ctx, pair * 2 + 1 - core)
        send(item, source, place, sibling, core_sems, (0, step, item), lambda: None)

    def go_straight(item):
        for step in range(1, pair_count):
            there = lax.rem(pair + step, pair_count) * 2 + core
            at = (0, step - 1, item)
            send(item, sources[item], homes[item], (ctx, there), pair_sems, at, lambda: None)
        straight_core(item, sources[item], homes[item], 0)

    locals_ = []
    for item in range(arity):
        copy = pltpu.make_async_copy(sources[item], outs[item].at[homes[item]], local_sem.at[item])
        copy.start()
        locals_.append(copy)
    spread(0, wide or range(arity))
    flows = []
    count = len(steps)
    for turn in range(1, count + 4):
        if turn < count:
            when(present(turn), functools.partial(spread, turn, wide or range(arity)))
        if turn == count:
            for item in narrow if wide else ():
                go_straight(item)
            for item in range(swaps):
                flow = Exchange(
                    swap_sources[item],
                    swap_outs[item],
                    refs[7 + 3 * item : 9 + 3 * item],
                    refs[9 + 3 * item],
                    pair_count,
                )
                flow.start()
                flows.append(flow)
        if 0 <= turn - 2 < count:
            when(present(turn - 2), functools.partial(collect, turn - 2))
        if square and 0 <= turn - 4 < count:
            when(present(turn - 4), functools.partial(collect_far, turn - 4))

    for item in narrow if wide else ():
        for step in range(1, pair_count):
            come = lax.rem(pair + pair_count - step, pair_count)
            place = slots[item](ctx, come * 2 + core)
            arrive(item, place, pair_sems, (0, step - 1, item))
            straight_core(item, outs[item].at[place], place, step)
    for item in narrow if wide else ():
        for step in range(pair_count):
            come = lax.rem(pair + pair_count - step, pair_count)
            arrive(item, slots[item](ctx, come * 2 + 1 - core), core_sems, (0, step, item))

    def from_core(step):
        for way in (0, *ways):
            come = ctx_source(ctx, way, square, ctx_size) if way else ctx
            for item in wide or range(arity):
                arrive(item, slots[item](come, origin(step) * 2 + 1 - core), core_sems, (way, step, item))

    for step in range(count):
        when(present(step), functools.partial(from_core, step))
    for flow in flows:
        flow.finish()
    for copy in locals_:
        copy.wait()
    for condition, *which in started:
        when(condition(), functools.partial(sent, *which))


def gather(pieces, slots, collective_id, swaps=(), wide=None):
    ctx_size, shard_count = lax.axis_size("ctx"), lax.axis_size("fsdp")
    pair_count = shard_count // 2
    arity = len(pieces)
    wide = range(arity) if wide is None else wide
    dma = pltpu.SemaphoreType.DMA
    moved = sum(piece.size for piece in pieces) * 2
    steps = 2 * pair_count - 1
    return pl.pallas_call(
        functools.partial(gather_kernel, arity, ctx_size, pair_count, slots, len(swaps), wide),
        in_specs=[pl.BlockSpec(memory_space=pltpu.VMEM)] * (arity + len(swaps)),
        out_specs=[pl.BlockSpec(memory_space=pl.ANY)] * (arity + len(swaps)),
        out_shape=[
            jax.ShapeDtypeStruct(
                ((ctx_size if item in wide else 1) * shard_count,) + piece.shape, piece.dtype
            )
            for item, piece in enumerate(pieces)
        ]
        + [jax.ShapeDtypeStruct(swap.shape, swap.dtype) for swap in swaps],
        scratch_shapes=[dma((2, pair_count - 1, arity))] * 2
        + [dma((ctx_size - 1, steps, arity))] * 2
        + [dma((ctx_size, steps, arity))] * 2
        + [dma((arity,))]
        + [dma((shard_count - 1,)), dma((shard_count - 1,)), dma] * len(swaps),
        compiler_params=pltpu.CompilerParams(collective_id=collective_id, has_side_effects=True),
        cost_estimate=pl.CostEstimate(
            flops=0, bytes_accessed=moved * ctx_size * shard_count * 4, transcendentals=0
        ),
    )(*pieces, *swaps)


class LineScatter:
    def __init__(self, source, out, half, room, sems, where, counts, last):
        self.count, self.ctx_size = counts
        self.source, self.out, self.half, self.room = source, out, half, room
        self.last = last
        self.core_sems, self.pair_sems = sems[0:2], sems[2:4]
        self.ctx, self.pair, self.core = where
        self.order = [*range(1, self.count), 0]

    def copy(self, source, target, device, sems, at):
        return pltpu.make_async_remote_copy(
            src_ref=source,
            dst_ref=target,
            send_sem=sems[0].at[at],
            recv_sem=sems[1].at[at],
            device_id=device,
            device_id_type=MESH_ID,
        )

    def here(self):
        return (self.ctx, self.pair * 2 + self.core)

    def toward(self, step):
        return lax.rem(self.pair + step, self.count)

    def start(self):
        self.copies = []
        for step in self.order:
            self.copies.append(
                self.copy(
                    self.source.at[self.toward(step) * 2 + 1 - self.core],
                    self.half.at[step],
                    (self.ctx, self.pair * 2 + 1 - self.core),
                    self.core_sems,
                    step,
                )
            )
            self.copies[-1].start()

    def fold(self, step):
        half = self.half.at[step]
        self.copy(half, half, self.here(), self.core_sems, step).wait_recv()
        mine = self.source[self.toward(step) * 2 + self.core].astype(jnp.float32)
        total = mine + half[...].astype(jnp.float32)
        if step == 0:
            self.out[...] = total
            return
        half[...] = total.astype(half.dtype)
        self.copies.append(
            self.copy(
                half,
                self.room.at[step - 1],
                (self.ctx, self.toward(step) * 2 + self.core),
                self.pair_sems,
                step - 1,
            )
        )
        self.copies[-1].start()

    def over_ctx(self, terms, room, landing, *sems):
        shard = self.pair * 2 + self.core
        copies = []

        def send(source, target, way, sems):
            there = lax.rem(self.ctx + way, self.ctx_size)
            copies.append(self.copy(source(there), target, (there, shard), sems, way - 1))
            copies[-1].start()

        def arrive(target, way, sems):
            self.copy(target, target, self.here(), sems, way - 1).wait_recv()

        terms[...] = self.out[...].astype(terms.dtype)
        for way in range(1, self.ctx_size):
            send(lambda there: terms.at[there], room.at[way - 1], way, sems[0:2])
        total = self.out[self.ctx]
        for way in range(1, self.ctx_size):
            arrive(room.at[way - 1], way, sems[0:2])
            total = total + room[way - 1].astype(jnp.float32)
        landing[self.ctx] = total.astype(landing.dtype)
        for way in range(1, self.ctx_size):
            send(lambda there: landing.at[self.ctx], landing.at[self.ctx], way, sems[2:4])
        for way in range(1, self.ctx_size):
            come = lax.rem(self.ctx + self.ctx_size - way, self.ctx_size)
            arrive(landing.at[come], way, sems[2:4])
        self.out[...] = landing[...].astype(jnp.float32)
        for copy in copies:
            copy.wait_send()

    def finish(self):
        for step in range(1, self.count):
            room = self.room.at[step - 1]
            self.copy(room, room, self.here(), self.pair_sems, step - 1).wait_recv()
            self.out[...] += room[...].astype(jnp.float32)
        if self.last:
            self.over_ctx(*self.last)
        for copy in self.copies:
            copy.wait_send()


def scatter_kernel(arity, ctx_size, pair_count, slot, spread_ctx, lines, *refs):
    sources, refs = refs[:arity], refs[arity:]
    line_sources, refs = refs[:lines], refs[lines:]
    outs, refs = refs[:arity], refs[arity:]
    line_outs, refs = refs[:lines], refs[lines:]
    halves, relays, asides, ends, finals = (refs[i * arity : (i + 1) * arity] for i in range(5))
    sems = refs[5 * arity : 5 * arity + 10]
    core_sems, relay_sems, ctx_sems, pair_sems, last_sems = (sems[2 * i : 2 * i + 2] for i in range(5))
    square, ways = peers_of(ctx_size)
    ctx, pair, core = greet(ctx_size, pair_count, True, False)
    order = list(range(1, pair_count)) + [0]
    started = []
    flows = []
    for item in range(lines):
        at = 5 * arity + 10 + 13 * item
        spread = len(line_sources[item].shape) == 4
        flows.append(
            LineScatter(
                line_sources[item],
                line_outs[item],
                *refs[at : at + 2],
                refs[at + 2 : at + 6],
                (ctx, pair, core),
                (pair_count, ctx_size),
                refs[at + 6 : at + 13] if spread else (),
            )
        )

    def send(source, target, device, pair_of_sems, at):
        copy = pltpu.make_async_remote_copy(
            src_ref=source,
            dst_ref=target,
            send_sem=pair_of_sems[0].at[at],
            recv_sem=pair_of_sems[1].at[at],
            device_id=device,
            device_id_type=MESH_ID,
        )
        copy.start()
        started.append(copy)

    def arrive(target, pair_of_sems, at):
        pltpu.make_async_remote_copy(
            src_ref=target,
            dst_ref=target,
            send_sem=pair_of_sems[0].at[at],
            recv_sem=pair_of_sems[1].at[at],
            device_id=(ctx, pair * 2 + core),
            device_id_type=MESH_ID,
        ).wait_recv()

    def toward(step):
        return lax.rem(pair + step, pair_count)

    def target_ctx(way):
        return ctx_target(ctx, way, square, ctx_size) if way else ctx

    def f32(value):
        return value.astype(jnp.float32)

    far_first = [3, 1, 2, 0] if square else list(ways) + [0]
    for step in order:
        for way in far_first:
            for item in range(arity):
                send(
                    sources[item].at[slot(target_ctx(way), toward(step) * 2 + 1 - core)],
                    halves[item].at[way, step],
                    (ctx, pair * 2 + 1 - core),
                    core_sems,
                    (way, step, item),
                )

    def fold_core(step):
        for way in far_first:
            for item in range(arity):
                half = halves[item].at[way, step]
                arrive(half, core_sems, (way, step, item))
                mine = sources[item][slot(target_ctx(way), toward(step) * 2 + core)]
                half[...] = (f32(mine) + f32(half[...])).astype(half.dtype)
                if square and way == 3:
                    there = ctx ^ (1 if step % 2 == 0 else 2)
                    send(
                        half,
                        relays[item].at[step],
                        (there, pair * 2 + core),
                        relay_sems,
                        (step, item),
                    )

    def fold_relay(step):
        for item in range(arity):
            if square:
                relay = relays[item].at[step]
                arrive(relay, relay_sems, (step, item))
                half = halves[item].at[2 if step % 2 == 0 else 1, step]
                half[...] = (f32(half[...]) + f32(relay[...])).astype(half.dtype)
            for way in ways:
                if square and way == 3:
                    continue
                send(
                    halves[item].at[way, step],
                    asides[item].at[way - 1, step],
                    (target_ctx(way), pair * 2 + core),
                    ctx_sems,
                    (way - 1, step, item),
                )

    def fold_ctx(step):
        for item in range(arity):
            half = halves[item].at[0, step]
            total = f32(half[...])
            for way in ways:
                if square and way == 3:
                    continue
                aside = asides[item].at[way - 1, step]
                arrive(aside, ctx_sems, (way - 1, step, item))
                total = total + f32(aside[...])
            if step:
                half[...] = total.astype(half.dtype)
                send(
                    half,
                    ends[item].at[step - 1],
                    (ctx, toward(step) * 2 + core),
                    pair_sems,
                    (step - 1, item),
                )
            else:
                for other in range(1, pair_count):
                    end = ends[item].at[other - 1]
                    arrive(end, pair_sems, (other - 1, item))
                    total = total + f32(end[...])
                if spread_ctx:
                    finals[item][...] = total.astype(finals[item].dtype)
                else:
                    outs[item][...] = total.astype(outs[item].dtype)

    for flow in flows:
        flow.start()
    for turn in range(pair_count + 2):
        if turn < pair_count:
            fold_core(order[turn])
        if 1 <= turn <= pair_count:
            fold_relay(order[turn - 1])
            for flow in flows:
                flow.fold(order[turn - 1])
        if turn >= 2:
            fold_ctx(order[turn - 2])
    if spread_ctx:
        for item in range(arity):
            for way in ways:
                send(
                    finals[item],
                    outs[item].at[ctx],
                    (target_ctx(way), pair * 2 + core),
                    last_sems,
                    (way - 1, item),
                )
            outs[item][ctx] = finals[item][...]
        for item in range(arity):
            for way in ways:
                arrive(outs[item].at[ctx_source(ctx, way, square, ctx_size)], last_sems, (way - 1, item))
    for flow in flows:
        flow.finish()
    for copy in started:
        copy.wait_send()


def scatter(terms, slot, collective_id, spread_ctx=False, out_dtype=None, lines=()):
    ctx_size, shard_count = lax.axis_size("ctx"), lax.axis_size("fsdp")
    pair_count = shard_count // 2
    arity = len(terms)
    dma = pltpu.SemaphoreType.DMA
    lead = (ctx_size,) if spread_ctx else ()
    asides = 2 if ctx_size == 4 else ctx_size - 1

    def room(*extent):
        return [pltpu.VMEM(extent + term.shape[1:], term.dtype) for term in terms]

    def line_room(line):
        if len(line.shape) == 3:
            return [pltpu.VMEM((8, HD), line.dtype)] * 3 + [dma((1,))] * 4
        cut = line.shape[2:]
        rooms = [pltpu.VMEM((count,) + cut, line.dtype) for count in (ctx_size, ctx_size - 1, ctx_size)]
        return rooms + [dma((ctx_size - 1,))] * 4

    moved = sum(term.size * term.dtype.itemsize for term in terms)
    return pl.pallas_call(
        functools.partial(scatter_kernel, arity, ctx_size, pair_count, slot, spread_ctx, len(lines)),
        in_specs=[pl.BlockSpec(memory_space=pltpu.VMEM)] * (arity + len(lines)),
        out_specs=[pl.BlockSpec(memory_space=pltpu.VMEM)] * (arity + len(lines)),
        out_shape=[
            jax.ShapeDtypeStruct(lead + term.shape[1:], out_dtype or term.dtype) for term in terms
        ]
        + [jax.ShapeDtypeStruct(line.shape[1:], jnp.float32) for line in lines],
        scratch_shapes=room(ctx_size, pair_count)
        + room(pair_count)
        + room(asides, pair_count)
        + room(pair_count - 1)
        + room()
        + [dma((ctx_size, pair_count, arity))] * 2
        + [dma((pair_count, arity))] * 2
        + [dma((ctx_size - 1, pair_count, arity))] * 2
        + [dma((pair_count - 1, arity))] * 2
        + [dma((ctx_size - 1, arity))] * 2
        + [
            scratch
            for line in lines
            for scratch in [
                pltpu.VMEM((pair_count,) + line.shape[1:], line.dtype),
                pltpu.VMEM((pair_count - 1,) + line.shape[1:], line.dtype),
            ]
            + [dma((pair_count,))] * 4
            + line_room(line)
        ],
        compiler_params=pltpu.CompilerParams(
            collective_id=collective_id, has_side_effects=True, vmem_limit_bytes=63 * 2**20
        ),
        cost_estimate=pl.CostEstimate(flops=0, bytes_accessed=moved * 16, transcendentals=0),
    )(*terms, *lines)


def line_sum_kernel(pair_count, source, out, half, room, *sems):
    where = greet(1, pair_count, False, False)
    flow = LineScatter(source, out, half, room, sems, where, (pair_count, 1), ())
    flow.start()
    for step in flow.order:
        flow.fold(step)
    flow.finish()


def line_sum(terms, collective_id):
    pair_count = lax.axis_size("fsdp") // 2
    extent = terms.shape[1:]
    dma = pltpu.SemaphoreType.DMA((pair_count,))
    return pl.pallas_call(
        functools.partial(line_sum_kernel, pair_count),
        in_specs=[pl.BlockSpec(memory_space=pltpu.VMEM)],
        out_specs=pl.BlockSpec(memory_space=pltpu.VMEM),
        out_shape=jax.ShapeDtypeStruct(extent, jnp.float32),
        scratch_shapes=[
            pltpu.VMEM((pair_count,) + extent, terms.dtype),
            pltpu.VMEM((pair_count - 1,) + extent, terms.dtype),
        ]
        + [dma] * 4,
        compiler_params=pltpu.CompilerParams(
            collective_id=collective_id, has_side_effects=True, vmem_limit_bytes=63 * 2**20
        ),
        cost_estimate=pl.CostEstimate(flops=0, bytes_accessed=terms.size * 16, transcendentals=0),
    )(terms)


def turned(values, cosine, signed_sine):
    return values * cosine + pltpu.roll(values, HD // 2, 1) * signed_sine


def turned_back(grads, cosine, signed_sine):
    return grads * cosine + pltpu.roll(grads * signed_sine, HD // 2, 1)


def slot_of(index):
    return index % SEQS, index // SEQS


def key_column(index, group, part):
    seq, half = slot_of(index)
    return (((seq * KVH + group) * 2 + half) * 2 + part) * HD


def project_kernel(rows, x_ref, gain_ref, w_hbm, bias_ref, cos_ref, sin_ref, normed_ref, q_ref, kv_ref, w_ref, q_acc, sems):
    wide = w_ref.shape[2]
    copies = []
    for part in range(w_ref.shape[0]):
        copy = pltpu.make_async_copy(
            w_hbm.at[:, part * wide : (part + 1) * wide], w_ref.at[part], sems.at[part]
        )
        copy.start()
        copies.append(copy)
    values = x_ref[...].astype(jnp.float32)
    scale = lax.rsqrt(jnp.mean(values * values, -1, keepdims=True) + EPS)
    normed = (values * scale * gain_ref[...]).astype(jnp.bfloat16)
    normed_ref[...] = normed
    cosine, sine = cos_ref[...], sin_ref[...]
    for part, copy in enumerate(copies):
        copy.wait()
        columns = jnp.dot(normed, w_ref[part], preferred_element_type=jnp.float32)
        columns = columns + bias_ref[:, part * wide : (part + 1) * wide]
        for index in range(wide // HD):
            head = part * (wide // HD) + index
            piece = columns[:, index * HD : (index + 1) * HD]
            if head < H + KVH:
                piece = turned(piece, cosine, sine)
            if head < H:
                piece = piece * (HD**-0.5)
            for slot in range(2 * SEQS):
                seq, half = slot_of(slot)
                own = piece[slot * rows : (slot + 1) * rows]
                if head < H:
                    group, member = head // (H // KVH), head % (H // KVH)
                    q_acc[seq, half, group, member * rows : (member + 1) * rows] = own
                else:
                    group, kind = (head - H) % KVH, (head - H) // KVH
                    at = key_column(slot, group, kind)
                    kv_ref[:, at : at + HD] = own.astype(jnp.bfloat16)
    q_ref[...] = q_acc[...].astype(jnp.bfloat16)


def project(tokens, gain, weight, bias, cosine, signed_sine, rows):
    vmem = pl.BlockSpec(memory_space=pltpu.VMEM)
    parts = 8
    grouped = (SEQS, 2, KVH, H // KVH * rows, HD)
    return pl.pallas_call(
        functools.partial(project_kernel, rows),
        in_specs=[vmem, vmem, pl.BlockSpec(memory_space=pl.ANY), vmem, vmem, vmem],
        out_specs=[vmem, vmem, vmem],
        out_shape=[
            jax.ShapeDtypeStruct(tokens.shape, jnp.bfloat16),
            jax.ShapeDtypeStruct(grouped, jnp.bfloat16),
            jax.ShapeDtypeStruct((rows, SEQS * KVH * 4 * HD), jnp.bfloat16),
        ],
        scratch_shapes=[
            pltpu.VMEM((parts, D, QKV // parts), jnp.bfloat16),
            pltpu.VMEM(grouped, jnp.float32),
            pltpu.SemaphoreType.DMA((parts,)),
        ],
        compiler_params=pltpu.CompilerParams(vmem_limit_bytes=40 * 2**20),
        cost_estimate=pl.CostEstimate(
            flops=2 * tokens.shape[0] * D * QKV, bytes_accessed=2 * D * QKV, transcendentals=0
        ),
        name="project",
    )(tokens, gain.reshape(1, -1), weight, bias.reshape(1, -1), cosine, signed_sine)


def unproject_kernel(rows, gq_ref, gkv_ref, cos_ref, sin_ref, w_hbm, x_ref, gain_ref, past_ref, gp_ref, gi_ref, gg_ref, gb_ref, w_ref, gp_acc, sem):
    copy = pltpu.make_async_copy(w_hbm, w_ref, sem)
    copy.start()
    cosine, sine = cos_ref[...], sin_ref[...]

    def rounded(values):
        return values.astype(jnp.bfloat16).astype(jnp.float32)

    for head in range(H + 2 * KVH):
        for slot in range(2 * SEQS):
            seq, half = slot_of(slot)
            at = slice(slot * rows, (slot + 1) * rows)
            if head < H:
                group, member = head // (H // KVH), head % (H // KVH)
                grad = gq_ref[seq, half, group, member * rows : (member + 1) * rows]
                grad = rounded(grad) * (HD**-0.5)
            else:
                group, kind = (head - H) % KVH, (head - H) // KVH
                column = key_column(slot, group, kind)
                grad = rounded(gkv_ref[:, column : column + HD])
            if head < H + KVH:
                grad = turned_back(grad, cosine[at], sine[at])
            gp_acc[at, head * HD : (head + 1) * HD] = grad
    low = gp_acc[...].astype(jnp.bfloat16)
    gp_ref[...] = low
    gb_ref[...] = jnp.sum(low.astype(jnp.float32), 0, keepdims=True)
    values = x_ref[...].astype(jnp.float32)
    scale = lax.rsqrt(jnp.mean(values * values, -1, keepdims=True) + EPS)
    unit = values * scale
    copy.wait()
    grad_normed = lax.dot_general(low, w_ref[...], CONTRACT_LAST, preferred_element_type=jnp.float32)
    gg_ref[...] = jnp.sum(grad_normed * unit, 0, keepdims=True)
    grad_unit = grad_normed * gain_ref[...]
    inner = jnp.mean(grad_unit * unit, -1, keepdims=True)
    gi_ref[...] = past_ref[...] + scale * (grad_unit - unit * inner)


def unproject(grad_queries, grad_kv, cosine, signed_sine, weight, tokens, gain, past, rows):
    vmem = pl.BlockSpec(memory_space=pltpu.VMEM)
    return pl.pallas_call(
        functools.partial(unproject_kernel, rows),
        in_specs=[vmem, vmem, vmem, vmem, pl.BlockSpec(memory_space=pl.ANY), vmem, vmem, vmem],
        out_specs=[vmem] * 4,
        out_shape=[
            jax.ShapeDtypeStruct((tokens.shape[0], QKV), jnp.bfloat16),
            jax.ShapeDtypeStruct(tokens.shape, jnp.float32),
            jax.ShapeDtypeStruct((1, D), jnp.float32),
            jax.ShapeDtypeStruct((1, QKV), jnp.float32),
        ],
        scratch_shapes=[
            pltpu.VMEM((D, QKV), jnp.bfloat16),
            pltpu.VMEM((tokens.shape[0], QKV), jnp.float32),
            pltpu.SemaphoreType.DMA,
        ],
        compiler_params=pltpu.CompilerParams(vmem_limit_bytes=40 * 2**20),
        cost_estimate=pl.CostEstimate(
            flops=2 * tokens.shape[0] * D * QKV, bytes_accessed=2 * D * QKV, transcendentals=0
        ),
        name="unproject",
    )(grad_queries, grad_kv, cosine, signed_sine, weight, tokens, gain.reshape(1, -1), past)


def pack_kernel(columns, gate_ref, up_ref, out_ref):
    width = out_ref.shape[2] // 2
    cut = out_ref.shape[1]
    for there in range(out_ref.shape[0]):
        for side, ref in enumerate((gate_ref, up_ref)):
            at = side * width
            out_ref[there, :, at + width - HD : at + width] = jnp.zeros((cut, HD), out_ref.dtype)
            out_ref[there, :, at : at + columns] = ref[:, there * columns : (there + 1) * columns]


def pack(gate, up, shard_count, columns, width):
    return pl.pallas_call(
        functools.partial(pack_kernel, columns),
        in_specs=[pl.BlockSpec(memory_space=pltpu.VMEM)] * 2,
        out_specs=pl.BlockSpec(memory_space=pltpu.VMEM),
        out_shape=jax.ShapeDtypeStruct((shard_count, gate.shape[0], 2 * width), gate.dtype),
        name="pack",
    )(gate, up)


def unpack_kernel(columns, in_ref, gate_ref, up_ref):
    width = in_ref.shape[3] // 2
    for there in range(in_ref.shape[1]):
        for side, ref in enumerate((gate_ref, up_ref)):
            part = in_ref[0, there, :, side * width : side * width + columns]
            ref[0, :, there * columns : (there + 1) * columns] = part.astype(jnp.float32)


def unpack(rows, columns):
    ctx_size, shard_count, cut, _ = rows.shape
    out = jax.ShapeDtypeStruct((ctx_size, cut, shard_count * columns), jnp.float32)
    return pl.pallas_call(
        functools.partial(unpack_kernel, columns),
        grid=(ctx_size,),
        in_specs=[pl.BlockSpec((1,) + rows.shape[1:], lambda c: (c, 0, 0, 0))],
        out_specs=[pl.BlockSpec((1, cut, shard_count * columns), lambda c: (c, 0, 0))] * 2,
        out_shape=[out, out],
        name="unpack",
    )(rows)


def shards(
    layer_input,
    block_order,
    first_gain,
    w_qkv,
    b_qkv,
    w_o,
    second_gain,
    w_gate,
    w_up,
    w_down,
    cotangent,
):
    ctx_size = lax.axis_size("ctx")
    shard_count = lax.axis_size("fsdp")
    own_ctx = lax.axis_index("ctx")
    own_shard = lax.axis_index("fsdp")
    rows_here = layer_input.shape[0]
    block_rows = rows_here * shard_count
    cut = D // (ctx_size * shard_count)
    columns = FF // shard_count
    cosine, signed_sine = turn_tables(
        block_order, own_ctx, ctx_size, block_rows, own_shard * rows_here, rows_here
    )
    tokens = by_slot(layer_input)
    grad_out = by_slot(cotangent)

    def by_rows(ctx, shard):
        return shard * ctx_size + ctx

    def by_tokens(ctx, shard):
        return ctx * shard_count + shard

    def own_cut(weight):
        return lax.dynamic_slice_in_dim(weight, own_ctx * cut, cut, 0)

    def mix_features(values):
        shaped = values.reshape(-1, shard_count, ctx_size, cut)
        return shaped.transpose(0, 2, 1, 3).reshape(-1, D)

    def unmix_features(values):
        shaped = values.reshape(-1, ctx_size, shard_count, cut)
        return shaped.transpose(0, 2, 1, 3).reshape(-1, D)

    small = jnp.concatenate([b_qkv, first_gain, second_gain]).reshape(ctx_size, -1)
    small_width = small.shape[1]
    small = lax.dynamic_slice_in_dim(small, own_ctx, 1, 0)
    small = jnp.pad(small, ((0, 0), (0, 16 * HD - small_width))).reshape(16, HD)
    width = -(-columns // HD) * HD
    w_qkv_all, small_all, gate_up_cut = gather(
        [own_cut(w_qkv), small],
        [by_rows, by_rows],
        1,
        swaps=[pack(own_cut(w_gate), own_cut(w_up), shard_count, columns, width)],
    )
    w_qkv_all = w_qkv_all.reshape(D, QKV)
    small_all = small_all.reshape(shard_count, ctx_size, -1)[:, :, :small_width]
    small_all = small_all.reshape(shard_count, -1).astype(jnp.float32)
    bias_width = QKV // shard_count
    gain_width = D // shard_count
    bias_all = small_all[:, :bias_width].reshape(-1)
    gain_one = small_all[:, bias_width : bias_width + gain_width].reshape(-1)
    gain_two = small_all[:, bias_width + gain_width :].reshape(-1)

    down_padded = jnp.pad(w_down, ((0, width - columns), (0, 0)))

    late_grad_out, w_qkv_all = lax.optimization_barrier((grad_out, w_qkv_all))
    cotangent_all = lax.all_gather(late_grad_out, "fsdp", axis=0, tiled=True)
    normed_one, queries, own_kv = project(
        tokens, gain_one, w_qkv_all, bias_all, cosine, signed_sine, rows_here
    )
    all_kv, w_o_all = gather([own_kv, own_cut(w_o)], [by_tokens, by_rows], 2)
    w_o_all = w_o_all.reshape(D, D)
    gate_up_cut, all_kv = lax.optimization_barrier((gate_up_cut, all_kv))
    gate_up_cols = lax.all_gather(
        gate_up_cut.reshape(shard_count * cut, 2 * width), "ctx", axis=0, tiled=True
    )
    all_kv = all_kv.reshape(-1, SEQS * KVH * 4 * HD)
    scalars = jnp.concatenate(
        [block_order.reshape(-1), jnp.stack([own_ctx, own_shard]).astype(jnp.int32)]
    )
    attended_grouped, stats = attend_forward(
        scalars, queries, all_kv, ctx_size, block_rows, rows_here
    )
    attended_low = from_groups(attended_grouped, rows_here).astype(jnp.bfloat16)
    middle = tokens.astype(jnp.float32) + jnp.dot(attended_low, w_o_all, preferred_element_type=jnp.float32)
    unit_two, scale_two, normed = normalize(middle, gain_two)
    normed_two = mix_features(normed.astype(jnp.bfloat16))

    (tokens_all,) = gather([normed_two], [lambda ctx, shard: shard], 6, wide=())
    tokens_all = tokens_all.reshape(-1, D)
    gate_up_part = jnp.dot(tokens_all, gate_up_cols, preferred_element_type=jnp.float32)
    gate_part, up_part = gate_up_part[:, :width], gate_up_part[:, width:]
    sigmoid_gate = jax.nn.sigmoid(gate_part)
    activated = gate_part * sigmoid_gate
    hidden = (activated * up_part).astype(jnp.bfloat16)
    grad_hidden = lax.dot_general(
        cotangent_all, down_padded, CONTRACT_LAST, preferred_element_type=jnp.float32
    )
    grad_gate = grad_hidden * up_part * sigmoid_gate * (1.0 + gate_part * (1.0 - sigmoid_gate))
    grad_gate_up = jnp.concatenate([grad_gate, grad_hidden * activated], -1).astype(jnp.bfloat16)
    gate_up_terms = lax.dot_general(
        tokens_all, grad_gate_up, CONTRACT_FIRST, preferred_element_type=jnp.float32
    ).astype(jnp.bfloat16)
    gate_up_rows = lax.psum_scatter(gate_up_terms, "ctx", scatter_dimension=0, tiled=True)
    grad_gate_up, hidden, gate_up_terms = lax.optimization_barrier(
        (grad_gate_up, hidden, gate_up_terms)
    )
    grad_tokens = lax.dot_general(
        grad_gate_up, gate_up_cols, CONTRACT_LAST, preferred_element_type=jnp.float32
    ).astype(jnp.bfloat16)
    grad_normed_two = line_sum(grad_tokens.reshape(shard_count, -1, D), 7)
    grad_normed_two, hidden = lax.optimization_barrier((grad_normed_two, hidden))
    down_terms = lax.dot_general(
        hidden, cotangent_all, CONTRACT_FIRST, preferred_element_type=jnp.float32
    ).astype(jnp.bfloat16)
    down_rows = lax.psum(down_terms, "ctx")
    mixed_terms = jnp.dot(hidden, down_padded, preferred_element_type=jnp.float32).astype(jnp.bfloat16)
    grad_normed_two, down_terms, mixed_terms = lax.optimization_barrier(
        (grad_normed_two, down_terms, mixed_terms)
    )
    grad_normed_two = unmix_features(grad_normed_two)
    grad_middle_norm, grad_gain_two = norm_back(grad_normed_two, unit_two, scale_two, gain_two)
    grad_middle = grad_out.astype(jnp.float32) + grad_middle_norm
    grad_branch_one = grad_middle.astype(jnp.bfloat16)
    grad_attended = lax.dot_general(
        grad_branch_one, w_o_all, CONTRACT_LAST, preferred_element_type=jnp.float32
    ).astype(jnp.bfloat16)
    gate_up_rows, grad_attended = lax.optimization_barrier((gate_up_rows, grad_attended))
    gate_up_rows = exchange(gate_up_rows.reshape(shard_count, cut, 2 * width), 5)
    gate_up_rows, grad_attended = lax.optimization_barrier((gate_up_rows, grad_attended))
    gate_up_rows = lax.all_gather(gate_up_rows, "ctx", axis=0, tiled=False)
    o_terms = lax.dot_general(
        attended_low, grad_branch_one, CONTRACT_FIRST, preferred_element_type=jnp.float32
    ).astype(jnp.bfloat16)
    grad_queries, grad_kv_full = attend_backward(
        scalars,
        queries,
        to_groups(grad_attended, rows_here),
        attended_grouped,
        stats,
        all_kv,
        ctx_size,
        block_rows,
        rows_here,
    )
    (grad_kv,) = scatter(
        [grad_kv_full.reshape(-1, rows_here, SEQS * KVH * 4 * HD)],
        by_tokens,
        3,
        out_dtype=jnp.float32,
    )
    mixed_terms, grad_kv = lax.optimization_barrier((mixed_terms, grad_kv))
    mixed_rows = lax.psum_scatter(mixed_terms, "fsdp", scatter_dimension=0, tiled=True)
    grad_projected, grad_input, grad_gain_one, grad_bias = unproject(
        grad_queries,
        grad_kv,
        cosine,
        signed_sine,
        w_qkv_all,
        tokens,
        gain_one,
        grad_middle,
        rows_here,
    )
    grad_input = from_slot(grad_input, rows_here)
    grad_bias = grad_bias.reshape(-1)
    qkv_terms = lax.dot_general(
        normed_one, grad_projected, CONTRACT_FIRST, preferred_element_type=jnp.float32
    ).astype(jnp.bfloat16)
    small_terms = jnp.concatenate(
        [
            part.reshape(shard_count, -1)
            for part in (grad_gain_one, grad_gain_two, grad_bias[:QK], grad_bias[QK:])
        ],
        1,
    )
    small_terms = small_terms.reshape(ctx_size * shard_count, small_width)
    small_terms = jnp.pad(small_terms, ((0, 0), (0, 8 * HD - small_width)))
    qkv_rows, o_rows, small_rows = scatter(
        [
            qkv_terms.reshape(-1, cut, QKV),
            o_terms.reshape(-1, cut, D),
            small_terms.reshape(-1, 8, HD),
        ],
        by_rows,
        4,
        spread_ctx=True,
    )
    mixed_out = middle + mixed_rows.astype(jnp.float32)
    output = from_slot(mixed_out.astype(jnp.bfloat16), rows_here)
    small_rows = small_rows.reshape(ctx_size, -1)[:, :small_width].reshape(-1)
    bias_start = 2 * gain_width
    value_start = bias_start + QK // shard_count

    gate_rows, up_rows = unpack(gate_up_rows, columns)
    return (
        output,
        grad_input,
        small_rows[:gain_width],
        qkv_rows.reshape(-1, QKV).astype(jnp.float32),
        small_rows[bias_start:value_start],
        small_rows[value_start:],
        o_rows.reshape(-1, D).astype(jnp.float32),
        small_rows[gain_width:bias_start],
        gate_rows.reshape(-1, FF),
        up_rows.reshape(-1, FF),
        down_rows[:columns].astype(jnp.float32),
    )


def solution(mesh):
    in_specs = (
        P(("ctx", "fsdp"), None, None),
        P(),
        P("fsdp"),
        P("fsdp", None),
        P("fsdp"),
        P("fsdp", None),
        P("fsdp"),
        P("fsdp", None),
        P("fsdp", None),
        P("fsdp", None),
        P(("ctx", "fsdp"), None, None),
    )
    out_specs = (
        P(("ctx", "fsdp"), None, None),
        P(("ctx", "fsdp"), None, None),
        P("fsdp"),
        P("fsdp", None),
        P("fsdp"),
        P("fsdp"),
        P("fsdp", None),
        P("fsdp"),
        P("fsdp", None),
        P("fsdp", None),
        P("fsdp", None),
    )
    return jax.shard_map(shards, mesh=mesh, in_specs=in_specs, out_specs=out_specs, check_vma=False)
```

```python
import functools

import jax
import jax.numpy as jnp
from jax import lax
from jax.experimental import pallas as pl
from jax.experimental.pallas import tpu as pltpu
from jax.sharding import PartitionSpec as P

D = 1536
H = 12
KVH = 2
HD = 128
FF = 8960
SEQS = 2
QKV = 2048
QK = 1792


EPS = 1e-06
THETA = 1000000.0
NEG_FILL = -1e30
MESH_ID = pl.DeviceIdType.MESH
CONTRACT_LAST = (((1,), (1,)), ((), ()))
CONTRACT_FIRST = (((0,), (0,)), ((), ()))


def by_slot(tokens):
    return tokens.transpose(1, 0, 2).reshape(-1, tokens.shape[2])


def from_slot(tokens, row_count):
    return tokens.reshape(2 * SEQS, row_count, -1).transpose(1, 0, 2)


def to_groups(tokens, row_count):
    shaped = tokens.reshape(2, SEQS, row_count, KVH, H // KVH, HD)
    return shaped.transpose(1, 0, 3, 4, 2, 5).reshape(SEQS, 2, KVH, H // KVH * row_count, HD)


def from_groups(grouped, row_count):
    shaped = grouped.reshape(SEQS, 2, KVH, H // KVH, row_count, HD).transpose(1, 0, 4, 2, 3, 5)
    return shaped.reshape(row_count * 2 * SEQS, H * HD)


def turn_tables(block_order, own_ctx, ctx_size, block_rows, first_row, row_count):
    half_width = HD // 2
    frequency = THETA ** (-jnp.arange(half_width, dtype=jnp.float32) * 2.0 / HD)
    frequency = jnp.tile(frequency, 2)[None, :]
    order = lax.dynamic_index_in_dim(block_order.reshape(SEQS, 2, ctx_size), own_ctx, 2, False)
    start = (order.T.reshape(-1) * block_rows + first_row).astype(jnp.float32)
    far = start[:, None] * frequency
    near = jnp.arange(row_count, dtype=jnp.float32)[:, None] * frequency
    far_cos, far_sin = jnp.cos(far)[:, None, :], jnp.sin(far)[:, None, :]
    near_cos, near_sin = jnp.cos(near)[None], jnp.sin(near)[None]
    sign = jnp.where(jnp.arange(HD) < half_width, -1.0, 1.0).astype(jnp.float32)
    cosine = far_cos * near_cos - far_sin * near_sin
    sine = (far_sin * near_cos + far_cos * near_sin) * sign
    return cosine.reshape(-1, HD), sine.reshape(-1, HD)


def normalize(values, gain):
    scale = lax.rsqrt(jnp.mean(values * values, -1, keepdims=True) + EPS)
    unit = values * scale
    return (unit, scale, unit * gain)


def norm_back(grad_out, unit, scale, gain):
    grad_unit = grad_out * gain
    inner = jnp.mean(grad_unit * unit, -1, keepdims=True)
    return (scale * (grad_unit - unit * inner), jnp.sum(grad_out * unit, 0))


def hidden_rows(scores, own_shard, rows_here):
    row = lax.broadcasted_iota(jnp.int32, scores.shape, 0)
    lane = lax.broadcasted_iota(jnp.int32, scores.shape, 1)
    return row > own_shard * rows_here + lax.rem(lane, rows_here)


def key_part(group, half_key, part):
    at = ((group * 2 + half_key) * 2 + part) * HD
    return slice(at, at + HD)


def attend_forward_kernel(ctx_size, block_rows, rows_here, scalars, q_ref, kv_ref, out_ref, stat_ref, best_ref, total_ref, accum_ref):
    seq = pl.program_id(0)
    blocks = 2 * ctx_size
    own_ctx = scalars[SEQS * blocks]
    own_shard = scalars[SEQS * blocks + 1]
    groups = range(KVH)
    best_ref[...] = jnp.full(best_ref.shape, NEG_FILL, jnp.float32)
    total_ref[...] = jnp.zeros(total_ref.shape, jnp.float32)
    accum_ref[...] = jnp.zeros(accum_ref.shape, jnp.float32)

    def step(key_ctx, half_key, half):
        order_key = scalars[seq * blocks + half_key * ctx_size + key_ctx]
        order_query = scalars[seq * blocks + half * ctx_size + own_ctx]

        def work(masked):
            rows = pl.ds(pl.multiple_of(key_ctx * block_rows, block_rows), block_rows)
            scores = [
                lax.dot_general(
                    kv_ref[rows, key_part(group, half_key, 0)],
                    q_ref[0, half, group],
                    CONTRACT_LAST,
                    preferred_element_type=jnp.float32,
                )
                for group in groups
            ]
            if masked:
                hidden = hidden_rows(scores[0], own_shard, rows_here)
                scores = [jnp.where(hidden, NEG_FILL, score) for score in scores]
            best = [best_ref[half, group] for group in groups]
            fresh = [
                jnp.maximum(best[group], jnp.max(scores[group], 0, keepdims=True)) for group in groups
            ]
            weights = [jnp.exp(scores[group] - fresh[group]) for group in groups]
            decay = [jnp.exp(best[group] - fresh[group]) for group in groups]
            added = [
                lax.dot_general(
                    kv_ref[rows, key_part(group, half_key, 1)],
                    weights[group].astype(jnp.bfloat16),
                    CONTRACT_FIRST,
                    preferred_element_type=jnp.float32,
                )
                for group in groups
            ]
            for group in groups:
                total_ref[half, group] = total_ref[half, group] * decay[group] + jnp.sum(
                    weights[group], 0, keepdims=True
                )
                accum_ref[half, group] = accum_ref[half, group] * decay[group] + added[group]
                best_ref[half, group] = fresh[group]

        @pl.when(order_key < order_query)
        def full():
            work(False)

        @pl.when(order_key == order_query)
        def diagonal():
            work(True)

    @pl.loop(0, ctx_size)
    def sweep(key_ctx):
        for half_key in range(2):
            for half in range(2):
                step(key_ctx, half_key, half)

    for half in range(2):
        for group in groups:
            totals = total_ref[half, group]
            out_ref[0, half, group] = (accum_ref[half, group] / totals).T
            stat_ref[0, half, group] = best_ref[half, group] + jnp.log(totals)


def group_blocks(lanes, key_rows):
    group = pl.BlockSpec((1, 2, KVH, lanes, HD), lambda s, _: (s, 0, 0, 0, 0))
    stat = pl.BlockSpec((1, 2, KVH, 1, lanes), lambda s, _: (s, 0, 0, 0, 0))
    keys = pl.BlockSpec((key_rows, KVH * 4 * HD), lambda s, _: (0, s))
    return group, stat, keys


def attend_forward(scalars, queries, all_kv, ctx_size, block_rows, rows_here):
    lanes = queries.shape[3]
    kernel = functools.partial(attend_forward_kernel, ctx_size, block_rows, rows_here)
    group, stat, keys = group_blocks(lanes, all_kv.shape[0])
    return pl.pallas_call(
        kernel,
        grid_spec=pltpu.PrefetchScalarGridSpec(
            num_scalar_prefetch=1,
            grid=(SEQS,),
            in_specs=[group, keys],
            out_specs=[group, stat],
            scratch_shapes=[
                pltpu.VMEM((2, KVH, 1, lanes), jnp.float32),
                pltpu.VMEM((2, KVH, 1, lanes), jnp.float32),
                pltpu.VMEM((2, KVH, HD, lanes), jnp.float32),
            ],
        ),
        out_shape=(
            jax.ShapeDtypeStruct(queries.shape, jnp.float32),
            jax.ShapeDtypeStruct((SEQS, 2, KVH, 1, lanes), jnp.float32),
        ),
        compiler_params=pltpu.CompilerParams(vmem_limit_bytes=60 * 2**20),
        name="attend_forward",
    )(scalars, queries, all_kv)


def attend_backward_kernel(ctx_size, block_rows, rows_here, scalars, q_ref, go_ref, att_ref, stat_ref, kv_ref, gq_ref, gkv_ref, delta_ref, gq_acc, gk_acc, gv_acc):
    seq = pl.program_id(0)
    blocks = 2 * ctx_size
    own_ctx = scalars[SEQS * blocks]
    own_shard = scalars[SEQS * blocks + 1]
    groups = range(KVH)
    gq_acc[...] = jnp.zeros(gq_acc.shape, jnp.float32)
    for half in range(2):
        for group in groups:
            product = go_ref[0, half, group].astype(jnp.float32) * att_ref[0, half, group]
            delta_ref[half, group] = jnp.sum(product.T, 0, keepdims=True)

    def step(key_ctx, half_key, half):
        order_key = scalars[seq * blocks + half_key * ctx_size + key_ctx]
        order_query = scalars[seq * blocks + half * ctx_size + own_ctx]

        def work(masked):
            rows = pl.ds(pl.multiple_of(key_ctx * block_rows, block_rows), block_rows)
            keys = [kv_ref[rows, key_part(group, half_key, 0)] for group in groups]
            queries = [q_ref[0, half, group] for group in groups]
            grad_out = [go_ref[0, half, group] for group in groups]
            scores = [
                lax.dot_general(
                    keys[group], queries[group], CONTRACT_LAST, preferred_element_type=jnp.float32
                )
                for group in groups
            ]
            grad_probs = [
                lax.dot_general(
                    kv_ref[rows, key_part(group, half_key, 1)],
                    grad_out[group],
                    CONTRACT_LAST,
                    preferred_element_type=jnp.float32,
                )
                for group in groups
            ]
            probs = [jnp.exp(scores[group] - stat_ref[0, half, group]) for group in groups]
            if masked:
                hidden = hidden_rows(scores[0], own_shard, rows_here)
                probs = [jnp.where(hidden, 0.0, prob) for prob in probs]
            grad_scores = [
                (probs[group] * (grad_probs[group] - delta_ref[half, group])).astype(jnp.bfloat16)
                for group in groups
            ]
            for group in groups:
                gv_acc[group] += jnp.dot(
                    probs[group].astype(jnp.bfloat16),
                    grad_out[group],
                    preferred_element_type=jnp.float32,
                )
                gk_acc[group] += jnp.dot(
                    grad_scores[group], queries[group], preferred_element_type=jnp.float32
                )
                gq_acc[half, group] += lax.dot_general(
                    keys[group], grad_scores[group], CONTRACT_FIRST, preferred_element_type=jnp.float32
                )

        @pl.when(order_key < order_query)
        def full():
            work(False)

        @pl.when(order_key == order_query)
        def diagonal():
            work(True)

    @pl.loop(0, ctx_size)
    def sweep(key_ctx):
        rows = pl.ds(pl.multiple_of(key_ctx * block_rows, block_rows), block_rows)
        for half_key in range(2):
            gk_acc[...] = jnp.zeros(gk_acc.shape, jnp.float32)
            gv_acc[...] = jnp.zeros(gv_acc.shape, jnp.float32)
            for half in range(2):
                step(key_ctx, half_key, half)
            for group in groups:
                gkv_ref[rows, key_part(group, half_key, 0)] = gk_acc[group].astype(jnp.bfloat16)
                gkv_ref[rows, key_part(group, half_key, 1)] = gv_acc[group].astype(jnp.bfloat16)

    for half in range(2):
        for group in groups:
            gq_ref[0, half, group] = gq_acc[half, group].T


def attend_backward(scalars, queries, grad_out, attended, stats, all_kv, ctx_size, block_rows, rows_here):
    lanes = queries.shape[3]
    kernel = functools.partial(attend_backward_kernel, ctx_size, block_rows, rows_here)
    group, stat, keys = group_blocks(lanes, all_kv.shape[0])
    return pl.pallas_call(
        kernel,
        grid_spec=pltpu.PrefetchScalarGridSpec(
            num_scalar_prefetch=1,
            grid=(SEQS,),
            in_specs=[group, group, group, stat, keys],
            out_specs=[group, keys],
            scratch_shapes=[
                pltpu.VMEM((2, KVH, 1, lanes), jnp.float32),
                pltpu.VMEM((2, KVH, HD, lanes), jnp.float32),
                pltpu.VMEM((KVH, block_rows, HD), jnp.float32),
                pltpu.VMEM((KVH, block_rows, HD), jnp.float32),
            ],
        ),
        out_shape=(
            jax.ShapeDtypeStruct(queries.shape, jnp.float32),
            jax.ShapeDtypeStruct(all_kv.shape, jnp.bfloat16),
        ),
        compiler_params=pltpu.CompilerParams(vmem_limit_bytes=60 * 2**20),
        name="attend_backward",
    )(scalars, queries, grad_out, attended, stats, all_kv)


def peers_of(ctx_size):
    return ctx_size == 4, range(1, ctx_size)


def ctx_target(position, way, square, ctx_size):
    return position ^ way if square else lax.rem(position + way, ctx_size)


def ctx_source(position, way, square, ctx_size):
    return position ^ way if square else lax.rem(position + ctx_size - way, ctx_size)


def greet(ctx_size, pair_count, with_ctx, all_shards):
    ctx = lax.axis_index("ctx")
    shard = lax.axis_index("fsdp")
    pair, core = shard // 2, shard % 2
    barrier = pltpu.get_barrier_semaphore()
    partners = [(ctx, pair * 2 + 1 - core)]
    for step in range(1, pair_count):
        there = lax.rem(pair + step, pair_count) * 2
        partners.append((ctx, there + core))
        if all_shards:
            partners.append((ctx, there + 1 - core))
    if with_ctx:
        for way in range(1, ctx_size):
            partners.append((lax.rem(ctx + way, ctx_size), shard))
    for partner in partners:
        pl.semaphore_signal(barrier, inc=1, device_id=partner, device_id_type=MESH_ID)
    pl.semaphore_wait(barrier, len(partners))
    return ctx, pair, core


class Exchange:
    def __init__(self, source, out, sems, own_sem, pair_count):
        self.source, self.out, self.sems, self.own_sem = source, out, sems, own_sem
        self.shard_count = 2 * pair_count

    def start(self):
        ctx, shard = lax.axis_index("ctx"), lax.axis_index("fsdp")
        self.own = pltpu.make_async_copy(self.source.at[shard], self.out.at[shard], self.own_sem)
        self.own.start()
        self.copies = []
        for step in range(1, self.shard_count):
            there = lax.rem(shard + step, self.shard_count)
            copy = pltpu.make_async_remote_copy(
                src_ref=self.source.at[there],
                dst_ref=self.out.at[shard],
                send_sem=self.sems[0].at[step - 1],
                recv_sem=self.sems[1].at[step - 1],
                device_id=(ctx, there),
                device_id_type=MESH_ID,
            )
            copy.start()
            self.copies.append(copy)

    def finish(self):
        ctx, shard = lax.axis_index("ctx"), lax.axis_index("fsdp")
        for step in range(1, self.shard_count):
            come = lax.rem(shard + self.shard_count - step, self.shard_count)
            pltpu.make_async_remote_copy(
                src_ref=self.out.at[come],
                dst_ref=self.out.at[come],
                send_sem=self.sems[0].at[step - 1],
                recv_sem=self.sems[1].at[step - 1],
                device_id=(ctx, shard),
                device_id_type=MESH_ID,
            ).wait_recv()
        self.own.wait()
        for copy in self.copies:
            copy.wait_send()


def gather_kernel(arity, ctx_size, pair_count, slots, swaps, wide, *refs):
    sources, refs = refs[:arity], refs[arity:]
    swap_sources, refs = refs[:swaps], refs[swaps:]
    outs, refs = refs[:arity], refs[arity:]
    swap_outs, refs = refs[:swaps], refs[swaps:]
    pair_sems, ctx_sems, core_sems = refs[0:2], refs[2:4], refs[4:6]
    local_sem = refs[6]
    square, ways = peers_of(ctx_size) if wide else (False, ())
    narrow = [item for item in range(arity) if item not in wide]
    near = [way for way in ways if not (square and way == 3)]
    ctx, pair, core = greet(ctx_size, pair_count, len(wide) > 0, swaps > 0)
    homes = [place(ctx, pair * 2 + core) for place in slots]
    started = []
    steps = [(0, 1)] + [(far, way) for far in range(1, pair_count) for way in (1, -1)]

    def present(step):
        far, way = steps[step]
        if far == 0:
            return None
        return pair >= far if way == 1 else pair + far < pair_count

    def origin(step):
        far, way = steps[step]
        return pair - far * way

    def when(condition, work):
        if condition is None:
            work()
        else:
            pl.when(condition)(work)

    def send(item, source, place, target, sems, at, condition):
        copy = pltpu.make_async_remote_copy(
            src_ref=source,
            dst_ref=outs[item].at[place],
            send_sem=sems[0].at[at],
            recv_sem=sems[1].at[at],
            device_id=target,
            device_id_type=MESH_ID,
        )
        copy.start()
        started.append((condition, item, sems, at))

    def sent(item, sems, at):
        pltpu.make_async_remote_copy(
            src_ref=outs[item].at[0],
            dst_ref=outs[item].at[0],
            send_sem=sems[0].at[at],
            recv_sem=sems[1].at[at],
            device_id=(ctx, pair * 2 + core),
            device_id_type=MESH_ID,
        ).wait_send()

    def arrive(item, place, sems, at):
        pltpu.make_async_remote_copy(
            src_ref=outs[item].at[place],
            dst_ref=outs[item].at[place],
            send_sem=sems[0].at[at],
            recv_sem=sems[1].at[at],
            device_id=(ctx, pair * 2 + core),
            device_id_type=MESH_ID,
        ).wait_recv()

    def pass_on(step, item, source, place):
        far, way = steps[step]
        for side in (1, -1) if far == 0 else (way,):

            def further(side=side):
                return pair + 1 < pair_count if side == 1 else pair >= 1

            def both(further=further):
                return further() if far == 0 else jnp.logical_and(further(), present(step))

            def work(side=side, both=both):
                send(
                    item,
                    source,
                    place,
                    (ctx, (pair + side) * 2 + core),
                    pair_sems,
                    ((side + 1) // 2, far, item),
                    both,
                )

            if far + 1 < pair_count:
                pl.when(further())(work)

    def to_core(item, source, from_ctx, way, step):
        send(
            item,
            source,
            slots[item](from_ctx, origin(step) * 2 + core),
            (ctx, pair * 2 + 1 - core),
            core_sems,
            (way, step, item),
            functools.partial(present, step),
        )

    def spread(step, items):
        for item in items:
            place = slots[item](ctx, origin(step) * 2 + core)
            source = sources[item]
            if step:
                far, way = steps[step]
                arrive(item, place, pair_sems, ((way + 1) // 2, far - 1, item))
                source = outs[item].at[place]
            pass_on(step, item, source, place)
            for way in near if item in wide else ():
                there = ctx_target(ctx, way, square, ctx_size)
                send(
                    item,
                    source,
                    place,
                    (there, pair * 2 + core),
                    ctx_sems,
                    (way - 1, step, item),
                    functools.partial(present, step),
                )
            to_core(item, source, ctx, 0, step)

    def collect(step):
        for way in near:
            for item in wide:
                come = ctx_source(ctx, way, square, ctx_size)
                place = slots[item](come, origin(step) * 2 + core)
                arrive(item, place, ctx_sems, (way - 1, step, item))
                source = outs[item].at[place]
                if square and (steps[step][0] % 2 == 0) == (way == 1):
                    send(
                        item,
                        source,
                        place,
                        (ctx ^ (3 - way), pair * 2 + core),
                        ctx_sems,
                        (2, step, item),
                        functools.partial(present, step),
                    )
                to_core(item, source, come, way, step)

    def collect_far(step):
        for item in wide:
            place = slots[item](ctx ^ 3, origin(step) * 2 + core)
            arrive(item, place, ctx_sems, (2, step, item))
            to_core(item, outs[item].at[place], ctx ^ 3, 3, step)

    def straight_core(item, source, place, step):
        sibling = (ctx, pair * 2 + 1 - core)
        send(item, source, place, sibling, core_sems, (0, step, item), lambda: None)

    def go_straight(item):
        for step in range(1, pair_count):
            there = lax.rem(pair + step, pair_count) * 2 + core
            at = (0, step - 1, item)
            send(item, sources[item], homes[item], (ctx, there), pair_sems, at, lambda: None)
        straight_core(item, sources[item], homes[item], 0)

    locals_ = []
    for item in range(arity):
        copy = pltpu.make_async_copy(sources[item], outs[item].at[homes[item]], local_sem.at[item])
        copy.start()
        locals_.append(copy)
    spread(0, wide or range(arity))
    flows = []
    count = len(steps)
    for turn in range(1, count + 4):
        if turn < count:
            when(present(turn), functools.partial(spread, turn, wide or range(arity)))
        if turn == count:
            for item in narrow if wide else ():
                go_straight(item)
            for item in range(swaps):
                flow = Exchange(
                    swap_sources[item],
                    swap_outs[item],
                    refs[7 + 3 * item : 9 + 3 * item],
                    refs[9 + 3 * item],
                    pair_count,
                )
                flow.start()
                flows.append(flow)
        if 0 <= turn - 2 < count:
            when(present(turn - 2), functools.partial(collect, turn - 2))
        if square and 0 <= turn - 4 < count:
            when(present(turn - 4), functools.partial(collect_far, turn - 4))

    for item in narrow if wide else ():
        for step in range(1, pair_count):
            come = lax.rem(pair + pair_count - step, pair_count)
            place = slots[item](ctx, come * 2 + core)
            arrive(item, place, pair_sems, (0, step - 1, item))
            straight_core(item, outs[item].at[place], place, step)
    for item in narrow if wide else ():
        for step in range(pair_count):
            come = lax.rem(pair + pair_count - step, pair_count)
            arrive(item, slots[item](ctx, come * 2 + 1 - core), core_sems, (0, step, item))

    def from_core(step):
        for way in (0, *ways):
            come = ctx_source(ctx, way, square, ctx_size) if way else ctx
            for item in wide or range(arity):
                arrive(item, slots[item](come, origin(step) * 2 + 1 - core), core_sems, (way, step, item))

    for step in range(count):
        when(present(step), functools.partial(from_core, step))
    for flow in flows:
        flow.finish()
    for copy in locals_:
        copy.wait()
    for condition, *which in started:
        when(condition(), functools.partial(sent, *which))


def gather(pieces, slots, collective_id, swaps=(), wide=None):
    ctx_size, shard_count = lax.axis_size("ctx"), lax.axis_size("fsdp")
    pair_count = shard_count // 2
    arity = len(pieces)
    wide = range(arity) if wide is None else wide
    dma = pltpu.SemaphoreType.DMA
    moved = sum(piece.size for piece in pieces) * 2
    steps = 2 * pair_count - 1
    return pl.pallas_call(
        functools.partial(gather_kernel, arity, ctx_size, pair_count, slots, len(swaps), wide),
        in_specs=[pl.BlockSpec(memory_space=pltpu.VMEM)] * (arity + len(swaps)),
        out_specs=[pl.BlockSpec(memory_space=pl.ANY)] * (arity + len(swaps)),
        out_shape=[
            jax.ShapeDtypeStruct(
                ((ctx_size if item in wide else 1) * shard_count,) + piece.shape, piece.dtype
            )
            for item, piece in enumerate(pieces)
        ]
        + [jax.ShapeDtypeStruct(swap.shape, swap.dtype) for swap in swaps],
        scratch_shapes=[dma((2, pair_count - 1, arity))] * 2
        + [dma((ctx_size - 1, steps, arity))] * 2
        + [dma((ctx_size, steps, arity))] * 2
        + [dma((arity,))]
        + [dma((shard_count - 1,)), dma((shard_count - 1,)), dma] * len(swaps),
        compiler_params=pltpu.CompilerParams(collective_id=collective_id, has_side_effects=True),
        cost_estimate=pl.CostEstimate(
            flops=0, bytes_accessed=moved * ctx_size * shard_count * 4, transcendentals=0
        ),
    )(*pieces, *swaps)


class LineScatter:
    def __init__(self, source, out, half, room, sems, where, counts, last):
        self.count, self.ctx_size = counts
        self.source, self.out, self.half, self.room = source, out, half, room
        self.last = last
        self.core_sems, self.pair_sems = sems[0:2], sems[2:4]
        self.ctx, self.pair, self.core = where
        self.order = [*range(1, self.count), 0]

    def copy(self, source, target, device, sems, at):
        return pltpu.make_async_remote_copy(
            src_ref=source,
            dst_ref=target,
            send_sem=sems[0].at[at],
            recv_sem=sems[1].at[at],
            device_id=device,
            device_id_type=MESH_ID,
        )

    def here(self):
        return (self.ctx, self.pair * 2 + self.core)

    def toward(self, step):
        return lax.rem(self.pair + step, self.count)

    def start(self):
        self.copies = []
        for step in self.order:
            self.copies.append(
                self.copy(
                    self.source.at[self.toward(step) * 2 + 1 - self.core],
                    self.half.at[step],
                    (self.ctx, self.pair * 2 + 1 - self.core),
                    self.core_sems,
                    step,
                )
            )
            self.copies[-1].start()

    def fold(self, step):
        half = self.half.at[step]
        self.copy(half, half, self.here(), self.core_sems, step).wait_recv()
        mine = self.source[self.toward(step) * 2 + self.core].astype(jnp.float32)
        total = mine + half[...].astype(jnp.float32)
        if step == 0:
            self.out[...] = total
            return
        half[...] = total.astype(half.dtype)
        self.copies.append(
            self.copy(
                half,
                self.room.at[step - 1],
                (self.ctx, self.toward(step) * 2 + self.core),
                self.pair_sems,
                step - 1,
            )
        )
        self.copies[-1].start()

    def over_ctx(self, terms, room, landing, *sems):
        shard = self.pair * 2 + self.core
        copies = []

        def send(source, target, way, sems):
            there = lax.rem(self.ctx + way, self.ctx_size)
            copies.append(self.copy(source(there), target, (there, shard), sems, way - 1))
            copies[-1].start()

        def arrive(target, way, sems):
            self.copy(target, target, self.here(), sems, way - 1).wait_recv()

        terms[...] = self.out[...].astype(terms.dtype)
        for way in range(1, self.ctx_size):
            send(lambda there: terms.at[there], room.at[way - 1], way, sems[0:2])
        total = self.out[self.ctx]
        for way in range(1, self.ctx_size):
            arrive(room.at[way - 1], way, sems[0:2])
            total = total + room[way - 1].astype(jnp.float32)
        landing[self.ctx] = total.astype(landing.dtype)
        for way in range(1, self.ctx_size):
            send(lambda there: landing.at[self.ctx], landing.at[self.ctx], way, sems[2:4])
        for way in range(1, self.ctx_size):
            come = lax.rem(self.ctx + self.ctx_size - way, self.ctx_size)
            arrive(landing.at[come], way, sems[2:4])
        self.out[...] = landing[...].astype(jnp.float32)
        for copy in copies:
            copy.wait_send()

    def finish(self):
        for step in range(1, self.count):
            room = self.room.at[step - 1]
            self.copy(room, room, self.here(), self.pair_sems, step - 1).wait_recv()
            self.out[...] += room[...].astype(jnp.float32)
        if self.last:
            self.over_ctx(*self.last)
        for copy in self.copies:
            copy.wait_send()


def scatter_kernel(arity, ctx_size, pair_count, slot, spread_ctx, lines, *refs):
    sources, refs = refs[:arity], refs[arity:]
    line_sources, refs = refs[:lines], refs[lines:]
    outs, refs = refs[:arity], refs[arity:]
    line_outs, refs = refs[:lines], refs[lines:]
    halves, relays, asides, ends, finals = (refs[i * arity : (i + 1) * arity] for i in range(5))
    sems = refs[5 * arity : 5 * arity + 10]
    core_sems, relay_sems, ctx_sems, pair_sems, last_sems = (sems[2 * i : 2 * i + 2] for i in range(5))
    square, ways = peers_of(ctx_size)
    ctx, pair, core = greet(ctx_size, pair_count, True, False)
    order = list(range(1, pair_count)) + [0]
    started = []
    flows = []
    for item in range(lines):
        at = 5 * arity + 10 + 13 * item
        spread = len(line_sources[item].shape) == 4
        flows.append(
            LineScatter(
                line_sources[item],
                line_outs[item],
                *refs[at : at + 2],
                refs[at + 2 : at + 6],
                (ctx, pair, core),
                (pair_count, ctx_size),
                refs[at + 6 : at + 13] if spread else (),
            )
        )

    def send(source, target, device, pair_of_sems, at):
        copy = pltpu.make_async_remote_copy(
            src_ref=source,
            dst_ref=target,
            send_sem=pair_of_sems[0].at[at],
            recv_sem=pair_of_sems[1].at[at],
            device_id=device,
            device_id_type=MESH_ID,
        )
        copy.start()
        started.append(copy)

    def arrive(target, pair_of_sems, at):
        pltpu.make_async_remote_copy(
            src_ref=target,
            dst_ref=target,
            send_sem=pair_of_sems[0].at[at],
            recv_sem=pair_of_sems[1].at[at],
            device_id=(ctx, pair * 2 + core),
            device_id_type=MESH_ID,
        ).wait_recv()

    def toward(step):
        return lax.rem(pair + step, pair_count)

    def target_ctx(way):
        return ctx_target(ctx, way, square, ctx_size) if way else ctx

    def f32(value):
        return value.astype(jnp.float32)

    far_first = [3, 1, 2, 0] if square else list(ways) + [0]
    for step in order:
        for way in far_first:
            for item in range(arity):
                send(
                    sources[item].at[slot(target_ctx(way), toward(step) * 2 + 1 - core)],
                    halves[item].at[way, step],
                    (ctx, pair * 2 + 1 - core),
                    core_sems,
                    (way, step, item),
                )

    def fold_core(step):
        for way in far_first:
            for item in range(arity):
                half = halves[item].at[way, step]
                arrive(half, core_sems, (way, step, item))
                mine = sources[item][slot(target_ctx(way), toward(step) * 2 + core)]
                half[...] = (f32(mine) + f32(half[...])).astype(half.dtype)
                if square and way == 3:
                    there = ctx ^ (1 if step % 2 == 0 else 2)
                    send(
                        half,
                        relays[item].at[step],
                        (there, pair * 2 + core),
                        relay_sems,
                        (step, item),
                    )

    def fold_relay(step):
        for item in range(arity):
            if square:
                relay = relays[item].at[step]
                arrive(relay, relay_sems, (step, item))
                half = halves[item].at[2 if step % 2 == 0 else 1, step]
                half[...] = (f32(half[...]) + f32(relay[...])).astype(half.dtype)
            for way in ways:
                if square and way == 3:
                    continue
                send(
                    halves[item].at[way, step],
                    asides[item].at[way - 1, step],
                    (target_ctx(way), pair * 2 + core),
                    ctx_sems,
                    (way - 1, step, item),
                )

    def fold_ctx(step):
        for item in range(arity):
            half = halves[item].at[0, step]
            total = f32(half[...])
            for way in ways:
                if square and way == 3:
                    continue
                aside = asides[item].at[way - 1, step]
                arrive(aside, ctx_sems, (way - 1, step, item))
                total = total + f32(aside[...])
            if step:
                half[...] = total.astype(half.dtype)
                send(
                    half,
                    ends[item].at[step - 1],
                    (ctx, toward(step) * 2 + core),
                    pair_sems,
                    (step - 1, item),
                )
            else:
                for other in range(1, pair_count):
                    end = ends[item].at[other - 1]
                    arrive(end, pair_sems, (other - 1, item))
                    total = total + f32(end[...])
                if spread_ctx:
                    finals[item][...] = total.astype(finals[item].dtype)
                else:
                    outs[item][...] = total.astype(outs[item].dtype)

    for flow in flows:
        flow.start()
    for turn in range(pair_count + 2):
        if turn < pair_count:
            fold_core(order[turn])
        if 1 <= turn <= pair_count:
            fold_relay(order[turn - 1])
            for flow in flows:
                flow.fold(order[turn - 1])
        if turn >= 2:
            fold_ctx(order[turn - 2])
    if spread_ctx:
        for item in range(arity):
            for way in ways:
                send(
                    finals[item],
                    outs[item].at[ctx],
                    (target_ctx(way), pair * 2 + core),
                    last_sems,
                    (way - 1, item),
                )
            outs[item][ctx] = finals[item][...]
        for item in range(arity):
            for way in ways:
                arrive(outs[item].at[ctx_source(ctx, way, square, ctx_size)], last_sems, (way - 1, item))
    for flow in flows:
        flow.finish()
    for copy in started:
        copy.wait_send()


def scatter(terms, slot, collective_id, spread_ctx=False, out_dtype=None, lines=()):
    ctx_size, shard_count = lax.axis_size("ctx"), lax.axis_size("fsdp")
    pair_count = shard_count // 2
    arity = len(terms)
    dma = pltpu.SemaphoreType.DMA
    lead = (ctx_size,) if spread_ctx else ()
    asides = 2 if ctx_size == 4 else ctx_size - 1

    def room(*extent):
        return [pltpu.VMEM(extent + term.shape[1:], term.dtype) for term in terms]

    def line_room(line):
        if len(line.shape) == 3:
            return [pltpu.VMEM((8, HD), line.dtype)] * 3 + [dma((1,))] * 4
        cut = line.shape[2:]
        rooms = [pltpu.VMEM((count,) + cut, line.dtype) for count in (ctx_size, ctx_size - 1, ctx_size)]
        return rooms + [dma((ctx_size - 1,))] * 4

    moved = sum(term.size * term.dtype.itemsize for term in terms)
    return pl.pallas_call(
        functools.partial(scatter_kernel, arity, ctx_size, pair_count, slot, spread_ctx, len(lines)),
        in_specs=[pl.BlockSpec(memory_space=pltpu.VMEM)] * (arity + len(lines)),
        out_specs=[pl.BlockSpec(memory_space=pltpu.VMEM)] * (arity + len(lines)),
        out_shape=[
            jax.ShapeDtypeStruct(lead + term.shape[1:], out_dtype or term.dtype) for term in terms
        ]
        + [jax.ShapeDtypeStruct(line.shape[1:], jnp.float32) for line in lines],
        scratch_shapes=room(ctx_size, pair_count)
        + room(pair_count)
        + room(asides, pair_count)
        + room(pair_count - 1)
        + room()
        + [dma((ctx_size, pair_count, arity))] * 2
        + [dma((pair_count, arity))] * 2
        + [dma((ctx_size - 1, pair_count, arity))] * 2
        + [dma((pair_count - 1, arity))] * 2
        + [dma((ctx_size - 1, arity))] * 2
        + [
            scratch
            for line in lines
            for scratch in [
                pltpu.VMEM((pair_count,) + line.shape[1:], line.dtype),
                pltpu.VMEM((pair_count - 1,) + line.shape[1:], line.dtype),
            ]
            + [dma((pair_count,))] * 4
            + line_room(line)
        ],
        compiler_params=pltpu.CompilerParams(
            collective_id=collective_id, has_side_effects=True, vmem_limit_bytes=63 * 2**20
        ),
        cost_estimate=pl.CostEstimate(flops=0, bytes_accessed=moved * 16, transcendentals=0),
    )(*terms, *lines)


def line_sum_kernel(pair_count, source, out, half, room, *sems):
    where = greet(1, pair_count, False, False)
    flow = LineScatter(source, out, half, room, sems, where, (pair_count, 1), ())
    flow.start()
    for step in flow.order:
        flow.fold(step)
    flow.finish()


def line_sum(terms, collective_id):
    pair_count = lax.axis_size("fsdp") // 2
    extent = terms.shape[1:]
    dma = pltpu.SemaphoreType.DMA((pair_count,))
    return pl.pallas_call(
        functools.partial(line_sum_kernel, pair_count),
        in_specs=[pl.BlockSpec(memory_space=pltpu.VMEM)],
        out_specs=pl.BlockSpec(memory_space=pltpu.VMEM),
        out_shape=jax.ShapeDtypeStruct(extent, jnp.float32),
        scratch_shapes=[
            pltpu.VMEM((pair_count,) + extent, terms.dtype),
            pltpu.VMEM((pair_count - 1,) + extent, terms.dtype),
        ]
        + [dma] * 4,
        compiler_params=pltpu.CompilerParams(
            collective_id=collective_id, has_side_effects=True, vmem_limit_bytes=63 * 2**20
        ),
        cost_estimate=pl.CostEstimate(flops=0, bytes_accessed=terms.size * 16, transcendentals=0),
    )(terms)


def turned(values, cosine, signed_sine):
    return values * cosine + pltpu.roll(values, HD // 2, 1) * signed_sine


def turned_back(grads, cosine, signed_sine):
    return grads * cosine + pltpu.roll(grads * signed_sine, HD // 2, 1)


def slot_of(index):
    return index % SEQS, index // SEQS


def key_column(index, group, part):
    seq, half = slot_of(index)
    return (((seq * KVH + group) * 2 + half) * 2 + part) * HD


def project_kernel(rows, x_ref, gain_ref, w_hbm, bias_ref, cos_ref, sin_ref, normed_ref, q_ref, kv_ref, w_ref, q_acc, sems):
    wide = w_ref.shape[2]
    copies = []
    for part in range(w_ref.shape[0]):
        copy = pltpu.make_async_copy(
            w_hbm.at[:, part * wide : (part + 1) * wide], w_ref.at[part], sems.at[part]
        )
        copy.start()
        copies.append(copy)
    values = x_ref[...].astype(jnp.float32)
    scale = lax.rsqrt(jnp.mean(values * values, -1, keepdims=True) + EPS)
    normed = (values * scale * gain_ref[...]).astype(jnp.bfloat16)
    normed_ref[...] = normed
    cosine, sine = cos_ref[...], sin_ref[...]
    for part, copy in enumerate(copies):
        copy.wait()
        columns = jnp.dot(normed, w_ref[part], preferred_element_type=jnp.float32)
        columns = columns + bias_ref[:, part * wide : (part + 1) * wide]
        for index in range(wide // HD):
            head = part * (wide // HD) + index
            piece = columns[:, index * HD : (index + 1) * HD]
            if head < H + KVH:
                piece = turned(piece, cosine, sine)
            if head < H:
                piece = piece * (HD**-0.5)
            for slot in range(2 * SEQS):
                seq, half = slot_of(slot)
                own = piece[slot * rows : (slot + 1) * rows]
                if head < H:
                    group, member = head // (H // KVH), head % (H // KVH)
                    q_acc[seq, half, group, member * rows : (member + 1) * rows] = own
                else:
                    group, kind = (head - H) % KVH, (head - H) // KVH
                    at = key_column(slot, group, kind)
                    kv_ref[:, at : at + HD] = own.astype(jnp.bfloat16)
    q_ref[...] = q_acc[...].astype(jnp.bfloat16)


def project(tokens, gain, weight, bias, cosine, signed_sine, rows):
    vmem = pl.BlockSpec(memory_space=pltpu.VMEM)
    parts = 8
    grouped = (SEQS, 2, KVH, H // KVH * rows, HD)
    return pl.pallas_call(
        functools.partial(project_kernel, rows),
        in_specs=[vmem, vmem, pl.BlockSpec(memory_space=pl.ANY), vmem, vmem, vmem],
        out_specs=[vmem, vmem, vmem],
        out_shape=[
            jax.ShapeDtypeStruct(tokens.shape, jnp.bfloat16),
            jax.ShapeDtypeStruct(grouped, jnp.bfloat16),
            jax.ShapeDtypeStruct((rows, SEQS * KVH * 4 * HD), jnp.bfloat16),
        ],
        scratch_shapes=[
            pltpu.VMEM((parts, D, QKV // parts), jnp.bfloat16),
            pltpu.VMEM(grouped, jnp.float32),
            pltpu.SemaphoreType.DMA((parts,)),
        ],
        compiler_params=pltpu.CompilerParams(vmem_limit_bytes=40 * 2**20),
        cost_estimate=pl.CostEstimate(
            flops=2 * tokens.shape[0] * D * QKV, bytes_accessed=2 * D * QKV, transcendentals=0
        ),
        name="project",
    )(tokens, gain.reshape(1, -1), weight, bias.reshape(1, -1), cosine, signed_sine)


def unproject_kernel(rows, gq_ref, gkv_ref, cos_ref, sin_ref, w_hbm, x_ref, gain_ref, past_ref, gp_ref, gi_ref, gg_ref, gb_ref, w_ref, gp_acc, sem):
    copy = pltpu.make_async_copy(w_hbm, w_ref, sem)
    copy.start()
    cosine, sine = cos_ref[...], sin_ref[...]

    def rounded(values):
        return values.astype(jnp.bfloat16).astype(jnp.float32)

    for head in range(H + 2 * KVH):
        for slot in range(2 * SEQS):
            seq, half = slot_of(slot)
            at = slice(slot * rows, (slot + 1) * rows)
            if head < H:
                group, member = head // (H // KVH), head % (H // KVH)
                grad = gq_ref[seq, half, group, member * rows : (member + 1) * rows]
                grad = rounded(grad) * (HD**-0.5)
            else:
                group, kind = (head - H) % KVH, (head - H) // KVH
                column = key_column(slot, group, kind)
                grad = rounded(gkv_ref[:, column : column + HD])
            if head < H + KVH:
                grad = turned_back(grad, cosine[at], sine[at])
            gp_acc[at, head * HD : (head + 1) * HD] = grad
    low = gp_acc[...].astype(jnp.bfloat16)
    gp_ref[...] = low
    gb_ref[...] = jnp.sum(low.astype(jnp.float32), 0, keepdims=True)
    values = x_ref[...].astype(jnp.float32)
    scale = lax.rsqrt(jnp.mean(values * values, -1, keepdims=True) + EPS)
    unit = values * scale
    copy.wait()
    grad_normed = lax.dot_general(low, w_ref[...], CONTRACT_LAST, preferred_element_type=jnp.float32)
    gg_ref[...] = jnp.sum(grad_normed * unit, 0, keepdims=True)
    grad_unit = grad_normed * gain_ref[...]
    inner = jnp.mean(grad_unit * unit, -1, keepdims=True)
    gi_ref[...] = past_ref[...] + scale * (grad_unit - unit * inner)


def unproject(grad_queries, grad_kv, cosine, signed_sine, weight, tokens, gain, past, rows):
    vmem = pl.BlockSpec(memory_space=pltpu.VMEM)
    return pl.pallas_call(
        functools.partial(unproject_kernel, rows),
        in_specs=[vmem, vmem, vmem, vmem, pl.BlockSpec(memory_space=pl.ANY), vmem, vmem, vmem],
        out_specs=[vmem] * 4,
        out_shape=[
            jax.ShapeDtypeStruct((tokens.shape[0], QKV), jnp.bfloat16),
            jax.ShapeDtypeStruct(tokens.shape, jnp.float32),
            jax.ShapeDtypeStruct((1, D), jnp.float32),
            jax.ShapeDtypeStruct((1, QKV), jnp.float32),
        ],
        scratch_shapes=[
            pltpu.VMEM((D, QKV), jnp.bfloat16),
            pltpu.VMEM((tokens.shape[0], QKV), jnp.float32),
            pltpu.SemaphoreType.DMA,
        ],
        compiler_params=pltpu.CompilerParams(vmem_limit_bytes=40 * 2**20),
        cost_estimate=pl.CostEstimate(
            flops=2 * tokens.shape[0] * D * QKV, bytes_accessed=2 * D * QKV, transcendentals=0
        ),
        name="unproject",
    )(grad_queries, grad_kv, cosine, signed_sine, weight, tokens, gain.reshape(1, -1), past)


def pack_kernel(columns, gate_ref, up_ref, out_ref):
    width = out_ref.shape[2] // 2
    cut = out_ref.shape[1]
    for there in range(out_ref.shape[0]):
        for side, ref in enumerate((gate_ref, up_ref)):
            at = side * width
            out_ref[there, :, at + width - HD : at + width] = jnp.zeros((cut, HD), out_ref.dtype)
            out_ref[there, :, at : at + columns] = ref[:, there * columns : (there + 1) * columns]


def pack(gate, up, shard_count, columns, width):
    return pl.pallas_call(
        functools.partial(pack_kernel, columns),
        in_specs=[pl.BlockSpec(memory_space=pltpu.VMEM)] * 2,
        out_specs=pl.BlockSpec(memory_space=pltpu.VMEM),
        out_shape=jax.ShapeDtypeStruct((shard_count, gate.shape[0], 2 * width), gate.dtype),
        name="pack",
    )(gate, up)


def unpack_kernel(columns, own_shard, in_ref, gate_ref, up_ref):
    width = in_ref.shape[3] // 2
    shard_count = in_ref.shape[1]
    for there in range(shard_count):
        step = lax.rem(own_shard[0] + shard_count - there, shard_count)
        for side, ref in enumerate((gate_ref, up_ref)):
            part = in_ref[0, step, :, side * width : side * width + columns]
            ref[0, :, there * columns : (there + 1) * columns] = part.astype(jnp.float32)


def unpack(own_shard, rows, columns):
    ctx_size, shard_count, cut, _ = rows.shape
    out = jax.ShapeDtypeStruct((ctx_size, cut, shard_count * columns), jnp.float32)
    return pl.pallas_call(
        functools.partial(unpack_kernel, columns),
        grid_spec=pltpu.PrefetchScalarGridSpec(
            num_scalar_prefetch=1,
            grid=(ctx_size,),
            in_specs=[pl.BlockSpec((1,) + rows.shape[1:], lambda c, _: (c, 0, 0, 0))],
            out_specs=[pl.BlockSpec((1, cut, shard_count * columns), lambda c, _: (c, 0, 0))] * 2,
        ),
        out_shape=[out, out],
        name="unpack",
    )(own_shard, rows)


def shards(
    layer_input,
    block_order,
    first_gain,
    w_qkv,
    b_qkv,
    w_o,
    second_gain,
    w_gate,
    w_up,
    w_down,
    cotangent,
):
    ctx_size = lax.axis_size("ctx")
    shard_count = lax.axis_size("fsdp")
    own_ctx = lax.axis_index("ctx")
    own_shard = lax.axis_index("fsdp")
    rows_here = layer_input.shape[0]
    block_rows = rows_here * shard_count
    cut = D // (ctx_size * shard_count)
    columns = FF // shard_count
    cosine, signed_sine = turn_tables(
        block_order, own_ctx, ctx_size, block_rows, own_shard * rows_here, rows_here
    )
    tokens = by_slot(layer_input)
    grad_out = by_slot(cotangent)

    def by_rows(ctx, shard):
        return shard * ctx_size + ctx

    def by_tokens(ctx, shard):
        return ctx * shard_count + shard

    def own_cut(weight):
        return lax.dynamic_slice_in_dim(weight, own_ctx * cut, cut, 0)

    def mix_features(values):
        shaped = values.reshape(-1, shard_count, ctx_size, cut)
        return shaped.transpose(0, 2, 1, 3).reshape(-1, D)

    def unmix_features(values):
        shaped = values.reshape(-1, ctx_size, shard_count, cut)
        return shaped.transpose(0, 2, 1, 3).reshape(-1, D)

    small = jnp.concatenate([b_qkv, first_gain, second_gain]).reshape(ctx_size, -1)
    small_width = small.shape[1]
    small = lax.dynamic_slice_in_dim(small, own_ctx, 1, 0)
    small = jnp.pad(small, ((0, 0), (0, 16 * HD - small_width))).reshape(16, HD)
    width = -(-columns // HD) * HD
    w_qkv_all, small_all, gate_up_cut = gather(
        [own_cut(w_qkv), small],
        [by_rows, by_rows],
        1,
        swaps=[pack(own_cut(w_gate), own_cut(w_up), shard_count, columns, width)],
    )
    w_qkv_all = w_qkv_all.reshape(D, QKV)
    small_all = small_all.reshape(shard_count, ctx_size, -1)[:, :, :small_width]
    small_all = small_all.reshape(shard_count, -1).astype(jnp.float32)
    bias_width = QKV // shard_count
    gain_width = D // shard_count
    bias_all = small_all[:, :bias_width].reshape(-1)
    gain_one = small_all[:, bias_width : bias_width + gain_width].reshape(-1)
    gain_two = small_all[:, bias_width + gain_width :].reshape(-1)

    down_padded = jnp.pad(w_down, ((0, width - columns), (0, 0)))

    late_w_o, w_qkv_all = lax.optimization_barrier((w_o, w_qkv_all))
    w_o_all = lax.all_gather(late_w_o, "fsdp", axis=0, tiled=True)
    normed_one, queries, own_kv = project(
        tokens, gain_one, w_qkv_all, bias_all, cosine, signed_sine, rows_here
    )
    (all_kv,) = gather([own_kv], [by_tokens], 2)
    gate_up_cut, all_kv = lax.optimization_barrier((gate_up_cut, all_kv))
    gate_up_cols = lax.all_gather(
        gate_up_cut.reshape(shard_count * cut, 2 * width), "ctx", axis=0, tiled=True
    )
    all_kv = all_kv.reshape(-1, SEQS * KVH * 4 * HD)
    scalars = jnp.concatenate(
        [block_order.reshape(-1), jnp.stack([own_ctx, own_shard]).astype(jnp.int32)]
    )
    attended_grouped, stats = attend_forward(
        scalars, queries, all_kv, ctx_size, block_rows, rows_here
    )
    attended_low = from_groups(attended_grouped, rows_here).astype(jnp.bfloat16)
    middle = tokens.astype(jnp.float32) + jnp.dot(attended_low, w_o_all, preferred_element_type=jnp.float32)
    unit_two, scale_two, normed = normalize(middle, gain_two)
    normed_two = mix_features(normed.astype(jnp.bfloat16))

    tokens_all, cotangent_all = gather(
        [normed_two, grad_out], [lambda ctx, shard: shard] * 2, 6, wide=()
    )
    tokens_all = tokens_all.reshape(-1, D)
    cotangent_all = cotangent_all.reshape(-1, D)
    gate_up_part = jnp.dot(tokens_all, gate_up_cols, preferred_element_type=jnp.float32)
    gate_part, up_part = gate_up_part[:, :width], gate_up_part[:, width:]
    sigmoid_gate = jax.nn.sigmoid(gate_part)
    activated = gate_part * sigmoid_gate
    hidden = (activated * up_part).astype(jnp.bfloat16)
    grad_hidden = lax.dot_general(
        cotangent_all, down_padded, CONTRACT_LAST, preferred_element_type=jnp.float32
    )
    grad_gate = grad_hidden * up_part * sigmoid_gate * (1.0 + gate_part * (1.0 - sigmoid_gate))
    grad_gate_up = jnp.concatenate([grad_gate, grad_hidden * activated], -1).astype(jnp.bfloat16)
    gate_up_terms = lax.dot_general(
        tokens_all, grad_gate_up, CONTRACT_FIRST, preferred_element_type=jnp.float32
    ).astype(jnp.bfloat16)
    gate_up_rows = lax.psum_scatter(gate_up_terms, "ctx", scatter_dimension=0, tiled=True)
    grad_gate_up, hidden, gate_up_terms = lax.optimization_barrier(
        (grad_gate_up, hidden, gate_up_terms)
    )
    grad_tokens = lax.dot_general(
        grad_gate_up, gate_up_cols, CONTRACT_LAST, preferred_element_type=jnp.float32
    ).astype(jnp.bfloat16)
    grad_normed_two = line_sum(grad_tokens.reshape(shard_count, -1, D), 7)
    grad_normed_two, hidden = lax.optimization_barrier((grad_normed_two, hidden))
    down_terms = lax.dot_general(
        hidden, cotangent_all, CONTRACT_FIRST, preferred_element_type=jnp.float32
    ).astype(jnp.bfloat16)
    down_rows = lax.psum(down_terms, "ctx")
    mixed_terms = jnp.dot(hidden, down_padded, preferred_element_type=jnp.float32).astype(jnp.bfloat16)
    grad_normed_two, down_terms, mixed_terms = lax.optimization_barrier(
        (grad_normed_two, down_terms, mixed_terms)
    )
    grad_normed_two = unmix_features(grad_normed_two)
    grad_middle_norm, grad_gain_two = norm_back(grad_normed_two, unit_two, scale_two, gain_two)
    grad_middle = grad_out.astype(jnp.float32) + grad_middle_norm
    grad_branch_one = grad_middle.astype(jnp.bfloat16)
    grad_attended = lax.dot_general(
        grad_branch_one, w_o_all, CONTRACT_LAST, preferred_element_type=jnp.float32
    ).astype(jnp.bfloat16)
    own_rows = gate_up_rows.reshape(shard_count, cut, 2 * width)
    swapped = [lax.dynamic_index_in_dim(own_rows, own_shard, 0, False)]
    for step in range(1, shard_count):
        there = lax.rem(own_shard + step, shard_count)
        swapped.append(
            lax.ppermute(
                lax.dynamic_index_in_dim(own_rows, there, 0, False),
                "fsdp",
                [(shard, (shard + step) % shard_count) for shard in range(shard_count)],
            )
        )
    o_terms = lax.dot_general(
        attended_low, grad_branch_one, CONTRACT_FIRST, preferred_element_type=jnp.float32
    ).astype(jnp.bfloat16)
    grad_queries, grad_kv_full = attend_backward(
        scalars,
        queries,
        to_groups(grad_attended, rows_here),
        attended_grouped,
        stats,
        all_kv,
        ctx_size,
        block_rows,
        rows_here,
    )
    (grad_kv,) = scatter(
        [grad_kv_full.reshape(-1, rows_here, SEQS * KVH * 4 * HD)],
        by_tokens,
        3,
        out_dtype=jnp.float32,
    )
    *swapped, mixed_terms, grad_kv = lax.optimization_barrier((*swapped, mixed_terms, grad_kv))
    gate_up_rows = lax.all_gather(jnp.stack(swapped), "ctx", axis=0, tiled=False)
    mixed_rows = lax.psum_scatter(mixed_terms, "fsdp", scatter_dimension=0, tiled=True)
    grad_projected, grad_input, grad_gain_one, grad_bias = unproject(
        grad_queries,
        grad_kv,
        cosine,
        signed_sine,
        w_qkv_all,
        tokens,
        gain_one,
        grad_middle,
        rows_here,
    )
    grad_input = from_slot(grad_input, rows_here)
    grad_bias = grad_bias.reshape(-1)
    qkv_terms = lax.dot_general(
        normed_one, grad_projected, CONTRACT_FIRST, preferred_element_type=jnp.float32
    ).astype(jnp.bfloat16)
    small_terms = jnp.concatenate(
        [
            part.reshape(shard_count, -1)
            for part in (grad_gain_one, grad_gain_two, grad_bias[:QK], grad_bias[QK:])
        ],
        1,
    )
    small_terms = small_terms.reshape(ctx_size * shard_count, small_width)
    small_terms = jnp.pad(small_terms, ((0, 0), (0, 8 * HD - small_width)))
    qkv_rows, o_rows, small_rows = scatter(
        [
            qkv_terms.reshape(-1, cut, QKV),
            o_terms.reshape(-1, cut, D),
            small_terms.reshape(-1, 8, HD),
        ],
        by_rows,
        4,
        spread_ctx=True,
    )
    mixed_out = middle + mixed_rows.astype(jnp.float32)
    output = from_slot(mixed_out.astype(jnp.bfloat16), rows_here)
    small_rows = small_rows.reshape(ctx_size, -1)[:, :small_width].reshape(-1)
    bias_start = 2 * gain_width
    value_start = bias_start + QK // shard_count

    gate_rows, up_rows = unpack(own_shard.reshape(1).astype(jnp.int32), gate_up_rows, columns)
    return (
        output,
        grad_input,
        small_rows[:gain_width],
        qkv_rows.reshape(-1, QKV).astype(jnp.float32),
        small_rows[bias_start:value_start],
        small_rows[value_start:],
        o_rows.reshape(-1, D).astype(jnp.float32),
        small_rows[gain_width:bias_start],
        gate_rows.reshape(-1, FF),
        up_rows.reshape(-1, FF),
        down_rows[:columns].astype(jnp.float32),
    )


def solution(mesh):
    in_specs = (
        P(("ctx", "fsdp"), None, None),
        P(),
        P("fsdp"),
        P("fsdp", None),
        P("fsdp"),
        P("fsdp", None),
        P("fsdp"),
        P("fsdp", None),
        P("fsdp", None),
        P("fsdp", None),
        P(("ctx", "fsdp"), None, None),
    )
    out_specs = (
        P(("ctx", "fsdp"), None, None),
        P(("ctx", "fsdp"), None, None),
        P("fsdp"),
        P("fsdp", None),
        P("fsdp"),
        P("fsdp"),
        P("fsdp", None),
        P("fsdp"),
        P("fsdp", None),
        P("fsdp", None),
        P("fsdp", None),
    )
    return jax.shard_map(shards, mesh=mesh, in_specs=in_specs, out_specs=out_specs, check_vma=False)
```

```python
import functools

import jax
import jax.numpy as jnp
from jax import lax
from jax.experimental import pallas as pl
from jax.experimental.pallas import tpu as pltpu
from jax.sharding import PartitionSpec as P

D = 1536
H = 12
KVH = 2
HD = 128
FF = 8960
SEQS = 2
QKV = 2048
QK = 1792


EPS = 1e-06
THETA = 1000000.0
NEG_FILL = -1e30
MESH_ID = pl.DeviceIdType.MESH
CONTRACT_LAST = (((1,), (1,)), ((), ()))
CONTRACT_FIRST = (((0,), (0,)), ((), ()))


def by_slot(tokens):
    return tokens.transpose(1, 0, 2).reshape(-1, tokens.shape[2])


def from_slot(tokens, row_count):
    return tokens.reshape(2 * SEQS, row_count, -1).transpose(1, 0, 2)


def to_groups(tokens, row_count):
    shaped = tokens.reshape(2, SEQS, row_count, KVH, H // KVH, HD)
    return shaped.transpose(1, 0, 3, 4, 2, 5).reshape(SEQS, 2, KVH, H // KVH * row_count, HD)


def from_groups(grouped, row_count):
    shaped = grouped.reshape(SEQS, 2, KVH, H // KVH, row_count, HD).transpose(1, 0, 4, 2, 3, 5)
    return shaped.reshape(row_count * 2 * SEQS, H * HD)


def turn_tables(block_order, own_ctx, ctx_size, block_rows, first_row, row_count):
    half_width = HD // 2
    frequency = THETA ** (-jnp.arange(half_width, dtype=jnp.float32) * 2.0 / HD)
    frequency = jnp.tile(frequency, 2)[None, :]
    order = lax.dynamic_index_in_dim(block_order.reshape(SEQS, 2, ctx_size), own_ctx, 2, False)
    start = (order.T.reshape(-1) * block_rows + first_row).astype(jnp.float32)
    far = start[:, None] * frequency
    near = jnp.arange(row_count, dtype=jnp.float32)[:, None] * frequency
    far_cos, far_sin = jnp.cos(far)[:, None, :], jnp.sin(far)[:, None, :]
    near_cos, near_sin = jnp.cos(near)[None], jnp.sin(near)[None]
    sign = jnp.where(jnp.arange(HD) < half_width, -1.0, 1.0).astype(jnp.float32)
    cosine = far_cos * near_cos - far_sin * near_sin
    sine = (far_sin * near_cos + far_cos * near_sin) * sign
    return cosine.reshape(-1, HD), sine.reshape(-1, HD)


def normalize(values, gain):
    scale = lax.rsqrt(jnp.mean(values * values, -1, keepdims=True) + EPS)
    unit = values * scale
    return (unit, scale, unit * gain)


def norm_back(grad_out, unit, scale, gain):
    grad_unit = grad_out * gain
    inner = jnp.mean(grad_unit * unit, -1, keepdims=True)
    return (scale * (grad_unit - unit * inner), jnp.sum(grad_out * unit, 0))


def hidden_rows(scores, own_shard, rows_here):
    row = lax.broadcasted_iota(jnp.int32, scores.shape, 0)
    lane = lax.broadcasted_iota(jnp.int32, scores.shape, 1)
    return row > own_shard * rows_here + lax.rem(lane, rows_here)


def key_part(group, half_key, part):
    at = ((group * 2 + half_key) * 2 + part) * HD
    return slice(at, at + HD)


def attend_forward_kernel(ctx_size, block_rows, rows_here, scalars, q_ref, kv_ref, out_ref, stat_ref, best_ref, total_ref, accum_ref):
    seq = pl.program_id(0)
    blocks = 2 * ctx_size
    own_ctx = scalars[SEQS * blocks]
    own_shard = scalars[SEQS * blocks + 1]
    groups = range(KVH)
    best_ref[...] = jnp.full(best_ref.shape, NEG_FILL, jnp.float32)
    total_ref[...] = jnp.zeros(total_ref.shape, jnp.float32)
    accum_ref[...] = jnp.zeros(accum_ref.shape, jnp.float32)

    def step(key_ctx, half_key, half):
        order_key = scalars[seq * blocks + half_key * ctx_size + key_ctx]
        order_query = scalars[seq * blocks + half * ctx_size + own_ctx]

        def work(masked):
            rows = pl.ds(pl.multiple_of(key_ctx * block_rows, block_rows), block_rows)
            scores = [
                lax.dot_general(
                    kv_ref[rows, key_part(group, half_key, 0)],
                    q_ref[0, half, group],
                    CONTRACT_LAST,
                    preferred_element_type=jnp.float32,
                )
                for group in groups
            ]
            if masked:
                hidden = hidden_rows(scores[0], own_shard, rows_here)
                scores = [jnp.where(hidden, NEG_FILL, score) for score in scores]
            best = [best_ref[half, group] for group in groups]
            fresh = [
                jnp.maximum(best[group], jnp.max(scores[group], 0, keepdims=True)) for group in groups
            ]
            weights = [jnp.exp(scores[group] - fresh[group]) for group in groups]
            decay = [jnp.exp(best[group] - fresh[group]) for group in groups]
            added = [
                lax.dot_general(
                    kv_ref[rows, key_part(group, half_key, 1)],
                    weights[group].astype(jnp.bfloat16),
                    CONTRACT_FIRST,
                    preferred_element_type=jnp.float32,
                )
                for group in groups
            ]
            for group in groups:
                total_ref[half, group] = total_ref[half, group] * decay[group] + jnp.sum(
                    weights[group], 0, keepdims=True
                )
                accum_ref[half, group] = accum_ref[half, group] * decay[group] + added[group]
                best_ref[half, group] = fresh[group]

        @pl.when(order_key < order_query)
        def full():
            work(False)

        @pl.when(order_key == order_query)
        def diagonal():
            work(True)

    @pl.loop(0, ctx_size)
    def sweep(key_ctx):
        for half_key in range(2):
            for half in range(2):
                step(key_ctx, half_key, half)

    for half in range(2):
        for group in groups:
            totals = total_ref[half, group]
            out_ref[0, half, group] = (accum_ref[half, group] / totals).T
            stat_ref[0, half, group] = best_ref[half, group] + jnp.log(totals)


def group_blocks(lanes, key_rows):
    group = pl.BlockSpec((1, 2, KVH, lanes, HD), lambda s, _: (s, 0, 0, 0, 0))
    stat = pl.BlockSpec((1, 2, KVH, 1, lanes), lambda s, _: (s, 0, 0, 0, 0))
    keys = pl.BlockSpec((key_rows, KVH * 4 * HD), lambda s, _: (0, s))
    return group, stat, keys


def attend_forward(scalars, queries, all_kv, ctx_size, block_rows, rows_here):
    lanes = queries.shape[3]
    kernel = functools.partial(attend_forward_kernel, ctx_size, block_rows, rows_here)
    group, stat, keys = group_blocks(lanes, all_kv.shape[0])
    return pl.pallas_call(
        kernel,
        grid_spec=pltpu.PrefetchScalarGridSpec(
            num_scalar_prefetch=1,
            grid=(SEQS,),
            in_specs=[group, keys],
            out_specs=[group, stat],
            scratch_shapes=[
                pltpu.VMEM((2, KVH, 1, lanes), jnp.float32),
                pltpu.VMEM((2, KVH, 1, lanes), jnp.float32),
                pltpu.VMEM((2, KVH, HD, lanes), jnp.float32),
            ],
        ),
        out_shape=(
            jax.ShapeDtypeStruct(queries.shape, jnp.float32),
            jax.ShapeDtypeStruct((SEQS, 2, KVH, 1, lanes), jnp.float32),
        ),
        compiler_params=pltpu.CompilerParams(vmem_limit_bytes=60 * 2**20),
        name="attend_forward",
    )(scalars, queries, all_kv)


def attend_backward_kernel(ctx_size, block_rows, rows_here, scalars, q_ref, go_ref, att_ref, stat_ref, kv_ref, gq_ref, gkv_ref, delta_ref, gq_acc, gk_acc, gv_acc):
    seq = pl.program_id(0)
    blocks = 2 * ctx_size
    own_ctx = scalars[SEQS * blocks]
    own_shard = scalars[SEQS * blocks + 1]
    groups = range(KVH)
    gq_acc[...] = jnp.zeros(gq_acc.shape, jnp.float32)
    for half in range(2):
        for group in groups:
            product = go_ref[0, half, group].astype(jnp.float32) * att_ref[0, half, group]
            delta_ref[half, group] = jnp.sum(product.T, 0, keepdims=True)

    def step(key_ctx, half_key, half):
        order_key = scalars[seq * blocks + half_key * ctx_size + key_ctx]
        order_query = scalars[seq * blocks + half * ctx_size + own_ctx]

        def work(masked):
            rows = pl.ds(pl.multiple_of(key_ctx * block_rows, block_rows), block_rows)
            keys = [kv_ref[rows, key_part(group, half_key, 0)] for group in groups]
            queries = [q_ref[0, half, group] for group in groups]
            grad_out = [go_ref[0, half, group] for group in groups]
            scores = [
                lax.dot_general(
                    keys[group], queries[group], CONTRACT_LAST, preferred_element_type=jnp.float32
                )
                for group in groups
            ]
            grad_probs = [
                lax.dot_general(
                    kv_ref[rows, key_part(group, half_key, 1)],
                    grad_out[group],
                    CONTRACT_LAST,
                    preferred_element_type=jnp.float32,
                )
                for group in groups
            ]
            probs = [jnp.exp(scores[group] - stat_ref[0, half, group]) for group in groups]
            if masked:
                hidden = hidden_rows(scores[0], own_shard, rows_here)
                probs = [jnp.where(hidden, 0.0, prob) for prob in probs]
            grad_scores = [
                (probs[group] * (grad_probs[group] - delta_ref[half, group])).astype(jnp.bfloat16)
                for group in groups
            ]
            for group in groups:
                gv_acc[group] += jnp.dot(
                    probs[group].astype(jnp.bfloat16),
                    grad_out[group],
                    preferred_element_type=jnp.float32,
                )
                gk_acc[group] += jnp.dot(
                    grad_scores[group], queries[group], preferred_element_type=jnp.float32
                )
                gq_acc[half, group] += lax.dot_general(
                    keys[group], grad_scores[group], CONTRACT_FIRST, preferred_element_type=jnp.float32
                )

        @pl.when(order_key < order_query)
        def full():
            work(False)

        @pl.when(order_key == order_query)
        def diagonal():
            work(True)

    @pl.loop(0, ctx_size)
    def sweep(key_ctx):
        rows = pl.ds(pl.multiple_of(key_ctx * block_rows, block_rows), block_rows)
        for half_key in range(2):
            gk_acc[...] = jnp.zeros(gk_acc.shape, jnp.float32)
            gv_acc[...] = jnp.zeros(gv_acc.shape, jnp.float32)
            for half in range(2):
                step(key_ctx, half_key, half)
            for group in groups:
                gkv_ref[rows, key_part(group, half_key, 0)] = gk_acc[group].astype(jnp.bfloat16)
                gkv_ref[rows, key_part(group, half_key, 1)] = gv_acc[group].astype(jnp.bfloat16)

    for half in range(2):
        for group in groups:
            gq_ref[0, half, group] = gq_acc[half, group].T


def attend_backward(scalars, queries, grad_out, attended, stats, all_kv, ctx_size, block_rows, rows_here):
    lanes = queries.shape[3]
    kernel = functools.partial(attend_backward_kernel, ctx_size, block_rows, rows_here)
    group, stat, keys = group_blocks(lanes, all_kv.shape[0])
    return pl.pallas_call(
        kernel,
        grid_spec=pltpu.PrefetchScalarGridSpec(
            num_scalar_prefetch=1,
            grid=(SEQS,),
            in_specs=[group, group, group, stat, keys],
            out_specs=[group, keys],
            scratch_shapes=[
                pltpu.VMEM((2, KVH, 1, lanes), jnp.float32),
                pltpu.VMEM((2, KVH, HD, lanes), jnp.float32),
                pltpu.VMEM((KVH, block_rows, HD), jnp.float32),
                pltpu.VMEM((KVH, block_rows, HD), jnp.float32),
            ],
        ),
        out_shape=(
            jax.ShapeDtypeStruct(queries.shape, jnp.float32),
            jax.ShapeDtypeStruct(all_kv.shape, jnp.bfloat16),
        ),
        compiler_params=pltpu.CompilerParams(vmem_limit_bytes=60 * 2**20),
        name="attend_backward",
    )(scalars, queries, grad_out, attended, stats, all_kv)


def peers_of(ctx_size):
    return ctx_size == 4, range(1, ctx_size)


def ctx_target(position, way, square, ctx_size):
    return position ^ way if square else lax.rem(position + way, ctx_size)


def ctx_source(position, way, square, ctx_size):
    return position ^ way if square else lax.rem(position + ctx_size - way, ctx_size)


def greet(ctx_size, pair_count, with_ctx, all_shards):
    ctx = lax.axis_index("ctx")
    shard = lax.axis_index("fsdp")
    pair, core = shard // 2, shard % 2
    barrier = pltpu.get_barrier_semaphore()
    partners = [(ctx, pair * 2 + 1 - core)]
    for step in range(1, pair_count):
        there = lax.rem(pair + step, pair_count) * 2
        partners.append((ctx, there + core))
        if all_shards:
            partners.append((ctx, there + 1 - core))
    if with_ctx:
        for way in range(1, ctx_size):
            partners.append((lax.rem(ctx + way, ctx_size), shard))
    for partner in partners:
        pl.semaphore_signal(barrier, inc=1, device_id=partner, device_id_type=MESH_ID)
    pl.semaphore_wait(barrier, len(partners))
    return ctx, pair, core


class Exchange:
    def __init__(self, source, out, sems, own_sem, pair_count):
        self.source, self.out, self.sems, self.own_sem = source, out, sems, own_sem
        self.shard_count = 2 * pair_count

    def start(self):
        ctx, shard = lax.axis_index("ctx"), lax.axis_index("fsdp")
        self.own = pltpu.make_async_copy(self.source.at[shard], self.out.at[shard], self.own_sem)
        self.own.start()
        self.copies = []
        for step in range(1, self.shard_count):
            there = lax.rem(shard + step, self.shard_count)
            copy = pltpu.make_async_remote_copy(
                src_ref=self.source.at[there],
                dst_ref=self.out.at[shard],
                send_sem=self.sems[0].at[step - 1],
                recv_sem=self.sems[1].at[step - 1],
                device_id=(ctx, there),
                device_id_type=MESH_ID,
            )
            copy.start()
            self.copies.append(copy)

    def finish(self):
        ctx, shard = lax.axis_index("ctx"), lax.axis_index("fsdp")
        for step in range(1, self.shard_count):
            come = lax.rem(shard + self.shard_count - step, self.shard_count)
            pltpu.make_async_remote_copy(
                src_ref=self.out.at[come],
                dst_ref=self.out.at[come],
                send_sem=self.sems[0].at[step - 1],
                recv_sem=self.sems[1].at[step - 1],
                device_id=(ctx, shard),
                device_id_type=MESH_ID,
            ).wait_recv()
        self.own.wait()
        for copy in self.copies:
            copy.wait_send()


def exchange_kernel(pair_count, source, out, send_sem, recv_sem, own_sem):
    greet(1, pair_count, False, True)
    flow = Exchange(source, out, (send_sem, recv_sem), own_sem, pair_count)
    flow.start()
    flow.finish()


def exchange(pieces, collective_id):
    shard_count = lax.axis_size("fsdp")
    dma = pltpu.SemaphoreType.DMA
    return pl.pallas_call(
        functools.partial(exchange_kernel, shard_count // 2),
        in_specs=[pl.BlockSpec(memory_space=pltpu.VMEM)],
        out_specs=pl.BlockSpec(memory_space=pl.ANY),
        out_shape=jax.ShapeDtypeStruct(pieces.shape, pieces.dtype),
        scratch_shapes=[dma((shard_count - 1,))] * 2 + [dma],
        compiler_params=pltpu.CompilerParams(collective_id=collective_id, has_side_effects=True),
        cost_estimate=pl.CostEstimate(
            flops=0, bytes_accessed=pieces.size * 64, transcendentals=0
        ),
    )(pieces)


def gather_kernel(arity, ctx_size, pair_count, slots, swaps, wide, *refs):
    sources, refs = refs[:arity], refs[arity:]
    swap_sources, refs = refs[:swaps], refs[swaps:]
    outs, refs = refs[:arity], refs[arity:]
    swap_outs, refs = refs[:swaps], refs[swaps:]
    pair_sems, ctx_sems, core_sems = refs[0:2], refs[2:4], refs[4:6]
    local_sem = refs[6]
    square, ways = peers_of(ctx_size) if wide else (False, ())
    narrow = [item for item in range(arity) if item not in wide]
    near = [way for way in ways if not (square and way == 3)]
    ctx, pair, core = greet(ctx_size, pair_count, len(wide) > 0, swaps > 0)
    homes = [place(ctx, pair * 2 + core) for place in slots]
    started = []
    steps = [(0, 1)] + [(far, way) for far in range(1, pair_count) for way in (1, -1)]

    def present(step):
        far, way = steps[step]
        if far == 0:
            return None
        return pair >= far if way == 1 else pair + far < pair_count

    def origin(step):
        far, way = steps[step]
        return pair - far * way

    def when(condition, work):
        if condition is None:
            work()
        else:
            pl.when(condition)(work)

    def send(item, source, place, target, sems, at, condition):
        copy = pltpu.make_async_remote_copy(
            src_ref=source,
            dst_ref=outs[item].at[place],
            send_sem=sems[0].at[at],
            recv_sem=sems[1].at[at],
            device_id=target,
            device_id_type=MESH_ID,
        )
        copy.start()
        started.append((condition, item, sems, at))

    def sent(item, sems, at):
        pltpu.make_async_remote_copy(
            src_ref=outs[item].at[0],
            dst_ref=outs[item].at[0],
            send_sem=sems[0].at[at],
            recv_sem=sems[1].at[at],
            device_id=(ctx, pair * 2 + core),
            device_id_type=MESH_ID,
        ).wait_send()

    def arrive(item, place, sems, at):
        pltpu.make_async_remote_copy(
            src_ref=outs[item].at[place],
            dst_ref=outs[item].at[place],
            send_sem=sems[0].at[at],
            recv_sem=sems[1].at[at],
            device_id=(ctx, pair * 2 + core),
            device_id_type=MESH_ID,
        ).wait_recv()

    def pass_on(step, item, source, place):
        far, way = steps[step]
        for side in (1, -1) if far == 0 else (way,):

            def further(side=side):
                return pair + 1 < pair_count if side == 1 else pair >= 1

            def both(further=further):
                return further() if far == 0 else jnp.logical_and(further(), present(step))

            def work(side=side, both=both):
                send(
                    item,
                    source,
                    place,
                    (ctx, (pair + side) * 2 + core),
                    pair_sems,
                    ((side + 1) // 2, far, item),
                    both,
                )

            if far + 1 < pair_count:
                pl.when(further())(work)

    def to_core(item, source, from_ctx, way, step):
        send(
            item,
            source,
            slots[item](from_ctx, origin(step) * 2 + core),
            (ctx, pair * 2 + 1 - core),
            core_sems,
            (way, step, item),
            functools.partial(present, step),
        )

    def spread(step, items):
        for item in items:
            place = slots[item](ctx, origin(step) * 2 + core)
            source = sources[item]
            if step:
                far, way = steps[step]
                arrive(item, place, pair_sems, ((way + 1) // 2, far - 1, item))
                source = outs[item].at[place]
            pass_on(step, item, source, place)
            for way in near if item in wide else ():
                there = ctx_target(ctx, way, square, ctx_size)
                send(
                    item,
                    source,
                    place,
                    (there, pair * 2 + core),
                    ctx_sems,
                    (way - 1, step, item),
                    functools.partial(present, step),
                )
            to_core(item, source, ctx, 0, step)

    def collect(step):
        for way in near:
            for item in wide:
                come = ctx_source(ctx, way, square, ctx_size)
                place = slots[item](come, origin(step) * 2 + core)
                arrive(item, place, ctx_sems, (way - 1, step, item))
                source = outs[item].at[place]
                if square and (steps[step][0] % 2 == 0) == (way == 1):
                    send(
                        item,
                        source,
                        place,
                        (ctx ^ (3 - way), pair * 2 + core),
                        ctx_sems,
                        (2, step, item),
                        functools.partial(present, step),
                    )
                to_core(item, source, come, way, step)

    def collect_far(step):
        for item in wide:
            place = slots[item](ctx ^ 3, origin(step) * 2 + core)
            arrive(item, place, ctx_sems, (2, step, item))
            to_core(item, outs[item].at[place], ctx ^ 3, 3, step)

    def straight_core(item, source, place, step):
        sibling = (ctx, pair * 2 + 1 - core)
        send(item, source, place, sibling, core_sems, (0, step, item), lambda: None)

    def go_straight(item):
        for step in range(1, pair_count):
            there = lax.rem(pair + step, pair_count) * 2 + core
            at = (0, step - 1, item)
            send(item, sources[item], homes[item], (ctx, there), pair_sems, at, lambda: None)
        straight_core(item, sources[item], homes[item], 0)

    locals_ = []
    for item in range(arity):
        copy = pltpu.make_async_copy(sources[item], outs[item].at[homes[item]], local_sem.at[item])
        copy.start()
        locals_.append(copy)
    spread(0, wide or range(arity))
    flows = []
    count = len(steps)
    for turn in range(1, count + 4):
        if turn < count:
            when(present(turn), functools.partial(spread, turn, wide or range(arity)))
        if turn == count:
            for item in narrow if wide else ():
                go_straight(item)
            for item in range(swaps):
                flow = Exchange(
                    swap_sources[item],
                    swap_outs[item],
                    refs[7 + 3 * item : 9 + 3 * item],
                    refs[9 + 3 * item],
                    pair_count,
                )
                flow.start()
                flows.append(flow)
        if 0 <= turn - 2 < count:
            when(present(turn - 2), functools.partial(collect, turn - 2))
        if square and 0 <= turn - 4 < count:
            when(present(turn - 4), functools.partial(collect_far, turn - 4))

    for item in narrow if wide else ():
        for step in range(1, pair_count):
            come = lax.rem(pair + pair_count - step, pair_count)
            place = slots[item](ctx, come * 2 + core)
            arrive(item, place, pair_sems, (0, step - 1, item))
            straight_core(item, outs[item].at[place], place, step)
    for item in narrow if wide else ():
        for step in range(pair_count):
            come = lax.rem(pair + pair_count - step, pair_count)
            arrive(item, slots[item](ctx, come * 2 + 1 - core), core_sems, (0, step, item))

    def from_core(step):
        for way in (0, *ways):
            come = ctx_source(ctx, way, square, ctx_size) if way else ctx
            for item in wide or range(arity):
                arrive(item, slots[item](come, origin(step) * 2 + 1 - core), core_sems, (way, step, item))

    for step in range(count):
        when(present(step), functools.partial(from_core, step))
    for flow in flows:
        flow.finish()
    for copy in locals_:
        copy.wait()
    for condition, *which in started:
        when(condition(), functools.partial(sent, *which))


def gather(pieces, slots, collective_id, swaps=(), wide=None):
    ctx_size, shard_count = lax.axis_size("ctx"), lax.axis_size("fsdp")
    pair_count = shard_count // 2
    arity = len(pieces)
    wide = range(arity) if wide is None else wide
    dma = pltpu.SemaphoreType.DMA
    moved = sum(piece.size for piece in pieces) * 2
    steps = 2 * pair_count - 1
    return pl.pallas_call(
        functools.partial(gather_kernel, arity, ctx_size, pair_count, slots, len(swaps), wide),
        in_specs=[pl.BlockSpec(memory_space=pltpu.VMEM)] * (arity + len(swaps)),
        out_specs=[pl.BlockSpec(memory_space=pl.ANY)] * (arity + len(swaps)),
        out_shape=[
            jax.ShapeDtypeStruct(
                ((ctx_size if item in wide else 1) * shard_count,) + piece.shape, piece.dtype
            )
            for item, piece in enumerate(pieces)
        ]
        + [jax.ShapeDtypeStruct(swap.shape, swap.dtype) for swap in swaps],
        scratch_shapes=[dma((2, pair_count - 1, arity))] * 2
        + [dma((ctx_size - 1, steps, arity))] * 2
        + [dma((ctx_size, steps, arity))] * 2
        + [dma((arity,))]
        + [dma((shard_count - 1,)), dma((shard_count - 1,)), dma] * len(swaps),
        compiler_params=pltpu.CompilerParams(collective_id=collective_id, has_side_effects=True),
        cost_estimate=pl.CostEstimate(
            flops=0, bytes_accessed=moved * ctx_size * shard_count * 4, transcendentals=0
        ),
    )(*pieces, *swaps)


class LineScatter:
    def __init__(self, source, out, half, room, sems, where, counts, last):
        self.count, self.ctx_size = counts
        self.source, self.out, self.half, self.room = source, out, half, room
        self.last = last
        self.core_sems, self.pair_sems = sems[0:2], sems[2:4]
        self.ctx, self.pair, self.core = where
        self.order = [*range(1, self.count), 0]

    def copy(self, source, target, device, sems, at):
        return pltpu.make_async_remote_copy(
            src_ref=source,
            dst_ref=target,
            send_sem=sems[0].at[at],
            recv_sem=sems[1].at[at],
            device_id=device,
            device_id_type=MESH_ID,
        )

    def here(self):
        return (self.ctx, self.pair * 2 + self.core)

    def toward(self, step):
        return lax.rem(self.pair + step, self.count)

    def start(self):
        self.copies = []
        for step in self.order:
            self.copies.append(
                self.copy(
                    self.source.at[self.toward(step) * 2 + 1 - self.core],
                    self.half.at[step],
                    (self.ctx, self.pair * 2 + 1 - self.core),
                    self.core_sems,
                    step,
                )
            )
            self.copies[-1].start()

    def fold(self, step):
        half = self.half.at[step]
        self.copy(half, half, self.here(), self.core_sems, step).wait_recv()
        mine = self.source[self.toward(step) * 2 + self.core].astype(jnp.float32)
        total = mine + half[...].astype(jnp.float32)
        if step == 0:
            self.out[...] = total
            return
        half[...] = total.astype(half.dtype)
        self.copies.append(
            self.copy(
                half,
                self.room.at[step - 1],
                (self.ctx, self.toward(step) * 2 + self.core),
                self.pair_sems,
                step - 1,
            )
        )
        self.copies[-1].start()

    def over_ctx(self, terms, room, landing, *sems):
        shard = self.pair * 2 + self.core
        copies = []

        def send(source, target, way, sems):
            there = lax.rem(self.ctx + way, self.ctx_size)
            copies.append(self.copy(source(there), target, (there, shard), sems, way - 1))
            copies[-1].start()

        def arrive(target, way, sems):
            self.copy(target, target, self.here(), sems, way - 1).wait_recv()

        terms[...] = self.out[...].astype(terms.dtype)
        for way in range(1, self.ctx_size):
            send(lambda there: terms.at[there], room.at[way - 1], way, sems[0:2])
        total = self.out[self.ctx]
        for way in range(1, self.ctx_size):
            arrive(room.at[way - 1], way, sems[0:2])
            total = total + room[way - 1].astype(jnp.float32)
        landing[self.ctx] = total.astype(landing.dtype)
        for way in range(1, self.ctx_size):
            send(lambda there: landing.at[self.ctx], landing.at[self.ctx], way, sems[2:4])
        for way in range(1, self.ctx_size):
            come = lax.rem(self.ctx + self.ctx_size - way, self.ctx_size)
            arrive(landing.at[come], way, sems[2:4])
        self.out[...] = landing[...].astype(jnp.float32)
        for copy in copies:
            copy.wait_send()

    def finish(self):
        for step in range(1, self.count):
            room = self.room.at[step - 1]
            self.copy(room, room, self.here(), self.pair_sems, step - 1).wait_recv()
            self.out[...] += room[...].astype(jnp.float32)
        if self.last:
            self.over_ctx(*self.last)
        for copy in self.copies:
            copy.wait_send()


def scatter_kernel(arity, ctx_size, pair_count, slot, spread_ctx, lines, *refs):
    sources, refs = refs[:arity], refs[arity:]
    line_sources, refs = refs[:lines], refs[lines:]
    outs, refs = refs[:arity], refs[arity:]
    line_outs, refs = refs[:lines], refs[lines:]
    halves, relays, asides, ends, finals = (refs[i * arity : (i + 1) * arity] for i in range(5))
    sems = refs[5 * arity : 5 * arity + 10]
    core_sems, relay_sems, ctx_sems, pair_sems, last_sems = (sems[2 * i : 2 * i + 2] for i in range(5))
    square, ways = peers_of(ctx_size)
    ctx, pair, core = greet(ctx_size, pair_count, True, False)
    order = list(range(1, pair_count)) + [0]
    started = []
    flows = []
    for item in range(lines):
        at = 5 * arity + 10 + 13 * item
        spread = len(line_sources[item].shape) == 4
        flows.append(
            LineScatter(
                line_sources[item],
                line_outs[item],
                *refs[at : at + 2],
                refs[at + 2 : at + 6],
                (ctx, pair, core),
                (pair_count, ctx_size),
                refs[at + 6 : at + 13] if spread else (),
            )
        )

    def send(source, target, device, pair_of_sems, at):
        copy = pltpu.make_async_remote_copy(
            src_ref=source,
            dst_ref=target,
            send_sem=pair_of_sems[0].at[at],
            recv_sem=pair_of_sems[1].at[at],
            device_id=device,
            device_id_type=MESH_ID,
        )
        copy.start()
        started.append(copy)

    def arrive(target, pair_of_sems, at):
        pltpu.make_async_remote_copy(
            src_ref=target,
            dst_ref=target,
            send_sem=pair_of_sems[0].at[at],
            recv_sem=pair_of_sems[1].at[at],
            device_id=(ctx, pair * 2 + core),
            device_id_type=MESH_ID,
        ).wait_recv()

    def toward(step):
        return lax.rem(pair + step, pair_count)

    def target_ctx(way):
        return ctx_target(ctx, way, square, ctx_size) if way else ctx

    def f32(value):
        return value.astype(jnp.float32)

    far_first = [3, 1, 2, 0] if square else list(ways) + [0]
    for step in order:
        for way in far_first:
            for item in range(arity):
                send(
                    sources[item].at[slot(target_ctx(way), toward(step) * 2 + 1 - core)],
                    halves[item].at[way, step],
                    (ctx, pair * 2 + 1 - core),
                    core_sems,
                    (way, step, item),
                )

    def fold_core(step):
        for way in far_first:
            for item in range(arity):
                half = halves[item].at[way, step]
                arrive(half, core_sems, (way, step, item))
                mine = sources[item][slot(target_ctx(way), toward(step) * 2 + core)]
                half[...] = (f32(mine) + f32(half[...])).astype(half.dtype)
                if square and way == 3:
                    there = ctx ^ (1 if step % 2 == 0 else 2)
                    send(
                        half,
                        relays[item].at[step],
                        (there, pair * 2 + core),
                        relay_sems,
                        (step, item),
                    )

    def fold_relay(step):
        for item in range(arity):
            if square:
                relay = relays[item].at[step]
                arrive(relay, relay_sems, (step, item))
                half = halves[item].at[2 if step % 2 == 0 else 1, step]
                half[...] = (f32(half[...]) + f32(relay[...])).astype(half.dtype)
            for way in ways:
                if square and way == 3:
                    continue
                send(
                    halves[item].at[way, step],
                    asides[item].at[way - 1, step],
                    (target_ctx(way), pair * 2 + core),
                    ctx_sems,
                    (way - 1, step, item),
                )

    def fold_ctx(step):
        for item in range(arity):
            half = halves[item].at[0, step]
            total = f32(half[...])
            for way in ways:
                if square and way == 3:
                    continue
                aside = asides[item].at[way - 1, step]
                arrive(aside, ctx_sems, (way - 1, step, item))
                total = total + f32(aside[...])
            if step:
                half[...] = total.astype(half.dtype)
                send(
                    half,
                    ends[item].at[step - 1],
                    (ctx, toward(step) * 2 + core),
                    pair_sems,
                    (step - 1, item),
                )
            else:
                for other in range(1, pair_count):
                    end = ends[item].at[other - 1]
                    arrive(end, pair_sems, (other - 1, item))
                    total = total + f32(end[...])
                if spread_ctx:
                    finals[item][...] = total.astype(finals[item].dtype)
                else:
                    outs[item][...] = total.astype(outs[item].dtype)

    for flow in flows:
        flow.start()
    for turn in range(pair_count + 2):
        if turn < pair_count:
            fold_core(order[turn])
        if 1 <= turn <= pair_count:
            fold_relay(order[turn - 1])
            for flow in flows:
                flow.fold(order[turn - 1])
        if turn >= 2:
            fold_ctx(order[turn - 2])
    if spread_ctx:
        for item in range(arity):
            for way in ways:
                send(
                    finals[item],
                    outs[item].at[ctx],
                    (target_ctx(way), pair * 2 + core),
                    last_sems,
                    (way - 1, item),
                )
            outs[item][ctx] = finals[item][...]
        for item in range(arity):
            for way in ways:
                arrive(outs[item].at[ctx_source(ctx, way, square, ctx_size)], last_sems, (way - 1, item))
    for flow in flows:
        flow.finish()
    for copy in started:
        copy.wait_send()


def scatter(terms, slot, collective_id, spread_ctx=False, out_dtype=None, lines=()):
    ctx_size, shard_count = lax.axis_size("ctx"), lax.axis_size("fsdp")
    pair_count = shard_count // 2
    arity = len(terms)
    dma = pltpu.SemaphoreType.DMA
    lead = (ctx_size,) if spread_ctx else ()
    asides = 2 if ctx_size == 4 else ctx_size - 1

    def room(*extent):
        return [pltpu.VMEM(extent + term.shape[1:], term.dtype) for term in terms]

    def line_room(line):
        if len(line.shape) == 3:
            return [pltpu.VMEM((8, HD), line.dtype)] * 3 + [dma((1,))] * 4
        cut = line.shape[2:]
        rooms = [pltpu.VMEM((count,) + cut, line.dtype) for count in (ctx_size, ctx_size - 1, ctx_size)]
        return rooms + [dma((ctx_size - 1,))] * 4

    moved = sum(term.size * term.dtype.itemsize for term in terms)
    return pl.pallas_call(
        functools.partial(scatter_kernel, arity, ctx_size, pair_count, slot, spread_ctx, len(lines)),
        in_specs=[pl.BlockSpec(memory_space=pltpu.VMEM)] * (arity + len(lines)),
        out_specs=[pl.BlockSpec(memory_space=pltpu.VMEM)] * (arity + len(lines)),
        out_shape=[
            jax.ShapeDtypeStruct(lead + term.shape[1:], out_dtype or term.dtype) for term in terms
        ]
        + [jax.ShapeDtypeStruct(line.shape[1:], jnp.float32) for line in lines],
        scratch_shapes=room(ctx_size, pair_count)
        + room(pair_count)
        + room(asides, pair_count)
        + room(pair_count - 1)
        + room()
        + [dma((ctx_size, pair_count, arity))] * 2
        + [dma((pair_count, arity))] * 2
        + [dma((ctx_size - 1, pair_count, arity))] * 2
        + [dma((pair_count - 1, arity))] * 2
        + [dma((ctx_size - 1, arity))] * 2
        + [
            scratch
            for line in lines
            for scratch in [
                pltpu.VMEM((pair_count,) + line.shape[1:], line.dtype),
                pltpu.VMEM((pair_count - 1,) + line.shape[1:], line.dtype),
            ]
            + [dma((pair_count,))] * 4
            + line_room(line)
        ],
        compiler_params=pltpu.CompilerParams(
            collective_id=collective_id, has_side_effects=True, vmem_limit_bytes=63 * 2**20
        ),
        cost_estimate=pl.CostEstimate(flops=0, bytes_accessed=moved * 16, transcendentals=0),
    )(*terms, *lines)


class CtxScatter:
    def __init__(self, source, out, relay, sums, asides, sems, where, ctx_size):
        self.source, self.out, self.relay, self.sums, self.asides = source, out, relay, sums, asides
        self.relay_sems, self.aside_sems = sems[0:2], sems[2:4]
        self.ctx, self.pair, self.core = where
        self.ctx_size = ctx_size
        self.square, ways = peers_of(ctx_size)
        self.near = [way for way in ways if not (self.square and way == 3)]
        self.parts = range(source.shape[1])
        self.copies = []

    def copy(self, source, target, ctx, sems, at):
        return pltpu.make_async_remote_copy(
            src_ref=source,
            dst_ref=target,
            send_sem=sems[0].at[at],
            recv_sem=sems[1].at[at],
            device_id=(ctx, self.pair * 2 + self.core),
            device_id_type=MESH_ID,
        )

    def send(self, *what):
        self.copies.append(self.copy(*what))
        self.copies[-1].start()

    def arrive(self, target, sems, at):
        self.copy(target, target, self.ctx, sems, at).wait_recv()

    def start(self):
        for part in self.parts if self.square else ():
            there = self.ctx ^ (1 if part % 2 == 0 else 2)
            self.send(
                self.source.at[self.ctx ^ 3, part], self.relay.at[part], there, self.relay_sems, part
            )

    def advance(self, part):
        for way in self.near:
            there = ctx_target(self.ctx, way, self.square, self.ctx_size)
            source = self.source.at[there, part]
            if self.square and (part % 2 == 0) == (way == 2):
                self.arrive(self.relay.at[part], self.relay_sems, part)
                total = source[...].astype(jnp.float32) + self.relay[part].astype(jnp.float32)
                self.sums[part] = total.astype(self.sums.dtype)
                source = self.sums.at[part]
            self.send(source, self.asides.at[way - 1, part], there, self.aside_sems, (way - 1, part))

    def close(self, part):
        total = self.source[self.ctx, part].astype(jnp.float32)
        for way in self.near:
            aside = self.asides.at[way - 1, part]
            self.arrive(aside, self.aside_sems, (way - 1, part))
            total = total + aside[...].astype(jnp.float32)
        self.out[part] = total.astype(self.out.dtype)

    def finish(self):
        for copy in self.copies:
            copy.wait_send()


def sum_tokens_kernel(pair_count, ctx_size, tokens, rows, tokens_out, rows_out, half, room, relay, sums, asides, *sems):
    where = greet(ctx_size, pair_count, True, False)
    line = LineScatter(tokens, tokens_out, half, room, sems[:4], where, (pair_count, 1), ())
    square = CtxScatter(rows, rows_out, relay, sums, asides, sems[4:], where, ctx_size)
    line.start()
    square.start()
    for step in line.order:
        line.fold(step)
    late = 2
    for part in range(rows.shape[1] + late):
        if part < rows.shape[1]:
            square.advance(part)
        if part >= late:
            square.close(part - late)
    line.finish()
    square.finish()


def sum_tokens(tokens, rows, collective_id):
    ctx_size, pair_count = lax.axis_size("ctx"), lax.axis_size("fsdp") // 2
    vmem = pl.BlockSpec(memory_space=pltpu.VMEM)
    extent, piece, parts = tokens.shape[1:], rows.shape[2:], rows.shape[1]
    asides = 2 if ctx_size == 4 else ctx_size - 1
    dma = pltpu.SemaphoreType.DMA
    return pl.pallas_call(
        functools.partial(sum_tokens_kernel, pair_count, ctx_size),
        in_specs=[vmem, vmem],
        out_specs=[vmem, vmem],
        out_shape=[
            jax.ShapeDtypeStruct(extent, jnp.float32),
            jax.ShapeDtypeStruct((parts,) + piece, rows.dtype),
        ],
        scratch_shapes=[
            pltpu.VMEM((pair_count,) + extent, tokens.dtype),
            pltpu.VMEM((pair_count - 1,) + extent, tokens.dtype),
            pltpu.VMEM((parts,) + piece, rows.dtype),
            pltpu.VMEM((parts,) + piece, rows.dtype),
            pltpu.VMEM((asides, parts) + piece, rows.dtype),
        ]
        + [dma((pair_count,))] * 4
        + [dma((parts,))] * 2
        + [dma((asides, parts))] * 2,
        compiler_params=pltpu.CompilerParams(
            collective_id=collective_id, has_side_effects=True, vmem_limit_bytes=63 * 2**20
        ),
        cost_estimate=pl.CostEstimate(flops=0, bytes_accessed=tokens.size * 32, transcendentals=0),
    )(tokens, rows)


def turned(values, cosine, signed_sine):
    return values * cosine + pltpu.roll(values, HD // 2, 1) * signed_sine


def turned_back(grads, cosine, signed_sine):
    return grads * cosine + pltpu.roll(grads * signed_sine, HD // 2, 1)


def slot_of(index):
    return index % SEQS, index // SEQS


def key_column(index, group, part):
    seq, half = slot_of(index)
    return (((seq * KVH + group) * 2 + half) * 2 + part) * HD


def project_kernel(rows, x_ref, gain_ref, w_hbm, bias_ref, cos_ref, sin_ref, normed_ref, q_ref, kv_ref, w_ref, q_acc, sems):
    wide = w_ref.shape[2]
    copies = []
    for part in range(w_ref.shape[0]):
        copy = pltpu.make_async_copy(
            w_hbm.at[:, part * wide : (part + 1) * wide], w_ref.at[part], sems.at[part]
        )
        copy.start()
        copies.append(copy)
    values = x_ref[...].astype(jnp.float32)
    scale = lax.rsqrt(jnp.mean(values * values, -1, keepdims=True) + EPS)
    normed = (values * scale * gain_ref[...]).astype(jnp.bfloat16)
    normed_ref[...] = normed
    cosine, sine = cos_ref[...], sin_ref[...]
    for part, copy in enumerate(copies):
        copy.wait()
        columns = jnp.dot(normed, w_ref[part], preferred_element_type=jnp.float32)
        columns = columns + bias_ref[:, part * wide : (part + 1) * wide]
        for index in range(wide // HD):
            head = part * (wide // HD) + index
            piece = columns[:, index * HD : (index + 1) * HD]
            if head < H + KVH:
                piece = turned(piece, cosine, sine)
            if head < H:
                piece = piece * (HD**-0.5)
            for slot in range(2 * SEQS):
                seq, half = slot_of(slot)
                own = piece[slot * rows : (slot + 1) * rows]
                if head < H:
                    group, member = head // (H // KVH), head % (H // KVH)
                    q_acc[seq, half, group, member * rows : (member + 1) * rows] = own
                else:
                    group, kind = (head - H) % KVH, (head - H) // KVH
                    at = key_column(slot, group, kind)
                    kv_ref[:, at : at + HD] = own.astype(jnp.bfloat16)
    q_ref[...] = q_acc[...].astype(jnp.bfloat16)


def project(tokens, gain, weight, bias, cosine, signed_sine, rows):
    vmem = pl.BlockSpec(memory_space=pltpu.VMEM)
    parts = 8
    grouped = (SEQS, 2, KVH, H // KVH * rows, HD)
    return pl.pallas_call(
        functools.partial(project_kernel, rows),
        in_specs=[vmem, vmem, pl.BlockSpec(memory_space=pl.ANY), vmem, vmem, vmem],
        out_specs=[vmem, vmem, vmem],
        out_shape=[
            jax.ShapeDtypeStruct(tokens.shape, jnp.bfloat16),
            jax.ShapeDtypeStruct(grouped, jnp.bfloat16),
            jax.ShapeDtypeStruct((rows, SEQS * KVH * 4 * HD), jnp.bfloat16),
        ],
        scratch_shapes=[
            pltpu.VMEM((parts, D, QKV // parts), jnp.bfloat16),
            pltpu.VMEM(grouped, jnp.float32),
            pltpu.SemaphoreType.DMA((parts,)),
        ],
        compiler_params=pltpu.CompilerParams(vmem_limit_bytes=40 * 2**20),
        cost_estimate=pl.CostEstimate(
            flops=2 * tokens.shape[0] * D * QKV, bytes_accessed=2 * D * QKV, transcendentals=0
        ),
        name="project",
    )(tokens, gain.reshape(1, -1), weight, bias.reshape(1, -1), cosine, signed_sine)


def unproject_kernel(rows, gq_ref, gkv_ref, cos_ref, sin_ref, w_hbm, x_ref, gain_ref, past_ref, gp_ref, gi_ref, gg_ref, gb_ref, w_ref, gp_acc, sem):
    copy = pltpu.make_async_copy(w_hbm, w_ref, sem)
    copy.start()
    cosine, sine = cos_ref[...], sin_ref[...]

    def rounded(values):
        return values.astype(jnp.bfloat16).astype(jnp.float32)

    for head in range(H + 2 * KVH):
        for slot in range(2 * SEQS):
            seq, half = slot_of(slot)
            at = slice(slot * rows, (slot + 1) * rows)
            if head < H:
                group, member = head // (H // KVH), head % (H // KVH)
                grad = gq_ref[seq, half, group, member * rows : (member + 1) * rows]
                grad = rounded(grad) * (HD**-0.5)
            else:
                group, kind = (head - H) % KVH, (head - H) // KVH
                column = key_column(slot, group, kind)
                grad = rounded(gkv_ref[:, column : column + HD])
            if head < H + KVH:
                grad = turned_back(grad, cosine[at], sine[at])
            gp_acc[at, head * HD : (head + 1) * HD] = grad
    low = gp_acc[...].astype(jnp.bfloat16)
    gp_ref[...] = low
    gb_ref[...] = jnp.sum(low.astype(jnp.float32), 0, keepdims=True)
    values = x_ref[...].astype(jnp.float32)
    scale = lax.rsqrt(jnp.mean(values * values, -1, keepdims=True) + EPS)
    unit = values * scale
    copy.wait()
    grad_normed = lax.dot_general(low, w_ref[...], CONTRACT_LAST, preferred_element_type=jnp.float32)
    gg_ref[...] = jnp.sum(grad_normed * unit, 0, keepdims=True)
    grad_unit = grad_normed * gain_ref[...]
    inner = jnp.mean(grad_unit * unit, -1, keepdims=True)
    gi_ref[...] = past_ref[...] + scale * (grad_unit - unit * inner)


def unproject(grad_queries, grad_kv, cosine, signed_sine, weight, tokens, gain, past, rows):
    vmem = pl.BlockSpec(memory_space=pltpu.VMEM)
    return pl.pallas_call(
        functools.partial(unproject_kernel, rows),
        in_specs=[vmem, vmem, vmem, vmem, pl.BlockSpec(memory_space=pl.ANY), vmem, vmem, vmem],
        out_specs=[vmem] * 4,
        out_shape=[
            jax.ShapeDtypeStruct((tokens.shape[0], QKV), jnp.bfloat16),
            jax.ShapeDtypeStruct(tokens.shape, jnp.float32),
            jax.ShapeDtypeStruct((1, D), jnp.float32),
            jax.ShapeDtypeStruct((1, QKV), jnp.float32),
        ],
        scratch_shapes=[
            pltpu.VMEM((D, QKV), jnp.bfloat16),
            pltpu.VMEM((tokens.shape[0], QKV), jnp.float32),
            pltpu.SemaphoreType.DMA,
        ],
        compiler_params=pltpu.CompilerParams(vmem_limit_bytes=40 * 2**20),
        cost_estimate=pl.CostEstimate(
            flops=2 * tokens.shape[0] * D * QKV, bytes_accessed=2 * D * QKV, transcendentals=0
        ),
        name="unproject",
    )(grad_queries, grad_kv, cosine, signed_sine, weight, tokens, gain.reshape(1, -1), past)


def pack_kernel(columns, gate_ref, up_ref, out_ref):
    width = out_ref.shape[2] // 2
    cut = out_ref.shape[1]
    for there in range(out_ref.shape[0]):
        for side, ref in enumerate((gate_ref, up_ref)):
            at = side * width
            out_ref[there, :, at + width - HD : at + width] = jnp.zeros((cut, HD), out_ref.dtype)
            out_ref[there, :, at : at + columns] = ref[:, there * columns : (there + 1) * columns]


def pack(gate, up, shard_count, columns, width):
    return pl.pallas_call(
        functools.partial(pack_kernel, columns),
        in_specs=[pl.BlockSpec(memory_space=pltpu.VMEM)] * 2,
        out_specs=pl.BlockSpec(memory_space=pltpu.VMEM),
        out_shape=jax.ShapeDtypeStruct((shard_count, gate.shape[0], 2 * width), gate.dtype),
        name="pack",
    )(gate, up)


def unpack_kernel(columns, in_ref, gate_ref, up_ref):
    width = in_ref.shape[3] // 2
    for there in range(in_ref.shape[1]):
        for side, ref in enumerate((gate_ref, up_ref)):
            part = in_ref[0, there, :, side * width : side * width + columns]
            ref[0, :, there * columns : (there + 1) * columns] = part.astype(jnp.float32)


def unpack(rows, columns):
    ctx_size, shard_count, cut, _ = rows.shape
    out = jax.ShapeDtypeStruct((ctx_size, cut, shard_count * columns), jnp.float32)
    return pl.pallas_call(
        functools.partial(unpack_kernel, columns),
        grid=(ctx_size,),
        in_specs=[pl.BlockSpec((1,) + rows.shape[1:], lambda c: (c, 0, 0, 0))],
        out_specs=[pl.BlockSpec((1, cut, shard_count * columns), lambda c: (c, 0, 0))] * 2,
        out_shape=[out, out],
        name="unpack",
    )(rows)


def shards(
    layer_input,
    block_order,
    first_gain,
    w_qkv,
    b_qkv,
    w_o,
    second_gain,
    w_gate,
    w_up,
    w_down,
    cotangent,
):
    ctx_size = lax.axis_size("ctx")
    shard_count = lax.axis_size("fsdp")
    own_ctx = lax.axis_index("ctx")
    own_shard = lax.axis_index("fsdp")
    rows_here = layer_input.shape[0]
    block_rows = rows_here * shard_count
    cut = D // (ctx_size * shard_count)
    columns = FF // shard_count
    cosine, signed_sine = turn_tables(
        block_order, own_ctx, ctx_size, block_rows, own_shard * rows_here, rows_here
    )
    tokens = by_slot(layer_input)
    grad_out = by_slot(cotangent)

    def by_rows(ctx, shard):
        return shard * ctx_size + ctx

    def by_tokens(ctx, shard):
        return ctx * shard_count + shard

    def own_cut(weight):
        return lax.dynamic_slice_in_dim(weight, own_ctx * cut, cut, 0)

    def mix_features(values):
        shaped = values.reshape(-1, shard_count, ctx_size, cut)
        return shaped.transpose(0, 2, 1, 3).reshape(-1, D)

    def unmix_features(values):
        shaped = values.reshape(-1, ctx_size, shard_count, cut)
        return shaped.transpose(0, 2, 1, 3).reshape(-1, D)

    small = jnp.concatenate([b_qkv, first_gain, second_gain]).reshape(ctx_size, -1)
    small_width = small.shape[1]
    small = lax.dynamic_slice_in_dim(small, own_ctx, 1, 0)
    small = jnp.pad(small, ((0, 0), (0, 16 * HD - small_width))).reshape(16, HD)
    width = -(-columns // HD) * HD
    w_qkv_all, small_all, gate_up_cut = gather(
        [own_cut(w_qkv), small],
        [by_rows, by_rows],
        1,
        swaps=[pack(own_cut(w_gate), own_cut(w_up), shard_count, columns, width)],
    )
    w_qkv_all = w_qkv_all.reshape(D, QKV)
    small_all = small_all.reshape(shard_count, ctx_size, -1)[:, :, :small_width]
    small_all = small_all.reshape(shard_count, -1).astype(jnp.float32)
    bias_width = QKV // shard_count
    gain_width = D // shard_count
    bias_all = small_all[:, :bias_width].reshape(-1)
    gain_one = small_all[:, bias_width : bias_width + gain_width].reshape(-1)
    gain_two = small_all[:, bias_width + gain_width :].reshape(-1)

    down_padded = jnp.pad(w_down, ((0, width - columns), (0, 0)))

    late_grad_out, w_qkv_all = lax.optimization_barrier((grad_out, w_qkv_all))
    cotangent_all = lax.all_gather(late_grad_out, "fsdp", axis=0, tiled=True)
    normed_one, queries, own_kv = project(
        tokens, gain_one, w_qkv_all, bias_all, cosine, signed_sine, rows_here
    )
    all_kv, w_o_all = gather([own_kv, own_cut(w_o)], [by_tokens, by_rows], 2)
    w_o_all = w_o_all.reshape(D, D)
    gate_up_cut, all_kv = lax.optimization_barrier((gate_up_cut, all_kv))
    gate_up_cols = lax.all_gather(
        gate_up_cut.reshape(shard_count * cut, 2 * width), "ctx", axis=0, tiled=True
    )
    all_kv = all_kv.reshape(-1, SEQS * KVH * 4 * HD)
    scalars = jnp.concatenate(
        [block_order.reshape(-1), jnp.stack([own_ctx, own_shard]).astype(jnp.int32)]
    )
    attended_grouped, stats = attend_forward(
        scalars, queries, all_kv, ctx_size, block_rows, rows_here
    )
    attended_low = from_groups(attended_grouped, rows_here).astype(jnp.bfloat16)
    middle = tokens.astype(jnp.float32) + jnp.dot(attended_low, w_o_all, preferred_element_type=jnp.float32)
    unit_two, scale_two, normed = normalize(middle, gain_two)
    normed_two = mix_features(normed.astype(jnp.bfloat16))

    (tokens_all,) = gather([normed_two], [lambda ctx, shard: shard], 6, wide=())
    tokens_all = tokens_all.reshape(-1, D)
    gate_up_part = jnp.dot(tokens_all, gate_up_cols, preferred_element_type=jnp.float32)
    gate_part, up_part = gate_up_part[:, :width], gate_up_part[:, width:]
    sigmoid_gate = jax.nn.sigmoid(gate_part)
    activated = gate_part * sigmoid_gate
    hidden = (activated * up_part).astype(jnp.bfloat16)
    grad_hidden = lax.dot_general(
        cotangent_all, down_padded, CONTRACT_LAST, preferred_element_type=jnp.float32
    )
    grad_gate = grad_hidden * up_part * sigmoid_gate * (1.0 + gate_part * (1.0 - sigmoid_gate))
    grad_gate_up = jnp.concatenate([grad_gate, grad_hidden * activated], -1).astype(jnp.bfloat16)
    down_terms = lax.dot_general(
        hidden, cotangent_all, CONTRACT_FIRST, preferred_element_type=jnp.float32
    ).astype(jnp.bfloat16)
    down_rows = lax.psum(down_terms, "ctx")
    grad_gate_up, hidden, down_terms = lax.optimization_barrier(
        (grad_gate_up, hidden, down_terms)
    )
    gate_up_terms = lax.dot_general(
        tokens_all, grad_gate_up, CONTRACT_FIRST, preferred_element_type=jnp.float32
    ).astype(jnp.bfloat16)
    grad_tokens = lax.dot_general(
        grad_gate_up, gate_up_cols, CONTRACT_LAST, preferred_element_type=jnp.float32
    ).astype(jnp.bfloat16)
    grad_normed_two, gate_up_rows = sum_tokens(
        grad_tokens.reshape(shard_count, -1, D),
        gate_up_terms.reshape(ctx_size, shard_count, cut, 2 * width),
        7,
    )
    grad_normed_two, hidden = lax.optimization_barrier((grad_normed_two, hidden))
    mixed_terms = jnp.dot(hidden, down_padded, preferred_element_type=jnp.float32).astype(jnp.bfloat16)
    grad_normed_two, mixed_terms = lax.optimization_barrier((grad_normed_two, mixed_terms))
    grad_normed_two = unmix_features(grad_normed_two)
    grad_middle_norm, grad_gain_two = norm_back(grad_normed_two, unit_two, scale_two, gain_two)
    grad_middle = grad_out.astype(jnp.float32) + grad_middle_norm
    grad_branch_one = grad_middle.astype(jnp.bfloat16)
    grad_attended = lax.dot_general(
        grad_branch_one, w_o_all, CONTRACT_LAST, preferred_element_type=jnp.float32
    ).astype(jnp.bfloat16)
    gate_up_rows, grad_attended = lax.optimization_barrier((gate_up_rows, grad_attended))
    gate_up_rows = exchange(gate_up_rows, 5)
    gate_up_rows, grad_attended = lax.optimization_barrier((gate_up_rows, grad_attended))
    gate_up_rows = lax.all_gather(gate_up_rows, "ctx", axis=0, tiled=False)
    o_terms = lax.dot_general(
        attended_low, grad_branch_one, CONTRACT_FIRST, preferred_element_type=jnp.float32
    ).astype(jnp.bfloat16)
    grad_queries, grad_kv_full = attend_backward(
        scalars,
        queries,
        to_groups(grad_attended, rows_here),
        attended_grouped,
        stats,
        all_kv,
        ctx_size,
        block_rows,
        rows_here,
    )
    (grad_kv,) = scatter(
        [grad_kv_full.reshape(-1, rows_here, SEQS * KVH * 4 * HD)],
        by_tokens,
        3,
        out_dtype=jnp.float32,
    )
    mixed_terms, grad_kv = lax.optimization_barrier((mixed_terms, grad_kv))
    mixed_rows = lax.psum_scatter(mixed_terms, "fsdp", scatter_dimension=0, tiled=True)
    grad_projected, grad_input, grad_gain_one, grad_bias = unproject(
        grad_queries,
        grad_kv,
        cosine,
        signed_sine,
        w_qkv_all,
        tokens,
        gain_one,
        grad_middle,
        rows_here,
    )
    grad_input = from_slot(grad_input, rows_here)
    grad_bias = grad_bias.reshape(-1)
    qkv_terms = lax.dot_general(
        normed_one, grad_projected, CONTRACT_FIRST, preferred_element_type=jnp.float32
    ).astype(jnp.bfloat16)
    small_terms = jnp.concatenate(
        [
            part.reshape(shard_count, -1)
            for part in (grad_gain_one, grad_gain_two, grad_bias[:QK], grad_bias[QK:])
        ],
        1,
    )
    small_terms = small_terms.reshape(ctx_size * shard_count, small_width)
    small_terms = jnp.pad(small_terms, ((0, 0), (0, 8 * HD - small_width)))
    qkv_rows, o_rows, small_rows = scatter(
        [
            qkv_terms.reshape(-1, cut, QKV),
            o_terms.reshape(-1, cut, D),
            small_terms.reshape(-1, 8, HD),
        ],
        by_rows,
        4,
        spread_ctx=True,
    )
    mixed_out = middle + mixed_rows.astype(jnp.float32)
    output = from_slot(mixed_out.astype(jnp.bfloat16), rows_here)
    small_rows = small_rows.reshape(ctx_size, -1)[:, :small_width].reshape(-1)
    bias_start = 2 * gain_width
    value_start = bias_start + QK // shard_count

    gate_rows, up_rows = unpack(gate_up_rows, columns)
    return (
        output,
        grad_input,
        small_rows[:gain_width],
        qkv_rows.reshape(-1, QKV).astype(jnp.float32),
        small_rows[bias_start:value_start],
        small_rows[value_start:],
        o_rows.reshape(-1, D).astype(jnp.float32),
        small_rows[gain_width:bias_start],
        gate_rows.reshape(-1, FF),
        up_rows.reshape(-1, FF),
        down_rows[:columns].astype(jnp.float32),
    )


def solution(mesh):
    in_specs = (
        P(("ctx", "fsdp"), None, None),
        P(),
        P("fsdp"),
        P("fsdp", None),
        P("fsdp"),
        P("fsdp", None),
        P("fsdp"),
        P("fsdp", None),
        P("fsdp", None),
        P("fsdp", None),
        P(("ctx", "fsdp"), None, None),
    )
    out_specs = (
        P(("ctx", "fsdp"), None, None),
        P(("ctx", "fsdp"), None, None),
        P("fsdp"),
        P("fsdp", None),
        P("fsdp"),
        P("fsdp"),
        P("fsdp", None),
        P("fsdp"),
        P("fsdp", None),
        P("fsdp", None),
        P("fsdp", None),
    )
    return jax.shard_map(shards, mesh=mesh, in_specs=in_specs, out_specs=out_specs, check_vma=False)
```

```python
import functools

import jax
import jax.numpy as jnp
from jax import lax
from jax.experimental import pallas as pl
from jax.experimental.pallas import tpu as pltpu
from jax.sharding import PartitionSpec as P

D = 1536
H = 12
KVH = 2
HD = 128
FF = 8960
SEQS = 2
QKV = 2048
QK = 1792


EPS = 1e-06
THETA = 1000000.0
NEG_FILL = -1e30
MESH_ID = pl.DeviceIdType.MESH
CONTRACT_LAST = (((1,), (1,)), ((), ()))
CONTRACT_FIRST = (((0,), (0,)), ((), ()))


def by_slot(tokens):
    return tokens.transpose(1, 0, 2).reshape(-1, tokens.shape[2])


def from_slot(tokens, row_count):
    return tokens.reshape(2 * SEQS, row_count, -1).transpose(1, 0, 2)


def to_groups(tokens, row_count):
    shaped = tokens.reshape(2, SEQS, row_count, KVH, H // KVH, HD)
    return shaped.transpose(1, 0, 3, 4, 2, 5).reshape(SEQS, 2, KVH, H // KVH * row_count, HD)


def from_groups(grouped, row_count):
    shaped = grouped.reshape(SEQS, 2, KVH, H // KVH, row_count, HD).transpose(1, 0, 4, 2, 3, 5)
    return shaped.reshape(row_count * 2 * SEQS, H * HD)


def turn_tables(block_order, own_ctx, ctx_size, block_rows, first_row, row_count):
    half_width = HD // 2
    frequency = THETA ** (-jnp.arange(half_width, dtype=jnp.float32) * 2.0 / HD)
    frequency = jnp.tile(frequency, 2)[None, :]
    order = lax.dynamic_index_in_dim(block_order.reshape(SEQS, 2, ctx_size), own_ctx, 2, False)
    start = (order.T.reshape(-1) * block_rows + first_row).astype(jnp.float32)
    far = start[:, None] * frequency
    near = jnp.arange(row_count, dtype=jnp.float32)[:, None] * frequency
    far_cos, far_sin = jnp.cos(far)[:, None, :], jnp.sin(far)[:, None, :]
    near_cos, near_sin = jnp.cos(near)[None], jnp.sin(near)[None]
    sign = jnp.where(jnp.arange(HD) < half_width, -1.0, 1.0).astype(jnp.float32)
    cosine = far_cos * near_cos - far_sin * near_sin
    sine = (far_sin * near_cos + far_cos * near_sin) * sign
    return cosine.reshape(-1, HD), sine.reshape(-1, HD)


def normalize(values, gain):
    scale = lax.rsqrt(jnp.mean(values * values, -1, keepdims=True) + EPS)
    unit = values * scale
    return (unit, scale, unit * gain)


def norm_back(grad_out, unit, scale, gain):
    grad_unit = grad_out * gain
    inner = jnp.mean(grad_unit * unit, -1, keepdims=True)
    return (scale * (grad_unit - unit * inner), jnp.sum(grad_out * unit, 0))


def hidden_rows(scores, own_shard, rows_here):
    row = lax.broadcasted_iota(jnp.int32, scores.shape, 0)
    lane = lax.broadcasted_iota(jnp.int32, scores.shape, 1)
    return row > own_shard * rows_here + lax.rem(lane, rows_here)


def key_part(group, half_key, part):
    at = ((group * 2 + half_key) * 2 + part) * HD
    return slice(at, at + HD)


def attend_forward_kernel(ctx_size, block_rows, rows_here, scalars, q_ref, kv_ref, out_ref, stat_ref, best_ref, total_ref, accum_ref):
    seq = pl.program_id(0)
    blocks = 2 * ctx_size
    own_ctx = scalars[SEQS * blocks]
    own_shard = scalars[SEQS * blocks + 1]
    groups = range(KVH)
    best_ref[...] = jnp.full(best_ref.shape, NEG_FILL, jnp.float32)
    total_ref[...] = jnp.zeros(total_ref.shape, jnp.float32)
    accum_ref[...] = jnp.zeros(accum_ref.shape, jnp.float32)

    def step(key_ctx, half_key, half):
        order_key = scalars[seq * blocks + half_key * ctx_size + key_ctx]
        order_query = scalars[seq * blocks + half * ctx_size + own_ctx]

        def work(masked):
            rows = pl.ds(pl.multiple_of(key_ctx * block_rows, block_rows), block_rows)
            scores = [
                lax.dot_general(
                    kv_ref[rows, key_part(group, half_key, 0)],
                    q_ref[0, half, group],
                    CONTRACT_LAST,
                    preferred_element_type=jnp.float32,
                )
                for group in groups
            ]
            if masked:
                hidden = hidden_rows(scores[0], own_shard, rows_here)
                scores = [jnp.where(hidden, NEG_FILL, score) for score in scores]
            best = [best_ref[half, group] for group in groups]
            fresh = [
                jnp.maximum(best[group], jnp.max(scores[group], 0, keepdims=True)) for group in groups
            ]
            weights = [jnp.exp(scores[group] - fresh[group]) for group in groups]
            decay = [jnp.exp(best[group] - fresh[group]) for group in groups]
            added = [
                lax.dot_general(
                    kv_ref[rows, key_part(group, half_key, 1)],
                    weights[group].astype(jnp.bfloat16),
                    CONTRACT_FIRST,
                    preferred_element_type=jnp.float32,
                )
                for group in groups
            ]
            for group in groups:
                total_ref[half, group] = total_ref[half, group] * decay[group] + jnp.sum(
                    weights[group], 0, keepdims=True
                )
                accum_ref[half, group] = accum_ref[half, group] * decay[group] + added[group]
                best_ref[half, group] = fresh[group]

        @pl.when(order_key < order_query)
        def full():
            work(False)

        @pl.when(order_key == order_query)
        def diagonal():
            work(True)

    @pl.loop(0, ctx_size)
    def sweep(key_ctx):
        for half_key in range(2):
            for half in range(2):
                step(key_ctx, half_key, half)

    for half in range(2):
        for group in groups:
            totals = total_ref[half, group]
            out_ref[0, half, group] = (accum_ref[half, group] / totals).T
            stat_ref[0, half, group] = best_ref[half, group] + jnp.log(totals)


def group_blocks(lanes, key_rows):
    group = pl.BlockSpec((1, 2, KVH, lanes, HD), lambda s, _: (s, 0, 0, 0, 0))
    stat = pl.BlockSpec((1, 2, KVH, 1, lanes), lambda s, _: (s, 0, 0, 0, 0))
    keys = pl.BlockSpec((key_rows, KVH * 4 * HD), lambda s, _: (0, s))
    return group, stat, keys


def attend_forward(scalars, queries, all_kv, ctx_size, block_rows, rows_here):
    lanes = queries.shape[3]
    kernel = functools.partial(attend_forward_kernel, ctx_size, block_rows, rows_here)
    group, stat, keys = group_blocks(lanes, all_kv.shape[0])
    return pl.pallas_call(
        kernel,
        grid_spec=pltpu.PrefetchScalarGridSpec(
            num_scalar_prefetch=1,
            grid=(SEQS,),
            in_specs=[group, keys],
            out_specs=[group, stat],
            scratch_shapes=[
                pltpu.VMEM((2, KVH, 1, lanes), jnp.float32),
                pltpu.VMEM((2, KVH, 1, lanes), jnp.float32),
                pltpu.VMEM((2, KVH, HD, lanes), jnp.float32),
            ],
        ),
        out_shape=(
            jax.ShapeDtypeStruct(queries.shape, jnp.float32),
            jax.ShapeDtypeStruct((SEQS, 2, KVH, 1, lanes), jnp.float32),
        ),
        compiler_params=pltpu.CompilerParams(vmem_limit_bytes=60 * 2**20),
        name="attend_forward",
    )(scalars, queries, all_kv)


def attend_backward_kernel(ctx_size, block_rows, rows_here, scalars, q_ref, go_ref, att_ref, stat_ref, kv_ref, gq_ref, gkv_ref, delta_ref, gq_acc, gk_acc, gv_acc):
    seq = pl.program_id(0)
    blocks = 2 * ctx_size
    own_ctx = scalars[SEQS * blocks]
    own_shard = scalars[SEQS * blocks + 1]
    groups = range(KVH)
    gq_acc[...] = jnp.zeros(gq_acc.shape, jnp.float32)
    for half in range(2):
        for group in groups:
            product = go_ref[0, half, group].astype(jnp.float32) * att_ref[0, half, group]
            delta_ref[half, group] = jnp.sum(product.T, 0, keepdims=True)

    def step(key_ctx, half_key, half):
        order_key = scalars[seq * blocks + half_key * ctx_size + key_ctx]
        order_query = scalars[seq * blocks + half * ctx_size + own_ctx]

        def work(masked):
            rows = pl.ds(pl.multiple_of(key_ctx * block_rows, block_rows), block_rows)
            keys = [kv_ref[rows, key_part(group, half_key, 0)] for group in groups]
            queries = [q_ref[0, half, group] for group in groups]
            grad_out = [go_ref[0, half, group] for group in groups]
            scores = [
                lax.dot_general(
                    keys[group], queries[group], CONTRACT_LAST, preferred_element_type=jnp.float32
                )
                for group in groups
            ]
            grad_probs = [
                lax.dot_general(
                    kv_ref[rows, key_part(group, half_key, 1)],
                    grad_out[group],
                    CONTRACT_LAST,
                    preferred_element_type=jnp.float32,
                )
                for group in groups
            ]
            probs = [jnp.exp(scores[group] - stat_ref[0, half, group]) for group in groups]
            if masked:
                hidden = hidden_rows(scores[0], own_shard, rows_here)
                probs = [jnp.where(hidden, 0.0, prob) for prob in probs]
            grad_scores = [
                (probs[group] * (grad_probs[group] - delta_ref[half, group])).astype(jnp.bfloat16)
                for group in groups
            ]
            for group in groups:
                gv_acc[group] += jnp.dot(
                    probs[group].astype(jnp.bfloat16),
                    grad_out[group],
                    preferred_element_type=jnp.float32,
                )
                gk_acc[group] += jnp.dot(
                    grad_scores[group], queries[group], preferred_element_type=jnp.float32
                )
                gq_acc[half, group] += lax.dot_general(
                    keys[group], grad_scores[group], CONTRACT_FIRST, preferred_element_type=jnp.float32
                )

        @pl.when(order_key < order_query)
        def full():
            work(False)

        @pl.when(order_key == order_query)
        def diagonal():
            work(True)

    @pl.loop(0, ctx_size)
    def sweep(key_ctx):
        rows = pl.ds(pl.multiple_of(key_ctx * block_rows, block_rows), block_rows)
        for half_key in range(2):
            gk_acc[...] = jnp.zeros(gk_acc.shape, jnp.float32)
            gv_acc[...] = jnp.zeros(gv_acc.shape, jnp.float32)
            for half in range(2):
                step(key_ctx, half_key, half)
            for group in groups:
                gkv_ref[rows, key_part(group, half_key, 0)] = gk_acc[group].astype(jnp.bfloat16)
                gkv_ref[rows, key_part(group, half_key, 1)] = gv_acc[group].astype(jnp.bfloat16)

    for half in range(2):
        for group in groups:
            gq_ref[0, half, group] = gq_acc[half, group].T


def attend_backward(scalars, queries, grad_out, attended, stats, all_kv, ctx_size, block_rows, rows_here):
    lanes = queries.shape[3]
    kernel = functools.partial(attend_backward_kernel, ctx_size, block_rows, rows_here)
    group, stat, keys = group_blocks(lanes, all_kv.shape[0])
    return pl.pallas_call(
        kernel,
        grid_spec=pltpu.PrefetchScalarGridSpec(
            num_scalar_prefetch=1,
            grid=(SEQS,),
            in_specs=[group, group, group, stat, keys],
            out_specs=[group, keys],
            scratch_shapes=[
                pltpu.VMEM((2, KVH, 1, lanes), jnp.float32),
                pltpu.VMEM((2, KVH, HD, lanes), jnp.float32),
                pltpu.VMEM((KVH, block_rows, HD), jnp.float32),
                pltpu.VMEM((KVH, block_rows, HD), jnp.float32),
            ],
        ),
        out_shape=(
            jax.ShapeDtypeStruct(queries.shape, jnp.float32),
            jax.ShapeDtypeStruct(all_kv.shape, jnp.bfloat16),
        ),
        compiler_params=pltpu.CompilerParams(vmem_limit_bytes=60 * 2**20),
        name="attend_backward",
    )(scalars, queries, grad_out, attended, stats, all_kv)


def peers_of(ctx_size):
    return ctx_size == 4, range(1, ctx_size)


def ctx_target(position, way, square, ctx_size):
    return position ^ way if square else lax.rem(position + way, ctx_size)


def ctx_source(position, way, square, ctx_size):
    return position ^ way if square else lax.rem(position + ctx_size - way, ctx_size)


def greet(ctx_size, pair_count, with_ctx, all_shards):
    ctx = lax.axis_index("ctx")
    shard = lax.axis_index("fsdp")
    pair, core = shard // 2, shard % 2
    barrier = pltpu.get_barrier_semaphore()
    partners = [(ctx, pair * 2 + 1 - core)]
    for step in range(1, pair_count):
        there = lax.rem(pair + step, pair_count) * 2
        partners.append((ctx, there + core))
        if all_shards:
            partners.append((ctx, there + 1 - core))
    if with_ctx:
        for way in range(1, ctx_size):
            partners.append((lax.rem(ctx + way, ctx_size), shard))
    for partner in partners:
        pl.semaphore_signal(barrier, inc=1, device_id=partner, device_id_type=MESH_ID)
    pl.semaphore_wait(barrier, len(partners))
    return ctx, pair, core


class Exchange:
    def __init__(self, source, out, sems, own_sem, pair_count):
        self.source, self.out, self.sems, self.own_sem = source, out, sems, own_sem
        self.shard_count = 2 * pair_count

    def start(self):
        ctx, shard = lax.axis_index("ctx"), lax.axis_index("fsdp")
        self.own = pltpu.make_async_copy(self.source.at[shard], self.out.at[shard], self.own_sem)
        self.own.start()
        self.copies = []
        for step in range(1, self.shard_count):
            there = lax.rem(shard + step, self.shard_count)
            copy = pltpu.make_async_remote_copy(
                src_ref=self.source.at[there],
                dst_ref=self.out.at[shard],
                send_sem=self.sems[0].at[step - 1],
                recv_sem=self.sems[1].at[step - 1],
                device_id=(ctx, there),
                device_id_type=MESH_ID,
            )
            copy.start()
            self.copies.append(copy)

    def finish(self):
        ctx, shard = lax.axis_index("ctx"), lax.axis_index("fsdp")
        for step in range(1, self.shard_count):
            come = lax.rem(shard + self.shard_count - step, self.shard_count)
            pltpu.make_async_remote_copy(
                src_ref=self.out.at[come],
                dst_ref=self.out.at[come],
                send_sem=self.sems[0].at[step - 1],
                recv_sem=self.sems[1].at[step - 1],
                device_id=(ctx, shard),
                device_id_type=MESH_ID,
            ).wait_recv()
        self.own.wait()
        for copy in self.copies:
            copy.wait_send()


def gather_kernel(arity, ctx_size, pair_count, slots, swaps, wide, *refs):
    sources, refs = refs[:arity], refs[arity:]
    swap_sources, refs = refs[:swaps], refs[swaps:]
    outs, refs = refs[:arity], refs[arity:]
    swap_outs, refs = refs[:swaps], refs[swaps:]
    pair_sems, ctx_sems, core_sems = refs[0:2], refs[2:4], refs[4:6]
    local_sem = refs[6]
    square, ways = peers_of(ctx_size) if wide else (False, ())
    narrow = [item for item in range(arity) if item not in wide]
    near = [way for way in ways if not (square and way == 3)]
    ctx, pair, core = greet(ctx_size, pair_count, len(wide) > 0, swaps > 0)
    homes = [place(ctx, pair * 2 + core) for place in slots]
    started = []
    steps = [(0, 1)] + [(far, way) for far in range(1, pair_count) for way in (1, -1)]

    def present(step):
        far, way = steps[step]
        if far == 0:
            return None
        return pair >= far if way == 1 else pair + far < pair_count

    def origin(step):
        far, way = steps[step]
        return pair - far * way

    def when(condition, work):
        if condition is None:
            work()
        else:
            pl.when(condition)(work)

    def send(item, source, place, target, sems, at, condition):
        copy = pltpu.make_async_remote_copy(
            src_ref=source,
            dst_ref=outs[item].at[place],
            send_sem=sems[0].at[at],
            recv_sem=sems[1].at[at],
            device_id=target,
            device_id_type=MESH_ID,
        )
        copy.start()
        started.append((condition, item, sems, at))

    def sent(item, sems, at):
        pltpu.make_async_remote_copy(
            src_ref=outs[item].at[0],
            dst_ref=outs[item].at[0],
            send_sem=sems[0].at[at],
            recv_sem=sems[1].at[at],
            device_id=(ctx, pair * 2 + core),
            device_id_type=MESH_ID,
        ).wait_send()

    def arrive(item, place, sems, at):
        pltpu.make_async_remote_copy(
            src_ref=outs[item].at[place],
            dst_ref=outs[item].at[place],
            send_sem=sems[0].at[at],
            recv_sem=sems[1].at[at],
            device_id=(ctx, pair * 2 + core),
            device_id_type=MESH_ID,
        ).wait_recv()

    def pass_on(step, item, source, place):
        far, way = steps[step]
        for side in (1, -1) if far == 0 else (way,):

            def further(side=side):
                return pair + 1 < pair_count if side == 1 else pair >= 1

            def both(further=further):
                return further() if far == 0 else jnp.logical_and(further(), present(step))

            def work(side=side, both=both):
                send(
                    item,
                    source,
                    place,
                    (ctx, (pair + side) * 2 + core),
                    pair_sems,
                    ((side + 1) // 2, far, item),
                    both,
                )

            if far + 1 < pair_count:
                pl.when(further())(work)

    def to_core(item, source, from_ctx, way, step):
        send(
            item,
            source,
            slots[item](from_ctx, origin(step) * 2 + core),
            (ctx, pair * 2 + 1 - core),
            core_sems,
            (way, step, item),
            functools.partial(present, step),
        )

    def spread(step, items):
        for item in items:
            place = slots[item](ctx, origin(step) * 2 + core)
            source = sources[item]
            if step:
                far, way = steps[step]
                arrive(item, place, pair_sems, ((way + 1) // 2, far - 1, item))
                source = outs[item].at[place]
            pass_on(step, item, source, place)
            for way in near if item in wide else ():
                there = ctx_target(ctx, way, square, ctx_size)
                send(
                    item,
                    source,
                    place,
                    (there, pair * 2 + core),
                    ctx_sems,
                    (way - 1, step, item),
                    functools.partial(present, step),
                )
            to_core(item, source, ctx, 0, step)

    def collect(step):
        for way in near:
            for item in wide:
                come = ctx_source(ctx, way, square, ctx_size)
                place = slots[item](come, origin(step) * 2 + core)
                arrive(item, place, ctx_sems, (way - 1, step, item))
                source = outs[item].at[place]
                if square and (steps[step][0] % 2 == 0) == (way == 1):
                    send(
                        item,
                        source,
                        place,
                        (ctx ^ (3 - way), pair * 2 + core),
                        ctx_sems,
                        (2, step, item),
                        functools.partial(present, step),
                    )
                to_core(item, source, come, way, step)

    def collect_far(step):
        for item in wide:
            place = slots[item](ctx ^ 3, origin(step) * 2 + core)
            arrive(item, place, ctx_sems, (2, step, item))
            to_core(item, outs[item].at[place], ctx ^ 3, 3, step)

    def straight_core(item, source, place, step):
        sibling = (ctx, pair * 2 + 1 - core)
        send(item, source, place, sibling, core_sems, (0, step, item), lambda: None)

    def go_straight(item):
        for step in range(1, pair_count):
            there = lax.rem(pair + step, pair_count) * 2 + core
            at = (0, step - 1, item)
            send(item, sources[item], homes[item], (ctx, there), pair_sems, at, lambda: None)
        straight_core(item, sources[item], homes[item], 0)

    locals_ = []
    for item in range(arity):
        copy = pltpu.make_async_copy(sources[item], outs[item].at[homes[item]], local_sem.at[item])
        copy.start()
        locals_.append(copy)
    spread(0, wide or range(arity))
    flows = []
    count = len(steps)
    for turn in range(1, count + 4):
        if turn < count:
            when(present(turn), functools.partial(spread, turn, wide or range(arity)))
        if turn == count:
            for item in narrow if wide else ():
                go_straight(item)
            for item in range(swaps):
                flow = Exchange(
                    swap_sources[item],
                    swap_outs[item],
                    refs[7 + 3 * item : 9 + 3 * item],
                    refs[9 + 3 * item],
                    pair_count,
                )
                flow.start()
                flows.append(flow)
        if 0 <= turn - 2 < count:
            when(present(turn - 2), functools.partial(collect, turn - 2))
        if square and 0 <= turn - 4 < count:
            when(present(turn - 4), functools.partial(collect_far, turn - 4))

    for item in narrow if wide else ():
        for step in range(1, pair_count):
            come = lax.rem(pair + pair_count - step, pair_count)
            place = slots[item](ctx, come * 2 + core)
            arrive(item, place, pair_sems, (0, step - 1, item))
            straight_core(item, outs[item].at[place], place, step)
    for item in narrow if wide else ():
        for step in range(pair_count):
            come = lax.rem(pair + pair_count - step, pair_count)
            arrive(item, slots[item](ctx, come * 2 + 1 - core), core_sems, (0, step, item))

    def from_core(step):
        for way in (0, *ways):
            come = ctx_source(ctx, way, square, ctx_size) if way else ctx
            for item in wide or range(arity):
                arrive(item, slots[item](come, origin(step) * 2 + 1 - core), core_sems, (way, step, item))

    for step in range(count):
        when(present(step), functools.partial(from_core, step))
    for flow in flows:
        flow.finish()
    for copy in locals_:
        copy.wait()
    for condition, *which in started:
        when(condition(), functools.partial(sent, *which))


def gather(pieces, slots, collective_id, swaps=(), wide=None):
    ctx_size, shard_count = lax.axis_size("ctx"), lax.axis_size("fsdp")
    pair_count = shard_count // 2
    arity = len(pieces)
    wide = range(arity) if wide is None else wide
    dma = pltpu.SemaphoreType.DMA
    moved = sum(piece.size for piece in pieces) * 2
    steps = 2 * pair_count - 1
    return pl.pallas_call(
        functools.partial(gather_kernel, arity, ctx_size, pair_count, slots, len(swaps), wide),
        in_specs=[pl.BlockSpec(memory_space=pltpu.VMEM)] * (arity + len(swaps)),
        out_specs=[pl.BlockSpec(memory_space=pl.ANY)] * (arity + len(swaps)),
        out_shape=[
            jax.ShapeDtypeStruct(
                ((ctx_size if item in wide else 1) * shard_count,) + piece.shape, piece.dtype
            )
            for item, piece in enumerate(pieces)
        ]
        + [jax.ShapeDtypeStruct(swap.shape, swap.dtype) for swap in swaps],
        scratch_shapes=[dma((2, pair_count - 1, arity))] * 2
        + [dma((ctx_size - 1, steps, arity))] * 2
        + [dma((ctx_size, steps, arity))] * 2
        + [dma((arity,))]
        + [dma((shard_count - 1,)), dma((shard_count - 1,)), dma] * len(swaps),
        compiler_params=pltpu.CompilerParams(collective_id=collective_id, has_side_effects=True),
        cost_estimate=pl.CostEstimate(
            flops=0, bytes_accessed=moved * ctx_size * shard_count * 4, transcendentals=0
        ),
    )(*pieces, *swaps)


class LineScatter:
    def __init__(self, source, out, half, room, sems, where, counts, last):
        self.count, self.ctx_size = counts
        self.source, self.out, self.half, self.room = source, out, half, room
        self.last = last
        self.core_sems, self.pair_sems = sems[0:2], sems[2:4]
        self.ctx, self.pair, self.core = where
        self.order = [*range(1, self.count), 0]

    def copy(self, source, target, device, sems, at):
        return pltpu.make_async_remote_copy(
            src_ref=source,
            dst_ref=target,
            send_sem=sems[0].at[at],
            recv_sem=sems[1].at[at],
            device_id=device,
            device_id_type=MESH_ID,
        )

    def here(self):
        return (self.ctx, self.pair * 2 + self.core)

    def toward(self, step):
        return lax.rem(self.pair + step, self.count)

    def start(self):
        self.copies = []
        for step in self.order:
            self.copies.append(
                self.copy(
                    self.source.at[self.toward(step) * 2 + 1 - self.core],
                    self.half.at[step],
                    (self.ctx, self.pair * 2 + 1 - self.core),
                    self.core_sems,
                    step,
                )
            )
            self.copies[-1].start()

    def fold(self, step):
        half = self.half.at[step]
        self.copy(half, half, self.here(), self.core_sems, step).wait_recv()
        mine = self.source[self.toward(step) * 2 + self.core].astype(jnp.float32)
        total = mine + half[...].astype(jnp.float32)
        if step == 0:
            self.out[...] = total
            return
        half[...] = total.astype(half.dtype)
        self.copies.append(
            self.copy(
                half,
                self.room.at[step - 1],
                (self.ctx, self.toward(step) * 2 + self.core),
                self.pair_sems,
                step - 1,
            )
        )
        self.copies[-1].start()

    def over_ctx(self, terms, room, landing, *sems):
        shard = self.pair * 2 + self.core
        copies = []

        def send(source, target, way, sems):
            there = lax.rem(self.ctx + way, self.ctx_size)
            copies.append(self.copy(source(there), target, (there, shard), sems, way - 1))
            copies[-1].start()

        def arrive(target, way, sems):
            self.copy(target, target, self.here(), sems, way - 1).wait_recv()

        terms[...] = self.out[...].astype(terms.dtype)
        for way in range(1, self.ctx_size):
            send(lambda there: terms.at[there], room.at[way - 1], way, sems[0:2])
        total = self.out[self.ctx]
        for way in range(1, self.ctx_size):
            arrive(room.at[way - 1], way, sems[0:2])
            total = total + room[way - 1].astype(jnp.float32)
        landing[self.ctx] = total.astype(landing.dtype)
        for way in range(1, self.ctx_size):
            send(lambda there: landing.at[self.ctx], landing.at[self.ctx], way, sems[2:4])
        for way in range(1, self.ctx_size):
            come = lax.rem(self.ctx + self.ctx_size - way, self.ctx_size)
            arrive(landing.at[come], way, sems[2:4])
        self.out[...] = landing[...].astype(jnp.float32)
        for copy in copies:
            copy.wait_send()

    def finish(self):
        for step in range(1, self.count):
            room = self.room.at[step - 1]
            self.copy(room, room, self.here(), self.pair_sems, step - 1).wait_recv()
            self.out[...] += room[...].astype(jnp.float32)
        if self.last:
            self.over_ctx(*self.last)
        for copy in self.copies:
            copy.wait_send()


def scatter_kernel(arity, ctx_size, pair_count, slot, spread_ctx, lines, swaps, *refs):
    sources, refs = refs[:arity], refs[arity:]
    line_sources, refs = refs[:lines], refs[lines:]
    swap_sources, refs = refs[:swaps], refs[swaps:]
    outs, refs = refs[:arity], refs[arity:]
    line_outs, refs = refs[:lines], refs[lines:]
    swap_outs, refs = refs[:swaps], refs[swaps:]
    halves, relays, asides, ends, finals = (refs[i * arity : (i + 1) * arity] for i in range(5))
    sems = refs[5 * arity : 5 * arity + 10]
    core_sems, relay_sems, ctx_sems, pair_sems, last_sems = (sems[2 * i : 2 * i + 2] for i in range(5))
    square, ways = peers_of(ctx_size)
    ctx, pair, core = greet(ctx_size, pair_count, True, swaps > 0)
    order = list(range(1, pair_count)) + [0]
    started = []
    flows = []
    for item in range(lines):
        at = 5 * arity + 10 + 13 * item
        spread = len(line_sources[item].shape) == 4
        flows.append(
            LineScatter(
                line_sources[item],
                line_outs[item],
                *refs[at : at + 2],
                refs[at + 2 : at + 6],
                (ctx, pair, core),
                (pair_count, ctx_size),
                refs[at + 6 : at + 13] if spread else (),
            )
        )

    def send(source, target, device, pair_of_sems, at):
        copy = pltpu.make_async_remote_copy(
            src_ref=source,
            dst_ref=target,
            send_sem=pair_of_sems[0].at[at],
            recv_sem=pair_of_sems[1].at[at],
            device_id=device,
            device_id_type=MESH_ID,
        )
        copy.start()
        started.append(copy)

    def arrive(target, pair_of_sems, at):
        pltpu.make_async_remote_copy(
            src_ref=target,
            dst_ref=target,
            send_sem=pair_of_sems[0].at[at],
            recv_sem=pair_of_sems[1].at[at],
            device_id=(ctx, pair * 2 + core),
            device_id_type=MESH_ID,
        ).wait_recv()

    def toward(step):
        return lax.rem(pair + step, pair_count)

    def target_ctx(way):
        return ctx_target(ctx, way, square, ctx_size) if way else ctx

    def f32(value):
        return value.astype(jnp.float32)

    far_first = [3, 1, 2, 0] if square else list(ways) + [0]
    for step in order:
        for way in far_first:
            for item in range(arity):
                send(
                    sources[item].at[slot(target_ctx(way), toward(step) * 2 + 1 - core)],
                    halves[item].at[way, step],
                    (ctx, pair * 2 + 1 - core),
                    core_sems,
                    (way, step, item),
                )

    def fold_core(step):
        for way in far_first:
            for item in range(arity):
                half = halves[item].at[way, step]
                arrive(half, core_sems, (way, step, item))
                mine = sources[item][slot(target_ctx(way), toward(step) * 2 + core)]
                half[...] = (f32(mine) + f32(half[...])).astype(half.dtype)
                if square and way == 3:
                    there = ctx ^ (1 if step % 2 == 0 else 2)
                    send(
                        half,
                        relays[item].at[step],
                        (there, pair * 2 + core),
                        relay_sems,
                        (step, item),
                    )

    def fold_relay(step):
        for item in range(arity):
            if square:
                relay = relays[item].at[step]
                arrive(relay, relay_sems, (step, item))
                half = halves[item].at[2 if step % 2 == 0 else 1, step]
                half[...] = (f32(half[...]) + f32(relay[...])).astype(half.dtype)
            for way in ways:
                if square and way == 3:
                    continue
                send(
                    halves[item].at[way, step],
                    asides[item].at[way - 1, step],
                    (target_ctx(way), pair * 2 + core),
                    ctx_sems,
                    (way - 1, step, item),
                )

    def fold_ctx(step):
        for item in range(arity):
            half = halves[item].at[0, step]
            total = f32(half[...])
            for way in ways:
                if square and way == 3:
                    continue
                aside = asides[item].at[way - 1, step]
                arrive(aside, ctx_sems, (way - 1, step, item))
                total = total + f32(aside[...])
            if step:
                half[...] = total.astype(half.dtype)
                send(
                    half,
                    ends[item].at[step - 1],
                    (ctx, toward(step) * 2 + core),
                    pair_sems,
                    (step - 1, item),
                )
            else:
                for other in range(1, pair_count):
                    end = ends[item].at[other - 1]
                    arrive(end, pair_sems, (other - 1, item))
                    total = total + f32(end[...])
                if spread_ctx:
                    finals[item][...] = total.astype(finals[item].dtype)
                else:
                    outs[item][...] = total.astype(outs[item].dtype)

    for flow in flows:
        flow.start()
    exchanges = []
    for item in range(swaps):
        at = 5 * arity + 10 + 13 * lines + 3 * item
        flow = Exchange(
            swap_sources[item], swap_outs[item], refs[at : at + 2], refs[at + 2], pair_count
        )
        flow.start()
        exchanges.append(flow)
    for turn in range(pair_count + 2):
        if turn < pair_count:
            fold_core(order[turn])
        if 1 <= turn <= pair_count:
            fold_relay(order[turn - 1])
            for flow in flows:
                flow.fold(order[turn - 1])
        if turn >= 2:
            fold_ctx(order[turn - 2])
    if spread_ctx:
        for item in range(arity):
            for way in ways:
                send(
                    finals[item],
                    outs[item].at[ctx],
                    (target_ctx(way), pair * 2 + core),
                    last_sems,
                    (way - 1, item),
                )
            outs[item][ctx] = finals[item][...]
        for item in range(arity):
            for way in ways:
                arrive(outs[item].at[ctx_source(ctx, way, square, ctx_size)], last_sems, (way - 1, item))
    for flow in (*flows, *exchanges):
        flow.finish()
    for copy in started:
        copy.wait_send()


def scatter(terms, slot, collective_id, spread_ctx=False, out_dtype=None, lines=(), swaps=()):
    ctx_size, shard_count = lax.axis_size("ctx"), lax.axis_size("fsdp")
    pair_count = shard_count // 2
    arity = len(terms)
    dma = pltpu.SemaphoreType.DMA
    lead = (ctx_size,) if spread_ctx else ()
    asides = 2 if ctx_size == 4 else ctx_size - 1

    def room(*extent):
        return [pltpu.VMEM(extent + term.shape[1:], term.dtype) for term in terms]

    def line_room(line):
        if len(line.shape) == 3:
            return [pltpu.VMEM((8, HD), line.dtype)] * 3 + [dma((1,))] * 4
        cut = line.shape[2:]
        rooms = [pltpu.VMEM((count,) + cut, line.dtype) for count in (ctx_size, ctx_size - 1, ctx_size)]
        return rooms + [dma((ctx_size - 1,))] * 4

    moved = sum(term.size * term.dtype.itemsize for term in terms)
    return pl.pallas_call(
        functools.partial(scatter_kernel, arity, ctx_size, pair_count, slot, spread_ctx, len(lines), len(swaps)),
        in_specs=[pl.BlockSpec(memory_space=pltpu.VMEM)] * (arity + len(lines) + len(swaps)),
        out_specs=[pl.BlockSpec(memory_space=pltpu.VMEM)] * (arity + len(lines))
        + [pl.BlockSpec(memory_space=pl.ANY)] * len(swaps),
        out_shape=[
            jax.ShapeDtypeStruct(lead + term.shape[1:], out_dtype or term.dtype) for term in terms
        ]
        + [jax.ShapeDtypeStruct(line.shape[1:], jnp.float32) for line in lines]
        + [jax.ShapeDtypeStruct(swap.shape, swap.dtype) for swap in swaps],
        scratch_shapes=room(ctx_size, pair_count)
        + room(pair_count)
        + room(asides, pair_count)
        + room(pair_count - 1)
        + room()
        + [dma((ctx_size, pair_count, arity))] * 2
        + [dma((pair_count, arity))] * 2
        + [dma((ctx_size - 1, pair_count, arity))] * 2
        + [dma((pair_count - 1, arity))] * 2
        + [dma((ctx_size - 1, arity))] * 2
        + [
            scratch
            for line in lines
            for scratch in [
                pltpu.VMEM((pair_count,) + line.shape[1:], line.dtype),
                pltpu.VMEM((pair_count - 1,) + line.shape[1:], line.dtype),
            ]
            + [dma((pair_count,))] * 4
            + line_room(line)
        ]
        + [dma((shard_count - 1,)), dma((shard_count - 1,)), dma] * len(swaps),
        compiler_params=pltpu.CompilerParams(
            collective_id=collective_id, has_side_effects=True, vmem_limit_bytes=63 * 2**20
        ),
        cost_estimate=pl.CostEstimate(flops=0, bytes_accessed=moved * 16, transcendentals=0),
    )(*terms, *lines, *swaps)


def line_sum_kernel(pair_count, source, out, half, room, *sems):
    where = greet(1, pair_count, False, False)
    flow = LineScatter(source, out, half, room, sems, where, (pair_count, 1), ())
    flow.start()
    for step in flow.order:
        flow.fold(step)
    flow.finish()


def line_sum(terms, collective_id):
    pair_count = lax.axis_size("fsdp") // 2
    extent = terms.shape[1:]
    dma = pltpu.SemaphoreType.DMA((pair_count,))
    return pl.pallas_call(
        functools.partial(line_sum_kernel, pair_count),
        in_specs=[pl.BlockSpec(memory_space=pltpu.VMEM)],
        out_specs=pl.BlockSpec(memory_space=pltpu.VMEM),
        out_shape=jax.ShapeDtypeStruct(extent, jnp.float32),
        scratch_shapes=[
            pltpu.VMEM((pair_count,) + extent, terms.dtype),
            pltpu.VMEM((pair_count - 1,) + extent, terms.dtype),
        ]
        + [dma] * 4,
        compiler_params=pltpu.CompilerParams(
            collective_id=collective_id, has_side_effects=True, vmem_limit_bytes=63 * 2**20
        ),
        cost_estimate=pl.CostEstimate(flops=0, bytes_accessed=terms.size * 16, transcendentals=0),
    )(terms)


def turned(values, cosine, signed_sine):
    return values * cosine + pltpu.roll(values, HD // 2, 1) * signed_sine


def turned_back(grads, cosine, signed_sine):
    return grads * cosine + pltpu.roll(grads * signed_sine, HD // 2, 1)


def slot_of(index):
    return index % SEQS, index // SEQS


def key_column(index, group, part):
    seq, half = slot_of(index)
    return (((seq * KVH + group) * 2 + half) * 2 + part) * HD


def project_kernel(rows, x_ref, gain_ref, w_hbm, bias_ref, cos_ref, sin_ref, normed_ref, q_ref, kv_ref, w_ref, q_acc, sems):
    wide = w_ref.shape[2]
    copies = []
    for part in range(w_ref.shape[0]):
        copy = pltpu.make_async_copy(
            w_hbm.at[:, part * wide : (part + 1) * wide], w_ref.at[part], sems.at[part]
        )
        copy.start()
        copies.append(copy)
    values = x_ref[...].astype(jnp.float32)
    scale = lax.rsqrt(jnp.mean(values * values, -1, keepdims=True) + EPS)
    normed = (values * scale * gain_ref[...]).astype(jnp.bfloat16)
    normed_ref[...] = normed
    cosine, sine = cos_ref[...], sin_ref[...]
    for part, copy in enumerate(copies):
        copy.wait()
        columns = jnp.dot(normed, w_ref[part], preferred_element_type=jnp.float32)
        columns = columns + bias_ref[:, part * wide : (part + 1) * wide]
        for index in range(wide // HD):
            head = part * (wide // HD) + index
            piece = columns[:, index * HD : (index + 1) * HD]
            if head < H + KVH:
                piece = turned(piece, cosine, sine)
            if head < H:
                piece = piece * (HD**-0.5)
            for slot in range(2 * SEQS):
                seq, half = slot_of(slot)
                own = piece[slot * rows : (slot + 1) * rows]
                if head < H:
                    group, member = head // (H // KVH), head % (H // KVH)
                    q_acc[seq, half, group, member * rows : (member + 1) * rows] = own
                else:
                    group, kind = (head - H) % KVH, (head - H) // KVH
                    at = key_column(slot, group, kind)
                    kv_ref[:, at : at + HD] = own.astype(jnp.bfloat16)
    q_ref[...] = q_acc[...].astype(jnp.bfloat16)


def project(tokens, gain, weight, bias, cosine, signed_sine, rows):
    vmem = pl.BlockSpec(memory_space=pltpu.VMEM)
    parts = 8
    grouped = (SEQS, 2, KVH, H // KVH * rows, HD)
    return pl.pallas_call(
        functools.partial(project_kernel, rows),
        in_specs=[vmem, vmem, pl.BlockSpec(memory_space=pl.ANY), vmem, vmem, vmem],
        out_specs=[vmem, vmem, vmem],
        out_shape=[
            jax.ShapeDtypeStruct(tokens.shape, jnp.bfloat16),
            jax.ShapeDtypeStruct(grouped, jnp.bfloat16),
            jax.ShapeDtypeStruct((rows, SEQS * KVH * 4 * HD), jnp.bfloat16),
        ],
        scratch_shapes=[
            pltpu.VMEM((parts, D, QKV // parts), jnp.bfloat16),
            pltpu.VMEM(grouped, jnp.float32),
            pltpu.SemaphoreType.DMA((parts,)),
        ],
        compiler_params=pltpu.CompilerParams(vmem_limit_bytes=62 * 2**20),
        cost_estimate=pl.CostEstimate(
            flops=2 * tokens.shape[0] * D * QKV, bytes_accessed=2 * D * QKV, transcendentals=0
        ),
        name="project",
    )(tokens, gain.reshape(1, -1), weight, bias.reshape(1, -1), cosine, signed_sine)


def unproject_kernel(rows, gq_ref, gkv_ref, cos_ref, sin_ref, w_hbm, x_ref, gain_ref, past_ref, gp_ref, gi_ref, gg_ref, gb_ref, w_ref, gp_acc, sem):
    copy = pltpu.make_async_copy(w_hbm, w_ref, sem)
    copy.start()
    cosine, sine = cos_ref[...], sin_ref[...]

    def rounded(values):
        return values.astype(jnp.bfloat16).astype(jnp.float32)

    for head in range(H + 2 * KVH):
        for slot in range(2 * SEQS):
            seq, half = slot_of(slot)
            at = slice(slot * rows, (slot + 1) * rows)
            if head < H:
                group, member = head // (H // KVH), head % (H // KVH)
                grad = gq_ref[seq, half, group, member * rows : (member + 1) * rows]
                grad = rounded(grad) * (HD**-0.5)
            else:
                group, kind = (head - H) % KVH, (head - H) // KVH
                column = key_column(slot, group, kind)
                grad = rounded(gkv_ref[:, column : column + HD])
            if head < H + KVH:
                grad = turned_back(grad, cosine[at], sine[at])
            gp_acc[at, head * HD : (head + 1) * HD] = grad
    low = gp_acc[...].astype(jnp.bfloat16)
    gp_ref[...] = low
    gb_ref[...] = jnp.sum(low.astype(jnp.float32), 0, keepdims=True)
    values = x_ref[...].astype(jnp.float32)
    scale = lax.rsqrt(jnp.mean(values * values, -1, keepdims=True) + EPS)
    unit = values * scale
    copy.wait()
    grad_normed = lax.dot_general(low, w_ref[...], CONTRACT_LAST, preferred_element_type=jnp.float32)
    gg_ref[...] = jnp.sum(grad_normed * unit, 0, keepdims=True)
    grad_unit = grad_normed * gain_ref[...]
    inner = jnp.mean(grad_unit * unit, -1, keepdims=True)
    gi_ref[...] = past_ref[...] + scale * (grad_unit - unit * inner)


def unproject(grad_queries, grad_kv, cosine, signed_sine, weight, tokens, gain, past, rows):
    vmem = pl.BlockSpec(memory_space=pltpu.VMEM)
    return pl.pallas_call(
        functools.partial(unproject_kernel, rows),
        in_specs=[vmem, vmem, vmem, vmem, pl.BlockSpec(memory_space=pl.ANY), vmem, vmem, vmem],
        out_specs=[vmem] * 4,
        out_shape=[
            jax.ShapeDtypeStruct((tokens.shape[0], QKV), jnp.bfloat16),
            jax.ShapeDtypeStruct(tokens.shape, jnp.float32),
            jax.ShapeDtypeStruct((1, D), jnp.float32),
            jax.ShapeDtypeStruct((1, QKV), jnp.float32),
        ],
        scratch_shapes=[
            pltpu.VMEM((D, QKV), jnp.bfloat16),
            pltpu.VMEM((tokens.shape[0], QKV), jnp.float32),
            pltpu.SemaphoreType.DMA,
        ],
        compiler_params=pltpu.CompilerParams(vmem_limit_bytes=62 * 2**20),
        cost_estimate=pl.CostEstimate(
            flops=2 * tokens.shape[0] * D * QKV, bytes_accessed=2 * D * QKV, transcendentals=0
        ),
        name="unproject",
    )(grad_queries, grad_kv, cosine, signed_sine, weight, tokens, gain.reshape(1, -1), past)


def pack_kernel(columns, gate_ref, up_ref, out_ref):
    width = out_ref.shape[2] // 2
    cut = out_ref.shape[1]
    for there in range(out_ref.shape[0]):
        for side, ref in enumerate((gate_ref, up_ref)):
            at = side * width
            out_ref[there, :, at + width - HD : at + width] = jnp.zeros((cut, HD), out_ref.dtype)
            out_ref[there, :, at : at + columns] = ref[:, there * columns : (there + 1) * columns]


def pack(gate, up, shard_count, columns, width):
    return pl.pallas_call(
        functools.partial(pack_kernel, columns),
        in_specs=[pl.BlockSpec(memory_space=pltpu.VMEM)] * 2,
        out_specs=pl.BlockSpec(memory_space=pltpu.VMEM),
        out_shape=jax.ShapeDtypeStruct((shard_count, gate.shape[0], 2 * width), gate.dtype),
        name="pack",
    )(gate, up)


def unpack_kernel(columns, in_ref, gate_ref, up_ref):
    width = in_ref.shape[3] // 2
    for there in range(in_ref.shape[1]):
        for side, ref in enumerate((gate_ref, up_ref)):
            part = in_ref[0, there, :, side * width : side * width + columns]
            ref[0, :, there * columns : (there + 1) * columns] = part.astype(jnp.float32)


def unpack(rows, columns):
    ctx_size, shard_count, cut, _ = rows.shape
    out = jax.ShapeDtypeStruct((ctx_size, cut, shard_count * columns), jnp.float32)
    return pl.pallas_call(
        functools.partial(unpack_kernel, columns),
        grid=(ctx_size,),
        in_specs=[pl.BlockSpec((1,) + rows.shape[1:], lambda c: (c, 0, 0, 0))],
        out_specs=[pl.BlockSpec((1, cut, shard_count * columns), lambda c: (c, 0, 0))] * 2,
        out_shape=[out, out],
        name="unpack",
    )(rows)


def shards(
    layer_input,
    block_order,
    first_gain,
    w_qkv,
    b_qkv,
    w_o,
    second_gain,
    w_gate,
    w_up,
    w_down,
    cotangent,
):
    ctx_size = lax.axis_size("ctx")
    shard_count = lax.axis_size("fsdp")
    own_ctx = lax.axis_index("ctx")
    own_shard = lax.axis_index("fsdp")
    rows_here = layer_input.shape[0]
    block_rows = rows_here * shard_count
    cut = D // (ctx_size * shard_count)
    columns = FF // shard_count
    cosine, signed_sine = turn_tables(
        block_order, own_ctx, ctx_size, block_rows, own_shard * rows_here, rows_here
    )
    tokens = by_slot(layer_input)
    grad_out = by_slot(cotangent)

    def by_rows(ctx, shard):
        return shard * ctx_size + ctx

    def by_tokens(ctx, shard):
        return ctx * shard_count + shard

    def own_cut(weight):
        return lax.dynamic_slice_in_dim(weight, own_ctx * cut, cut, 0)

    def mix_features(values):
        shaped = values.reshape(-1, shard_count, ctx_size, cut)
        return shaped.transpose(0, 2, 1, 3).reshape(-1, D)

    def unmix_features(values):
        shaped = values.reshape(-1, ctx_size, shard_count, cut)
        return shaped.transpose(0, 2, 1, 3).reshape(-1, D)

    small = jnp.concatenate([b_qkv, first_gain, second_gain]).reshape(ctx_size, -1)
    small_width = small.shape[1]
    small = lax.dynamic_slice_in_dim(small, own_ctx, 1, 0)
    small = jnp.pad(small, ((0, 0), (0, 16 * HD - small_width))).reshape(16, HD)
    width = -(-columns // HD) * HD
    w_qkv_all, w_o_all, small_all, gate_up_cut = gather(
        [own_cut(w_qkv), own_cut(w_o), small],
        [by_rows, by_rows, by_rows],
        1,
        swaps=[pack(own_cut(w_gate), own_cut(w_up), shard_count, columns, width)],
    )
    w_qkv_all = w_qkv_all.reshape(D, QKV)
    w_o_all = w_o_all.reshape(D, D)
    small_all = small_all.reshape(shard_count, ctx_size, -1)[:, :, :small_width]
    small_all = small_all.reshape(shard_count, -1).astype(jnp.float32)
    bias_width = QKV // shard_count
    gain_width = D // shard_count
    bias_all = small_all[:, :bias_width].reshape(-1)
    gain_one = small_all[:, bias_width : bias_width + gain_width].reshape(-1)
    gain_two = small_all[:, bias_width + gain_width :].reshape(-1)

    down_padded = jnp.pad(w_down, ((0, width - columns), (0, 0)))

    late_grad_out, w_qkv_all = lax.optimization_barrier((grad_out, w_qkv_all))
    cotangent_all = lax.all_gather(late_grad_out, "fsdp", axis=0, tiled=True)
    normed_one, queries, own_kv = project(
        tokens, gain_one, w_qkv_all, bias_all, cosine, signed_sine, rows_here
    )
    (all_kv,) = gather([own_kv], [by_tokens], 2)
    gate_up_cut, all_kv = lax.optimization_barrier((gate_up_cut, all_kv))
    gate_up_cols = lax.all_gather(
        gate_up_cut.reshape(shard_count * cut, 2 * width), "ctx", axis=0, tiled=True
    )
    all_kv = all_kv.reshape(-1, SEQS * KVH * 4 * HD)
    scalars = jnp.concatenate(
        [block_order.reshape(-1), jnp.stack([own_ctx, own_shard]).astype(jnp.int32)]
    )
    attended_grouped, stats = attend_forward(
        scalars, queries, all_kv, ctx_size, block_rows, rows_here
    )
    attended_low = from_groups(attended_grouped, rows_here).astype(jnp.bfloat16)
    middle = tokens.astype(jnp.float32) + jnp.dot(attended_low, w_o_all, preferred_element_type=jnp.float32)
    unit_two, scale_two, normed = normalize(middle, gain_two)
    normed_two = mix_features(normed.astype(jnp.bfloat16))

    (tokens_all,) = gather([normed_two], [lambda ctx, shard: shard], 6, wide=())
    tokens_all = tokens_all.reshape(-1, D)
    gate_up_part = jnp.dot(tokens_all, gate_up_cols, preferred_element_type=jnp.float32)
    gate_part, up_part = gate_up_part[:, :width], gate_up_part[:, width:]
    sigmoid_gate = jax.nn.sigmoid(gate_part)
    activated = gate_part * sigmoid_gate
    hidden = (activated * up_part).astype(jnp.bfloat16)
    grad_hidden = lax.dot_general(
        cotangent_all, down_padded, CONTRACT_LAST, preferred_element_type=jnp.float32
    )
    grad_gate = grad_hidden * up_part * sigmoid_gate * (1.0 + gate_part * (1.0 - sigmoid_gate))
    grad_gate_up = jnp.concatenate([grad_gate, grad_hidden * activated], -1).astype(jnp.bfloat16)
    gate_up_terms = lax.dot_general(
        tokens_all, grad_gate_up, CONTRACT_FIRST, preferred_element_type=jnp.float32
    ).astype(jnp.bfloat16)
    gate_up_rows = lax.psum_scatter(gate_up_terms, "ctx", scatter_dimension=0, tiled=True)
    grad_gate_up, hidden, gate_up_terms = lax.optimization_barrier(
        (grad_gate_up, hidden, gate_up_terms)
    )
    grad_tokens = lax.dot_general(
        grad_gate_up, gate_up_cols, CONTRACT_LAST, preferred_element_type=jnp.float32
    ).astype(jnp.bfloat16)
    grad_normed_two = line_sum(grad_tokens.reshape(shard_count, -1, D), 7)
    grad_normed_two, hidden = lax.optimization_barrier((grad_normed_two, hidden))
    down_terms = lax.dot_general(
        hidden, cotangent_all, CONTRACT_FIRST, preferred_element_type=jnp.float32
    ).astype(jnp.bfloat16)
    down_rows = lax.psum(down_terms, "ctx")
    mixed_terms = jnp.dot(hidden, down_padded, preferred_element_type=jnp.float32).astype(jnp.bfloat16)
    grad_normed_two, down_terms, mixed_terms = lax.optimization_barrier(
        (grad_normed_two, down_terms, mixed_terms)
    )
    grad_normed_two = unmix_features(grad_normed_two)
    grad_middle_norm, grad_gain_two = norm_back(grad_normed_two, unit_two, scale_two, gain_two)
    grad_middle = grad_out.astype(jnp.float32) + grad_middle_norm
    grad_branch_one = grad_middle.astype(jnp.bfloat16)
    grad_attended = lax.dot_general(
        grad_branch_one, w_o_all, CONTRACT_LAST, preferred_element_type=jnp.float32
    ).astype(jnp.bfloat16)
    o_terms = lax.dot_general(
        attended_low, grad_branch_one, CONTRACT_FIRST, preferred_element_type=jnp.float32
    ).astype(jnp.bfloat16)
    grad_queries, grad_kv_full = attend_backward(
        scalars,
        queries,
        to_groups(grad_attended, rows_here),
        attended_grouped,
        stats,
        all_kv,
        ctx_size,
        block_rows,
        rows_here,
    )
    grad_kv, gate_up_rows = scatter(
        [grad_kv_full.reshape(-1, rows_here, SEQS * KVH * 4 * HD)],
        by_tokens,
        3,
        out_dtype=jnp.float32,
        swaps=[gate_up_rows.reshape(shard_count, cut, 2 * width)],
    )
    gate_up_rows = lax.all_gather(gate_up_rows, "ctx", axis=0, tiled=False)
    mixed_terms, grad_kv = lax.optimization_barrier((mixed_terms, grad_kv))
    mixed_rows = lax.psum_scatter(mixed_terms, "fsdp", scatter_dimension=0, tiled=True)
    grad_projected, grad_input, grad_gain_one, grad_bias = unproject(
        grad_queries,
        grad_kv,
        cosine,
        signed_sine,
        w_qkv_all,
        tokens,
        gain_one,
        grad_middle,
        rows_here,
    )
    grad_input = from_slot(grad_input, rows_here)
    grad_bias = grad_bias.reshape(-1)
    qkv_terms = lax.dot_general(
        normed_one, grad_projected, CONTRACT_FIRST, preferred_element_type=jnp.float32
    ).astype(jnp.bfloat16)
    small_terms = jnp.concatenate(
        [
            part.reshape(shard_count, -1)
            for part in (grad_gain_one, grad_gain_two, grad_bias[:QK], grad_bias[QK:])
        ],
        1,
    )
    small_terms = small_terms.reshape(ctx_size * shard_count, small_width)
    small_terms = jnp.pad(small_terms, ((0, 0), (0, 8 * HD - small_width)))
    qkv_rows, o_rows, small_rows = scatter(
        [
            qkv_terms.reshape(-1, cut, QKV),
            o_terms.reshape(-1, cut, D),
            small_terms.reshape(-1, 8, HD),
        ],
        by_rows,
        4,
        spread_ctx=True,
    )
    mixed_out = middle + mixed_rows.astype(jnp.float32)
    output = from_slot(mixed_out.astype(jnp.bfloat16), rows_here)
    small_rows = small_rows.reshape(ctx_size, -1)[:, :small_width].reshape(-1)
    bias_start = 2 * gain_width
    value_start = bias_start + QK // shard_count

    gate_rows, up_rows = unpack(gate_up_rows, columns)
    return (
        output,
        grad_input,
        small_rows[:gain_width],
        qkv_rows.reshape(-1, QKV).astype(jnp.float32),
        small_rows[bias_start:value_start],
        small_rows[value_start:],
        o_rows.reshape(-1, D).astype(jnp.float32),
        small_rows[gain_width:bias_start],
        gate_rows.reshape(-1, FF),
        up_rows.reshape(-1, FF),
        down_rows[:columns].astype(jnp.float32),
    )


def solution(mesh):
    in_specs = (
        P(("ctx", "fsdp"), None, None),
        P(),
        P("fsdp"),
        P("fsdp", None),
        P("fsdp"),
        P("fsdp", None),
        P("fsdp"),
        P("fsdp", None),
        P("fsdp", None),
        P("fsdp", None),
        P(("ctx", "fsdp"), None, None),
    )
    out_specs = (
        P(("ctx", "fsdp"), None, None),
        P(("ctx", "fsdp"), None, None),
        P("fsdp"),
        P("fsdp", None),
        P("fsdp"),
        P("fsdp"),
        P("fsdp", None),
        P("fsdp"),
        P("fsdp", None),
        P("fsdp", None),
        P("fsdp", None),
    )
    return jax.shard_map(shards, mesh=mesh, in_specs=in_specs, out_specs=out_specs, check_vma=False)
```

```python
import functools

import jax
import jax.numpy as jnp
from jax import lax
from jax.experimental import pallas as pl
from jax.experimental.pallas import tpu as pltpu
from jax.sharding import PartitionSpec as P

D = 1536
H = 12
KVH = 2
HD = 128
FF = 8960
SEQS = 2
QKV = 2048
QK = 1792


EPS = 1e-06
THETA = 1000000.0
NEG_FILL = -1e30
MESH_ID = pl.DeviceIdType.MESH
CONTRACT_LAST = (((1,), (1,)), ((), ()))
CONTRACT_FIRST = (((0,), (0,)), ((), ()))


def by_slot(tokens):
    return tokens.transpose(1, 0, 2).reshape(-1, tokens.shape[2])


def from_slot(tokens, row_count):
    return tokens.reshape(2 * SEQS, row_count, -1).transpose(1, 0, 2)


def to_groups(tokens, row_count):
    shaped = tokens.reshape(2, SEQS, row_count, KVH, H // KVH, HD)
    return shaped.transpose(1, 0, 3, 4, 2, 5).reshape(SEQS, 2, KVH, H // KVH * row_count, HD)


def from_groups(grouped, row_count):
    shaped = grouped.reshape(SEQS, 2, KVH, H // KVH, row_count, HD).transpose(1, 0, 4, 2, 3, 5)
    return shaped.reshape(row_count * 2 * SEQS, H * HD)


def turn_tables(block_order, own_ctx, ctx_size, block_rows, first_row, row_count):
    half_width = HD // 2
    frequency = THETA ** (-jnp.arange(half_width, dtype=jnp.float32) * 2.0 / HD)
    frequency = jnp.tile(frequency, 2)[None, :]
    order = lax.dynamic_index_in_dim(block_order.reshape(SEQS, 2, ctx_size), own_ctx, 2, False)
    start = (order.T.reshape(-1) * block_rows + first_row).astype(jnp.float32)
    far = start[:, None] * frequency
    near = jnp.arange(row_count, dtype=jnp.float32)[:, None] * frequency
    far_cos, far_sin = jnp.cos(far)[:, None, :], jnp.sin(far)[:, None, :]
    near_cos, near_sin = jnp.cos(near)[None], jnp.sin(near)[None]
    sign = jnp.where(jnp.arange(HD) < half_width, -1.0, 1.0).astype(jnp.float32)
    cosine = far_cos * near_cos - far_sin * near_sin
    sine = (far_sin * near_cos + far_cos * near_sin) * sign
    return cosine.reshape(-1, HD), sine.reshape(-1, HD)


def normalize(values, gain):
    scale = lax.rsqrt(jnp.mean(values * values, -1, keepdims=True) + EPS)
    unit = values * scale
    return (unit, scale, unit * gain)


def norm_back(grad_out, unit, scale, gain):
    grad_unit = grad_out * gain
    inner = jnp.mean(grad_unit * unit, -1, keepdims=True)
    return (scale * (grad_unit - unit * inner), jnp.sum(grad_out * unit, 0))


def hidden_rows(scores, own_shard, rows_here):
    row = lax.broadcasted_iota(jnp.int32, scores.shape, 0)
    lane = lax.broadcasted_iota(jnp.int32, scores.shape, 1)
    return row > own_shard * rows_here + lax.rem(lane, rows_here)


def key_part(group, half_key, part):
    at = ((group * 2 + half_key) * 2 + part) * HD
    return slice(at, at + HD)


def attend_forward_kernel(ctx_size, block_rows, rows_here, scalars, q_ref, kv_ref, out_ref, stat_ref, best_ref, total_ref, accum_ref):
    seq = pl.program_id(0)
    blocks = 2 * ctx_size
    own_ctx = scalars[SEQS * blocks]
    own_shard = scalars[SEQS * blocks + 1]
    groups = range(KVH)
    best_ref[...] = jnp.full(best_ref.shape, NEG_FILL, jnp.float32)
    total_ref[...] = jnp.zeros(total_ref.shape, jnp.float32)
    accum_ref[...] = jnp.zeros(accum_ref.shape, jnp.float32)

    def step(key_ctx, half_key, half):
        order_key = scalars[seq * blocks + half_key * ctx_size + key_ctx]
        order_query = scalars[seq * blocks + half * ctx_size + own_ctx]

        def work(masked):
            rows = pl.ds(pl.multiple_of(key_ctx * block_rows, block_rows), block_rows)
            scores = [
                lax.dot_general(
                    kv_ref[rows, key_part(group, half_key, 0)],
                    q_ref[0, half, group],
                    CONTRACT_LAST,
                    preferred_element_type=jnp.float32,
                )
                for group in groups
            ]
            if masked:
                hidden = hidden_rows(scores[0], own_shard, rows_here)
                scores = [jnp.where(hidden, NEG_FILL, score) for score in scores]
            best = [best_ref[half, group] for group in groups]
            fresh = [
                jnp.maximum(best[group], jnp.max(scores[group], 0, keepdims=True)) for group in groups
            ]
            weights = [jnp.exp(scores[group] - fresh[group]) for group in groups]
            decay = [jnp.exp(best[group] - fresh[group]) for group in groups]
            added = [
                lax.dot_general(
                    kv_ref[rows, key_part(group, half_key, 1)],
                    weights[group].astype(jnp.bfloat16),
                    CONTRACT_FIRST,
                    preferred_element_type=jnp.float32,
                )
                for group in groups
            ]
            for group in groups:
                total_ref[half, group] = total_ref[half, group] * decay[group] + jnp.sum(
                    weights[group], 0, keepdims=True
                )
                accum_ref[half, group] = accum_ref[half, group] * decay[group] + added[group]
                best_ref[half, group] = fresh[group]

        @pl.when(order_key < order_query)
        def full():
            work(False)

        @pl.when(order_key == order_query)
        def diagonal():
            work(True)

    @pl.loop(0, ctx_size)
    def sweep(key_ctx):
        for half_key in range(2):
            for half in range(2):
                step(key_ctx, half_key, half)

    for half in range(2):
        for group in groups:
            totals = total_ref[half, group]
            out_ref[0, half, group] = (accum_ref[half, group] / totals).T
            stat_ref[0, half, group] = best_ref[half, group] + jnp.log(totals)


def group_blocks(lanes, key_rows):
    group = pl.BlockSpec((1, 2, KVH, lanes, HD), lambda s, _: (s, 0, 0, 0, 0))
    stat = pl.BlockSpec((1, 2, KVH, 1, lanes), lambda s, _: (s, 0, 0, 0, 0))
    keys = pl.BlockSpec((key_rows, KVH * 4 * HD), lambda s, _: (0, s))
    return group, stat, keys


def attend_forward(scalars, queries, all_kv, ctx_size, block_rows, rows_here):
    lanes = queries.shape[3]
    kernel = functools.partial(attend_forward_kernel, ctx_size, block_rows, rows_here)
    group, stat, keys = group_blocks(lanes, all_kv.shape[0])
    return pl.pallas_call(
        kernel,
        grid_spec=pltpu.PrefetchScalarGridSpec(
            num_scalar_prefetch=1,
            grid=(SEQS,),
            in_specs=[group, keys],
            out_specs=[group, stat],
            scratch_shapes=[
                pltpu.VMEM((2, KVH, 1, lanes), jnp.float32),
                pltpu.VMEM((2, KVH, 1, lanes), jnp.float32),
                pltpu.VMEM((2, KVH, HD, lanes), jnp.float32),
            ],
        ),
        out_shape=(
            jax.ShapeDtypeStruct(queries.shape, jnp.float32),
            jax.ShapeDtypeStruct((SEQS, 2, KVH, 1, lanes), jnp.float32),
        ),
        compiler_params=pltpu.CompilerParams(vmem_limit_bytes=60 * 2**20),
        name="attend_forward",
    )(scalars, queries, all_kv)


def attend_backward_kernel(ctx_size, block_rows, rows_here, scalars, q_ref, go_ref, att_ref, stat_ref, kv_ref, gq_ref, gkv_ref, delta_ref, gq_acc, gk_acc, gv_acc):
    seq = pl.program_id(0)
    blocks = 2 * ctx_size
    own_ctx = scalars[SEQS * blocks]
    own_shard = scalars[SEQS * blocks + 1]
    groups = range(KVH)
    gq_acc[...] = jnp.zeros(gq_acc.shape, jnp.float32)
    for half in range(2):
        for group in groups:
            product = go_ref[0, half, group].astype(jnp.float32) * att_ref[0, half, group]
            delta_ref[half, group] = jnp.sum(product.T, 0, keepdims=True)

    def step(key_ctx, half_key, half):
        order_key = scalars[seq * blocks + half_key * ctx_size + key_ctx]
        order_query = scalars[seq * blocks + half * ctx_size + own_ctx]

        def work(masked):
            rows = pl.ds(pl.multiple_of(key_ctx * block_rows, block_rows), block_rows)
            keys = [kv_ref[rows, key_part(group, half_key, 0)] for group in groups]
            queries = [q_ref[0, half, group] for group in groups]
            grad_out = [go_ref[0, half, group] for group in groups]
            scores = [
                lax.dot_general(
                    keys[group], queries[group], CONTRACT_LAST, preferred_element_type=jnp.float32
                )
                for group in groups
            ]
            grad_probs = [
                lax.dot_general(
                    kv_ref[rows, key_part(group, half_key, 1)],
                    grad_out[group],
                    CONTRACT_LAST,
                    preferred_element_type=jnp.float32,
                )
                for group in groups
            ]
            probs = [jnp.exp(scores[group] - stat_ref[0, half, group]) for group in groups]
            if masked:
                hidden = hidden_rows(scores[0], own_shard, rows_here)
                probs = [jnp.where(hidden, 0.0, prob) for prob in probs]
            grad_scores = [
                (probs[group] * (grad_probs[group] - delta_ref[half, group])).astype(jnp.bfloat16)
                for group in groups
            ]
            for group in groups:
                gv_acc[group] += jnp.dot(
                    probs[group].astype(jnp.bfloat16),
                    grad_out[group],
                    preferred_element_type=jnp.float32,
                )
                gk_acc[group] += jnp.dot(
                    grad_scores[group], queries[group], preferred_element_type=jnp.float32
                )
                gq_acc[half, group] += lax.dot_general(
                    keys[group], grad_scores[group], CONTRACT_FIRST, preferred_element_type=jnp.float32
                )

        @pl.when(order_key < order_query)
        def full():
            work(False)

        @pl.when(order_key == order_query)
        def diagonal():
            work(True)

    @pl.loop(0, ctx_size)
    def sweep(key_ctx):
        rows = pl.ds(pl.multiple_of(key_ctx * block_rows, block_rows), block_rows)
        for half_key in range(2):
            gk_acc[...] = jnp.zeros(gk_acc.shape, jnp.float32)
            gv_acc[...] = jnp.zeros(gv_acc.shape, jnp.float32)
            for half in range(2):
                step(key_ctx, half_key, half)
            for group in groups:
                gkv_ref[rows, key_part(group, half_key, 0)] = gk_acc[group].astype(jnp.bfloat16)
                gkv_ref[rows, key_part(group, half_key, 1)] = gv_acc[group].astype(jnp.bfloat16)

    for half in range(2):
        for group in groups:
            gq_ref[0, half, group] = gq_acc[half, group].T


def attend_backward(scalars, queries, grad_out, attended, stats, all_kv, ctx_size, block_rows, rows_here):
    lanes = queries.shape[3]
    kernel = functools.partial(attend_backward_kernel, ctx_size, block_rows, rows_here)
    group, stat, keys = group_blocks(lanes, all_kv.shape[0])
    return pl.pallas_call(
        kernel,
        grid_spec=pltpu.PrefetchScalarGridSpec(
            num_scalar_prefetch=1,
            grid=(SEQS,),
            in_specs=[group, group, group, stat, keys],
            out_specs=[group, keys],
            scratch_shapes=[
                pltpu.VMEM((2, KVH, 1, lanes), jnp.float32),
                pltpu.VMEM((2, KVH, HD, lanes), jnp.float32),
                pltpu.VMEM((KVH, block_rows, HD), jnp.float32),
                pltpu.VMEM((KVH, block_rows, HD), jnp.float32),
            ],
        ),
        out_shape=(
            jax.ShapeDtypeStruct(queries.shape, jnp.float32),
            jax.ShapeDtypeStruct(all_kv.shape, jnp.bfloat16),
        ),
        compiler_params=pltpu.CompilerParams(vmem_limit_bytes=60 * 2**20),
        name="attend_backward",
    )(scalars, queries, grad_out, attended, stats, all_kv)


def peers_of(ctx_size):
    return ctx_size == 4, range(1, ctx_size)


def ctx_target(position, way, square, ctx_size):
    return position ^ way if square else lax.rem(position + way, ctx_size)


def ctx_source(position, way, square, ctx_size):
    return position ^ way if square else lax.rem(position + ctx_size - way, ctx_size)


def greet(ctx_size, pair_count, with_ctx, all_shards):
    ctx = lax.axis_index("ctx")
    shard = lax.axis_index("fsdp")
    pair, core = shard // 2, shard % 2
    barrier = pltpu.get_barrier_semaphore()
    partners = [(ctx, pair * 2 + 1 - core)]
    for step in range(1, pair_count):
        there = lax.rem(pair + step, pair_count) * 2
        partners.append((ctx, there + core))
        if all_shards:
            partners.append((ctx, there + 1 - core))
    if with_ctx:
        for way in range(1, ctx_size):
            partners.append((lax.rem(ctx + way, ctx_size), shard))
    for partner in partners:
        pl.semaphore_signal(barrier, inc=1, device_id=partner, device_id_type=MESH_ID)
    pl.semaphore_wait(barrier, len(partners))
    return ctx, pair, core


class Exchange:
    def __init__(self, source, out, sems, own_sem, pair_count):
        self.source, self.out, self.sems, self.own_sem = source, out, sems, own_sem
        self.shard_count = 2 * pair_count

    def start(self):
        ctx, shard = lax.axis_index("ctx"), lax.axis_index("fsdp")
        self.own = pltpu.make_async_copy(self.source.at[shard], self.out.at[shard], self.own_sem)
        self.own.start()
        self.copies = []
        for step in range(1, self.shard_count):
            there = lax.rem(shard + step, self.shard_count)
            copy = pltpu.make_async_remote_copy(
                src_ref=self.source.at[there],
                dst_ref=self.out.at[shard],
                send_sem=self.sems[0].at[step - 1],
                recv_sem=self.sems[1].at[step - 1],
                device_id=(ctx, there),
                device_id_type=MESH_ID,
            )
            copy.start()
            self.copies.append(copy)

    def finish(self):
        ctx, shard = lax.axis_index("ctx"), lax.axis_index("fsdp")
        for step in range(1, self.shard_count):
            come = lax.rem(shard + self.shard_count - step, self.shard_count)
            pltpu.make_async_remote_copy(
                src_ref=self.out.at[come],
                dst_ref=self.out.at[come],
                send_sem=self.sems[0].at[step - 1],
                recv_sem=self.sems[1].at[step - 1],
                device_id=(ctx, shard),
                device_id_type=MESH_ID,
            ).wait_recv()
        self.own.wait()
        for copy in self.copies:
            copy.wait_send()


def pack(gate_ref, up_ref, out_ref, columns):
    width = out_ref.shape[2] // 2
    for there in range(out_ref.shape[0]):
        for side, ref in enumerate((gate_ref, up_ref)):
            at = side * width
            out_ref[there, :, at + width - HD : at + width] = jnp.zeros(
                (out_ref.shape[1], HD), out_ref.dtype
            )
            out_ref[there, :, at : at + columns] = ref[:, there * columns : (there + 1) * columns]


def gather_kernel(arity, ctx_size, pair_count, slots, swaps, wide, *refs):
    sources, refs = refs[:arity], refs[arity:]
    swap_sources, refs = refs[:swaps], refs[swaps:]
    outs, refs = refs[:arity], refs[arity:]
    swap_outs, refs = refs[: swaps // 2], refs[swaps // 2 :]
    pair_sems, ctx_sems, core_sems = refs[0:2], refs[2:4], refs[4:6]
    local_sem = refs[6]
    square, ways = peers_of(ctx_size) if wide else (False, ())
    narrow = [item for item in range(arity) if item not in wide]
    near = [way for way in ways if not (square and way == 3)]
    if swaps:
        gate_rows, up_rows, packed, pack_sem = refs[10:14]
        own_ctx = lax.axis_index("ctx")
        cut = gate_rows.shape[0]
        loads = []
        for item, room in enumerate((gate_rows, up_rows)):
            rows = swap_sources[item]
            if rows.shape[0] != cut:
                rows = rows.at[pl.ds(pl.multiple_of(own_ctx * cut, cut), cut)]
            loads.append(pltpu.make_async_copy(rows, room, pack_sem.at[item]))
            loads[-1].start()
    ctx, pair, core = greet(ctx_size, pair_count, len(wide) > 0, swaps > 0)
    homes = [place(ctx, pair * 2 + core) for place in slots]
    started = []
    steps = [(0, 1)] + [(far, way) for far in range(1, pair_count) for way in (1, -1)]

    def present(step):
        far, way = steps[step]
        if far == 0:
            return None
        return pair >= far if way == 1 else pair + far < pair_count

    def origin(step):
        far, way = steps[step]
        return pair - far * way

    def when(condition, work):
        if condition is None:
            work()
        else:
            pl.when(condition)(work)

    def send(item, source, place, target, sems, at, condition):
        copy = pltpu.make_async_remote_copy(
            src_ref=source,
            dst_ref=outs[item].at[place],
            send_sem=sems[0].at[at],
            recv_sem=sems[1].at[at],
            device_id=target,
            device_id_type=MESH_ID,
        )
        copy.start()
        started.append((condition, item, sems, at))

    def sent(item, sems, at):
        pltpu.make_async_remote_copy(
            src_ref=outs[item].at[0],
            dst_ref=outs[item].at[0],
            send_sem=sems[0].at[at],
            recv_sem=sems[1].at[at],
            device_id=(ctx, pair * 2 + core),
            device_id_type=MESH_ID,
        ).wait_send()

    def arrive(item, place, sems, at):
        pltpu.make_async_remote_copy(
            src_ref=outs[item].at[place],
            dst_ref=outs[item].at[place],
            send_sem=sems[0].at[at],
            recv_sem=sems[1].at[at],
            device_id=(ctx, pair * 2 + core),
            device_id_type=MESH_ID,
        ).wait_recv()

    def pass_on(step, item, source, place):
        far, way = steps[step]
        for side in (1, -1) if far == 0 else (way,):

            def further(side=side):
                return pair + 1 < pair_count if side == 1 else pair >= 1

            def both(further=further):
                return further() if far == 0 else jnp.logical_and(further(), present(step))

            def work(side=side, both=both):
                send(
                    item,
                    source,
                    place,
                    (ctx, (pair + side) * 2 + core),
                    pair_sems,
                    ((side + 1) // 2, far, item),
                    both,
                )

            if far + 1 < pair_count:
                pl.when(further())(work)

    def to_core(item, source, from_ctx, way, step):
        send(
            item,
            source,
            slots[item](from_ctx, origin(step) * 2 + core),
            (ctx, pair * 2 + 1 - core),
            core_sems,
            (way, step, item),
            functools.partial(present, step),
        )

    def spread(step, items):
        for item in items:
            place = slots[item](ctx, origin(step) * 2 + core)
            source = sources[item]
            if step:
                far, way = steps[step]
                arrive(item, place, pair_sems, ((way + 1) // 2, far - 1, item))
                source = outs[item].at[place]
            pass_on(step, item, source, place)
            for way in near if item in wide else ():
                there = ctx_target(ctx, way, square, ctx_size)
                send(
                    item,
                    source,
                    place,
                    (there, pair * 2 + core),
                    ctx_sems,
                    (way - 1, step, item),
                    functools.partial(present, step),
                )
            to_core(item, source, ctx, 0, step)

    def collect(step):
        for way in near:
            for item in wide:
                come = ctx_source(ctx, way, square, ctx_size)
                place = slots[item](come, origin(step) * 2 + core)
                arrive(item, place, ctx_sems, (way - 1, step, item))
                source = outs[item].at[place]
                if square and (steps[step][0] % 2 == 0) == (way == 1):
                    send(
                        item,
                        source,
                        place,
                        (ctx ^ (3 - way), pair * 2 + core),
                        ctx_sems,
                        (2, step, item),
                        functools.partial(present, step),
                    )
                to_core(item, source, come, way, step)

    def collect_far(step):
        for item in wide:
            place = slots[item](ctx ^ 3, origin(step) * 2 + core)
            arrive(item, place, ctx_sems, (2, step, item))
            to_core(item, outs[item].at[place], ctx ^ 3, 3, step)

    def straight_core(item, source, place, step):
        sibling = (ctx, pair * 2 + 1 - core)
        send(item, source, place, sibling, core_sems, (0, step, item), lambda: None)

    def go_straight(item):
        for step in range(1, pair_count):
            there = lax.rem(pair + step, pair_count) * 2 + core
            at = (0, step - 1, item)
            send(item, sources[item], homes[item], (ctx, there), pair_sems, at, lambda: None)
        straight_core(item, sources[item], homes[item], 0)

    locals_ = []
    for item in range(arity):
        copy = pltpu.make_async_copy(sources[item], outs[item].at[homes[item]], local_sem.at[item])
        copy.start()
        locals_.append(copy)
    spread(0, wide or range(arity))
    if swaps:
        for load in loads:
            load.wait()
        pack(gate_rows, up_rows, packed, gate_rows.shape[1] // (2 * pair_count))
    flows = []
    count = len(steps)
    for turn in range(1, count + 4):
        if turn < count:
            when(present(turn), functools.partial(spread, turn, wide or range(arity)))
        if turn == count:
            for item in narrow if wide else ():
                go_straight(item)
            if swaps:
                flow = Exchange(packed, swap_outs[0], refs[7:9], refs[9], pair_count)
                flow.start()
                flows.append(flow)
        if 0 <= turn - 2 < count:
            when(present(turn - 2), functools.partial(collect, turn - 2))
        if square and 0 <= turn - 4 < count:
            when(present(turn - 4), functools.partial(collect_far, turn - 4))

    for item in narrow if wide else ():
        for step in range(1, pair_count):
            come = lax.rem(pair + pair_count - step, pair_count)
            place = slots[item](ctx, come * 2 + core)
            arrive(item, place, pair_sems, (0, step - 1, item))
            straight_core(item, outs[item].at[place], place, step)
    for item in narrow if wide else ():
        for step in range(pair_count):
            come = lax.rem(pair + pair_count - step, pair_count)
            arrive(item, slots[item](ctx, come * 2 + 1 - core), core_sems, (0, step, item))

    def from_core(step):
        for way in (0, *ways):
            come = ctx_source(ctx, way, square, ctx_size) if way else ctx
            for item in wide or range(arity):
                arrive(item, slots[item](come, origin(step) * 2 + 1 - core), core_sems, (way, step, item))

    for step in range(count):
        when(present(step), functools.partial(from_core, step))
    for flow in flows:
        flow.finish()
    for copy in locals_:
        copy.wait()
    for condition, *which in started:
        when(condition(), functools.partial(sent, *which))


def gather(pieces, slots, collective_id, swaps=(), wide=None):
    ctx_size, shard_count = lax.axis_size("ctx"), lax.axis_size("fsdp")
    pair_count = shard_count // 2
    arity = len(pieces)
    wide = range(arity) if wide is None else wide
    dma = pltpu.SemaphoreType.DMA
    moved = sum(piece.size for piece in pieces) * 2
    steps = 2 * pair_count - 1
    if swaps:
        cut = pieces[0].shape[0]
        columns = swaps[0].shape[1] // shard_count
        packed = (shard_count, cut, 2 * (-(-columns // HD) * HD))
    return pl.pallas_call(
        functools.partial(gather_kernel, arity, ctx_size, pair_count, slots, len(swaps), wide),
        in_specs=[pl.BlockSpec(memory_space=pltpu.VMEM)] * arity
        + [pl.BlockSpec(memory_space=pl.ANY)] * len(swaps),
        out_specs=[pl.BlockSpec(memory_space=pl.ANY)] * (arity + len(swaps) // 2),
        out_shape=[
            jax.ShapeDtypeStruct(
                ((ctx_size if item in wide else 1) * shard_count,) + piece.shape, piece.dtype
            )
            for item, piece in enumerate(pieces)
        ]
        + [jax.ShapeDtypeStruct(packed, swap.dtype) for swap in swaps[:1]],
        scratch_shapes=[dma((2, pair_count - 1, arity))] * 2
        + [dma((ctx_size - 1, steps, arity))] * 2
        + [dma((ctx_size, steps, arity))] * 2
        + [dma((arity,))]
        + [dma((shard_count - 1,)), dma((shard_count - 1,)), dma] * (len(swaps) // 2)
        + [pltpu.VMEM((cut, swap.shape[1]), swap.dtype) for swap in swaps]
        + [pltpu.VMEM(packed, swap.dtype) for swap in swaps[:1]]
        + [dma((2,))] * (len(swaps) // 2),
        compiler_params=pltpu.CompilerParams(collective_id=collective_id, has_side_effects=True),
        cost_estimate=pl.CostEstimate(
            flops=0, bytes_accessed=moved * ctx_size * shard_count * 4, transcendentals=0
        ),
    )(*pieces, *swaps)


class LineScatter:
    def __init__(self, source, out, half, room, sems, where, counts, last):
        self.count, self.ctx_size = counts
        self.source, self.out, self.half, self.room = source, out, half, room
        self.last = last
        self.core_sems, self.pair_sems = sems[0:2], sems[2:4]
        self.ctx, self.pair, self.core = where
        self.order = [*range(1, self.count), 0]

    def copy(self, source, target, device, sems, at):
        return pltpu.make_async_remote_copy(
            src_ref=source,
            dst_ref=target,
            send_sem=sems[0].at[at],
            recv_sem=sems[1].at[at],
            device_id=device,
            device_id_type=MESH_ID,
        )

    def here(self):
        return (self.ctx, self.pair * 2 + self.core)

    def toward(self, step):
        return lax.rem(self.pair + step, self.count)

    def start(self):
        self.copies = []
        for step in self.order:
            self.copies.append(
                self.copy(
                    self.source.at[self.toward(step) * 2 + 1 - self.core],
                    self.half.at[step],
                    (self.ctx, self.pair * 2 + 1 - self.core),
                    self.core_sems,
                    step,
                )
            )
            self.copies[-1].start()

    def fold(self, step):
        half = self.half.at[step]
        self.copy(half, half, self.here(), self.core_sems, step).wait_recv()
        mine = self.source[self.toward(step) * 2 + self.core].astype(jnp.float32)
        total = mine + half[...].astype(jnp.float32)
        if step == 0:
            self.out[...] = total
            return
        half[...] = total.astype(half.dtype)
        self.copies.append(
            self.copy(
                half,
                self.room.at[step - 1],
                (self.ctx, self.toward(step) * 2 + self.core),
                self.pair_sems,
                step - 1,
            )
        )
        self.copies[-1].start()

    def over_ctx(self, terms, room, landing, *sems):
        shard = self.pair * 2 + self.core
        copies = []

        def send(source, target, way, sems):
            there = lax.rem(self.ctx + way, self.ctx_size)
            copies.append(self.copy(source(there), target, (there, shard), sems, way - 1))
            copies[-1].start()

        def arrive(target, way, sems):
            self.copy(target, target, self.here(), sems, way - 1).wait_recv()

        terms[...] = self.out[...].astype(terms.dtype)
        for way in range(1, self.ctx_size):
            send(lambda there: terms.at[there], room.at[way - 1], way, sems[0:2])
        total = self.out[self.ctx]
        for way in range(1, self.ctx_size):
            arrive(room.at[way - 1], way, sems[0:2])
            total = total + room[way - 1].astype(jnp.float32)
        landing[self.ctx] = total.astype(landing.dtype)
        for way in range(1, self.ctx_size):
            send(lambda there: landing.at[self.ctx], landing.at[self.ctx], way, sems[2:4])
        for way in range(1, self.ctx_size):
            come = lax.rem(self.ctx + self.ctx_size - way, self.ctx_size)
            arrive(landing.at[come], way, sems[2:4])
        self.out[...] = landing[...].astype(jnp.float32)
        for copy in copies:
            copy.wait_send()

    def finish(self):
        for step in range(1, self.count):
            room = self.room.at[step - 1]
            self.copy(room, room, self.here(), self.pair_sems, step - 1).wait_recv()
            self.out[...] += room[...].astype(jnp.float32)
        if self.last:
            self.over_ctx(*self.last)
        for copy in self.copies:
            copy.wait_send()


def scatter_kernel(arity, ctx_size, pair_count, slot, spread_ctx, lines, swaps, *refs):
    sources, refs = refs[:arity], refs[arity:]
    line_sources, refs = refs[:lines], refs[lines:]
    swap_sources, refs = refs[:swaps], refs[swaps:]
    outs, refs = refs[:arity], refs[arity:]
    line_outs, refs = refs[:lines], refs[lines:]
    swap_outs, refs = refs[:swaps], refs[swaps:]
    halves, relays, asides, ends, finals = (refs[i * arity : (i + 1) * arity] for i in range(5))
    sems = refs[5 * arity : 5 * arity + 10]
    core_sems, relay_sems, ctx_sems, pair_sems, last_sems = (sems[2 * i : 2 * i + 2] for i in range(5))
    square, ways = peers_of(ctx_size)
    ctx, pair, core = greet(ctx_size, pair_count, True, swaps > 0)
    order = list(range(1, pair_count)) + [0]
    started = []
    flows = []
    for item in range(lines):
        at = 5 * arity + 10 + 13 * item
        spread = len(line_sources[item].shape) == 4
        flows.append(
            LineScatter(
                line_sources[item],
                line_outs[item],
                *refs[at : at + 2],
                refs[at + 2 : at + 6],
                (ctx, pair, core),
                (pair_count, ctx_size),
                refs[at + 6 : at + 13] if spread else (),
            )
        )

    def send(source, target, device, pair_of_sems, at):
        copy = pltpu.make_async_remote_copy(
            src_ref=source,
            dst_ref=target,
            send_sem=pair_of_sems[0].at[at],
            recv_sem=pair_of_sems[1].at[at],
            device_id=device,
            device_id_type=MESH_ID,
        )
        copy.start()
        started.append(copy)

    def arrive(target, pair_of_sems, at):
        pltpu.make_async_remote_copy(
            src_ref=target,
            dst_ref=target,
            send_sem=pair_of_sems[0].at[at],
            recv_sem=pair_of_sems[1].at[at],
            device_id=(ctx, pair * 2 + core),
            device_id_type=MESH_ID,
        ).wait_recv()

    def toward(step):
        return lax.rem(pair + step, pair_count)

    def target_ctx(way):
        return ctx_target(ctx, way, square, ctx_size) if way else ctx

    def f32(value):
        return value.astype(jnp.float32)

    far_first = [3, 1, 2, 0] if square else list(ways) + [0]
    for step in order:
        for way in far_first:
            for item in range(arity):
                send(
                    sources[item].at[slot(target_ctx(way), toward(step) * 2 + 1 - core)],
                    halves[item].at[way, step],
                    (ctx, pair * 2 + 1 - core),
                    core_sems,
                    (way, step, item),
                )

    def fold_core(step):
        for way in far_first:
            for item in range(arity):
                half = halves[item].at[way, step]
                arrive(half, core_sems, (way, step, item))
                mine = sources[item][slot(target_ctx(way), toward(step) * 2 + core)]
                half[...] = (f32(mine) + f32(half[...])).astype(half.dtype)
                if square and way == 3:
                    there = ctx ^ (1 if step % 2 == 0 else 2)
                    send(
                        half,
                        relays[item].at[step],
                        (there, pair * 2 + core),
                        relay_sems,
                        (step, item),
                    )

    def fold_relay(step):
        for item in range(arity):
            if square:
                relay = relays[item].at[step]
                arrive(relay, relay_sems, (step, item))
                half = halves[item].at[2 if step % 2 == 0 else 1, step]
                half[...] = (f32(half[...]) + f32(relay[...])).astype(half.dtype)
            for way in ways:
                if square and way == 3:
                    continue
                send(
                    halves[item].at[way, step],
                    asides[item].at[way - 1, step],
                    (target_ctx(way), pair * 2 + core),
                    ctx_sems,
                    (way - 1, step, item),
                )

    def fold_ctx(step):
        for item in range(arity):
            half = halves[item].at[0, step]
            total = f32(half[...])
            for way in ways:
                if square and way == 3:
                    continue
                aside = asides[item].at[way - 1, step]
                arrive(aside, ctx_sems, (way - 1, step, item))
                total = total + f32(aside[...])
            if step:
                half[...] = total.astype(half.dtype)
                send(
                    half,
                    ends[item].at[step - 1],
                    (ctx, toward(step) * 2 + core),
                    pair_sems,
                    (step - 1, item),
                )
            else:
                for other in range(1, pair_count):
                    end = ends[item].at[other - 1]
                    arrive(end, pair_sems, (other - 1, item))
                    total = total + f32(end[...])
                if spread_ctx:
                    finals[item][...] = total.astype(finals[item].dtype)
                else:
                    outs[item][...] = total.astype(outs[item].dtype)

    for flow in flows:
        flow.start()
    exchanges = []
    for item in range(swaps):
        at = 5 * arity + 10 + 13 * lines + 3 * item
        flow = Exchange(
            swap_sources[item], swap_outs[item], refs[at : at + 2], refs[at + 2], pair_count
        )
        flow.start()
        exchanges.append(flow)
    for turn in range(pair_count + 2):
        if turn < pair_count:
            fold_core(order[turn])
        if 1 <= turn <= pair_count:
            fold_relay(order[turn - 1])
            for flow in flows:
                flow.fold(order[turn - 1])
        if turn >= 2:
            fold_ctx(order[turn - 2])
    if spread_ctx:
        for item in range(arity):
            for way in ways:
                send(
                    finals[item],
                    outs[item].at[ctx],
                    (target_ctx(way), pair * 2 + core),
                    last_sems,
                    (way - 1, item),
                )
            outs[item][ctx] = finals[item][...]
        for item in range(arity):
            for way in ways:
                arrive(outs[item].at[ctx_source(ctx, way, square, ctx_size)], last_sems, (way - 1, item))
    for flow in (*flows, *exchanges):
        flow.finish()
    for copy in started:
        copy.wait_send()


def scatter(terms, slot, collective_id, spread_ctx=False, out_dtype=None, lines=(), swaps=()):
    ctx_size, shard_count = lax.axis_size("ctx"), lax.axis_size("fsdp")
    pair_count = shard_count // 2
    arity = len(terms)
    dma = pltpu.SemaphoreType.DMA
    lead = (ctx_size,) if spread_ctx else ()
    asides = 2 if ctx_size == 4 else ctx_size - 1

    def room(*extent):
        return [pltpu.VMEM(extent + term.shape[1:], term.dtype) for term in terms]

    def line_room(line):
        if len(line.shape) == 3:
            return [pltpu.VMEM((8, HD), line.dtype)] * 3 + [dma((1,))] * 4
        cut = line.shape[2:]
        rooms = [pltpu.VMEM((count,) + cut, line.dtype) for count in (ctx_size, ctx_size - 1, ctx_size)]
        return rooms + [dma((ctx_size - 1,))] * 4

    moved = sum(term.size * term.dtype.itemsize for term in terms)
    return pl.pallas_call(
        functools.partial(scatter_kernel, arity, ctx_size, pair_count, slot, spread_ctx, len(lines), len(swaps)),
        in_specs=[pl.BlockSpec(memory_space=pltpu.VMEM)] * (arity + len(lines) + len(swaps)),
        out_specs=[pl.BlockSpec(memory_space=pltpu.VMEM)] * (arity + len(lines))
        + [pl.BlockSpec(memory_space=pl.ANY)] * len(swaps),
        out_shape=[
            jax.ShapeDtypeStruct(lead + term.shape[1:], out_dtype or term.dtype) for term in terms
        ]
        + [jax.ShapeDtypeStruct(line.shape[1:], jnp.float32) for line in lines]
        + [jax.ShapeDtypeStruct(swap.shape, swap.dtype) for swap in swaps],
        scratch_shapes=room(ctx_size, pair_count)
        + room(pair_count)
        + room(asides, pair_count)
        + room(pair_count - 1)
        + room()
        + [dma((ctx_size, pair_count, arity))] * 2
        + [dma((pair_count, arity))] * 2
        + [dma((ctx_size - 1, pair_count, arity))] * 2
        + [dma((pair_count - 1, arity))] * 2
        + [dma((ctx_size - 1, arity))] * 2
        + [
            scratch
            for line in lines
            for scratch in [
                pltpu.VMEM((pair_count,) + line.shape[1:], line.dtype),
                pltpu.VMEM((pair_count - 1,) + line.shape[1:], line.dtype),
            ]
            + [dma((pair_count,))] * 4
            + line_room(line)
        ]
        + [dma((shard_count - 1,)), dma((shard_count - 1,)), dma] * len(swaps),
        compiler_params=pltpu.CompilerParams(
            collective_id=collective_id, has_side_effects=True, vmem_limit_bytes=63 * 2**20
        ),
        cost_estimate=pl.CostEstimate(flops=0, bytes_accessed=moved * 16, transcendentals=0),
    )(*terms, *lines, *swaps)


def line_sum_kernel(pair_count, source, out, half, room, *sems):
    where = greet(1, pair_count, False, False)
    flow = LineScatter(source, out, half, room, sems, where, (pair_count, 1), ())
    flow.start()
    for step in flow.order:
        flow.fold(step)
    flow.finish()


def line_sum(terms, collective_id):
    pair_count = lax.axis_size("fsdp") // 2
    extent = terms.shape[1:]
    dma = pltpu.SemaphoreType.DMA((pair_count,))
    return pl.pallas_call(
        functools.partial(line_sum_kernel, pair_count),
        in_specs=[pl.BlockSpec(memory_space=pltpu.VMEM)],
        out_specs=pl.BlockSpec(memory_space=pltpu.VMEM),
        out_shape=jax.ShapeDtypeStruct(extent, jnp.float32),
        scratch_shapes=[
            pltpu.VMEM((pair_count,) + extent, terms.dtype),
            pltpu.VMEM((pair_count - 1,) + extent, terms.dtype),
        ]
        + [dma] * 4,
        compiler_params=pltpu.CompilerParams(
            collective_id=collective_id, has_side_effects=True, vmem_limit_bytes=63 * 2**20
        ),
        cost_estimate=pl.CostEstimate(flops=0, bytes_accessed=terms.size * 16, transcendentals=0),
    )(terms)


def turned(values, cosine, signed_sine):
    return values * cosine + pltpu.roll(values, HD // 2, 1) * signed_sine


def turned_back(grads, cosine, signed_sine):
    return grads * cosine + pltpu.roll(grads * signed_sine, HD // 2, 1)


def slot_of(index):
    return index % SEQS, index // SEQS


def key_column(index, group, part):
    seq, half = slot_of(index)
    return (((seq * KVH + group) * 2 + half) * 2 + part) * HD


def project_kernel(rows, x_ref, gain_ref, w_hbm, bias_ref, cos_ref, sin_ref, normed_ref, q_ref, kv_ref, w_ref, q_acc, sems):
    wide = w_ref.shape[2]
    copies = []
    for part in range(w_ref.shape[0]):
        copy = pltpu.make_async_copy(
            w_hbm.at[:, part * wide : (part + 1) * wide], w_ref.at[part], sems.at[part]
        )
        copy.start()
        copies.append(copy)
    values = x_ref[...].astype(jnp.float32)
    scale = lax.rsqrt(jnp.mean(values * values, -1, keepdims=True) + EPS)
    normed = (values * scale * gain_ref[...]).astype(jnp.bfloat16)
    normed_ref[...] = normed
    cosine, sine = cos_ref[...], sin_ref[...]
    for part, copy in enumerate(copies):
        copy.wait()
        columns = jnp.dot(normed, w_ref[part], preferred_element_type=jnp.float32)
        columns = columns + bias_ref[:, part * wide : (part + 1) * wide]
        for index in range(wide // HD):
            head = part * (wide // HD) + index
            piece = columns[:, index * HD : (index + 1) * HD]
            if head < H + KVH:
                piece = turned(piece, cosine, sine)
            if head < H:
                piece = piece * (HD**-0.5)
            for slot in range(2 * SEQS):
                seq, half = slot_of(slot)
                own = piece[slot * rows : (slot + 1) * rows]
                if head < H:
                    group, member = head // (H // KVH), head % (H // KVH)
                    q_acc[seq, half, group, member * rows : (member + 1) * rows] = own
                else:
                    group, kind = (head - H) % KVH, (head - H) // KVH
                    at = key_column(slot, group, kind)
                    kv_ref[:, at : at + HD] = own.astype(jnp.bfloat16)
    q_ref[...] = q_acc[...].astype(jnp.bfloat16)


def project(tokens, gain, weight, bias, cosine, signed_sine, rows):
    vmem = pl.BlockSpec(memory_space=pltpu.VMEM)
    parts = 8
    grouped = (SEQS, 2, KVH, H // KVH * rows, HD)
    return pl.pallas_call(
        functools.partial(project_kernel, rows),
        in_specs=[vmem, vmem, pl.BlockSpec(memory_space=pl.ANY), vmem, vmem, vmem],
        out_specs=[vmem, vmem, vmem],
        out_shape=[
            jax.ShapeDtypeStruct(tokens.shape, jnp.bfloat16),
            jax.ShapeDtypeStruct(grouped, jnp.bfloat16),
            jax.ShapeDtypeStruct((rows, SEQS * KVH * 4 * HD), jnp.bfloat16),
        ],
        scratch_shapes=[
            pltpu.VMEM((parts, D, QKV // parts), jnp.bfloat16),
            pltpu.VMEM(grouped, jnp.float32),
            pltpu.SemaphoreType.DMA((parts,)),
        ],
        compiler_params=pltpu.CompilerParams(vmem_limit_bytes=62 * 2**20),
        cost_estimate=pl.CostEstimate(
            flops=2 * tokens.shape[0] * D * QKV, bytes_accessed=2 * D * QKV, transcendentals=0
        ),
        name="project",
    )(tokens, gain.reshape(1, -1), weight, bias.reshape(1, -1), cosine, signed_sine)


def unproject_kernel(rows, gq_ref, gkv_ref, cos_ref, sin_ref, w_hbm, x_ref, gain_ref, past_ref, gp_ref, gi_ref, gg_ref, gb_ref, w_ref, gp_acc, sem):
    copy = pltpu.make_async_copy(w_hbm, w_ref, sem)
    copy.start()
    cosine, sine = cos_ref[...], sin_ref[...]

    def rounded(values):
        return values.astype(jnp.bfloat16).astype(jnp.float32)

    for head in range(H + 2 * KVH):
        for slot in range(2 * SEQS):
            seq, half = slot_of(slot)
            at = slice(slot * rows, (slot + 1) * rows)
            if head < H:
                group, member = head // (H // KVH), head % (H // KVH)
                grad = gq_ref[seq, half, group, member * rows : (member + 1) * rows]
                grad = rounded(grad) * (HD**-0.5)
            else:
                group, kind = (head - H) % KVH, (head - H) // KVH
                column = key_column(slot, group, kind)
                grad = rounded(gkv_ref[:, column : column + HD])
            if head < H + KVH:
                grad = turned_back(grad, cosine[at], sine[at])
            gp_acc[at, head * HD : (head + 1) * HD] = grad
    low = gp_acc[...].astype(jnp.bfloat16)
    gp_ref[...] = low
    gb_ref[...] = jnp.sum(low.astype(jnp.float32), 0, keepdims=True)
    values = x_ref[...].astype(jnp.float32)
    scale = lax.rsqrt(jnp.mean(values * values, -1, keepdims=True) + EPS)
    unit = values * scale
    copy.wait()
    grad_normed = lax.dot_general(low, w_ref[...], CONTRACT_LAST, preferred_element_type=jnp.float32)
    gg_ref[...] = jnp.sum(grad_normed * unit, 0, keepdims=True)
    grad_unit = grad_normed * gain_ref[...]
    inner = jnp.mean(grad_unit * unit, -1, keepdims=True)
    gi_ref[...] = past_ref[...] + scale * (grad_unit - unit * inner)


def unproject(grad_queries, grad_kv, cosine, signed_sine, weight, tokens, gain, past, rows):
    vmem = pl.BlockSpec(memory_space=pltpu.VMEM)
    return pl.pallas_call(
        functools.partial(unproject_kernel, rows),
        in_specs=[vmem, vmem, vmem, vmem, pl.BlockSpec(memory_space=pl.ANY), vmem, vmem, vmem],
        out_specs=[vmem] * 4,
        out_shape=[
            jax.ShapeDtypeStruct((tokens.shape[0], QKV), jnp.bfloat16),
            jax.ShapeDtypeStruct(tokens.shape, jnp.float32),
            jax.ShapeDtypeStruct((1, D), jnp.float32),
            jax.ShapeDtypeStruct((1, QKV), jnp.float32),
        ],
        scratch_shapes=[
            pltpu.VMEM((D, QKV), jnp.bfloat16),
            pltpu.VMEM((tokens.shape[0], QKV), jnp.float32),
            pltpu.SemaphoreType.DMA,
        ],
        compiler_params=pltpu.CompilerParams(vmem_limit_bytes=62 * 2**20),
        cost_estimate=pl.CostEstimate(
            flops=2 * tokens.shape[0] * D * QKV, bytes_accessed=2 * D * QKV, transcendentals=0
        ),
        name="unproject",
    )(grad_queries, grad_kv, cosine, signed_sine, weight, tokens, gain.reshape(1, -1), past)


def unpack_kernel(columns, in_ref, gate_ref, up_ref):
    width = in_ref.shape[3] // 2
    for there in range(in_ref.shape[1]):
        for side, ref in enumerate((gate_ref, up_ref)):
            part = in_ref[0, there, :, side * width : side * width + columns]
            ref[0, :, there * columns : (there + 1) * columns] = part.astype(jnp.float32)


def unpack(rows, columns):
    ctx_size, shard_count, cut, _ = rows.shape
    out = jax.ShapeDtypeStruct((ctx_size, cut, shard_count * columns), jnp.float32)
    return pl.pallas_call(
        functools.partial(unpack_kernel, columns),
        grid=(ctx_size,),
        in_specs=[pl.BlockSpec((1,) + rows.shape[1:], lambda c: (c, 0, 0, 0))],
        out_specs=[pl.BlockSpec((1, cut, shard_count * columns), lambda c: (c, 0, 0))] * 2,
        out_shape=[out, out],
        name="unpack",
    )(rows)


def shards(
    layer_input,
    block_order,
    first_gain,
    w_qkv,
    b_qkv,
    w_o,
    second_gain,
    w_gate,
    w_up,
    w_down,
    cotangent,
):
    ctx_size = lax.axis_size("ctx")
    shard_count = lax.axis_size("fsdp")
    own_ctx = lax.axis_index("ctx")
    own_shard = lax.axis_index("fsdp")
    rows_here = layer_input.shape[0]
    block_rows = rows_here * shard_count
    cut = D // (ctx_size * shard_count)
    columns = FF // shard_count
    cosine, signed_sine = turn_tables(
        block_order, own_ctx, ctx_size, block_rows, own_shard * rows_here, rows_here
    )
    tokens = by_slot(layer_input)
    grad_out = by_slot(cotangent)

    def by_rows(ctx, shard):
        return shard * ctx_size + ctx

    def by_tokens(ctx, shard):
        return ctx * shard_count + shard

    def own_cut(weight):
        return lax.dynamic_slice_in_dim(weight, own_ctx * cut, cut, 0)

    def mix_features(values):
        shaped = values.reshape(-1, shard_count, ctx_size, cut)
        return shaped.transpose(0, 2, 1, 3).reshape(-1, D)

    def unmix_features(values):
        shaped = values.reshape(-1, ctx_size, shard_count, cut)
        return shaped.transpose(0, 2, 1, 3).reshape(-1, D)

    small = jnp.concatenate([b_qkv, first_gain, second_gain]).reshape(ctx_size, -1)
    small_width = small.shape[1]
    small = lax.dynamic_slice_in_dim(small, own_ctx, 1, 0)
    small = jnp.pad(small, ((0, 0), (0, 16 * HD - small_width))).reshape(16, HD)
    width = -(-columns // HD) * HD
    w_qkv_all, w_o_all, small_all, gate_up_cut = gather(
        [own_cut(w_qkv), own_cut(w_o), small],
        [by_rows, by_rows, by_rows],
        1,
        swaps=[w_gate, w_up] if cut % 8 == 0 else [own_cut(w_gate), own_cut(w_up)],
    )
    w_qkv_all = w_qkv_all.reshape(D, QKV)
    w_o_all = w_o_all.reshape(D, D)
    small_all = small_all.reshape(shard_count, ctx_size, -1)[:, :, :small_width]
    small_all = small_all.reshape(shard_count, -1).astype(jnp.float32)
    bias_width = QKV // shard_count
    gain_width = D // shard_count
    bias_all = small_all[:, :bias_width].reshape(-1)
    gain_one = small_all[:, bias_width : bias_width + gain_width].reshape(-1)
    gain_two = small_all[:, bias_width + gain_width :].reshape(-1)

    down_padded = jnp.pad(w_down, ((0, width - columns), (0, 0)))

    late_grad_out, w_qkv_all = lax.optimization_barrier((grad_out, w_qkv_all))
    cotangent_all = lax.all_gather(late_grad_out, "fsdp", axis=0, tiled=True)
    normed_one, queries, own_kv = project(
        tokens, gain_one, w_qkv_all, bias_all, cosine, signed_sine, rows_here
    )
    (all_kv,) = gather([own_kv], [by_tokens], 2)
    gate_up_cols = lax.all_gather(
        gate_up_cut.reshape(shard_count * cut, 2 * width), "ctx", axis=0, tiled=True
    )
    all_kv = all_kv.reshape(-1, SEQS * KVH * 4 * HD)
    scalars = jnp.concatenate(
        [block_order.reshape(-1), jnp.stack([own_ctx, own_shard]).astype(jnp.int32)]
    )
    attended_grouped, stats = attend_forward(
        scalars, queries, all_kv, ctx_size, block_rows, rows_here
    )
    attended_low = from_groups(attended_grouped, rows_here).astype(jnp.bfloat16)
    middle = tokens.astype(jnp.float32) + jnp.dot(attended_low, w_o_all, preferred_element_type=jnp.float32)
    unit_two, scale_two, normed = normalize(middle, gain_two)
    normed_two = mix_features(normed.astype(jnp.bfloat16))

    (tokens_all,) = gather([normed_two], [lambda ctx, shard: shard], 6, wide=())
    tokens_all = tokens_all.reshape(-1, D)
    gate_up_part = jnp.dot(tokens_all, gate_up_cols, preferred_element_type=jnp.float32)
    gate_part, up_part = gate_up_part[:, :width], gate_up_part[:, width:]
    sigmoid_gate = jax.nn.sigmoid(gate_part)
    activated = gate_part * sigmoid_gate
    hidden = (activated * up_part).astype(jnp.bfloat16)
    grad_hidden = lax.dot_general(
        cotangent_all, down_padded, CONTRACT_LAST, preferred_element_type=jnp.float32
    )
    grad_gate = grad_hidden * up_part * sigmoid_gate * (1.0 + gate_part * (1.0 - sigmoid_gate))
    grad_gate_up = jnp.concatenate([grad_gate, grad_hidden * activated], -1).astype(jnp.bfloat16)
    gate_up_terms = lax.dot_general(
        tokens_all, grad_gate_up, CONTRACT_FIRST, preferred_element_type=jnp.float32
    ).astype(jnp.bfloat16)
    gate_up_rows = lax.psum_scatter(gate_up_terms, "ctx", scatter_dimension=0, tiled=True)
    grad_gate_up, hidden, gate_up_terms = lax.optimization_barrier(
        (grad_gate_up, hidden, gate_up_terms)
    )
    grad_tokens = lax.dot_general(
        grad_gate_up, gate_up_cols, CONTRACT_LAST, preferred_element_type=jnp.float32
    ).astype(jnp.bfloat16)
    grad_normed_two = line_sum(grad_tokens.reshape(shard_count, -1, D), 7)
    grad_normed_two, hidden = lax.optimization_barrier((grad_normed_two, hidden))
    down_terms = lax.dot_general(
        hidden, cotangent_all, CONTRACT_FIRST, preferred_element_type=jnp.float32
    ).astype(jnp.bfloat16)
    down_rows = lax.psum(down_terms, "ctx")
    mixed_terms = jnp.dot(hidden, down_padded, preferred_element_type=jnp.float32).astype(jnp.bfloat16)
    grad_normed_two, down_terms, mixed_terms = lax.optimization_barrier(
        (grad_normed_two, down_terms, mixed_terms)
    )
    grad_normed_two = unmix_features(grad_normed_two)
    grad_middle_norm, grad_gain_two = norm_back(grad_normed_two, unit_two, scale_two, gain_two)
    grad_middle = grad_out.astype(jnp.float32) + grad_middle_norm
    grad_branch_one = grad_middle.astype(jnp.bfloat16)
    grad_attended = lax.dot_general(
        grad_branch_one, w_o_all, CONTRACT_LAST, preferred_element_type=jnp.float32
    ).astype(jnp.bfloat16)
    o_terms = lax.dot_general(
        attended_low, grad_branch_one, CONTRACT_FIRST, preferred_element_type=jnp.float32
    ).astype(jnp.bfloat16)
    grad_queries, grad_kv_full = attend_backward(
        scalars,
        queries,
        to_groups(grad_attended, rows_here),
        attended_grouped,
        stats,
        all_kv,
        ctx_size,
        block_rows,
        rows_here,
    )
    grad_kv, gate_up_rows = scatter(
        [grad_kv_full.reshape(-1, rows_here, SEQS * KVH * 4 * HD)],
        by_tokens,
        3,
        out_dtype=jnp.float32,
        swaps=[gate_up_rows.reshape(shard_count, cut, 2 * width)],
    )
    gate_up_rows = lax.all_gather(gate_up_rows, "ctx", axis=0, tiled=False)
    mixed_rows = lax.psum_scatter(mixed_terms, "fsdp", scatter_dimension=0, tiled=True)
    grad_projected, grad_input, grad_gain_one, grad_bias = unproject(
        grad_queries,
        grad_kv,
        cosine,
        signed_sine,
        w_qkv_all,
        tokens,
        gain_one,
        grad_middle,
        rows_here,
    )
    grad_input = from_slot(grad_input, rows_here)
    grad_bias = grad_bias.reshape(-1)
    qkv_terms = lax.dot_general(
        normed_one, grad_projected, CONTRACT_FIRST, preferred_element_type=jnp.float32
    ).astype(jnp.bfloat16)
    small_terms = jnp.concatenate(
        [
            part.reshape(shard_count, -1)
            for part in (grad_gain_one, grad_gain_two, grad_bias[:QK], grad_bias[QK:])
        ],
        1,
    )
    small_terms = small_terms.reshape(ctx_size * shard_count, small_width)
    small_terms = jnp.pad(small_terms, ((0, 0), (0, 8 * HD - small_width)))
    qkv_rows, o_rows, small_rows = scatter(
        [
            qkv_terms.reshape(-1, cut, QKV),
            o_terms.reshape(-1, cut, D),
            small_terms.reshape(-1, 8, HD),
        ],
        by_rows,
        4,
        spread_ctx=True,
    )
    mixed_rows, small_rows = lax.optimization_barrier((mixed_rows, small_rows))
    mixed_out = middle + mixed_rows.astype(jnp.float32)
    output = from_slot(mixed_out.astype(jnp.bfloat16), rows_here)
    small_rows = small_rows.reshape(ctx_size, -1)[:, :small_width].reshape(-1)
    bias_start = 2 * gain_width
    value_start = bias_start + QK // shard_count

    gate_rows, up_rows = unpack(gate_up_rows, columns)
    return (
        output,
        grad_input,
        small_rows[:gain_width],
        qkv_rows.reshape(-1, QKV).astype(jnp.float32),
        small_rows[bias_start:value_start],
        small_rows[value_start:],
        o_rows.reshape(-1, D).astype(jnp.float32),
        small_rows[gain_width:bias_start],
        gate_rows.reshape(-1, FF),
        up_rows.reshape(-1, FF),
        down_rows[:columns].astype(jnp.float32),
    )


def solution(mesh):
    in_specs = (
        P(("ctx", "fsdp"), None, None),
        P(),
        P("fsdp"),
        P("fsdp", None),
        P("fsdp"),
        P("fsdp", None),
        P("fsdp"),
        P("fsdp", None),
        P("fsdp", None),
        P("fsdp", None),
        P(("ctx", "fsdp"), None, None),
    )
    out_specs = (
        P(("ctx", "fsdp"), None, None),
        P(("ctx", "fsdp"), None, None),
        P("fsdp"),
        P("fsdp", None),
        P("fsdp"),
        P("fsdp"),
        P("fsdp", None),
        P("fsdp"),
        P("fsdp", None),
        P("fsdp", None),
        P("fsdp", None),
    )
    return jax.shard_map(shards, mesh=mesh, in_specs=in_specs, out_specs=out_specs, check_vma=False)
```
